128 devices in a mesh: seq: 16 (over y, z_lo, core), zero: 8 (over x, z_hi).
Axes of the slice: x: 4, y: 4, z: 4 (z_hi: 2, z_lo: 2; z = z_hi * 2 + z_lo), core: 2. Of those that a mesh axis runs over, the one named last changes fastest.
Arguments:
- hidden: bfloat16 [8, 2048, 1280], P('zero', 'seq'), may hold values from -6 to 6
- output_grad: bfloat16 [8, 2048, 2560], P('zero', 'seq'), may hold values from -6 to 6
- input_weight: bfloat16 [1280, 2856], P('zero'), may hold values from -0.15625 to 0.15625
- step_bias: float32 [40], replicated, may hold values from -7 to -2
- decay_log: float32 [40], replicated, may hold values from -4 to 1
- skip_gain: float32 [40], replicated, may hold values from 0.5 to 1.5
Outputs:
- hidden_grad: bfloat16 [8, 2048, 1280], P('zero', 'seq')
- weight_grad: float32 [1280, 2856], P(('seq', 'zero'))
- head_grads: float32 [3, 40], replicated
The draws below stay inside these ranges and needn't reach their ends.
All inputs are finite; a program needn't handle non-finite values.
Results may differ from the reference program's by a relative error of at most 0.0049.
Values may be sent and summed in bfloat16 or wider, within the bound.
A program may use at most 192 MiB of HBM per device.

```python
import jax
import jax.numpy as jnp
from jax import lax

D = 1280
HEADS = 40
HEAD_DIM = 64
STATE = 128
GROUP = 128
INNER = 2560
PROJ = 2856
LENGTH = 2048
SEQS = 8


def levels(key, shape, split, smallest, top_value):
    loudness = 1.0
    for position, blocks in split:
        steps = jax.random.uniform(jax.random.fold_in(jax.random.fold_in(key, 6), position), (blocks,), jnp.float32, smallest / len(split), top_value / len(split))
        loudness = loudness * jnp.repeat(jnp.exp(steps), shape[position] // blocks).reshape((-1,) + (1,) * (len(shape) - 1 - position))
    return loudness


def normal_values(stream_key, shape, deviation, bound, split=(), dtype=jnp.bfloat16):
    drawn = jax.random.normal(stream_key, shape, jnp.float32) * deviation
    if len(split) > 0:
        drawn = levels(stream_key, shape, split, -0.22, 0.18) * drawn
    return jnp.clip(drawn, min=-bound, max=bound).astype(dtype)


def setup_inputs(seed: int = 0) -> dict:
    seeds = jax.random.split(jax.random.key(seed), 7)
    return {
        "hidden": normal_values(seeds[0], (SEQS, LENGTH, D), 1.0, 6.0, ((0, 8), (1, 16))),
        "output_grad": normal_values(seeds[1], (SEQS, LENGTH, INNER), 1.0, 6.0, ((0, 8), (1, 16))),
        "input_weight": normal_values(seeds[2], (D, PROJ), D ** -0.5, 0.15625, ((0, 8),)),
        "step_bias": jnp.clip(jax.random.uniform(seeds[3], (HEADS,), jnp.float32, -7.0, -2.0), -7.0, -2.0),
        "decay_log": jnp.clip(jax.random.uniform(seeds[4], (HEADS,), jnp.float32, -4.0, 1.0), -4.0, 1.0),
        "skip_gain": jnp.clip(jax.random.uniform(seeds[5], (HEADS,), jnp.float32, 0.5, 1.5), 0.5, 1.5),
    }


highest = lax.Precision.HIGHEST

def state_mixer(columns, step_bias, decay_log, skip_gain, initial):
    length = columns.shape[0]
    blocks = length // GROUP
    values = jax.nn.silu(columns[:, :INNER])
    input_map = jax.nn.silu(columns[:, INNER:INNER + STATE]).reshape(blocks, GROUP, STATE)
    output_map = jax.nn.silu(columns[:, INNER + STATE:INNER + 2 * STATE]).reshape(blocks, GROUP, STATE)
    step_size = jax.nn.softplus(columns[:, INNER + 2 * STATE:] + step_bias)
    log_decay = -jnp.exp(decay_log) * step_size
    head_values = values.reshape(blocks, GROUP, HEADS, HEAD_DIM)
    scaled = head_values * step_size.reshape(blocks, GROUP, HEADS)[:, :, :, None]
    cumulative = jnp.cumsum(log_decay.reshape(blocks, GROUP, HEADS), axis=1)
    causal = (lax.broadcasted_iota(jnp.int32, (GROUP, GROUP), 0) >= lax.broadcasted_iota(jnp.int32, (GROUP, GROUP), 1))[None, :, :, None]
    differences = cumulative[:, :, None, :] - cumulative[:, None, :, :]
    within = jnp.where(causal, jnp.exp(jnp.where(causal, differences, 0.0)), 0.0)
    scores = jnp.einsum('kqn,ksn->kqs', output_map, input_map, precision=highest)
    inside = jnp.einsum('kqsh,kshp->kqhp', scores[:, :, :, None] * within, scaled, precision=highest)
    tail_decay = jnp.exp(cumulative[:, -1:, :] - cumulative)
    group_states = jnp.einsum('kshp,ksn->khpn', scaled * tail_decay[:, :, :, None], input_map, precision=highest)
    totals = cumulative[:, -1, :]

    def advance(running, inputs):
        block_total, block_state = inputs
        return (jnp.exp(block_total)[:, None, None] * running + block_state, running)
    final_state, entering = lax.scan(advance, initial, (totals, group_states))
    from_state = jnp.einsum('kqn,khpn->kqhp', output_map, entering, precision=highest) * jnp.exp(cumulative)[:, :, :, None]
    mixed_out = inside + from_state + skip_gain[None, None, :, None] * head_values
    return (mixed_out.reshape(length, INNER), final_state, lax.optimization_barrier(jnp.sum(totals, axis=0)))

def reference(hidden, output_grad, input_weight, step_bias, decay_log, skip_gain):
    initial = jnp.zeros((HEADS, HEAD_DIM, STATE), jnp.float32)

    def one_sequence(running, inputs):
        weight_sum, head_sum = running
        tokens, cotangent = inputs
        projected = jnp.dot(tokens, input_weight, preferred_element_type=jnp.float32)

        def forward(columns, bias_part, log_part, gain_part):
            return state_mixer(columns, bias_part, log_part, gain_part, initial)[0]
        unused, pullback = jax.vjp(forward, projected, step_bias, decay_log, skip_gain)
        column_grad, bias_grad, log_grad, gain_grad = pullback(cotangent.astype(jnp.float32))
        rounded = column_grad.astype(jnp.bfloat16)
        token_grad = lax.dot_general(rounded, input_weight, (((1,), (1,)), ((), ())), preferred_element_type=jnp.float32).astype(jnp.bfloat16)
        weight_sum = weight_sum + lax.dot_general(tokens, rounded, (((0,), (0,)), ((), ())), preferred_element_type=jnp.float32)
        head_sum = head_sum + jnp.stack([bias_grad, log_grad, gain_grad])
        return ((weight_sum, head_sum), token_grad)
    starting = (jnp.zeros((D, PROJ), jnp.float32), jnp.zeros((3, HEADS), jnp.float32))
    (weight_grad, head_grads), hidden_grad = lax.scan(one_sequence, starting, (hidden, output_grad))
    return (hidden_grad, weight_grad, head_grads)
```

```python
import functools

import jax
import jax.numpy as jnp
from jax import lax
from jax.experimental import pallas as pl
from jax.experimental.pallas import tpu as pltpu
from jax.sharding import Mesh
from jax.sharding import PartitionSpec as P

HEADS = 40
STATE = 128
INNER = 2560
D = 1280
COLS = 640
ZERO = ("zero_0", "zero_1")
SEQ = ("seq_0", "seq_1", "seq_2")
SEQ_ZERO = ("seq_0", "seq_1", "seq_2", "zero_0", "zero_1")
MESH = pl.DeviceIdType.MESH
F32 = jnp.float32
BF16 = jnp.bfloat16
highest = lax.Precision.HIGHEST
NN = (((1,), (0,)), ((), ()))
NT = (((1,), (1,)), ((), ()))
TN = (((0,), (0,)), ((), ()))


def mm(a, b, dims=NN, precision=None):
    return lax.dot_general(a, b, dims, preferred_element_type=F32, precision=precision)


def ds(start, size, align=None):
    return pl.ds(pl.multiple_of(start, align or size), size)


def silu_grad(v):
    sig = jax.nn.sigmoid(v)
    return sig * (1.0 + v * (1.0 - sig))


def kernel(
    hid_ref, cot_ref, w_ref, par_ref,
    hg_ref, wg_ref, hd_ref,
    hidf, hidt, cot, wf, proj, bmf, cmf, stp, lgd, cums, sexp, ecs, tls, vv, xb, xt, oe, tot,
    sl, dl, stt, tts, str_, ttr, q1s, dxin, dbf, dcf, sb, db, dd, ipr, rr, rdt, gacc,
    t1s, t1r, t1d, t1dr, t2s, t2r, shr, hgp, hgs, hgr,
    dwa, dwb, sa1, ra1p, ra1m, sa2p, sa2m, ra2p, ra2m,
    sa3, ra3, sa4, ra4, sd, rd, heads_y, heads_x, heads_z, heads_g,
    ss, rs, ls,
):
    y, zl, c = (lax.axis_index(n) for n in SEQ)
    x, zh = (lax.axis_index(n) for n in ZERO)
    r = zl * 2 + c
    a = lax.rem(zl + zh, 2)
    g = a * 2 + c
    pending = []

    def send(i, src, dst, where, recv=None):
        copy = pltpu.make_async_remote_copy(
            src_ref=src, dst_ref=dst, send_sem=ss.at[i], recv_sem=rs.at[i if recv is None else recv],
            device_id=where, device_id_type=MESH,
        )
        copy.start()
        pending.append(copy)
        return copy

    def rank(k):
        zlk = lax.rem(zl + k // 2, 2)
        ck = lax.rem(c + k % 2, 2)
        return zlk, ck, {"seq_1": zlk, "seq_2": ck}

    def xdev(k):
        return {"zero_0": lax.rem(x + k + 4, 4)}

    def ydev(k):
        return {"seq_0": lax.rem(y + k + 4, 4)}

    zpair = {"seq_1": 1 - zl, "zero_1": 1 - zh}
    core = {"seq_2": 1 - c}

    def shard(xk, zk):
        return ds((lax.rem(xk + 4, 4) * 2 + zk) * 160, 160)

    mine = ds(r * 128, 128)
    own = shard(x, zh)
    other = shard(x, 1 - zh)
    w_z = send(6, w_ref, wf.at[own, :], zpair)
    w_p = send(7, w_ref, wf.at[own, :], xdev(1))
    w_m = send(8, w_ref, wf.at[own, :], xdev(-1))
    h_z = send(1, hid_ref, hidf.at[mine, :], rank(2)[2])
    h_c = send(0, hid_ref, hidf.at[mine, :], core)
    cots = []
    for k in (2, 3, 1):
        zlk, ck, dev = rank(k)
        gk = lax.rem(zlk + zh, 2) * 2 + ck
        cots.append(send(2 + k, cot_ref.at[:, ds(gk * COLS, COLS)], cot.at[mine, :], dev))
    local = [
        pltpu.make_async_copy(w_ref, wf.at[own, :], ls.at[0]),
        pltpu.make_async_copy(hid_ref, hidf.at[mine, :], ls.at[1]),
        pltpu.make_async_copy(cot_ref.at[:, ds(g * COLS, COLS)], cot.at[mine, :], ls.at[2]),
    ]
    for copy in local:
        copy.start()
    w_z.wait_recv()
    w_zp = send(9, wf.at[other, :], wf.at[other, :], xdev(1))
    w_zm = send(10, wf.at[other, :], wf.at[other, :], xdev(-1))
    h_z.wait_recv()
    zrows = ds((rank(2)[0] * 2 + c) * 128, 128)
    h_f = send(2, hidf.at[zrows, :], hidf.at[zrows, :], core)
    half = 512
    w_p.wait_recv()
    piece = wf.at[shard(x - 1, zh), 0:half]
    f1 = send(11, piece, piece, xdev(1))
    w_m.wait_recv()
    piece = wf.at[shard(x + 1, zh), half:1024]
    f2 = send(12, piece, piece, xdev(-1))
    for copy in local:
        copy.wait()
    h_c.wait_recv()
    h_f.wait_recv()
    for copy in cots:
        copy.wait_recv()

    def turn(i, carry):
        hidt[:, ds(i * 128, 128)] = hidf[ds(i * 128, 128), :].T
        return carry

    lax.fori_loop(0, 4, turn, 0)
    w_zp.wait_recv()
    piece = wf.at[shard(x - 1, 1 - zh), 0:half]
    f3 = send(13, piece, piece, xdev(1))
    w_zm.wait_recv()
    piece = wf.at[shard(x + 1, 1 - zh), half:1024]
    f4 = send(14, piece, piece, xdev(-1))
    for copy in (f1, f2, f3, f4):
        copy.wait_recv()

    rowi = lax.broadcasted_iota(jnp.int32, (128, 128), 0)
    coli = lax.broadcasted_iota(jnp.int32, (128, 128), 1)
    low = coli < 64
    causal = rowi >= coli
    anti = rowi <= coli
    tri = causal.astype(F32)
    upper = anti.astype(F32)
    strict = (rowi > coli).astype(F32)
    bias = par_ref[0:1, :]
    neg = -jnp.exp(par_ref[1:2, :])
    skip = par_ref[2:3, :]

    def pair(v, j, width=128):
        return jnp.where(low[0 : v.shape[0]], v[:, 2 * j : 2 * j + 1], v[:, 2 * j + 1 : 2 * j + 2])

    def forward(b, carry):
        rows = ds(b * 128, 128)
        p = mm(hidf[rows, :], wf[...])
        proj[rows, :] = p
        bm = jax.nn.silu(p[:, 640:768])
        cm = jax.nn.silu(p[:, 768:896])
        bmf[rows, :] = bm
        cmf[rows, :] = cm
        pre = p[:, 896:1024] + bias
        step = jnp.maximum(pre, 0.0) + jnp.log1p(jnp.exp(-jnp.abs(pre)))
        lg = neg * step
        cum = mm(tri, lg, NN, highest)
        stp[rows, :] = step
        lgd[rows, :] = lg
        cums[rows, :] = cum
        for j in range(5):
            cj = slice(128 * j, 128 * j + 128)
            ce = pair(cum, j)
            se = pair(step, j)
            ec = jnp.exp(ce)
            tl = jnp.exp(ce[127:128, :] - ce)
            val = jax.nn.silu(proj[rows, cj])
            xs = val * se
            sexp[rows, cj] = se
            ecs[rows, cj] = ec
            tls[rows, cj] = tl
            vv[rows, cj] = val
            xb[rows, cj] = xs.astype(BF16)
            xt[rows, cj] = (xs * tl).astype(BF16)
            oe[rows, cj] = (cot[rows, cj].astype(F32) * ec).astype(BF16)
            tot[ds(b * 8, 8), cj] = jnp.broadcast_to(ce[127:128, :], (8, 128))
        sl[b] = mm(bm.astype(BF16), xt[rows, :], TN)
        dl[b] = mm(cm.astype(BF16), oe[rows, :], TN)
        return carry

    lax.fori_loop(0, 4, forward, 0)

    def total(b, cj):
        return tot[8 * b : 8 * b + 1, cj]

    for j in range(5):
        cj = slice(128 * j, 128 * j + 128)
        s = sl[0, :, cj]
        d = dl[3, :, cj]
        for b in range(1, 4):
            s = jnp.exp(total(b, cj)) * s + sl[b, :, cj]
            d = jnp.exp(total(3 - b, cj)) * d + dl[3 - b, :, cj]
        stt[0, :, cj] = s.astype(BF16)
        stt[1, :, cj] = d.astype(BF16)
    tts[...] = tot[0:8, :] + tot[8:16, :] + tot[16:24, :] + tot[24:32, :]
    states = []
    for k in (1, 2, 3):
        wraps = lax.div(y + k, 4)
        states.append(send(14 + k, stt.at[wraps], str_.at[k - 1], ydev(k)))
        states.append(send(17 + k, tts, ttr.at[k - 1], ydev(k)))

    def inside(b, carry):
        rows = ds(b * 128, 128)
        bm = bmf[rows, :]
        cm = cmf[rows, :]
        scores = mm(cm, bm, NT, highest)
        scores_t = scores.T
        cum = cums[rows, :]
        cum_t = cum.T
        ds_ = jnp.zeros((128, 128), F32)
        for j in range(5):
            cj = slice(128 * j, 128 * j + 128)
            c0, c1 = cum[:, 2 * j : 2 * j + 1], cum[:, 2 * j + 1 : 2 * j + 2]
            r0, r1 = cum_t[2 * j : 2 * j + 1, :], cum_t[2 * j + 1 : 2 * j + 2, :]
            w0 = jnp.where(causal, jnp.exp(jnp.where(causal, c0 - r0, 0.0)), 0.0)
            w1 = jnp.where(causal, jnp.exp(jnp.where(causal, c1 - r1, 0.0)), 0.0)
            u0 = jnp.where(anti, jnp.exp(jnp.where(anti, r0 - c0, 0.0)), 0.0)
            u1 = jnp.where(anti, jnp.exp(jnp.where(anti, r1 - c1, 0.0)), 0.0)
            m = jnp.concatenate([scores * w0, scores * w1], axis=1).astype(BF16)
            mt = jnp.concatenate([scores_t * u0, scores_t * u1], axis=1).astype(BF16)
            x16 = xb[rows, cj]
            o16 = cot[rows, cj]
            zero = jnp.zeros_like(x16)
            xd = jnp.concatenate([jnp.where(low, x16, zero), jnp.where(low, zero, x16)], axis=0)
            od = jnp.concatenate([jnp.where(low, o16, zero), jnp.where(low, zero, o16)], axis=0)
            yy = mm(m, xd)
            pp = mm(o16, xd, NT)
            dx = mm(mt, od)
            ds_ = ds_ + w0 * pp[:, 0:128] + w1 * pp[:, 128:256]
            dxin[rows, cj] = dx
            q1s[rows, cj] = o16.astype(F32) * yy - x16.astype(F32) * dx
        dcf[rows, :] = mm(ds_, bm, NN, highest)
        dbf[rows, :] = mm(ds_, cm, TN, highest)
        return carry

    lax.fori_loop(0, 4, inside, 0)
    for copy in states:
        copy.wait_recv()

    lanes = lax.broadcasted_iota(jnp.int32, (256, 128), 0)
    outl = lax.broadcasted_iota(jnp.int32, (256, 128), 1)

    def sums(z, j):
        hi = z.astype(BF16)
        lo = (z - hi.astype(F32)).astype(BF16)
        pick = (outl == 2 * j + lax.rem(lax.div(lanes, 64), 2)).astype(F32).astype(BF16)
        return mm(jnp.concatenate([hi, lo], axis=1), pick)

    yes = [jnp.where(y >= k, 1.0, 0.0).astype(F32) for k in (1, 2, 3)]
    no = [jnp.where(y + k <= 3, 1.0, 0.0).astype(F32) for k in (1, 2, 3)]
    inner = [jnp.zeros((8, 128), F32) for _ in range(4)]
    for j in range(5):
        cj = slice(128 * j, 128 * j + 128)
        t = [ttr[k, 0:1, cj] for k in range(3)]
        got = [str_[k, :, cj].astype(F32) for k in range(3)]
        s = yes[0] * got[0] + (yes[1] * jnp.exp(t[0])) * got[1] + (yes[2] * jnp.exp(t[0] + t[1])) * got[2]
        d = no[0] * got[2] + (no[1] * jnp.exp(t[2])) * got[1] + (no[2] * jnp.exp(t[2] + t[1])) * got[0]
        for b in (3, 2, 1, 0):
            db[b, :, cj] = d.astype(BF16)
            dd[b] = d
            d = jnp.exp(total(b, cj)) * d + dl[b, :, cj]
        for b in range(4):
            sb[b, :, cj] = s.astype(BF16)
            grown = jnp.exp(total(b, cj)) * s
            inner[b] = inner[b] + sums((grown * dd[b]).reshape(16, 8, 128).sum(axis=0), j)
            s = grown + sl[b, :, cj]
    for b in range(4):
        ipr[8 * b : 8 * b + 8, :] = jnp.broadcast_to(inner[b].sum(axis=0, keepdims=True), (8, 128))

    gacc[...] = jnp.zeros_like(gacc)
    ownl = coli < 10

    def outside(b, carry):
        bias_sum, decay_sum = carry
        rows = ds(b * 128, 128)
        b16 = bmf[rows, :].astype(BF16)
        c16 = cmf[rows, :].astype(BF16)
        red = jnp.zeros((384, 128), F32)
        for j in range(5):
            cj = slice(128 * j, 128 * j + 128)
            o = cot[rows, cj].astype(F32)
            yst = mm(c16, sb[b, :, cj]) * ecs[rows, cj]
            dxst = mm(b16, db[b, :, cj]) * tls[rows, cj]
            se = sexp[rows, cj]
            val = vv[rows, cj]
            dxs = dxin[rows, cj] + dxst
            z = jnp.concatenate([q1s[rows, cj] + o * yst, xb[rows, cj].astype(F32) * dxst, dxs * val], axis=0)
            red = red + sums(z, j)
            dval = dxs * se + pair(skip, j) * o
            rr[rows, cj] = (dval * silu_grad(proj[rows, cj])).astype(BF16)
            gacc[:, cj] = gacc[:, cj] + (o * val).reshape(16, 8, 128).sum(axis=0)
        dcf[rows, :] = dcf[rows, :] + mm(oe[rows, :], sb[b], NT)
        dbf[rows, :] = dbf[rows, :] + mm(xt[rows, :], db[b], NT)
        dlog = mm(upper, red[0:128], NN, highest) + mm(strict, red[128:256], NN, highest)
        dlog = dlog + ipr[ds(b * 8, 8), :][0:1, :]
        dlog = jnp.where(ownl, dlog, 0.0)
        ddt = (red[256:384] + neg * dlog) * jax.nn.sigmoid(proj[rows, 896:1024] + bias)
        ddt = jnp.where(ownl, ddt, 0.0)
        rdt[rows, :] = ddt.astype(BF16)
        bias_sum = bias_sum + ddt.reshape(16, 8, 128).sum(axis=0)
        decay_sum = decay_sum + (dlog * lgd[rows, :]).reshape(16, 8, 128).sum(axis=0)
        return bias_sum, decay_sum

    zero8 = jnp.zeros((8, 128), F32)
    bias_sum, decay_sum = lax.fori_loop(0, 4, outside, (zero8, zero8))
    gain_sum = zero8
    for j in range(5):
        gain_sum = gain_sum + sums(gacc[:, 128 * j : 128 * j + 128], j)
    row8 = lax.broadcasted_iota(jnp.int32, (8, 128), 0)
    packed = jnp.where(
        row8 == 0, bias_sum.sum(axis=0, keepdims=True),
        jnp.where(row8 == 1, decay_sum.sum(axis=0, keepdims=True),
                  jnp.where(row8 == 2, gain_sum.sum(axis=0, keepdims=True), 0.0)),
    )
    place = jnp.where(jnp.logical_and(rowi < 10, coli == rowi + 10 * g), 1.0, 0.0).astype(F32)
    heads_y[y] = mm(packed, place, NN, highest)
    head_y = [send(50 + k, heads_y.at[y], heads_y.at[y], ydev(k)) for k in (1, 2, 3)]

    first = c == 0
    spread = mm(rdt[...], place.astype(BF16)).astype(BF16)
    t1d[...] = spread
    t1s[...] = jnp.where(first, dcf[...], dbf[...])
    t1 = [send(21, t1s, t1r, core), send(22, t1d, t1dr, core)]

    def weights(target, lo, hi):
        def step(i, carry):
            rows = ds(i * 320, 320)
            target[rows, :] = mm(hidt[rows, :], rr[:, lo:hi])
            return carry

        lax.fori_loop(0, 4, step, 0)

    def ring_first(n, target, index, dev):
        far = ds(lax.rem(index + 2, 4) * 320, 320)
        sa1[n] = target[far, :].astype(BF16)
        return (
            send(24 + 4 * n, sa1.at[n, 0:160, :], ra1p.at[n], dev(1)),
            send(25 + 4 * n, sa1.at[n, 160:320, :], ra1m.at[n], dev(-1)),
        )

    def ring_second(n, target, index, dev, firsts):
        nxt = lax.rem(index + 1, 4) * 320
        prv = lax.rem(index + 3, 4) * 320
        firsts[0].wait_recv()
        sa2p[n, 0:160, :] = (target[ds(nxt, 160, 160), :] + ra1p[n].astype(F32)).astype(BF16)
        sa2p[n, 160:320, :] = target[ds(nxt + 160, 160, 160), :].astype(BF16)
        up = send(26 + 4 * n, sa2p.at[n], ra2p.at[n], dev(1))
        firsts[1].wait_recv()
        sa2m[n, 0:160, :] = target[ds(prv, 160, 160), :].astype(BF16)
        sa2m[n, 160:320, :] = (target[ds(prv + 160, 160, 160), :] + ra1m[n].astype(F32)).astype(BF16)
        down = send(27 + 4 * n, sa2m.at[n], ra2m.at[n], dev(-1))
        return up, down

    def second_stage(n, target, index, seconds, other_index, dev):
        for copy in seconds:
            copy.wait_recv()
        here = ds(index * 320, 320)
        summed = target[here, :] + ra2p[n].astype(F32) + ra2m[n].astype(F32)
        target[here, :] = summed
        sa3[n] = summed.astype(BF16)
        return [
            send(31 + 3 * n + k, sa3.at[n, ds(lax.rem(other_index + k, 4) * 80, 80), :], ra3.at[n, k - 1], dev(k))
            for k in (1, 2, 3)
        ]

    def third_stage(n, target, index, other_index, thirds):
        for copy in thirds:
            copy.wait_recv()
        rows = ds(index * 320 + other_index * 80, 80)
        sa4[n] = target[rows, :] + ra3[n, 0].astype(F32) + ra3[n, 1].astype(F32) + ra3[n, 2].astype(F32)
        return send(38 + n, sa4.at[n, ds((1 - zh) * 40, 40), :], ra4.at[n], zpair)

    weights(dwa, 0, 384)
    a1 = ring_first(0, dwa, y, ydev)
    for copy in t1:
        copy.wait_recv()
    mixed = jnp.where(first, dbf[...], dcf[...]) + t1r[...]
    dt2 = spread.astype(F32) + t1dr[...].astype(F32)
    north = a == 0
    t2s[...] = jnp.where(north, dt2, mixed).astype(BF16)
    t2 = send(23, t2s, t2r, rank(2)[2])

    def token(i, carry):
        rows = ds(i * 128, 128)
        hgp[rows, :] = mm(rr[rows, 0:640], wf[:, 0:640], NT) + mm(rdt[rows, :], wf[:, 896:1024], NT)
        return carry

    lax.fori_loop(0, 4, token, 0)
    a2 = ring_second(0, dwa, y, ydev, a1)
    t2.wait_recv()
    came = t2r[...].astype(F32)
    tile = proj[:, ds(640 + 128 * c, 128)]
    upper_pick = ((mixed + came) * silu_grad(tile)).astype(BF16).astype(F32)
    lower_pick = jnp.where(first, dt2 + came, 0.0)
    rr[:, 640:768] = jnp.where(north, upper_pick, lower_pick).astype(BF16)
    shr[...] = jnp.where(north, upper_pick, 0.0).astype(BF16)
    weights(dwb, 384, 768)
    b1 = ring_first(1, dwb, x, xdev)

    def shared(i, carry):
        rows = ds(i * 128, 128)
        hgp[rows, :] = hgp[rows, :] + mm(shr[rows, :], wf[:, ds(640 + 128 * c, 128)], NT)
        return carry

    lax.fori_loop(0, 4, shared, 0)
    hgc = []
    for k in (2, 3, 1):
        zlk, ck, dev = rank(k)
        hgs[k - 1] = hgp[ds((zlk * 2 + ck) * 128, 128), :].astype(BF16)
        hgc.append(send(47 + k, hgs.at[k - 1], hgr.at[k - 1], dev))
    b2 = ring_second(1, dwb, x, xdev, b1)
    a3 = second_stage(0, dwa, y, a2, x, xdev)
    for copy in head_y:
        copy.wait_recv()
    heads_x[x] = (heads_y[0] + heads_y[1]) + (heads_y[2] + heads_y[3])
    head_x = [send(53 + k, heads_x.at[x], heads_x.at[x], xdev(k)) for k in (1, 2, 3)]
    b3 = second_stage(1, dwb, x, b2, y, ydev)
    a4 = third_stage(0, dwa, y, x, a3)
    for copy in head_x:
        copy.wait_recv()
    heads_z[zh] = (heads_x[0] + heads_x[1]) + (heads_x[2] + heads_x[3])
    head_z = send(57, heads_z.at[zh], heads_z.at[zh], zpair)
    b4 = third_stage(1, dwb, x, y, b3)

    pick = lax.div(x, 2)
    part = lax.rem(x, 2) * 2 + zh
    to_me = [
        jnp.logical_and(x == r, zh == pick),
        jnp.logical_and(jnp.logical_and(x == y, y == r), zh == pick),
    ]
    moves = []

    def last(n, fourth, outer, inner_index):
        fourth.wait_recv()
        chunk = sa4[n, ds(zh * 40, 40), :] + ra4[n]
        for i in range(4):
            sd[n, i, 0:10, :] = chunk[10 * i : 10 * i + 10, :]
            dev = {
                "seq_0": outer,
                "seq_1": lax.div(inner_index, 2),
                "seq_2": lax.rem(inner_index, 2),
                "zero_0": zh * 2 + i // 2,
                "zero_1": jnp.int32(i % 2),
            }
            copy = pltpu.make_async_remote_copy(
                src_ref=sd.at[n, i], dst_ref=rd.at[n, g], send_sem=ss.at[40 + 4 * n + i],
                recv_sem=rs.at[40 + 4 * n + g], device_id=dev, device_id_type=MESH,
            )
            keep = jnp.logical_and(to_me[n], part == i)

            @pl.when(jnp.logical_not(keep))
            def _():
                copy.start()

            @pl.when(keep)
            def _():
                rd[n, g] = sd[n, i]

            moves.append((copy, keep))

    last(0, a4, y, x)
    head_z.wait_recv()
    heads_g[r] = heads_z[0] + heads_z[1]
    head_g = [send(57 + k, heads_g.at[r], heads_g.at[r], rank(k)[2]) for k in (1, 2, 3)]
    last(1, b4, x, y)
    for copy in hgc:
        copy.wait_recv()
    out = hgp[mine, :] + hgr[0].astype(F32) + hgr[1].astype(F32) + hgr[2].astype(F32)
    hg_ref[...] = out.astype(BF16)
    for copy in head_g:
        copy.wait_recv()
    hd_ref[...] = (heads_g[0] + heads_g[1]) + (heads_g[2] + heads_g[3])
    for n in range(2):
        for k in range(4):
            copy = pltpu.make_async_remote_copy(
                src_ref=sd.at[n, 0], dst_ref=rd.at[n, k], send_sem=ss.at[40 + 4 * n],
                recv_sem=rs.at[40 + 4 * n + k], device_id=core, device_id_type=MESH,
            )

            @pl.when(jnp.logical_not(jnp.logical_and(to_me[n], g == k)))
            def _():
                copy.wait_recv()

    for k in range(4):
        wg_ref[:, 640 * k : 640 * k + 384] = rd[0, k, 0:10, :]
        wg_ref[:, 640 * k + 384 : 640 * k + 640] = rd[1, k, 0:10, 0:256]
    wg_ref[:, 2560:2688] = rd[1, 0, 0:10, 256:384]
    wg_ref[:, 2688:2816] = rd[1, 1, 0:10, 256:384]
    wg_ref[:, 2816:2856] = rd[1, 2, 0:10, 256:296]
    for copy in pending:
        copy.wait_send()
    for copy, keep in moves:

        @pl.when(jnp.logical_not(keep))
        def _():
            copy.wait_send()


def scratch():
    def v(shape, dtype=F32):
        return pltpu.VMEM(shape, dtype)

    return [
        v((512, D), BF16), v((D, 512), BF16), v((512, COLS), BF16), v((D, 1024), BF16), v((512, 1024)),
        v((512, 128)), v((512, 128)), v((512, 128)), v((512, 128)), v((512, 128)),
        v((512, COLS)), v((512, COLS)), v((512, COLS)), v((512, COLS)),
        v((512, COLS), BF16), v((512, COLS), BF16), v((512, COLS), BF16), v((32, COLS)),
        v((4, 128, COLS)), v((4, 128, COLS)), v((2, 128, COLS), BF16), v((8, COLS)),
        v((3, 128, COLS), BF16), v((3, 8, COLS)),
        v((512, COLS)), v((512, COLS)), v((512, 128)), v((512, 128)),
        v((4, 128, COLS), BF16), v((4, 128, COLS), BF16), v((4, 128, 128)), v((32, 128)),
        v((512, 768), BF16), v((512, 128), BF16), v((8, COLS)),
        v((512, 128)), v((512, 128)), v((512, 128), BF16), v((512, 128), BF16),
        v((512, 128), BF16), v((512, 128), BF16), v((512, 128), BF16),
        v((512, D)), v((3, 128, D), BF16), v((3, 128, D), BF16),
        v((D, 384)), v((D, 384)), v((2, 320, 384), BF16), v((2, 160, 384), BF16), v((2, 160, 384), BF16),
        v((2, 320, 384), BF16), v((2, 320, 384), BF16), v((2, 320, 384), BF16), v((2, 320, 384), BF16),
        v((2, 320, 384), BF16), v((2, 3, 80, 384), BF16), v((2, 80, 384)), v((2, 40, 384)),
        v((2, 4, 16, 384)), v((2, 4, 16, 384)),
        v((4, 8, 128)), v((4, 8, 128)), v((2, 8, 128)), v((4, 8, 128)),
        pltpu.SemaphoreType.DMA((64,)), pltpu.SemaphoreType.DMA((64,)), pltpu.SemaphoreType.DMA((4,)),
    ]


def body(hidden, output_grad, input_weight, step_bias, decay_log, skip_gain):
    zl, c = lax.axis_index("seq_1"), lax.axis_index("seq_2")
    zh = lax.axis_index("zero_1")
    g = lax.rem(zl + zh, 2) * 2 + c
    w = jnp.concatenate(
        [
            lax.dynamic_slice(input_weight, (0, g * COLS), (160, COLS)),
            input_weight[:, INNER : INNER + 2 * STATE],
            lax.dynamic_slice(input_weight, (0, INNER + 2 * STATE + 10 * g), (160, 10)),
            jnp.zeros((160, 118), BF16),
        ],
        axis=1,
    )
    own = lax.dynamic_slice(jnp.stack([step_bias, decay_log, skip_gain]), (0, 10 * g), (3, 10))
    par = jnp.pad(own, ((0, 5), (0, 118)))
    anyspace = pl.BlockSpec(memory_space=pl.ANY)
    vmem = pl.BlockSpec(memory_space=pltpu.VMEM)
    hg, wg, hd = pl.pallas_call(
        kernel,
        out_shape=(
            jax.ShapeDtypeStruct((128, D), BF16),
            jax.ShapeDtypeStruct((10, 2856), F32),
            jax.ShapeDtypeStruct((8, 128), F32),
        ),
        in_specs=[anyspace, anyspace, anyspace, vmem],
        out_specs=(vmem, vmem, vmem),
        scratch_shapes=scratch(),
        compiler_params=pltpu.CompilerParams(has_side_effects=True, vmem_limit_bytes=64000000),
    )(hidden[0], output_grad[0], w, par)
    return (hg[None], wg, hd[0:3, 0:HEADS])


def solution(mesh):
    torus = Mesh(
        mesh.devices.reshape(4, 2, 2, 4, 2), ("seq_0", "seq_1", "seq_2", "zero_0", "zero_1")
    )
    in_specs = (P(ZERO, SEQ, None), P(ZERO, SEQ, None), P(ZERO, None), P(), P(), P())
    out_specs = (P(ZERO, SEQ, None), P(SEQ_ZERO, None), P())
    return jax.shard_map(body, mesh=torus, in_specs=in_specs, out_specs=out_specs, check_vma=False)
```

```python
import functools

import jax
import jax.numpy as jnp
from jax import lax
from jax.experimental import pallas as pl
from jax.experimental.pallas import tpu as pltpu
from jax.sharding import Mesh
from jax.sharding import PartitionSpec as P

HEADS = 40
STATE = 128
INNER = 2560
D = 1280
COLS = 640
ZERO = ("zero_0", "zero_1")
SEQ = ("seq_0", "seq_1", "seq_2")
SEQ_ZERO = ("seq_0", "seq_1", "seq_2", "zero_0", "zero_1")
MESH = pl.DeviceIdType.MESH
F32 = jnp.float32
BF16 = jnp.bfloat16
highest = lax.Precision.HIGHEST
NN = (((1,), (0,)), ((), ()))
NT = (((1,), (1,)), ((), ()))
TN = (((0,), (0,)), ((), ()))


def mm(a, b, dims=NN, precision=None):
    return lax.dot_general(a, b, dims, preferred_element_type=F32, precision=precision)


def ds(start, size, align=None):
    return pl.ds(pl.multiple_of(start, align or size), size)


def silu_grad(v):
    sig = jax.nn.sigmoid(v)
    return sig * (1.0 + v * (1.0 - sig))


def kernel(
    hid_ref, cot_ref, w_ref, bias_ref, decay_ref, skip_ref,
    hg_ref, wg_ref, hd_ref,
    hidf, hidt, cot, wraw, wf, projs, projv, bmf, cmf, lgd, cums, cumt, stp, gs, gts, dgs,
    sexp, ecs, tls, vv, xb, xt, oe, tot,
    sl, dl, stt, tts, str_, ttr, q1s, dxin, dbf, dcf, sb, db, dd, red,
    rr, rdt, t1s, t1r, t1d, t1dr, t2s, t2r, shr, hgp, hgs, hgr,
    dwa, sa1, ra1p, ra1m, sa2p, sa2m, ra2p, ra2m, sa3, ra3, sa4, ra4, sd, rd,
    dwb, sb1, rb1p, rb1m, sb2p, sb2m, rb2p, rb2m, sb3, rb3, sb4, rb4, sdb, rdb,
    dwc, sc1, rc1p, rc1m, sc2p, sc2m, rc2p, rc2m, sc3, rc3, sc4, rc4, sdc, rdc,
    heads_y, heads_x, heads_z, heads_g,
    ss, rs, ls,
):
    y, zl, c = (lax.axis_index(n) for n in SEQ)
    x, zh = (lax.axis_index(n) for n in ZERO)
    r = zl * 2 + c
    a = lax.rem(zl + zh, 2)
    g = a * 2 + c
    pending = []

    def send(i, src, dst, where):
        copy = pltpu.make_async_remote_copy(
            src_ref=src, dst_ref=dst, send_sem=ss.at[i], recv_sem=rs.at[i],
            device_id=where, device_id_type=MESH,
        )
        copy.start()
        pending.append(copy)
        return copy

    def rank(k):
        zlk = lax.rem(zl + k // 2, 2)
        ck = lax.rem(c + k % 2, 2)
        return zlk, ck, {"seq_1": zlk, "seq_2": ck}

    def xdev(k):
        return {"zero_0": lax.rem(x + k + 4, 4)}

    def ydev(k):
        return {"seq_0": lax.rem(y + k + 4, 4)}

    zpair = {"seq_1": 1 - zl, "zero_1": 1 - zh}
    core = {"seq_2": 1 - c}
    here_id = ds(r * 128, 128)

    def shard(xk, zk, lo=0, size=160):
        return ds((lax.rem(xk + 4, 4) * 2 + zk) * 160 + lo, size, 16)

    own = shard(x, zh)
    lane0 = 640 + 256 * c
    local = [
        pltpu.make_async_copy(w_ref, wraw, ls.at[0]),
        pltpu.make_async_copy(w_ref.at[:, ds(g * COLS, COLS, 128)], wf.at[own, 0:640], ls.at[1]),
        pltpu.make_async_copy(w_ref.at[:, ds(2560 + 128 * c, 128)], wf.at[own, ds(lane0, 128)], ls.at[2]),
        pltpu.make_async_copy(hid_ref, hidf.at[here_id, :], ls.at[3]),
        pltpu.make_async_copy(cot_ref.at[:, ds(g * COLS, COLS, 128)], cot.at[here_id, :], ls.at[4]),
    ]
    for copy in local:
        copy.start()

    pick = lax.div(x, 2)
    part = lax.rem(x, 2) * 2 + zh
    to_me = [
        jnp.logical_and(x == r, zh == pick),
        jnp.logical_and(jnp.logical_and(x == y, y == r), zh == pick),
    ]

    barrier = pltpu.get_barrier_semaphore()

    def greet(dev):
        pl.semaphore_signal(barrier, inc=1, device_id=dev, device_id_type=MESH)

    greet(zpair)
    for k in (1, 2, 3):
        greet(xdev(k))
        greet(ydev(k))
        greet(rank(k)[2])
    for n in range(2):
        for k in range(4):
            greet({
                "seq_0": y if n == 0 else r, "seq_1": jnp.int32(k // 2), "seq_2": jnp.int32(k % 2),
                "zero_0": r if n == 0 else y, "zero_1": pick,
            })

    coli = lax.broadcasted_iota(jnp.int32, (128, 128), 1)
    rowi = lax.broadcasted_iota(jnp.int32, (128, 128), 0)
    local[0].wait()
    tail = jnp.concatenate([wraw[:, 2816:2856].astype(F32), jnp.zeros((160, 88), F32)], axis=1)
    tail = pltpu.roll(tail, lax.rem(128 - 10 * g, 128), 1)
    keep10 = lax.broadcasted_iota(jnp.int32, (160, 128), 1) < 10
    wf[own, 768:896] = jnp.where(keep10, tail, 0.0).astype(BF16)

    def lanes10(ref):
        full = jnp.concatenate([ref[...], jnp.zeros((1, 88), F32)], axis=1)
        return pltpu.roll(jnp.broadcast_to(full, (8, 128)), lax.rem(128 - 10 * g, 128), 1)[0:1, :]

    bias = lanes10(bias_ref)
    neg = -jnp.exp(lanes10(decay_ref))
    skip = lanes10(skip_ref)
    for copy in local[1:]:
        copy.wait()
    pl.semaphore_wait(barrier, 18)

    def cols(m):
        return (ds(640 + 128 * c, 256, 128), slice(0, 256), slice(256, 512), slice(512, 640))[m]

    w = {}

    def wsend(m, i, rows, dev):
        ref = wf.at[rows, cols(m)]
        w[m, i] = send(9 * m + i, ref, ref, dev)

    def w_own_x(m):
        wsend(m, 1, own, xdev(1))
        wsend(m, 2, own, xdev(-1))

    def w_own_z(m):
        wsend(m, 0, own, zpair)

    def w_other(m):
        w[m, 0].wait_recv()
        wsend(m, 3, shard(x, 1 - zh), xdev(1))
        wsend(m, 4, shard(x, 1 - zh), xdev(-1))

    def w_forward(m):
        w[m, 1].wait_recv()
        wsend(m, 5, shard(x - 1, zh, 0, 80), xdev(1))
        w[m, 2].wait_recv()
        wsend(m, 6, shard(x + 1, zh, 80, 80), xdev(-1))

    def w_forward_other(m):
        w[m, 3].wait_recv()
        wsend(m, 7, shard(x - 1, 1 - zh, 0, 80), xdev(1))
        w[m, 4].wait_recv()
        wsend(m, 8, shard(x + 1, 1 - zh, 80, 80), xdev(-1))

    def w_across(m):
        wsend(m, 3, shard(x - 1, zh), zpair)
        wsend(m, 4, shard(x + 1, zh), zpair)

    def w_across_far(m):
        w[m, 5].wait_recv()
        wsend(m, 7, shard(x + 2, zh, 0, 80), zpair)
        w[m, 6].wait_recv()
        wsend(m, 8, shard(x + 2, zh, 80, 80), zpair)

    def w_done(m, which):
        for i in which:
            w[m, i].wait_recv()

    w_own_z(0)
    w_own_x(0)
    h_z = send(37, hid_ref, hidf.at[here_id, :], rank(2)[2])
    h_c = send(36, hid_ref, hidf.at[here_id, :], core)
    cots = []
    for k in (2, 3, 1):
        zlk, ck, dev = rank(k)
        gk = lax.rem(zlk + zh, 2) * 2 + ck
        cots.append(send(38 + k, cot_ref.at[:, ds(gk * COLS, COLS, 128)], cot.at[here_id, :], dev))
    w_own_z(1)
    w_own_x(1)
    w_other(0)
    w_own_x(2)
    w_own_z(2)
    w_forward(0)
    w_other(1)
    h_z.wait_recv()
    zrows = ds((rank(2)[0] * 2 + c) * 128, 128)
    h_f = send(38, hidf.at[zrows, :], hidf.at[zrows, :], core)
    w_own_x(3)
    w_own_z(3)
    w_forward_other(0)
    w_forward(1)
    w_done(0, (5, 6, 7, 8))
    mate = send(42, wf.at[:, ds(lane0, 128)], wf.at[:, ds(lane0, 128)], core)
    w_forward(2)
    w_across(2)
    h_c.wait_recv()
    h_f.wait_recv()
    w_forward_other(1)
    mate.wait_recv()

    low = coli < 64
    causal = rowi >= coli
    anti = rowi <= coli
    tri = causal.astype(F32)
    upper = anti.astype(F32)
    strict = (rowi > coli).astype(F32)

    def pair(v, j):
        return jnp.where(low[0 : v.shape[0]], v[:, 2 * j : 2 * j + 1], v[:, 2 * j + 1 : 2 * j + 2])

    def blocks(f, unroll=True):
        if unroll:
            for b in range(4):
                f(b, pl.ds(b * 128, 128))
        else:
            def step(b, carry):
                f(b, ds(b * 128, 128))
                return carry

            lax.fori_loop(0, 4, step, 0)

    def common(b, rows):
        p = mm(hidf[rows, :], wf[:, 640:1024])
        projs[rows, :] = p
        bm = jax.nn.silu(p[:, 0:128])
        cm = jax.nn.silu(p[:, 256:384])
        bmf[rows, :] = bm
        cmf[rows, :] = cm
        pre = p[:, 128:256] + bias
        step = jnp.maximum(pre, 0.0) + jnp.log1p(jnp.exp(-jnp.abs(pre)))
        lg = neg * step
        cum = mm(tri, lg, NN, highest)
        stp[rows, :] = step
        lgd[rows, :] = lg
        cums[rows, :] = cum
        cumt[b] = cum.T[0:16, :]
        scores = mm(cm, bm, NT, highest)
        gs[b] = scores
        gts[b] = scores.T
        dgs[b] = jnp.zeros((128, 128), F32)
        red[b] = jnp.zeros((384, 128), F32)

    blocks(common)
    for j in range(5):
        cj = slice(128 * j, 128 * j + 128)
        for b in range(4):
            last_row = cums[128 * b + 127 : 128 * b + 128, :]
            tot[8 * b : 8 * b + 8, cj] = pair(jnp.broadcast_to(last_row, (8, 128)), j)
    tts[...] = tot[0:8, :] + tot[8:16, :] + tot[16:24, :] + tot[24:32, :]
    totals = [send(43 + k, tts, ttr.at[k - 1], ydev(k)) for k in (1, 2, 3)]

    def total(b, cj):
        return tot[8 * b : 8 * b + 1, cj]

    states = {}

    def pair_forward(j):
        cj = slice(128 * j, 128 * j + 128)

        def project(b, rows):
            projv[rows, cj] = mm(hidf[rows, :], wf[:, cj])

        def local_part(b, rows):
            ce = pair(cums[rows, :], j)
            se = pair(stp[rows, :], j)
            ec = jnp.exp(ce)
            tl = jnp.exp(ce[127:128, :] - ce)
            val = jax.nn.silu(projv[rows, cj])
            xs = val * se
            sexp[rows, cj] = se
            ecs[rows, cj] = ec
            tls[rows, cj] = tl
            vv[rows, cj] = val
            xb[rows, cj] = xs.astype(BF16)
            x16 = (xs * tl).astype(BF16)
            o16 = (cot[rows, cj].astype(F32) * ec).astype(BF16)
            xt[rows, cj] = x16
            oe[rows, cj] = o16
            sl[b, :, cj] = mm(bmf[rows, :].astype(BF16), x16, TN)
            dl[b, :, cj] = mm(cmf[rows, :].astype(BF16), o16, TN)

        blocks(project)
        blocks(local_part)
        s = sl[0, :, cj]
        d = dl[3, :, cj]
        for b in range(1, 4):
            s = jnp.exp(total(b, cj)) * s + sl[b, :, cj]
            d = jnp.exp(total(3 - b, cj)) * d + dl[3 - b, :, cj]
        stt[0, :, cj] = s.astype(BF16)
        stt[1, :, cj] = d.astype(BF16)
        for k in (1, 2, 3):
            wraps = lax.div(y + k, 4)
            states[j, k] = send(47 + 3 * j + k - 1, stt.at[wraps, :, cj], str_.at[k - 1, :, cj], ydev(k))

    def pair_inside(j):
        cj = slice(128 * j, 128 * j + 128)

        def inside(b, rows):
            cum = cums[rows, :]
            c0, c1 = cum[:, 2 * j : 2 * j + 1], cum[:, 2 * j + 1 : 2 * j + 2]
            r0, r1 = cumt[b, 2 * j : 2 * j + 1, :], cumt[b, 2 * j + 1 : 2 * j + 2, :]
            w0 = jnp.where(causal, jnp.exp(jnp.where(causal, c0 - r0, 0.0)), 0.0)
            w1 = jnp.where(causal, jnp.exp(jnp.where(causal, c1 - r1, 0.0)), 0.0)
            u0 = jnp.where(anti, jnp.exp(jnp.where(anti, r0 - c0, 0.0)), 0.0)
            u1 = jnp.where(anti, jnp.exp(jnp.where(anti, r1 - c1, 0.0)), 0.0)
            scores, scores_t = gs[b], gts[b]
            m = jnp.concatenate([scores * w0, scores * w1], axis=1).astype(BF16)
            mt = jnp.concatenate([scores_t * u0, scores_t * u1], axis=1).astype(BF16)
            x16 = xb[rows, cj]
            o16 = cot[rows, cj]
            zero = jnp.zeros_like(x16)
            xd = jnp.concatenate([jnp.where(low, x16, zero), jnp.where(low, zero, x16)], axis=0)
            od = jnp.concatenate([jnp.where(low, o16, zero), jnp.where(low, zero, o16)], axis=0)
            yy = mm(m, xd)
            pp = mm(o16, xd, NT)
            dx = mm(mt, od)
            dgs[b] = dgs[b] + w0 * pp[:, 0:128] + w1 * pp[:, 128:256]
            dxin[rows, cj] = dx
            q1s[rows, cj] = o16.astype(F32) * yy - x16.astype(F32) * dx

        blocks(inside)

    for copy in cots:
        copy.wait_recv()
    w_done(1, (5, 6, 7, 8))
    w_forward(3)
    w_across(3)
    pair_forward(0)
    w_across_far(2)
    pair_inside(0)
    w_across_far(3)
    pair_forward(1)
    pair_inside(1)
    w_done(2, (0, 3, 4, 7, 8))
    pair_forward(2)
    pair_inside(2)
    pair_forward(3)
    pair_inside(3)
    w_done(3, (0, 3, 4, 7, 8))
    pair_forward(4)
    pair_inside(4)

    def turn(b, rows):
        hidt[:, rows] = hidf[rows, :].T
        dcf[rows, :] = mm(dgs[b], bmf[rows, :], NN, highest)
        dbf[rows, :] = mm(dgs[b], cmf[rows, :], TN, highest)

    blocks(turn)
    for copy in totals:
        copy.wait_recv()

    lanes = lax.broadcasted_iota(jnp.int32, (256, 128), 0)
    outl = lax.broadcasted_iota(jnp.int32, (256, 128), 1)

    def sums(z, j):
        hi = z.astype(BF16)
        lo = (z - hi.astype(F32)).astype(BF16)
        choose = (outl == 2 * j + lax.rem(lax.div(lanes, 64), 2)).astype(F32).astype(BF16)
        return mm(jnp.concatenate([hi, lo], axis=1), choose)

    yes = [jnp.where(y >= k, 1.0, 0.0).astype(F32) for k in (1, 2, 3)]
    no = [jnp.where(y + k <= 3, 1.0, 0.0).astype(F32) for k in (1, 2, 3)]
    inner = [jnp.zeros((8, 128), F32) for _ in range(4)]
    gain = [jnp.zeros((8, 128), F32)]

    def pair_outside(j):
        cj = slice(128 * j, 128 * j + 128)
        for k in (1, 2, 3):
            states[j, k].wait_recv()
        t = [ttr[k, 0:1, cj] for k in range(3)]
        got = [str_[k, :, cj].astype(F32) for k in range(3)]
        s = yes[0] * got[0] + (yes[1] * jnp.exp(t[0])) * got[1] + (yes[2] * jnp.exp(t[0] + t[1])) * got[2]
        d = no[0] * got[2] + (no[1] * jnp.exp(t[2])) * got[1] + (no[2] * jnp.exp(t[2] + t[1])) * got[0]
        for b in (3, 2, 1, 0):
            db[b, :, cj] = d.astype(BF16)
            dd[b] = d
            d = jnp.exp(total(b, cj)) * d + dl[b, :, cj]
        for b in range(4):
            sb[b, :, cj] = s.astype(BF16)
            grown = jnp.exp(total(b, cj)) * s
            inner[b] = inner[b] + sums((grown * dd[b]).reshape(16, 8, 128).sum(axis=0), j)
            s = grown + sl[b, :, cj]

        def outside(b, rows):
            o = cot[rows, cj].astype(F32)
            yst = mm(cmf[rows, :].astype(BF16), sb[b, :, cj]) * ecs[rows, cj]
            dxst = mm(bmf[rows, :].astype(BF16), db[b, :, cj]) * tls[rows, cj]
            val = vv[rows, cj]
            dxs = dxin[rows, cj] + dxst
            z = jnp.concatenate([q1s[rows, cj] + o * yst, xb[rows, cj].astype(F32) * dxst, dxs * val], axis=0)
            red[b] = red[b] + sums(z, j)
            dval = dxs * sexp[rows, cj] + pair(skip, j) * o
            rr[rows, cj] = (dval * silu_grad(projv[rows, cj])).astype(BF16)
            gain[0] = gain[0] + sums((o * val).reshape(16, 8, 128).sum(axis=0), j)

        blocks(outside)

    class Stream:
        def __init__(self, base, lo, hi, kind, bufs):
            self.base, self.lo, self.hi, self.kind = base, lo, hi, kind
            (self.dw, self.s1, self.r1p, self.r1m, self.s2p, self.s2m, self.r2p, self.r2m,
             self.s3, self.r3, self.s4, self.r4, self.sd, self.rd) = bufs
            self.index, self.dev, self.index2, self.dev2 = (y, ydev, x, xdev) if kind == 0 else (x, xdev, y, ydev)

        def first(self):
            for i in (2, 1, 3, 0):
                rows = ds(lax.rem(self.index + i, 4) * 320, 320)
                self.dw[rows, :] = mm(hidt[rows, :], rr[:, self.lo : self.hi])
                if i == 2:
                    self.s1[...] = self.dw[rows, :].astype(BF16)
                    self.one = (
                        send(self.base, self.s1.at[0:160, :], self.r1p, self.dev(1)),
                        send(self.base + 1, self.s1.at[160:320, :], self.r1m, self.dev(-1)),
                    )

        def second(self):
            nxt = lax.rem(self.index + 1, 4) * 320
            prv = lax.rem(self.index + 3, 4) * 320
            self.one[0].wait_recv()
            self.s2p[0:160, :] = (self.dw[ds(nxt, 160), :] + self.r1p[...].astype(F32)).astype(BF16)
            self.s2p[160:320, :] = self.dw[ds(nxt + 160, 160), :].astype(BF16)
            up = send(self.base + 2, self.s2p, self.r2p, self.dev(1))
            self.one[1].wait_recv()
            self.s2m[0:160, :] = self.dw[ds(prv, 160), :].astype(BF16)
            self.s2m[160:320, :] = (self.dw[ds(prv + 160, 160), :] + self.r1m[...].astype(F32)).astype(BF16)
            self.two = (up, send(self.base + 3, self.s2m, self.r2m, self.dev(-1)))

        def third(self):
            for copy in self.two:
                copy.wait_recv()
            here = ds(self.index * 320, 320)
            summed = self.dw[here, :] + self.r2p[...].astype(F32) + self.r2m[...].astype(F32)
            self.dw[here, :] = summed
            self.s3[...] = summed.astype(BF16)
            self.three = [
                send(self.base + 3 + k, self.s3.at[ds(lax.rem(self.index2 + k, 4) * 80, 80), :], self.r3.at[k - 1], self.dev2(k))
                for k in (2, 1, 3)
            ]

        def fourth(self):
            for copy in self.three:
                copy.wait_recv()
            rows = ds(self.index * 320 + self.index2 * 80, 80)
            self.s4[...] = self.dw[rows, :] + self.r3[0].astype(F32) + self.r3[1].astype(F32) + self.r3[2].astype(F32)
            self.four = send(self.base + 7, self.s4.at[ds((1 - zh) * 40, 40), :], self.r4, zpair)

        def owners(self):
            self.four.wait_recv()
            chunk = self.s4[ds(zh * 40, 40), :] + self.r4[...]
            self.moves = []
            for i in range(4):
                self.sd[i, 0:10, :] = chunk[10 * i : 10 * i + 10, :]
                dev = {
                    "seq_0": self.index,
                    "seq_1": lax.div(self.index2, 2),
                    "seq_2": lax.rem(self.index2, 2),
                    "zero_0": zh * 2 + i // 2,
                    "zero_1": jnp.int32(i % 2),
                }
                copy = pltpu.make_async_remote_copy(
                    src_ref=self.sd.at[i], dst_ref=self.rd.at[g], send_sem=ss.at[self.base + 8 + i],
                    recv_sem=rs.at[self.base + 8 + g], device_id=dev, device_id_type=MESH,
                )
                keep = jnp.logical_and(to_me[self.kind], part == i)

                @pl.when(jnp.logical_not(keep))
                def _():
                    copy.start()

                @pl.when(keep)
                def _():
                    self.rd[g] = self.sd[i]

                self.moves.append((copy, keep))

        def finish(self):
            for k in range(4):
                copy = pltpu.make_async_remote_copy(
                    src_ref=self.sd.at[0], dst_ref=self.rd.at[k], send_sem=ss.at[self.base + 8],
                    recv_sem=rs.at[self.base + 8 + k], device_id=core, device_id_type=MESH,
                )

                @pl.when(jnp.logical_not(jnp.logical_and(to_me[self.kind], g == k)))
                def _():
                    copy.wait_recv()

        def close(self):
            for copy, keep in self.moves:

                @pl.when(jnp.logical_not(keep))
                def _():
                    copy.wait_send()

    alpha = Stream(62, 0, 384, 0, (dwa, sa1, ra1p, ra1m, sa2p, sa2m, ra2p, ra2m, sa3, ra3, sa4, ra4, sd, rd))
    beta = Stream(74, 384, 640, 1, (dwb, sb1, rb1p, rb1m, sb2p, sb2m, rb2p, rb2m, sb3, rb3, sb4, rb4, sdb, rdb))
    gamma = Stream(86, 640, 768, 1, (dwc, sc1, rc1p, rc1m, sc2p, sc2m, rc2p, rc2m, sc3, rc3, sc4, rc4, sdc, rdc))

    pair_outside(0)
    pair_outside(1)
    pair_outside(2)
    alpha.first()
    pair_outside(3)
    pair_outside(4)
    beta.first()
    alpha.second()

    ownl = coli < 10
    bias_sum = decay_sum = jnp.zeros((8, 128), F32)
    for b in range(4):
        rows = slice(128 * b, 128 * b + 128)
        dcf[rows, :] = dcf[rows, :] + mm(oe[rows, :], sb[b], NT)
        dbf[rows, :] = dbf[rows, :] + mm(xt[rows, :], db[b], NT)
        dlog = mm(upper, red[b, 0:128], NN, highest) + mm(strict, red[b, 128:256], NN, highest)
        dlog = jnp.where(ownl, dlog + inner[b].sum(axis=0, keepdims=True), 0.0)
        ddt = (red[b, 256:384] + neg * dlog) * jax.nn.sigmoid(projs[rows, 128:256] + bias)
        ddt = jnp.where(ownl, ddt, 0.0)
        rdt[rows, :] = ddt.astype(BF16)
        bias_sum = bias_sum + ddt.reshape(16, 8, 128).sum(axis=0)
        decay_sum = decay_sum + (dlog * lgd[rows, :]).reshape(16, 8, 128).sum(axis=0)
    first = c == 0
    place = jnp.where(jnp.logical_and(rowi < 10, coli == rowi + 10 * g), 1.0, 0.0).astype(F32)
    spread = mm(rdt[...], place.astype(BF16)).astype(BF16)
    t1d[...] = spread
    t1s[...] = jnp.where(first, dcf[...], dbf[...])
    t1 = [send(98, t1s, t1r, core), send(99, t1d, t1dr, core)]
    row8 = lax.broadcasted_iota(jnp.int32, (8, 128), 0)
    packed = jnp.where(
        row8 == 0, bias_sum.sum(axis=0, keepdims=True),
        jnp.where(row8 == 1, decay_sum.sum(axis=0, keepdims=True),
                  jnp.where(row8 == 2, gain[0].sum(axis=0, keepdims=True), 0.0)),
    )
    heads_y[y] = mm(packed, place, NN, highest)
    head_y = [send(100 + k, heads_y.at[y], heads_y.at[y], ydev(k)) for k in (1, 2, 3)]
    beta.second()
    for copy in t1:
        copy.wait_recv()
    mixed = jnp.where(first, dbf[...], dcf[...]) + t1r[...]
    dt2 = spread.astype(F32) + t1dr[...].astype(F32)
    north = a == 0
    t2s[...] = jnp.where(north, dt2, mixed).astype(BF16)
    t2 = send(104, t2s, t2r, rank(2)[2])

    def token(b, rows):
        hgp[rows, :] = mm(rr[rows, 0:640], wf[:, 0:640], NT) + mm(rdt[rows, :], wf[:, 768:896], NT)

    blocks(token, False)
    t2.wait_recv()
    came = t2r[...].astype(F32)
    tile = projs[:, ds(256 * c, 128, 128)]
    upper_pick = ((mixed + came) * silu_grad(tile)).astype(BF16).astype(F32)
    lower_pick = jnp.where(first, dt2 + came, 0.0)
    rr[:, 640:768] = jnp.where(north, upper_pick, lower_pick).astype(BF16)
    shr[...] = jnp.where(north, upper_pick, 0.0).astype(BF16)
    gamma.first()
    hgc = []
    for k in (2, 3, 1):
        zlk, ck, dev = rank(k)
        rows = ds((zlk * 2 + ck) * 128, 128)
        hgs[k - 1] = (hgp[rows, :] + mm(shr[rows, :], wf[:, ds(lane0, 128)], NT)).astype(BF16)
        hgc.append(send(104 + k, hgs.at[k - 1], hgr.at[k - 1], dev))
    hgp[here_id, :] = hgp[here_id, :] + mm(shr[here_id, :], wf[:, ds(lane0, 128)], NT)
    gamma.second()
    alpha.third()
    beta.third()
    for copy in head_y:
        copy.wait_recv()
    heads_x[x] = (heads_y[0] + heads_y[1]) + (heads_y[2] + heads_y[3])
    head_x = [send(107 + k, heads_x.at[x], heads_x.at[x], xdev(k)) for k in (1, 2, 3)]
    gamma.third()
    beta.fourth()
    alpha.fourth()
    for copy in head_x:
        copy.wait_recv()
    heads_z[zh] = (heads_x[0] + heads_x[1]) + (heads_x[2] + heads_x[3])
    head_z = send(111, heads_z.at[zh], heads_z.at[zh], zpair)
    gamma.fourth()
    beta.owners()
    alpha.owners()
    gamma.owners()
    head_z.wait_recv()
    heads_g[r] = heads_z[0] + heads_z[1]
    head_g = [send(111 + k, heads_g.at[r], heads_g.at[r], rank(k)[2]) for k in (1, 2, 3)]
    for copy in hgc:
        copy.wait_recv()
    out = hgp[here_id, :] + hgr[0].astype(F32) + hgr[1].astype(F32) + hgr[2].astype(F32)
    hg_ref[...] = out.astype(BF16)
    beta.finish()
    for k in range(4):
        wg_ref[:, 640 * k + 384 : 640 * k + 640] = rdb[k, 0:10, :]
    alpha.finish()
    for k in range(4):
        wg_ref[:, 640 * k : 640 * k + 384] = rd[k, 0:10, :]
    gamma.finish()
    wg_ref[:, 2560:2688] = rdc[0, 0:10, :]
    wg_ref[:, 2688:2816] = rdc[1, 0:10, :]
    wg_ref[:, 2816:2856] = rdc[2, 0:10, 0:40]
    for copy in head_g:
        copy.wait_recv()
    hd_ref[...] = (heads_g[0] + heads_g[1]) + (heads_g[2] + heads_g[3])
    for copy in pending:
        copy.wait_send()
    for stream in (alpha, beta, gamma):
        stream.close()


def scratch():
    def v(shape, dtype=F32):
        return pltpu.VMEM(shape, dtype)

    def stream(n):
        half, whole = v((160, n), BF16), v((320, n), BF16)
        return [
            v((D, n)), whole, half, half, whole, whole, whole, whole, whole,
            v((3, 80, n), BF16), v((80, n)), v((40, n)), v((4, 16, n)), v((4, 16, n)),
        ]

    wide, wide16 = v((512, COLS)), v((512, COLS), BF16)
    thin, thin16 = v((512, 128)), v((512, 128), BF16)
    return [
        v((512, D), BF16), v((D, 512), BF16), wide16, v((160, 2856), BF16), v((D, 1024), BF16),
        v((512, 384)), wide, thin, thin, thin, thin, v((4, 16, 128)), thin,
        v((4, 128, 128)), v((4, 128, 128)), v((4, 128, 128)),
        wide, wide, wide, wide, wide16, wide16, wide16, v((32, COLS)),
        v((4, 128, COLS)), v((4, 128, COLS)), v((2, 128, COLS), BF16), v((8, COLS)),
        v((3, 128, COLS), BF16), v((3, 8, COLS)), wide, wide, thin, thin,
        v((4, 128, COLS), BF16), v((4, 128, COLS), BF16), v((4, 128, 128)), v((4, 384, 128)),
        v((512, 768), BF16), thin16, thin, thin, thin16, thin16, thin16, thin16, thin16,
        v((512, D)), v((3, 128, D), BF16), v((3, 128, D), BF16),
        *stream(384), *stream(256), *stream(128),
        v((4, 8, 128)), v((4, 8, 128)), v((2, 8, 128)), v((4, 8, 128)),
        pltpu.SemaphoreType.DMA((116,)), pltpu.SemaphoreType.DMA((116,)), pltpu.SemaphoreType.DMA((8,)),
    ]


def body(hidden, output_grad, input_weight, step_bias, decay_log, skip_gain):
    anyspace = pl.BlockSpec(memory_space=pl.ANY)
    vmem = pl.BlockSpec(memory_space=pltpu.VMEM)
    hg, wg, hd = pl.pallas_call(
        kernel,
        out_shape=(
            jax.ShapeDtypeStruct((128, D), BF16),
            jax.ShapeDtypeStruct((10, 2856), F32),
            jax.ShapeDtypeStruct((8, 128), F32),
        ),
        in_specs=[anyspace, anyspace, anyspace, vmem, vmem, vmem],
        out_specs=(vmem, vmem, vmem),
        scratch_shapes=scratch(),
        compiler_params=pltpu.CompilerParams(has_side_effects=True, collective_id=0, vmem_limit_bytes=64000000),
    )(hidden[0], output_grad[0], input_weight, step_bias[None], decay_log[None], skip_gain[None])
    return (hg[None], wg, hd[0:3, 0:HEADS])


def solution(mesh):
    torus = Mesh(
        mesh.devices.reshape(4, 2, 2, 4, 2), ("seq_0", "seq_1", "seq_2", "zero_0", "zero_1")
    )
    in_specs = (P(ZERO, SEQ, None), P(ZERO, SEQ, None), P(ZERO, None), P(), P(), P())
    out_specs = (P(ZERO, SEQ, None), P(SEQ_ZERO, None), P())
    return jax.shard_map(body, mesh=torus, in_specs=in_specs, out_specs=out_specs, check_vma=False)
```

```python
import functools

import jax
import jax.numpy as jnp
from jax import lax
from jax.experimental import pallas as pl
from jax.experimental.pallas import tpu as pltpu
from jax.sharding import Mesh
from jax.sharding import PartitionSpec as P

HEADS = 40
STATE = 128
INNER = 2560
D = 1280
COLS = 640
ZERO = ("zero_0", "zero_1")
SEQ = ("seq_0", "seq_1", "seq_2")
SEQ_ZERO = ("seq_0", "seq_1", "seq_2", "zero_0", "zero_1")
MESH = pl.DeviceIdType.MESH
F32 = jnp.float32
BF16 = jnp.bfloat16
highest = lax.Precision.HIGHEST
NN = (((1,), (0,)), ((), ()))
NT = (((1,), (1,)), ((), ()))
TN = (((0,), (0,)), ((), ()))


def mm(a, b, dims=NN, precision=None):
    return lax.dot_general(a, b, dims, preferred_element_type=F32, precision=precision)


def ds(start, size, align=None):
    return pl.ds(pl.multiple_of(start, align or size), size)


def silu_grad(v):
    sig = jax.nn.sigmoid(v)
    return sig * (1.0 + v * (1.0 - sig))


def kernel(
    hid_ref, cot_ref, w_ref, bias_ref, decay_ref, skip_ref,
    hg_ref, wg_ref, hd_ref,
    hidf, hidt, hidx, cot, wraw, wf, projs, projv, bmf, cmf, lgd, cums, cumt, stp, gs, gts, dgs,
    sexp, ecs, tls, vv, xb, xt, oe, tot,
    sl, dl, stt, tts, str_, ttr, q1s, dxin, dbf, dcf, sb, db, dd, red,
    rr, rdt, t1s, t1r, t1d, t1dr, t2s, t2r, shr, hgp, hgs, hgr,
    dwa, sa1, ra1p, ra1m, sa2p, sa2m, ra2p, ra2m, sa3, ra3, sa4, ra4, sd, rd,
    dwb, sb1, rb1p, rb1m, sb2p, sb2m, rb2p, rb2m, sb3, rb3, sb4, rb4, sdb, rdb,
    dwc, sc1, rc1p, rc1m, sc2p, sc2m, rc2p, rc2m, sc3, rc3, sc4, rc4, sdc, rdc,
    heads_y, heads_x, heads_z, heads_g, extras, hgo, wgo, hdo,
    ss, rs, ls,
):
    y, zl, c = (lax.axis_index(n) for n in SEQ)
    x, zh = (lax.axis_index(n) for n in ZERO)
    r = zl * 2 + c
    a = lax.rem(zl + zh, 2)
    g = a * 2 + c
    pending = []

    def send(i, src, dst, where):
        copy = pltpu.make_async_remote_copy(
            src_ref=src, dst_ref=dst, send_sem=ss.at[i], recv_sem=rs.at[i],
            device_id=where, device_id_type=MESH,
        )
        copy.start()
        pending.append(copy)
        return copy

    def rank(k):
        zlk = lax.rem(zl + k // 2, 2)
        ck = lax.rem(c + k % 2, 2)
        return zlk, ck, {"seq_1": zlk, "seq_2": ck}

    def xdev(k):
        return {"zero_0": lax.rem(x + k + 4, 4)}

    def ydev(k):
        return {"seq_0": lax.rem(y + k + 4, 4)}

    zpair = {"seq_1": 1 - zl, "zero_1": 1 - zh}
    core = {"seq_2": 1 - c}
    here_id = ds(r * 128, 128)

    def shard(xk, zk, lo=0, size=160):
        return ds((lax.rem(xk + 4, 4) * 2 + zk) * 160 + lo, size, 16)

    own = shard(x, zh)
    lane0 = 640 + 256 * c
    local = [
        pltpu.make_async_copy(w_ref, wraw, ls.at[0]),
        pltpu.make_async_copy(w_ref.at[:, ds(g * COLS, COLS, 128)], wf.at[own, 0:640], ls.at[1]),
        pltpu.make_async_copy(w_ref.at[:, ds(2560 + 128 * c, 128)], wf.at[own, ds(lane0, 128)], ls.at[2]),
        pltpu.make_async_copy(hid_ref, hidf.at[here_id, :], ls.at[3]),
        pltpu.make_async_copy(cot_ref.at[:, ds(g * COLS, COLS, 128)], cot.at[here_id, :], ls.at[4]),
    ]
    for copy in local:
        copy.start()

    barrier = pltpu.get_barrier_semaphore()

    def greet(dev):
        pl.semaphore_signal(barrier, inc=1, device_id=dev, device_id_type=MESH)

    greet(zpair)
    for k in (1, 2, 3):
        greet(xdev(k))
        greet(ydev(k))
        greet(rank(k)[2])
    coli = lax.broadcasted_iota(jnp.int32, (128, 128), 1)
    rowi = lax.broadcasted_iota(jnp.int32, (128, 128), 0)
    local[0].wait()
    tail = jnp.concatenate([wraw[:, 2816:2856].astype(F32), jnp.zeros((160, 88), F32)], axis=1)
    tail = pltpu.roll(tail, lax.rem(128 - 10 * g, 128), 1)
    keep10 = lax.broadcasted_iota(jnp.int32, (160, 128), 1) < 10
    wf[own, 768:896] = jnp.where(keep10, tail, 0.0).astype(BF16)

    def lanes10(ref):
        full = jnp.concatenate([ref[...], jnp.zeros((1, 88), F32)], axis=1)
        return pltpu.roll(jnp.broadcast_to(full, (8, 128)), lax.rem(128 - 10 * g, 128), 1)[0:1, :]

    bias = lanes10(bias_ref)
    neg = -jnp.exp(lanes10(decay_ref))
    skip = lanes10(skip_ref)
    for copy in local[1:]:
        copy.wait()
    pl.semaphore_wait(barrier, 10)

    def cols(m):
        return (ds(640 + 128 * c, 256, 128), slice(0, 256), slice(256, 512), slice(512, 640))[m]

    w = {}

    def wsend(m, i, rows, dev):
        ref = wf.at[rows, cols(m)]
        w[m, i] = send(9 * m + i, ref, ref, dev)

    def w_own_x(m):
        wsend(m, 1, own, xdev(1))
        wsend(m, 2, own, xdev(-1))

    def w_own_z(m):
        wsend(m, 0, own, zpair)

    def w_other(m):
        w[m, 0].wait_recv()
        wsend(m, 3, shard(x, 1 - zh), xdev(1))
        wsend(m, 4, shard(x, 1 - zh), xdev(-1))

    def w_forward(m):
        w[m, 1].wait_recv()
        wsend(m, 5, shard(x - 1, zh, 0, 80), xdev(1))
        w[m, 2].wait_recv()
        wsend(m, 6, shard(x + 1, zh, 80, 80), xdev(-1))

    def w_forward_other(m):
        w[m, 3].wait_recv()
        wsend(m, 7, shard(x - 1, 1 - zh, 0, 80), xdev(1))
        w[m, 4].wait_recv()
        wsend(m, 8, shard(x + 1, 1 - zh, 80, 80), xdev(-1))

    def w_across(m):
        wsend(m, 3, shard(x - 1, zh), zpair)
        wsend(m, 4, shard(x + 1, zh), zpair)

    def w_across_far(m):
        w[m, 5].wait_recv()
        wsend(m, 7, shard(x + 2, zh, 0, 80), zpair)
        w[m, 6].wait_recv()
        wsend(m, 8, shard(x + 2, zh, 80, 80), zpair)

    def w_done(m, which):
        for i in which:
            w[m, i].wait_recv()

    w_own_z(0)
    w_own_x(0)
    h_z = send(37, hid_ref, hidf.at[here_id, :], rank(2)[2])
    w_own_z(1)
    w_own_x(1)
    h_c = send(36, hid_ref, hidf.at[here_id, :], core)
    cots = []
    for k in (2, 3, 1):
        zlk, ck, dev = rank(k)
        gk = lax.rem(zlk + zh, 2) * 2 + ck
        cots.append(send(38 + k, cot_ref.at[:, ds(gk * COLS, COLS, 128)], cot.at[here_id, :], dev))
    w_other(0)
    w_forward(0)
    w_own_x(2)
    w_own_z(2)
    w_other(1)
    w_forward_other(0)
    w_forward(1)
    h_z.wait_recv()
    zrows = ds((rank(2)[0] * 2 + c) * 128, 128)
    h_f = send(38, hidf.at[zrows, :], hidf.at[zrows, :], core)
    w_own_x(3)
    w_own_z(3)
    w_done(0, (5, 6, 7, 8))
    mate = send(42, wf.at[:, ds(lane0, 128)], wf.at[:, ds(lane0, 128)], core)
    w_forward(2)
    w_across(2)
    w_forward_other(1)
    h_c.wait_recv()
    h_f.wait_recv()
    mate.wait_recv()

    low = coli < 64
    causal = rowi >= coli
    anti = rowi <= coli
    tri = causal.astype(F32)
    upper = anti.astype(F32)
    strict = (rowi > coli).astype(F32)

    def pair(v, j):
        return jnp.where(low[0 : v.shape[0]], v[:, 2 * j : 2 * j + 1], v[:, 2 * j + 1 : 2 * j + 2])

    def blocks(f, unroll=True):
        if unroll:
            for b in range(4):
                f(b, pl.ds(b * 128, 128))
        else:
            def step(b, carry):
                f(b, ds(b * 128, 128))
                return carry

            lax.fori_loop(0, 4, step, 0)

    def common(b, rows):
        p = mm(hidf[rows, :], wf[:, 640:1024])
        projs[rows, :] = p
        bm = jax.nn.silu(p[:, 0:128])
        cm = jax.nn.silu(p[:, 256:384])
        bmf[rows, :] = bm
        cmf[rows, :] = cm
        pre = p[:, 128:256] + bias
        step = jnp.maximum(pre, 0.0) + jnp.log1p(jnp.exp(-jnp.abs(pre)))
        lg = neg * step
        cum = mm(tri, lg, NN, highest)
        stp[rows, :] = step
        lgd[rows, :] = lg
        cums[rows, :] = cum
        cumt[b] = cum.T[0:16, :]
        scores = mm(cm, bm, NT, highest)
        gs[b] = scores
        gts[b] = scores.T
        dgs[b] = jnp.zeros((128, 128), F32)
        red[b] = jnp.zeros((384, 128), F32)

    blocks(common)
    for j in range(5):
        cj = slice(128 * j, 128 * j + 128)
        for b in range(4):
            last_row = cums[128 * b + 127 : 128 * b + 128, :]
            tot[8 * b : 8 * b + 8, cj] = pair(jnp.broadcast_to(last_row, (8, 128)), j)
    tts[...] = tot[0:8, :] + tot[8:16, :] + tot[16:24, :] + tot[24:32, :]
    totals = [send(43 + k, tts, ttr.at[k - 1], ydev(k)) for k in (1, 2, 3)]

    def total(b, cj):
        return tot[8 * b : 8 * b + 1, cj]

    states = {}

    def pair_forward(j):
        cj = slice(128 * j, 128 * j + 128)

        def local_part(b, rows):
            ce = pair(cums[rows, :], j)
            se = pair(stp[rows, :], j)
            ec = jnp.exp(ce)
            tl = jnp.exp(ce[127:128, :] - ce)
            val = jax.nn.silu(projv[rows, cj])
            xs = val * se
            sexp[rows, cj] = se
            ecs[rows, cj] = ec
            tls[rows, cj] = tl
            vv[rows, cj] = val
            xb[rows, cj] = xs.astype(BF16)
            x16 = (xs * tl).astype(BF16)
            o16 = (cot[rows, cj].astype(F32) * ec).astype(BF16)
            xt[rows, cj] = x16
            oe[rows, cj] = o16
            sl[b, :, cj] = mm(bmf[rows, :].astype(BF16), x16, TN)
            dl[b, :, cj] = mm(cmf[rows, :].astype(BF16), o16, TN)

        projv[:, cj] = mm(hidf[...], wf[:, cj])
        blocks(local_part)
        s = sl[0, :, cj]
        d = dl[3, :, cj]
        for b in range(1, 4):
            s = jnp.exp(total(b, cj)) * s + sl[b, :, cj]
            d = jnp.exp(total(3 - b, cj)) * d + dl[3 - b, :, cj]
        stt[0, :, cj] = s.astype(BF16)
        stt[1, :, cj] = d.astype(BF16)
        for k in (1, 2, 3):
            wraps = lax.div(y + k, 4)
            states[j, k] = send(47 + 3 * j + k - 1, stt.at[wraps, :, cj], str_.at[k - 1, :, cj], ydev(k))

    def pair_inside(j):
        cj = slice(128 * j, 128 * j + 128)

        def inside(b, rows):
            cum = cums[rows, :]
            c0, c1 = cum[:, 2 * j : 2 * j + 1], cum[:, 2 * j + 1 : 2 * j + 2]
            r0, r1 = cumt[b, 2 * j : 2 * j + 1, :], cumt[b, 2 * j + 1 : 2 * j + 2, :]
            w0 = jnp.where(causal, jnp.exp(jnp.where(causal, c0 - r0, 0.0)), 0.0)
            w1 = jnp.where(causal, jnp.exp(jnp.where(causal, c1 - r1, 0.0)), 0.0)
            u0 = jnp.where(anti, jnp.exp(jnp.where(anti, r0 - c0, 0.0)), 0.0)
            u1 = jnp.where(anti, jnp.exp(jnp.where(anti, r1 - c1, 0.0)), 0.0)
            scores, scores_t = gs[b], gts[b]
            m = jnp.concatenate([scores * w0, scores * w1], axis=1).astype(BF16)
            mt = jnp.concatenate([scores_t * u0, scores_t * u1], axis=1).astype(BF16)
            x16 = xb[rows, cj]
            o16 = cot[rows, cj]
            zero = jnp.zeros_like(x16)
            xd = jnp.concatenate([jnp.where(low, x16, zero), jnp.where(low, zero, x16)], axis=0)
            od = jnp.concatenate([jnp.where(low, o16, zero), jnp.where(low, zero, o16)], axis=0)
            yy = mm(m, xd)
            pp = mm(o16, xd, NT)
            dx = mm(mt, od)
            dgs[b] = dgs[b] + w0 * pp[:, 0:128] + w1 * pp[:, 128:256]
            dxin[rows, cj] = dx
            q1s[rows, cj] = o16.astype(F32) * yy - x16.astype(F32) * dx

        blocks(inside)

    w_forward(3)
    w_across(3)

    i320 = lax.broadcasted_iota(jnp.int32, (320, 320), 0)
    k320 = lax.broadcasted_iota(jnp.int32, (320, 320), 1)
    tens = lax.shift_right_logical(i320 * 6554, 16)
    source = ((tens & 3) * 8 + lax.shift_right_logical(tens, 2)) * 10 + i320 - tens * 10
    perm = jnp.where(k320 == source, 1.0, 0.0).astype(F32).astype(BF16)
    for q in range(4):
        hidt[320 * q : 320 * q + 320, :] = mm(perm, hidf[:, 320 * q : 320 * q + 320], NT).astype(BF16)
    for copy in cots:
        copy.wait_recv()
    w_done(1, (5, 6, 7, 8))
    pair_forward(0)
    w_across_far(2)
    pair_inside(0)
    for p in range(4):
        for q in range(4):
            hidx[320 * p + 80 * q : 320 * p + 80 * q + 80, :] = hidt[320 * q + 80 * p : 320 * q + 80 * p + 80, :]
    w_across_far(3)
    pair_forward(1)
    pair_inside(1)
    w_done(2, (0, 3, 4, 7, 8))
    pair_forward(2)
    pair_inside(2)
    pair_forward(3)
    pair_inside(3)
    w_done(3, (0, 3, 4, 7, 8))
    pair_forward(4)
    pair_inside(4)

    def turn(b, rows):
        dcf[rows, :] = mm(dgs[b], bmf[rows, :], NN, highest)
        dbf[rows, :] = mm(dgs[b], cmf[rows, :], TN, highest)

    blocks(turn)
    for copy in totals:
        copy.wait_recv()

    lanes = lax.broadcasted_iota(jnp.int32, (256, 128), 0)
    outl = lax.broadcasted_iota(jnp.int32, (256, 128), 1)

    def sums(z, j):
        hi = z.astype(BF16)
        lo = (z - hi.astype(F32)).astype(BF16)
        choose = (outl == 2 * j + lax.rem(lax.div(lanes, 64), 2)).astype(F32).astype(BF16)
        return mm(jnp.concatenate([hi, lo], axis=1), choose)

    yes = [jnp.where(y >= k, 1.0, 0.0).astype(F32) for k in (1, 2, 3)]
    no = [jnp.where(y + k <= 3, 1.0, 0.0).astype(F32) for k in (1, 2, 3)]
    inner = [jnp.zeros((8, 128), F32) for _ in range(4)]
    gain = [jnp.zeros((8, 128), F32)]

    def pair_outside(j):
        cj = slice(128 * j, 128 * j + 128)
        for k in (1, 2, 3):
            states[j, k].wait_recv()
        t = [ttr[k, 0:1, cj] for k in range(3)]
        got = [str_[k, :, cj].astype(F32) for k in range(3)]
        s = yes[0] * got[0] + (yes[1] * jnp.exp(t[0])) * got[1] + (yes[2] * jnp.exp(t[0] + t[1])) * got[2]
        d = no[0] * got[2] + (no[1] * jnp.exp(t[2])) * got[1] + (no[2] * jnp.exp(t[2] + t[1])) * got[0]
        for b in (3, 2, 1, 0):
            db[b, :, cj] = d.astype(BF16)
            dd[b] = d
            d = jnp.exp(total(b, cj)) * d + dl[b, :, cj]
        for b in range(4):
            sb[b, :, cj] = s.astype(BF16)
            grown = jnp.exp(total(b, cj)) * s
            inner[b] = inner[b] + sums((grown * dd[b]).reshape(16, 8, 128).sum(axis=0), j)
            s = grown + sl[b, :, cj]

        def outside(b, rows):
            o = cot[rows, cj].astype(F32)
            yst = mm(cmf[rows, :].astype(BF16), sb[b, :, cj]) * ecs[rows, cj]
            dxst = mm(bmf[rows, :].astype(BF16), db[b, :, cj]) * tls[rows, cj]
            val = vv[rows, cj]
            dxs = dxin[rows, cj] + dxst
            z = jnp.concatenate([q1s[rows, cj] + o * yst, xb[rows, cj].astype(F32) * dxst, dxs * val], axis=0)
            red[b] = red[b] + sums(z, j)
            dval = dxs * sexp[rows, cj] + pair(skip, j) * o
            rr[rows, cj] = (dval * silu_grad(projv[rows, cj])).astype(BF16)
            gain[0] = gain[0] + sums((o * val).reshape(16, 8, 128).sum(axis=0), j)

        blocks(outside)

    class Stream:
        def __init__(self, base, lo, hi, kind, bufs):
            self.base, self.lo, self.hi, self.left = base, lo, hi, hidx if kind else hidt
            (self.dw, self.s1, self.r1p, self.r1m, self.s2p, self.s2m, self.r2p, self.r2m,
             self.s3, self.r3, self.s4, self.r4, self.sd, self.rd) = bufs
            self.index, self.dev, self.index2, self.dev2 = (y, ydev, x, xdev) if kind == 0 else (x, xdev, y, ydev)

        def first(self):
            for i in (2, 1, 3, 0):
                rows = ds(lax.rem(self.index + i, 4) * 320, 320)
                self.dw[rows, :] = mm(self.left[rows, :], rr[:, self.lo : self.hi])
                if i == 2:
                    self.s1[...] = self.dw[rows, :].astype(BF16)
                    self.one = (
                        send(self.base, self.s1.at[0:160, :], self.r1p, self.dev(1)),
                        send(self.base + 1, self.s1.at[160:320, :], self.r1m, self.dev(-1)),
                    )

        def second(self):
            nxt = lax.rem(self.index + 1, 4) * 320
            prv = lax.rem(self.index + 3, 4) * 320
            self.one[0].wait_recv()
            self.s2p[0:160, :] = (self.dw[ds(nxt, 160), :] + self.r1p[...].astype(F32)).astype(BF16)
            self.s2p[160:320, :] = self.dw[ds(nxt + 160, 160), :].astype(BF16)
            up = send(self.base + 2, self.s2p, self.r2p, self.dev(1))
            self.one[1].wait_recv()
            self.s2m[0:160, :] = self.dw[ds(prv, 160), :].astype(BF16)
            self.s2m[160:320, :] = (self.dw[ds(prv + 160, 160), :] + self.r1m[...].astype(F32)).astype(BF16)
            self.two = (up, send(self.base + 3, self.s2m, self.r2m, self.dev(-1)))

        def third(self):
            for copy in self.two:
                copy.wait_recv()
            here = ds(self.index * 320, 320)
            summed = self.dw[here, :] + self.r2p[...].astype(F32) + self.r2m[...].astype(F32)
            self.dw[here, :] = summed
            self.s3[...] = summed.astype(BF16)
            self.three = [
                send(self.base + 3 + k, self.s3.at[ds(lax.rem(self.index2 + k, 4) * 80, 80), :], self.r3.at[k - 1], self.dev2(k))
                for k in (2, 1, 3)
            ]

        def fourth(self):
            for copy in self.three:
                copy.wait_recv()
            rows = ds(self.index * 320 + self.index2 * 80, 80)
            self.s4[...] = self.dw[rows, :] + self.r3[0].astype(F32) + self.r3[1].astype(F32) + self.r3[2].astype(F32)
            self.four = send(self.base + 11, self.s4.at[ds((1 - zh) * 40, 40), :], self.r4, zpair)

        def owners(self):
            self.four.wait_recv()
            chunk = self.s4[ds(zh * 40, 40), :] + self.r4[...]
            for i in range(4):
                self.sd[i, 0:10, :] = chunk[10 * i : 10 * i + 10, :]
            self.rd[g] = self.sd[r]
            self.five = [
                send(self.base + 7 + k, self.sd.at[(rank(k)[0] * 2 + rank(k)[1])], self.rd.at[g], rank(k)[2])
                for k in (2, 3, 1)
            ]

        def finish(self):
            for copy in self.five:
                copy.wait_recv()

    alpha = Stream(62, 0, 384, 0, (dwa, sa1, ra1p, ra1m, sa2p, sa2m, ra2p, ra2m, sa3, ra3, sa4, ra4, sd, rd))
    beta = Stream(74, 384, 640, 1, (dwb, sb1, rb1p, rb1m, sb2p, sb2m, rb2p, rb2m, sb3, rb3, sb4, rb4, sdb, rdb))
    gamma = Stream(86, 640, 768, 1, (dwc, sc1, rc1p, rc1m, sc2p, sc2m, rc2p, rc2m, sc3, rc3, sc4, rc4, sdc, rdc))

    pair_outside(0)
    pair_outside(1)
    pair_outside(2)
    alpha.first()
    pair_outside(3)
    pair_outside(4)

    ownl = coli < 10
    bias_sum = decay_sum = jnp.zeros((8, 128), F32)
    for b in range(4):
        rows = slice(128 * b, 128 * b + 128)
        dcf[rows, :] = dcf[rows, :] + mm(oe[rows, :], sb[b], NT)
        dbf[rows, :] = dbf[rows, :] + mm(xt[rows, :], db[b], NT)
        dlog = mm(upper, red[b, 0:128], NN, highest) + mm(strict, red[b, 128:256], NN, highest)
        dlog = jnp.where(ownl, dlog + inner[b].sum(axis=0, keepdims=True), 0.0)
        ddt = (red[b, 256:384] + neg * dlog) * jax.nn.sigmoid(projs[rows, 128:256] + bias)
        ddt = jnp.where(ownl, ddt, 0.0)
        rdt[rows, :] = ddt.astype(BF16)
        bias_sum = bias_sum + ddt.reshape(16, 8, 128).sum(axis=0)
        decay_sum = decay_sum + (dlog * lgd[rows, :]).reshape(16, 8, 128).sum(axis=0)
    first = c == 0
    place = jnp.where(jnp.logical_and(rowi < 10, coli == rowi + 10 * g), 1.0, 0.0).astype(F32)
    spread = mm(rdt[...], place.astype(BF16)).astype(BF16)
    t1d[...] = spread
    t1s[...] = jnp.where(first, dcf[...], dbf[...])
    t1 = [send(98, t1s, t1r, core), send(99, t1d, t1dr, core)]
    beta.first()
    row8 = lax.broadcasted_iota(jnp.int32, (8, 128), 0)
    packed = jnp.where(
        row8 == 0, bias_sum.sum(axis=0, keepdims=True),
        jnp.where(row8 == 1, decay_sum.sum(axis=0, keepdims=True),
                  jnp.where(row8 == 2, gain[0].sum(axis=0, keepdims=True), 0.0)),
    )
    heads_y[y] = mm(packed, place, NN, highest)
    head_y = [send(100 + k, heads_y.at[y], heads_y.at[y], ydev(k)) for k in (1, 2, 3)]
    alpha.second()
    for copy in t1:
        copy.wait_recv()
    mixed = jnp.where(first, dbf[...], dcf[...]) + t1r[...]
    dt2 = spread.astype(F32) + t1dr[...].astype(F32)
    north = a == 0
    t2s[...] = jnp.where(north, dt2, mixed).astype(BF16)
    t2 = send(104, t2s, t2r, rank(2)[2])
    for n in range(5):
        part = slice(256 * n, 256 * n + 256)
        hgp[:, part] = mm(rr[:, 0:640], wf[part, 0:640], NT) + mm(rdt[...], wf[part, 768:896], NT)
    mate_row = ds((zl * 2 + 1 - c) * 128, 128)
    far_mate = ds(((1 - zl) * 2 + 1 - c) * 128, 128)
    far_row = ds(((1 - zl) * 2 + c) * 128, 128)
    hgs[1] = hgp[far_mate, :].astype(BF16)
    hg_far = send(106, hgs.at[1], hgr.at[1], core)
    hgs[0] = hgp[mate_row, :].astype(BF16)
    hg_near = send(105, hgs.at[0], hgr.at[0], core)
    beta.second()
    hg_far.wait_recv()
    hgs[2] = (hgp[far_row, :] + hgr[1].astype(F32)).astype(BF16)
    t2.wait_recv()
    hg_z = send(107, hgs.at[2], hgr.at[2], rank(2)[2])
    came = t2r[...].astype(F32)
    tile = projs[:, ds(256 * c, 128, 128)]
    upper_pick = ((mixed + came) * silu_grad(tile)).astype(BF16).astype(F32)
    lower_pick = jnp.where(first, dt2 + came, 0.0)
    rr[:, 640:768] = jnp.where(north, upper_pick, lower_pick).astype(BF16)
    shr[...] = jnp.where(north, upper_pick, lower_pick).astype(BF16)
    gamma.first()
    extras[g] = shr[here_id, :]
    extra = [
        send(111 + k, shr.at[ds((rank(k)[0] * 2 + rank(k)[1]) * 128, 128), :], extras.at[g], rank(k)[2])
        for k in (2, 3, 1)
    ]
    alpha.third()
    gamma.second()
    beta.third()
    for copy in head_y:
        copy.wait_recv()
    heads_x[x] = (heads_y[0] + heads_y[1]) + (heads_y[2] + heads_y[3])
    head_x = [send(107 + k, heads_x.at[x], heads_x.at[x], xdev(k)) for k in (1, 2, 3)]
    alpha.fourth()
    for copy in extra:
        copy.wait_recv()
    hgp[here_id, :] = hgp[here_id, :] + mm(extras[0], wf[:, 640:768], NT) + mm(extras[1], wf[:, 896:1024], NT)
    gamma.third()
    beta.fourth()
    for copy in head_x:
        copy.wait_recv()
    heads_z[zh] = (heads_x[0] + heads_x[1]) + (heads_x[2] + heads_x[3])
    head_z = send(111, heads_z.at[zh], heads_z.at[zh], zpair)
    alpha.owners()
    gamma.fourth()
    beta.owners()
    hg_near.wait_recv()
    hg_z.wait_recv()
    hgo[...] = (hgp[here_id, :] + hgr[0].astype(F32) + hgr[2].astype(F32)).astype(BF16)
    hg_out = pltpu.make_async_copy(hgo, hg_ref, ls.at[5])
    hg_out.start()
    head_z.wait_recv()
    heads_g[r] = heads_z[0] + heads_z[1]
    head_g = [send(114 + k, heads_g.at[r], heads_g.at[r], rank(k)[2]) for k in (1, 2, 3)]
    gamma.owners()
    alpha.finish()
    for k in range(4):
        wgo[:, 640 * k : 640 * k + 384] = rd[k, 0:10, :]
    beta.finish()
    for k in range(4):
        wgo[:, 640 * k + 384 : 640 * k + 640] = rdb[k, 0:10, :]
    for copy in head_g:
        copy.wait_recv()
    hdo[...] = (heads_g[0] + heads_g[1]) + (heads_g[2] + heads_g[3])
    hd_out = pltpu.make_async_copy(hdo, hd_ref, ls.at[6])
    hd_out.start()
    gamma.finish()
    wgo[:, 2560:2688] = rdc[0, 0:10, :]
    wgo[:, 2688:2816] = rdc[1, 0:10, :]
    wgo[:, 2816:2856] = rdc[2, 0:10, 0:40]
    wg_out = pltpu.make_async_copy(wgo, wg_ref, ls.at[7])
    wg_out.start()
    for copy in pending:
        copy.wait_send()
    hg_out.wait()
    hd_out.wait()
    wg_out.wait()


def scratch():
    def v(shape, dtype=F32):
        return pltpu.VMEM(shape, dtype)

    def stream(n):
        half, whole = v((160, n), BF16), v((320, n), BF16)
        return [
            v((D, n)), whole, half, half, whole, whole, whole, whole, whole,
            v((3, 80, n), BF16), v((80, n)), v((40, n)), v((4, 16, n)), v((4, 16, n)),
        ]

    wide, wide16 = v((512, COLS)), v((512, COLS), BF16)
    thin, thin16 = v((512, 128)), v((512, 128), BF16)
    return [
        v((512, D), BF16), v((D, 512), BF16), v((D, 512), BF16), wide16, v((160, 2856), BF16), v((D, 1024), BF16),
        v((512, 384)), wide, thin, thin, thin, thin, v((4, 16, 128)), thin,
        v((4, 128, 128)), v((4, 128, 128)), v((4, 128, 128)),
        wide, wide, wide, wide, wide16, wide16, wide16, v((32, COLS)),
        v((4, 128, COLS)), v((4, 128, COLS)), v((2, 128, COLS), BF16), v((8, COLS)),
        v((3, 128, COLS), BF16), v((3, 8, COLS)), wide, wide, thin, thin,
        v((4, 128, COLS), BF16), v((4, 128, COLS), BF16), v((4, 128, 128)), v((4, 384, 128)),
        v((512, 768), BF16), thin16, thin, thin, thin16, thin16, thin16, thin16, thin16,
        v((512, D)), v((3, 128, D), BF16), v((3, 128, D), BF16),
        *stream(384), *stream(256), *stream(128),
        v((4, 8, 128)), v((4, 8, 128)), v((2, 8, 128)), v((4, 8, 128)), v((4, 128, 128), BF16),
        v((128, D), BF16), v((10, 2856)), v((8, 128)),
        pltpu.SemaphoreType.DMA((120,)), pltpu.SemaphoreType.DMA((120,)), pltpu.SemaphoreType.DMA((8,)),
    ]


def body(hidden, output_grad, input_weight, step_bias, decay_log, skip_gain):
    anyspace = pl.BlockSpec(memory_space=pl.ANY)
    vmem = pl.BlockSpec(memory_space=pltpu.VMEM)
    hg, wg, hd = pl.pallas_call(
        kernel,
        out_shape=(
            jax.ShapeDtypeStruct((128, D), BF16),
            jax.ShapeDtypeStruct((10, 2856), F32),
            jax.ShapeDtypeStruct((8, 128), F32),
        ),
        in_specs=[anyspace, anyspace, anyspace, vmem, vmem, vmem],
        out_specs=(anyspace, anyspace, anyspace),
        scratch_shapes=scratch(),
        compiler_params=pltpu.CompilerParams(has_side_effects=True, collective_id=0, vmem_limit_bytes=64000000),
    )(hidden[0], output_grad[0], input_weight, step_bias[None], decay_log[None], skip_gain[None])
    return (hg[None], wg, hd[0:3, 0:HEADS])


def solution(mesh):
    torus = Mesh(
        mesh.devices.reshape(4, 2, 2, 4, 2), ("seq_0", "seq_1", "seq_2", "zero_0", "zero_1")
    )
    in_specs = (P(ZERO, SEQ, None), P(ZERO, SEQ, None), P(ZERO, None), P(), P(), P())
    out_specs = (P(ZERO, SEQ, None), P(SEQ_ZERO, None), P())
    return jax.shard_map(body, mesh=torus, in_specs=in_specs, out_specs=out_specs, check_vma=False)
```

```python
import functools

import jax
import jax.numpy as jnp
from jax import lax
from jax.experimental import pallas as pl
from jax.experimental.pallas import tpu as pltpu
from jax.sharding import Mesh
from jax.sharding import PartitionSpec as P

HEADS = 40
STATE = 128
INNER = 2560
D = 1280
COLS = 640
ZERO = ("zero_0", "zero_1")
SEQ = ("seq_0", "seq_1", "seq_2")
SEQ_ZERO = ("seq_0", "seq_1", "seq_2", "zero_0", "zero_1")
MESH = pl.DeviceIdType.MESH
F32 = jnp.float32
BF16 = jnp.bfloat16
highest = lax.Precision.HIGHEST
NN = (((1,), (0,)), ((), ()))
NT = (((1,), (1,)), ((), ()))
TN = (((0,), (0,)), ((), ()))


def mm(a, b, dims=NN, precision=None):
    return lax.dot_general(a, b, dims, preferred_element_type=F32, precision=precision)


def ds(start, size, align=None):
    return pl.ds(pl.multiple_of(start, align or size), size)


def silu_grad(v):
    sig = jax.nn.sigmoid(v)
    return sig * (1.0 + v * (1.0 - sig))


def kernel(
    hid_ref, cot_ref, w_ref, bias_ref, decay_ref, skip_ref,
    hg_ref, wg_ref, hd_ref,
    hidf, hidt, hidx, cot, wraw, wf, projs, projv, bmf, cmf, lgd, cums, cumt, stp, gs, gts, dgs,
    sexp, ecs, tls, vv, xb, xt, oe, tot,
    sl, dl, stt, tts, str_, ttr, q1s, dxin, dbf, dcf, sb, db, dd, red,
    rr, rdt, t1s, t1r, t1d, t1dr, t2s, t2r, shr, hgp, hgs, hgr,
    dwa, sa1, ra1, sa2, ra2, sa3, ra3, sa4, ra4, sda, rda,
    dwb, sb1, rb1, sb2, rb2, sb3, rb3, sb4, rb4, sdb, rdb,
    dwc, sc1, rc1, sc2, rc2, sc3, rc3, sc4, rc4, sdc, rdc,
    heads_y, heads_x, heads_z, heads_g, extras, hgo, wgo, hdo,
    ss, rs, ls,
):
    y, zl, c = (lax.axis_index(n) for n in SEQ)
    x, zh = (lax.axis_index(n) for n in ZERO)
    r = zl * 2 + c
    a = lax.rem(zl + zh, 2)
    g = a * 2 + c

    def send(i, src, dst, where, group):
        copy = pltpu.make_async_remote_copy(
            src_ref=src, dst_ref=dst, send_sem=ss.at[group], recv_sem=rs.at[i],
            device_id=where, device_id_type=MESH,
        )
        copy.start()
        return copy

    def bytes_of(ref, i=0, group=0):
        return pltpu.make_async_remote_copy(
            src_ref=ref, dst_ref=ref, send_sem=ss.at[group], recv_sem=rs.at[i],
            device_id={"seq_2": 1 - c}, device_id_type=MESH,
        )

    def got(i, ref):
        bytes_of(ref, i=i).wait_recv()

    def sent(group, ref):
        bytes_of(ref, group=group).wait_send()

    def rank(k):
        zlk = lax.rem(zl + k // 2, 2)
        ck = lax.rem(c + k % 2, 2)
        return zlk, ck, {"seq_1": zlk, "seq_2": ck}

    def xdev(k):
        return {"zero_0": lax.rem(x + k + 4, 4)}

    def ydev(k):
        return {"seq_0": lax.rem(y + k + 4, 4)}

    zpair = {"seq_1": 1 - zl, "zero_1": 1 - zh}
    core = {"seq_2": 1 - c}
    here_id = ds(r * 128, 128)

    def shard(xk, zk, lo=0, size=160):
        return ds((lax.rem(xk + 4, 4) * 2 + zk) * 160 + lo, size, 16)

    own = shard(x, zh)
    lane0 = 640 + 256 * c
    local = [
        pltpu.make_async_copy(w_ref, wraw, ls.at[0]),
        pltpu.make_async_copy(w_ref.at[:, ds(g * COLS, COLS, 128)], wf.at[own, 0:640], ls.at[1]),
        pltpu.make_async_copy(w_ref.at[:, ds(2560 + 128 * c, 128)], wf.at[own, ds(lane0, 128)], ls.at[2]),
        pltpu.make_async_copy(hid_ref, hidf.at[here_id, :], ls.at[3]),
        pltpu.make_async_copy(cot_ref.at[:, ds(g * COLS, COLS, 128)], cot.at[here_id, :], ls.at[4]),
    ]
    for copy in local:
        copy.start()

    barrier = pltpu.get_barrier_semaphore()

    def greet(dev):
        pl.semaphore_signal(barrier, inc=1, device_id=dev, device_id_type=MESH)

    greet(zpair)
    for k in (1, 2, 3):
        greet(xdev(k))
        greet(ydev(k))
        greet(rank(k)[2])
    coli = lax.broadcasted_iota(jnp.int32, (128, 128), 1)
    rowi = lax.broadcasted_iota(jnp.int32, (128, 128), 0)
    local[0].wait()
    tail = jnp.concatenate([wraw[:, 2816:2856].astype(F32), jnp.zeros((160, 88), F32)], axis=1)
    tail = pltpu.roll(tail, lax.rem(128 - 10 * g, 128), 1)
    keep10 = lax.broadcasted_iota(jnp.int32, (160, 128), 1) < 10
    wf[own, 768:896] = jnp.where(keep10, tail, 0.0).astype(BF16)

    def lanes10(ref):
        full = jnp.concatenate([ref[...], jnp.zeros((1, 88), F32)], axis=1)
        return pltpu.roll(jnp.broadcast_to(full, (8, 128)), lax.rem(128 - 10 * g, 128), 1)[0:1, :]

    bias = lanes10(bias_ref)
    neg = -jnp.exp(lanes10(decay_ref))
    skip = lanes10(skip_ref)
    for copy in local[1:]:
        copy.wait()
    pl.semaphore_wait(barrier, 10)

    def cols(m):
        return (ds(640 + 128 * c, 256, 128), slice(0, 256), slice(256, 512), slice(512, 640))[m]

    w = {}

    def wsend(m, i, rows, dev):
        ref = wf.at[rows, cols(m)]
        slot = min(i, 5) if m < 2 else {1: 1, 2: 2, 5: 3, 6: 4}.get(i, 5)
        w[m, i] = send(6 * m + slot, ref, ref, dev, m)

    def w_own_x(m):
        wsend(m, 1, own, xdev(1))
        wsend(m, 2, own, xdev(-1))

    def w_own_z(m):
        wsend(m, 0, own, zpair)

    def w_other(m):
        w[m, 0].wait_recv()
        wsend(m, 3, shard(x, 1 - zh), xdev(1))
        wsend(m, 4, shard(x, 1 - zh), xdev(-1))

    def w_forward(m):
        w[m, 1].wait_recv()
        wsend(m, 5, shard(x - 1, zh, 0, 80), xdev(1))
        w[m, 2].wait_recv()
        wsend(m, 6, shard(x + 1, zh, 80, 80), xdev(-1))

    def w_forward_other(m):
        w[m, 3].wait_recv()
        wsend(m, 7, shard(x - 1, 1 - zh, 0, 80), xdev(1))
        w[m, 4].wait_recv()
        wsend(m, 8, shard(x + 1, 1 - zh, 80, 80), xdev(-1))

    def w_across(m):
        wsend(m, 3, shard(x - 1, zh), zpair)
        wsend(m, 4, shard(x + 1, zh), zpair)

    def w_across_far(m):
        w[m, 5].wait_recv()
        wsend(m, 7, shard(x + 2, zh, 0, 80), zpair)
        w[m, 6].wait_recv()
        wsend(m, 8, shard(x + 2, zh, 80, 80), zpair)

    def w_done(m):
        got(6 * m + 5, wf.at[0 : 320 if m < 2 else 640, cols(m)])

    w_own_z(0)
    w_own_x(0)
    h_z = send(24, hid_ref, hidf.at[here_id, :], rank(2)[2], 4)
    w_own_z(1)
    w_own_x(1)
    h_c = send(25, hid_ref, hidf.at[here_id, :], core, 4)
    for k in (2, 3, 1):
        zlk, ck, dev = rank(k)
        gk = lax.rem(zlk + zh, 2) * 2 + ck
        send(27, cot_ref.at[:, ds(gk * COLS, COLS, 128)], cot.at[here_id, :], dev, 5)
    w_own_z(2)
    w_own_z(3)
    w_other(0)
    w_forward(0)
    w_forward_other(0)
    w_other(1)
    w_own_x(2)
    w_forward(1)
    h_z.wait_recv()
    zrows = ds((rank(2)[0] * 2 + c) * 128, 128)
    h_f = send(26, hidf.at[zrows, :], hidf.at[zrows, :], core, 4)
    w_own_x(3)
    w_done(0)
    mate = send(28, wf.at[:, ds(lane0, 128)], wf.at[:, ds(lane0, 128)], core, 6)
    w_forward_other(1)
    w_forward(2)
    w_across(2)
    h_c.wait_recv()
    h_f.wait_recv()
    mate.wait_recv()

    low = coli < 64
    causal = rowi >= coli
    anti = rowi <= coli
    tri = causal.astype(F32)
    upper = anti.astype(F32)
    strict = (rowi > coli).astype(F32)

    def pair(v, j):
        return jnp.where(low[0 : v.shape[0]], v[:, 2 * j : 2 * j + 1], v[:, 2 * j + 1 : 2 * j + 2])

    def blocks(f, unroll=True):
        if unroll:
            for b in range(4):
                f(b, pl.ds(b * 128, 128))
        else:
            def step(b, carry):
                f(b, ds(b * 128, 128))
                return carry

            lax.fori_loop(0, 4, step, 0)

    def common(b, rows):
        p = mm(hidf[rows, :], wf[:, 640:1024])
        projs[rows, :] = p
        bm = jax.nn.silu(p[:, 0:128])
        cm = jax.nn.silu(p[:, 256:384])
        bmf[rows, :] = bm
        cmf[rows, :] = cm
        pre = p[:, 128:256] + bias
        step = jnp.maximum(pre, 0.0) + jnp.log1p(jnp.exp(-jnp.abs(pre)))
        lg = neg * step
        cum = mm(tri, lg, NN, highest)
        stp[rows, :] = step
        lgd[rows, :] = lg
        cums[rows, :] = cum
        cumt[b] = cum.T[0:16, :]
        scores = mm(cm, bm, NT, highest)
        gs[b] = scores
        gts[b] = scores.T
        dgs[b] = jnp.zeros((128, 128), F32)
        red[b] = jnp.zeros((384, 128), F32)

    blocks(common)
    for j in range(5):
        cj = slice(128 * j, 128 * j + 128)
        for b in range(4):
            last_row = cums[128 * b + 127 : 128 * b + 128, :]
            tot[8 * b : 8 * b + 8, cj] = pair(jnp.broadcast_to(last_row, (8, 128)), j)
    tts[...] = tot[0:8, :] + tot[8:16, :] + tot[16:24, :] + tot[24:32, :]
    for k in (1, 2, 3):
        send(29, tts, ttr.at[k - 1], ydev(k), 7)

    def total(b, cj):
        return tot[8 * b : 8 * b + 1, cj]

    def pair_forward(j):
        cj = slice(128 * j, 128 * j + 128)

        def project(b, rows):
            projv[rows, cj] = mm(hidf[rows, :], wf[:, cj])

        def local_part(b, rows):
            ce = pair(cums[rows, :], j)
            se = pair(stp[rows, :], j)
            ec = jnp.exp(ce)
            tl = jnp.exp(ce[127:128, :] - ce)
            val = jax.nn.silu(projv[rows, cj])
            xs = val * se
            sexp[rows, cj] = se
            ecs[rows, cj] = ec
            tls[rows, cj] = tl
            vv[rows, cj] = val
            xb[rows, cj] = xs.astype(BF16)
            x16 = (xs * tl).astype(BF16)
            o16 = (cot[rows, cj].astype(F32) * ec).astype(BF16)
            xt[rows, cj] = x16
            oe[rows, cj] = o16
            sl[b, :, cj] = mm(bmf[rows, :].astype(BF16), x16, TN)
            dl[b, :, cj] = mm(cmf[rows, :].astype(BF16), o16, TN)

        blocks(project)
        blocks(local_part)
        s = sl[0, :, cj]
        d = dl[3, :, cj]
        for b in range(1, 4):
            s = jnp.exp(total(b, cj)) * s + sl[b, :, cj]
            d = jnp.exp(total(3 - b, cj)) * d + dl[3 - b, :, cj]
        stt[0, :, cj] = s.astype(BF16)
        stt[1, :, cj] = d.astype(BF16)
        for k in (1, 2, 3):
            wraps = lax.div(y + k, 4)
            send(30 + j, stt.at[wraps, :, cj], str_.at[k - 1, :, cj], ydev(k), 8)

    def pair_inside(j):
        cj = slice(128 * j, 128 * j + 128)

        def inside(b, rows):
            cum = cums[rows, :]
            c0, c1 = cum[:, 2 * j : 2 * j + 1], cum[:, 2 * j + 1 : 2 * j + 2]
            r0, r1 = cumt[b, 2 * j : 2 * j + 1, :], cumt[b, 2 * j + 1 : 2 * j + 2, :]
            w0 = jnp.where(causal, jnp.exp(jnp.where(causal, c0 - r0, 0.0)), 0.0)
            w1 = jnp.where(causal, jnp.exp(jnp.where(causal, c1 - r1, 0.0)), 0.0)
            u0 = jnp.where(anti, jnp.exp(jnp.where(anti, r0 - c0, 0.0)), 0.0)
            u1 = jnp.where(anti, jnp.exp(jnp.where(anti, r1 - c1, 0.0)), 0.0)
            scores, scores_t = gs[b], gts[b]
            m = jnp.concatenate([scores * w0, scores * w1], axis=1).astype(BF16)
            mt = jnp.concatenate([scores_t * u0, scores_t * u1], axis=1).astype(BF16)
            x16 = xb[rows, cj]
            o16 = cot[rows, cj]
            zero = jnp.zeros_like(x16)
            xd = jnp.concatenate([jnp.where(low, x16, zero), jnp.where(low, zero, x16)], axis=0)
            od = jnp.concatenate([jnp.where(low, o16, zero), jnp.where(low, zero, o16)], axis=0)
            yy = mm(m, xd)
            pp = mm(o16, xd, NT)
            dx = mm(mt, od)
            dgs[b] = dgs[b] + w0 * pp[:, 0:128] + w1 * pp[:, 128:256]
            dxin[rows, cj] = dx
            q1s[rows, cj] = o16.astype(F32) * yy - x16.astype(F32) * dx

        blocks(inside)

    w_forward(3)
    w_across(3)

    i320 = lax.broadcasted_iota(jnp.int32, (320, 320), 0)
    k320 = lax.broadcasted_iota(jnp.int32, (320, 320), 1)
    tens = lax.shift_right_logical(i320 * 6554, 16)
    source = ((tens & 3) * 8 + lax.shift_right_logical(tens, 2)) * 10 + i320 - tens * 10
    perm = jnp.where(k320 == source, 1.0, 0.0).astype(F32).astype(BF16)
    for q in range(4):
        hidt[320 * q : 320 * q + 320, :] = mm(perm, hidf[:, 320 * q : 320 * q + 320], NT).astype(BF16)
    got(27, cot.at[0:384, :])
    w_done(1)
    pair_forward(0)
    w_across_far(2)
    pair_inside(0)
    for p in range(4):
        for q in range(4):
            hidx[320 * p + 80 * q : 320 * p + 80 * q + 80, :] = hidt[320 * q + 80 * p : 320 * q + 80 * p + 80, :]
    w_across_far(3)
    pair_forward(1)
    pair_inside(1)
    w_done(2)
    pair_forward(2)
    pair_inside(2)
    pair_forward(3)
    pair_inside(3)
    w_done(3)
    pair_forward(4)
    pair_inside(4)

    def turn(b, rows):
        dcf[rows, :] = mm(dgs[b], bmf[rows, :], NN, highest)
        dbf[rows, :] = mm(dgs[b], cmf[rows, :], TN, highest)

    blocks(turn)
    got(29, ttr)

    lanes = lax.broadcasted_iota(jnp.int32, (256, 128), 0)
    outl = lax.broadcasted_iota(jnp.int32, (256, 128), 1)

    def sums(z, j):
        hi = z.astype(BF16)
        lo = (z - hi.astype(F32)).astype(BF16)
        choose = (outl == 2 * j + lax.rem(lax.div(lanes, 64), 2)).astype(F32).astype(BF16)
        return mm(jnp.concatenate([hi, lo], axis=1), choose)

    yes = [jnp.where(y >= k, 1.0, 0.0).astype(F32) for k in (1, 2, 3)]
    no = [jnp.where(y + k <= 3, 1.0, 0.0).astype(F32) for k in (1, 2, 3)]
    inner = [jnp.zeros((8, 128), F32) for _ in range(4)]
    gain = [jnp.zeros((8, 128), F32)]

    def pair_outside(j):
        cj = slice(128 * j, 128 * j + 128)
        got(30 + j, str_.at[:, :, cj])
        t = [ttr[k, 0:1, cj] for k in range(3)]
        came = [str_[k, :, cj].astype(F32) for k in range(3)]
        s = yes[0] * came[0] + (yes[1] * jnp.exp(t[0])) * came[1] + (yes[2] * jnp.exp(t[0] + t[1])) * came[2]
        d = no[0] * came[2] + (no[1] * jnp.exp(t[2])) * came[1] + (no[2] * jnp.exp(t[2] + t[1])) * came[0]
        for b in (3, 2, 1, 0):
            db[b, :, cj] = d.astype(BF16)
            dd[b] = d
            d = jnp.exp(total(b, cj)) * d + dl[b, :, cj]
        for b in range(4):
            sb[b, :, cj] = s.astype(BF16)
            grown = jnp.exp(total(b, cj)) * s
            inner[b] = inner[b] + sums((grown * dd[b]).reshape(16, 8, 128).sum(axis=0), j)
            s = grown + sl[b, :, cj]

        def outside(b, rows):
            o = cot[rows, cj].astype(F32)
            yst = mm(cmf[rows, :].astype(BF16), sb[b, :, cj]) * ecs[rows, cj]
            dxst = mm(bmf[rows, :].astype(BF16), db[b, :, cj]) * tls[rows, cj]
            val = vv[rows, cj]
            dxs = dxin[rows, cj] + dxst
            z = jnp.concatenate([q1s[rows, cj] + o * yst, xb[rows, cj].astype(F32) * dxst, dxs * val], axis=0)
            red[b] = red[b] + sums(z, j)
            dval = dxs * sexp[rows, cj] + pair(skip, j) * o
            rr[rows, cj] = (dval * silu_grad(projv[rows, cj])).astype(BF16)
            gain[0] = gain[0] + sums((o * val).reshape(16, 8, 128).sum(axis=0), j)

        blocks(outside)

    class Stream:
        def __init__(self, base, group, lo, hi, kind, bufs):
            self.base, self.group, self.lo, self.hi, self.left = base, group, lo, hi, hidx if kind else hidt
            self.dw, self.s1, self.r1, self.s2, self.r2, self.s3, self.r3, self.s4, self.r4, self.sd, self.rd = bufs
            self.index, self.dev, self.index2, self.dev2 = (y, ydev, x, xdev) if kind == 0 else (x, xdev, y, ydev)

        def send(self, i, src, dst, dev):
            return send(self.base + i, src, dst, dev, self.group)

        def first(self):
            for i in (2, 1, 3, 0):
                rows = ds(lax.rem(self.index + i, 4) * 320, 320)
                self.dw[rows, :] = mm(self.left[rows, :], rr[:, self.lo : self.hi])
                if i == 2:
                    self.s1[...] = self.dw[rows, :].astype(BF16)
                    self.one = (
                        self.send(0, self.s1.at[0:160, :], self.r1.at[0], self.dev(1)),
                        self.send(1, self.s1.at[160:320, :], self.r1.at[1], self.dev(-1)),
                    )

        def second(self):
            nxt = lax.rem(self.index + 1, 4) * 320
            prv = lax.rem(self.index + 3, 4) * 320
            self.one[0].wait_recv()
            self.s2[0, 0:160, :] = (self.dw[ds(nxt, 160), :] + self.r1[0].astype(F32)).astype(BF16)
            self.s2[0, 160:320, :] = self.dw[ds(nxt + 160, 160), :].astype(BF16)
            self.send(2, self.s2.at[0], self.r2.at[0], self.dev(1))
            self.one[1].wait_recv()
            self.s2[1, 0:160, :] = self.dw[ds(prv, 160), :].astype(BF16)
            self.s2[1, 160:320, :] = (self.dw[ds(prv + 160, 160), :] + self.r1[1].astype(F32)).astype(BF16)
            self.send(2, self.s2.at[1], self.r2.at[1], self.dev(-1))

        def third(self):
            got(self.base + 2, self.r2)
            here = ds(self.index * 320, 320)
            summed = self.dw[here, :] + self.r2[0].astype(F32) + self.r2[1].astype(F32)
            self.dw[here, :] = summed
            self.s3[...] = summed.astype(BF16)
            for k in (2, 1, 3):
                piece = self.s3.at[ds(lax.rem(self.index2 + k, 4) * 80, 80), :]
                self.send(3, piece, self.r3.at[k - 1], self.dev2(k))

        def fourth(self):
            got(self.base + 3, self.r3)
            rows = ds(self.index * 320 + self.index2 * 80, 80)
            self.s4[...] = self.dw[rows, :] + self.r3[0].astype(F32) + self.r3[1].astype(F32) + self.r3[2].astype(F32)
            self.four = self.send(4, self.s4.at[ds((1 - zh) * 40, 40), :], self.r4, zpair)

        def owners(self):
            self.four.wait_recv()
            chunk = self.s4[ds(zh * 40, 40), :] + self.r4[...]
            for i in range(4):
                self.sd[i, 0:10, :] = chunk[10 * i : 10 * i + 10, :]
            self.rd[g] = self.sd[r]
            for k in (2, 3, 1):
                zlk, ck, dev = rank(k)
                self.send(5, self.sd.at[zlk * 2 + ck], self.rd.at[g], dev)

        def finish(self):
            got(self.base + 5, self.rd.at[0:3])

        def close(self):
            sent(self.group, self.dw.at[0:688, :])

    alpha = Stream(46, 13, 0, 384, 0, (dwa, sa1, ra1, sa2, ra2, sa3, ra3, sa4, ra4, sda, rda))
    beta = Stream(52, 14, 384, 640, 1, (dwb, sb1, rb1, sb2, rb2, sb3, rb3, sb4, rb4, sdb, rdb))
    gamma = Stream(58, 15, 640, 768, 1, (dwc, sc1, rc1, sc2, rc2, sc3, rc3, sc4, rc4, sdc, rdc))

    pair_outside(0)
    pair_outside(1)
    pair_outside(2)
    alpha.first()
    pair_outside(3)
    pair_outside(4)

    ownl = coli < 10
    bias_sum = decay_sum = jnp.zeros((8, 128), F32)
    for b in range(4):
        rows = slice(128 * b, 128 * b + 128)
        dcf[rows, :] = dcf[rows, :] + mm(oe[rows, :], sb[b], NT)
        dbf[rows, :] = dbf[rows, :] + mm(xt[rows, :], db[b], NT)
        dlog = mm(upper, red[b, 0:128], NN, highest) + mm(strict, red[b, 128:256], NN, highest)
        dlog = jnp.where(ownl, dlog + inner[b].sum(axis=0, keepdims=True), 0.0)
        ddt = (red[b, 256:384] + neg * dlog) * jax.nn.sigmoid(projs[rows, 128:256] + bias)
        ddt = jnp.where(ownl, ddt, 0.0)
        rdt[rows, :] = ddt.astype(BF16)
        bias_sum = bias_sum + ddt.reshape(16, 8, 128).sum(axis=0)
        decay_sum = decay_sum + (dlog * lgd[rows, :]).reshape(16, 8, 128).sum(axis=0)
    first = c == 0
    place = jnp.where(jnp.logical_and(rowi < 10, coli == rowi + 10 * g), 1.0, 0.0).astype(F32)
    spread = mm(rdt[...], place.astype(BF16)).astype(BF16)
    t1d[...] = spread
    t1s[...] = jnp.where(first, dcf[...], dbf[...])
    t1 = [send(35, t1s, t1r, core, 9), send(36, t1d, t1dr, core, 9)]
    beta.first()
    row8 = lax.broadcasted_iota(jnp.int32, (8, 128), 0)
    packed = jnp.where(
        row8 == 0, bias_sum.sum(axis=0, keepdims=True),
        jnp.where(row8 == 1, decay_sum.sum(axis=0, keepdims=True),
                  jnp.where(row8 == 2, gain[0].sum(axis=0, keepdims=True), 0.0)),
    )
    heads_y[y] = mm(packed, place, NN, highest)
    for k in (1, 2, 3):
        send(38, heads_y.at[y], heads_y.at[y], ydev(k), 10)
    alpha.second()
    for copy in t1:
        copy.wait_recv()
    mixed = jnp.where(first, dbf[...], dcf[...]) + t1r[...]
    dt2 = spread.astype(F32) + t1dr[...].astype(F32)
    north = a == 0
    t2s[...] = jnp.where(north, dt2, mixed).astype(BF16)
    t2 = send(37, t2s, t2r, rank(2)[2], 9)
    for n in range(5):
        part = slice(256 * n, 256 * n + 256)
        hgp[:, part] = mm(rr[:, 0:640], wf[part, 0:640], NT) + mm(rdt[...], wf[part, 768:896], NT)
    mate_row = ds((zl * 2 + 1 - c) * 128, 128)
    far_mate = ds(((1 - zl) * 2 + 1 - c) * 128, 128)
    far_row = ds(((1 - zl) * 2 + c) * 128, 128)
    hgs[1] = hgp[far_mate, :].astype(BF16)
    hg_far = send(43, hgs.at[1], hgr.at[1], core, 11)
    hgs[0] = hgp[mate_row, :].astype(BF16)
    hg_near = send(42, hgs.at[0], hgr.at[0], core, 11)
    beta.second()
    hg_far.wait_recv()
    hgs[2] = (hgp[far_row, :] + hgr[1].astype(F32)).astype(BF16)
    t2.wait_recv()
    came = t2r[...].astype(F32)
    tile = projs[:, ds(256 * c, 128, 128)]
    upper_pick = ((mixed + came) * silu_grad(tile)).astype(BF16).astype(F32)
    lower_pick = jnp.where(first, dt2 + came, 0.0)
    rr[:, 640:768] = jnp.where(north, upper_pick, lower_pick).astype(BF16)
    shr[...] = jnp.where(north, upper_pick, lower_pick).astype(BF16)
    for k in (2, 3, 1):
        zlk, ck, dev = rank(k)
        send(45, shr.at[ds((zlk * 2 + ck) * 128, 128), :], extras.at[g], dev, 12)
    hg_z = send(44, hgs.at[2], hgr.at[2], rank(2)[2], 11)
    gamma.first()
    extras[g] = shr[here_id, :]
    alpha.third()
    gamma.second()
    beta.third()
    got(38, heads_y.at[0:3])
    heads_x[x] = (heads_y[0] + heads_y[1]) + (heads_y[2] + heads_y[3])
    for k in (1, 2, 3):
        send(39, heads_x.at[x], heads_x.at[x], xdev(k), 10)
    alpha.fourth()
    gamma.third()
    got(45, extras.at[0:3])
    hgp[here_id, :] = hgp[here_id, :] + mm(extras[0], wf[:, 640:768], NT) + mm(extras[1], wf[:, 896:1024], NT)
    beta.fourth()
    got(39, heads_x.at[0:3])
    heads_z[zh] = (heads_x[0] + heads_x[1]) + (heads_x[2] + heads_x[3])
    head_z = send(40, heads_z.at[zh], heads_z.at[zh], zpair, 10)
    alpha.owners()
    gamma.fourth()
    beta.owners()
    hg_near.wait_recv()
    hg_z.wait_recv()
    hgo[...] = (hgp[here_id, :] + hgr[0].astype(F32) + hgr[2].astype(F32)).astype(BF16)
    hg_out = pltpu.make_async_copy(hgo, hg_ref, ls.at[5])
    hg_out.start()
    head_z.wait_recv()
    heads_g[r] = heads_z[0] + heads_z[1]
    for k in (1, 2, 3):
        send(41, heads_g.at[r], heads_g.at[r], rank(k)[2], 10)
    gamma.owners()
    alpha.finish()
    for k in range(4):
        wgo[:, 640 * k : 640 * k + 384] = rda[k, 0:10, :]
    beta.finish()
    for k in range(4):
        wgo[:, 640 * k + 384 : 640 * k + 640] = rdb[k, 0:10, :]
    got(41, heads_g.at[0:3])
    hdo[...] = (heads_g[0] + heads_g[1]) + (heads_g[2] + heads_g[3])
    hd_out = pltpu.make_async_copy(hdo, hd_ref, ls.at[6])
    hd_out.start()
    gamma.finish()
    wgo[:, 2560:2688] = rdc[0, 0:10, :]
    wgo[:, 2688:2816] = rdc[1, 0:10, :]
    wgo[:, 2816:2856] = rdc[2, 0:10, 0:40]
    wg_out = pltpu.make_async_copy(wgo, wg_ref, ls.at[7])
    wg_out.start()
    for m in range(4):
        sent(m, wf.at[0:1120, cols(m)])
    sent(4, hidf.at[0:384, :])
    sent(5, cot.at[0:384, :])
    sent(6, wf.at[:, ds(lane0, 128)])
    sent(7, ttr)
    sent(8, str_)
    sent(9, dwc.at[0:1024, :])
    sent(10, bmf.at[0:80, :])
    sent(11, hgs)
    sent(12, extras.at[0:3])
    for stream in (alpha, beta, gamma):
        stream.close()
    hg_out.wait()
    hd_out.wait()
    wg_out.wait()


def scratch():
    def v(shape, dtype=F32):
        return pltpu.VMEM(shape, dtype)

    def stream(n):
        return [
            v((D, n)), v((320, n), BF16), v((2, 160, n), BF16), v((2, 320, n), BF16), v((2, 320, n), BF16),
            v((320, n), BF16), v((3, 80, n), BF16), v((80, n)), v((40, n)), v((4, 16, n)), v((4, 16, n)),
        ]

    wide, wide16 = v((512, COLS)), v((512, COLS), BF16)
    thin, thin16 = v((512, 128)), v((512, 128), BF16)
    return [
        v((512, D), BF16), v((D, 512), BF16), v((D, 512), BF16), wide16, v((160, 2856), BF16), v((D, 1024), BF16),
        v((512, 384)), wide, thin, thin, thin, thin, v((4, 16, 128)), thin,
        v((4, 128, 128)), v((4, 128, 128)), v((4, 128, 128)),
        wide, wide, wide, wide, wide16, wide16, wide16, v((32, COLS)),
        v((4, 128, COLS)), v((4, 128, COLS)), v((2, 128, COLS), BF16), v((8, COLS)),
        v((3, 128, COLS), BF16), v((3, 8, COLS)), wide, wide, thin, thin,
        v((4, 128, COLS), BF16), v((4, 128, COLS), BF16), v((4, 128, 128)), v((4, 384, 128)),
        v((512, 768), BF16), thin16, thin, thin, thin16, thin16, thin16, thin16, thin16,
        v((512, D)), v((3, 128, D), BF16), v((3, 128, D), BF16),
        *stream(384), *stream(256), *stream(128),
        v((4, 8, 128)), v((4, 8, 128)), v((2, 8, 128)), v((4, 8, 128)), v((4, 128, 128), BF16),
        v((128, D), BF16), v((10, 2856)), v((8, 128)),
        pltpu.SemaphoreType.DMA((16,)), pltpu.SemaphoreType.DMA((64,)), pltpu.SemaphoreType.DMA((8,)),
    ]


def emit(hg_ref, wg_ref, hd_ref, hg_out, wg_out, hd_out):
    hg_out[...] = hg_ref[...]
    wg_out[...] = wg_ref[...]
    hd_out[...] = hd_ref[0:3, 0:HEADS]


def body(hidden, output_grad, input_weight, step_bias, decay_log, skip_gain):
    anyspace = pl.BlockSpec(memory_space=pl.ANY)
    vmem = pl.BlockSpec(memory_space=pltpu.VMEM)
    hg, wg, hd = pl.pallas_call(
        kernel,
        out_shape=(
            jax.ShapeDtypeStruct((128, D), BF16),
            jax.ShapeDtypeStruct((10, 2856), F32),
            jax.ShapeDtypeStruct((8, 128), F32),
        ),
        in_specs=[anyspace, anyspace, anyspace, vmem, vmem, vmem],
        out_specs=(anyspace, anyspace, anyspace),
        scratch_shapes=scratch(),
        compiler_params=pltpu.CompilerParams(has_side_effects=True, collective_id=0, vmem_limit_bytes=64000000),
    )(hidden[0], output_grad[0], input_weight, step_bias[None], decay_log[None], skip_gain[None])
    hg, wg, hd = pl.pallas_call(
        emit,
        out_shape=(
            jax.ShapeDtypeStruct((128, D), BF16),
            jax.ShapeDtypeStruct((10, 2856), F32),
            jax.ShapeDtypeStruct((3, HEADS), F32),
        ),
        in_specs=[vmem, vmem, vmem],
        out_specs=(vmem, vmem, vmem),
    )(hg, wg, hd)
    return (hg[None], wg, hd)


def solution(mesh):
    torus = Mesh(
        mesh.devices.reshape(4, 2, 2, 4, 2), ("seq_0", "seq_1", "seq_2", "zero_0", "zero_1")
    )
    in_specs = (P(ZERO, SEQ, None), P(ZERO, SEQ, None), P(ZERO, None), P(), P(), P())
    out_specs = (P(ZERO, SEQ, None), P(SEQ_ZERO, None), P())
    return jax.shard_map(body, mesh=torus, in_specs=in_specs, out_specs=out_specs, check_vma=False)
```

```python
import functools

import jax
import jax.numpy as jnp
from jax import lax
from jax.experimental import pallas as pl
from jax.experimental.pallas import tpu as pltpu
from jax.sharding import Mesh
from jax.sharding import PartitionSpec as P

HEADS = 40
STATE = 128
INNER = 2560
D = 1280
COLS = 640
ZERO = ("zero_0", "zero_1")
SEQ = ("seq_0", "seq_1", "seq_2")
SEQ_ZERO = ("seq_0", "seq_1", "seq_2", "zero_0", "zero_1")
MESH = pl.DeviceIdType.MESH
F32 = jnp.float32
BF16 = jnp.bfloat16
highest = lax.Precision.HIGHEST
NN = (((1,), (0,)), ((), ()))
NT = (((1,), (1,)), ((), ()))
TN = (((0,), (0,)), ((), ()))


def mm(a, b, dims=NN, precision=None):
    return lax.dot_general(a, b, dims, preferred_element_type=F32, precision=precision)


def ds(start, size, align=None):
    return pl.ds(pl.multiple_of(start, align or size), size)


def silu_grad(v):
    sig = jax.nn.sigmoid(v)
    return sig * (1.0 + v * (1.0 - sig))


def kernel(
    hid_ref, cot_ref, w_ref, bias_ref, decay_ref, skip_ref,
    hg_ref, wg_ref, hd_ref,
    hidf, hidt, hidx, cot, wraw, wf, projs, projv, bmf, cmf, lgd, cums, cumt, stp, gs, gts, dgs,
    sexp, ecs, tls, vv, xb, xt, oe, tot,
    sl, dl, stt, tts, str_, ttr, q1s, dxin, dbf, dcf, sb, db, dd, red,
    rr, t1s, t1r, hgp, hgs, hgr,
    dwa, sa1, ra1, sa2, ra2, sa3, ra3, sa4, ra4, sda, rda,
    dwb, sb1, rb1, sb2, rb2, sb3, rb3, sb4, rb4, sdb, rdb,
    dwc, sc1, rc1, sc2, rc2, sc3, rc3, sc4, rc4, sdc, rdc,
    heads_y, heads_x, heads_z, heads_g, hgo, wgo, hdo,
    ss, rs, ls,
):
    y, zl, c = (lax.axis_index(n) for n in SEQ)
    x, zh = (lax.axis_index(n) for n in ZERO)
    r = zl * 2 + c
    a = lax.rem(zl + zh, 2)
    g = a * 2 + c

    def send(i, src, dst, where, group):
        copy = pltpu.make_async_remote_copy(
            src_ref=src, dst_ref=dst, send_sem=ss.at[group], recv_sem=rs.at[i],
            device_id=where, device_id_type=MESH,
        )
        copy.start()
        return copy

    def bytes_of(ref, i=0, group=0):
        return pltpu.make_async_remote_copy(
            src_ref=ref, dst_ref=ref, send_sem=ss.at[group], recv_sem=rs.at[i],
            device_id={"seq_2": 1 - c}, device_id_type=MESH,
        )

    def got(i, ref):
        bytes_of(ref, i=i).wait_recv()

    def sent(group, ref):
        bytes_of(ref, group=group).wait_send()

    def rank(k):
        zlk = lax.rem(zl + k // 2, 2)
        ck = lax.rem(c + k % 2, 2)
        return zlk, ck, {"seq_1": zlk, "seq_2": ck}

    def xdev(k):
        return {"zero_0": lax.rem(x + k + 4, 4)}

    def ydev(k):
        return {"seq_0": lax.rem(y + k + 4, 4)}

    zpair = {"seq_1": 1 - zl, "zero_1": 1 - zh}
    core = {"seq_2": 1 - c}
    here_id = ds(r * 128, 128)

    def shard(xk, zk, lo=0, size=160):
        return ds((lax.rem(xk + 4, 4) * 2 + zk) * 160 + lo, size, 16)

    own = shard(x, zh)
    lane0 = 640 + 256 * c
    local = [
        pltpu.make_async_copy(w_ref, wraw, ls.at[0]),
        pltpu.make_async_copy(w_ref.at[:, ds(g * COLS, COLS, 128)], wf.at[own, 0:640], ls.at[1]),
        pltpu.make_async_copy(w_ref.at[:, ds(2560 + 128 * c, 128)], wf.at[own, ds(lane0, 128)], ls.at[2]),
        pltpu.make_async_copy(hid_ref, hidf.at[here_id, :], ls.at[3]),
        pltpu.make_async_copy(cot_ref.at[:, ds(g * COLS, COLS, 128)], cot.at[here_id, :], ls.at[4]),
    ]
    for copy in local:
        copy.start()

    barrier = pltpu.get_barrier_semaphore()

    def greet(dev):
        pl.semaphore_signal(barrier, inc=1, device_id=dev, device_id_type=MESH)

    greet(zpair)
    for k in (1, 2, 3):
        greet(xdev(k))
        greet(ydev(k))
        greet(rank(k)[2])
    coli = lax.broadcasted_iota(jnp.int32, (128, 128), 1)
    rowi = lax.broadcasted_iota(jnp.int32, (128, 128), 0)
    local[0].wait()
    tail = jnp.concatenate([wraw[:, 2816:2856].astype(F32), jnp.zeros((160, 88), F32)], axis=1)
    tail = pltpu.roll(tail, lax.rem(128 - 10 * g, 128), 1)
    keep10 = lax.broadcasted_iota(jnp.int32, (160, 128), 1) < 10
    wf[own, 768:896] = jnp.where(keep10, tail, 0.0).astype(BF16)

    def lanes10(ref):
        full = jnp.concatenate([ref[...], jnp.zeros((1, 88), F32)], axis=1)
        return pltpu.roll(jnp.broadcast_to(full, (8, 128)), lax.rem(128 - 10 * g, 128), 1)[0:1, :]

    bias = lanes10(bias_ref)
    neg = -jnp.exp(lanes10(decay_ref))
    skip = lanes10(skip_ref)
    for copy in local[1:]:
        copy.wait()
    pl.semaphore_wait(barrier, 10)

    def cols(m):
        return (ds(640 + 128 * c, 256, 128), slice(0, 256), slice(256, 512), slice(512, 640))[m]

    w = {}

    def wsend(m, i, rows, dev):
        ref = wf.at[rows, cols(m)]
        slot = min(i, 5) if m < 2 else {1: 1, 2: 2, 5: 3, 6: 4}.get(i, 5)
        w[m, i] = send(6 * m + slot, ref, ref, dev, m)

    def w_own_x(m):
        wsend(m, 1, own, xdev(1))
        wsend(m, 2, own, xdev(-1))

    def w_own_z(m):
        wsend(m, 0, own, zpair)

    def w_other(m):
        w[m, 0].wait_recv()
        wsend(m, 3, shard(x, 1 - zh), xdev(1))
        wsend(m, 4, shard(x, 1 - zh), xdev(-1))

    def w_forward(m):
        w[m, 1].wait_recv()
        wsend(m, 5, shard(x - 1, zh, 0, 80), xdev(1))
        w[m, 2].wait_recv()
        wsend(m, 6, shard(x + 1, zh, 80, 80), xdev(-1))

    def w_forward_other(m):
        w[m, 3].wait_recv()
        wsend(m, 7, shard(x - 1, 1 - zh, 0, 80), xdev(1))
        w[m, 4].wait_recv()
        wsend(m, 8, shard(x + 1, 1 - zh, 80, 80), xdev(-1))

    def w_across(m):
        wsend(m, 3, shard(x - 1, zh), zpair)
        wsend(m, 4, shard(x + 1, zh), zpair)

    def w_across_far(m):
        w[m, 5].wait_recv()
        wsend(m, 7, shard(x + 2, zh, 0, 80), zpair)
        w[m, 6].wait_recv()
        wsend(m, 8, shard(x + 2, zh, 80, 80), zpair)

    def w_done(m):
        got(6 * m + 5, wf.at[0 : 320 if m < 2 else 640, cols(m)])

    w_own_z(0)
    w_own_x(0)
    h_z = send(24, hid_ref, hidf.at[here_id, :], rank(2)[2], 4)
    w_own_x(2)
    w_own_z(1)
    h_c = send(25, hid_ref, hidf.at[here_id, :], core, 4)
    for k in (2, 3, 1):
        zlk, ck, dev = rank(k)
        gk = lax.rem(zlk + zh, 2) * 2 + ck
        send(27, cot_ref.at[:, ds(gk * COLS, COLS, 128)], cot.at[here_id, :], dev, 5)
    w_own_z(2)
    w_own_z(3)
    w_other(0)
    w_forward(0)
    w_forward(2)
    w_across(2)
    w_own_x(3)
    w_forward_other(0)
    w_own_x(1)
    h_z.wait_recv()
    zrows = ds((rank(2)[0] * 2 + c) * 128, 128)
    h_f = send(26, hidf.at[zrows, :], hidf.at[zrows, :], core, 4)
    w_across_far(2)
    w_forward(3)
    w_across(3)
    w_other(1)
    w_done(0)
    mate = send(28, wf.at[:, ds(lane0, 128)], wf.at[:, ds(lane0, 128)], core, 6)
    h_c.wait_recv()
    h_f.wait_recv()
    mate.wait_recv()

    low = coli < 64
    causal = rowi >= coli
    anti = rowi <= coli
    tri = causal.astype(F32)
    upper = anti.astype(F32)
    strict = (rowi > coli).astype(F32)

    def pair(v, j):
        return jnp.where(low[0 : v.shape[0]], v[:, 2 * j : 2 * j + 1], v[:, 2 * j + 1 : 2 * j + 2])

    def blocks(f, unroll=True):
        if unroll:
            for b in range(4):
                f(b, pl.ds(b * 128, 128))
        else:
            def step(b, carry):
                f(b, ds(b * 128, 128))
                return carry

            lax.fori_loop(0, 4, step, 0)

    def common(b, rows):
        p = mm(hidf[rows, :], wf[:, 640:1024])
        projs[rows, :] = p
        bm = jax.nn.silu(p[:, 0:128])
        cm = jax.nn.silu(p[:, 256:384])
        bmf[rows, :] = bm
        cmf[rows, :] = cm
        pre = p[:, 128:256] + bias
        step = jnp.maximum(pre, 0.0) + jnp.log1p(jnp.exp(-jnp.abs(pre)))
        lg = neg * step
        cum = mm(tri, lg, NN, highest)
        stp[rows, :] = step
        lgd[rows, :] = lg
        cums[rows, :] = cum
        cumt[b] = cum.T[0:16, :]
        scores = mm(cm, bm, NT, highest)
        gs[b] = scores
        gts[b] = scores.T
        dgs[b] = jnp.zeros((128, 128), F32)
        red[b] = jnp.zeros((384, 128), F32)

    common(0, pl.ds(0, 128))
    w_forward(1)
    w_across_far(3)
    common(1, pl.ds(128, 128))
    common(2, pl.ds(256, 128))
    w_forward_other(1)
    common(3, pl.ds(384, 128))
    for j in range(5):
        cj = slice(128 * j, 128 * j + 128)
        for b in range(4):
            last_row = cums[128 * b + 127 : 128 * b + 128, :]
            tot[8 * b : 8 * b + 8, cj] = pair(jnp.broadcast_to(last_row, (8, 128)), j)
    tts[...] = tot[0:8, :] + tot[8:16, :] + tot[16:24, :] + tot[24:32, :]
    for k in (1, 2, 3):
        send(29, tts, ttr.at[k - 1], ydev(k), 7)

    def total(b, cj):
        return tot[8 * b : 8 * b + 1, cj]

    def pair_forward(j):
        cj = slice(128 * j, 128 * j + 128)

        def project(b, rows):
            projv[rows, cj] = mm(hidf[rows, :], wf[:, cj])

        def local_part(b, rows):
            ce = pair(cums[rows, :], j)
            se = pair(stp[rows, :], j)
            ec = jnp.exp(ce)
            tl = jnp.exp(ce[127:128, :] - ce)
            val = jax.nn.silu(projv[rows, cj])
            xs = val * se
            sexp[rows, cj] = se
            ecs[rows, cj] = ec
            tls[rows, cj] = tl
            vv[rows, cj] = val
            xb[rows, cj] = xs.astype(BF16)
            x16 = (xs * tl).astype(BF16)
            o16 = (cot[rows, cj].astype(F32) * ec).astype(BF16)
            xt[rows, cj] = x16
            oe[rows, cj] = o16
            sl[b, :, cj] = mm(bmf[rows, :].astype(BF16), x16, TN)
            dl[b, :, cj] = mm(cmf[rows, :].astype(BF16), o16, TN)

        blocks(project)
        blocks(local_part)
        s = sl[0, :, cj]
        d = dl[3, :, cj]
        for b in range(1, 4):
            s = jnp.exp(total(b, cj)) * s + sl[b, :, cj]
            d = jnp.exp(total(3 - b, cj)) * d + dl[3 - b, :, cj]
        stt[0, :, cj] = s.astype(BF16)
        stt[1, :, cj] = d.astype(BF16)
        for k in (1, 2, 3):
            wraps = lax.div(y + k, 4)
            send(30 + j, stt.at[wraps, :, cj], str_.at[k - 1, :, cj], ydev(k), 8)

    def pair_inside(j):
        cj = slice(128 * j, 128 * j + 128)

        def inside(b, rows):
            cum = cums[rows, :]
            c0, c1 = cum[:, 2 * j : 2 * j + 1], cum[:, 2 * j + 1 : 2 * j + 2]
            r0, r1 = cumt[b, 2 * j : 2 * j + 1, :], cumt[b, 2 * j + 1 : 2 * j + 2, :]
            w0 = jnp.where(causal, jnp.exp(jnp.where(causal, c0 - r0, 0.0)), 0.0)
            w1 = jnp.where(causal, jnp.exp(jnp.where(causal, c1 - r1, 0.0)), 0.0)
            u0 = jnp.where(anti, jnp.exp(jnp.where(anti, r0 - c0, 0.0)), 0.0)
            u1 = jnp.where(anti, jnp.exp(jnp.where(anti, r1 - c1, 0.0)), 0.0)
            scores, scores_t = gs[b], gts[b]
            m = jnp.concatenate([scores * w0, scores * w1], axis=1).astype(BF16)
            mt = jnp.concatenate([scores_t * u0, scores_t * u1], axis=1).astype(BF16)
            x16 = xb[rows, cj]
            o16 = cot[rows, cj]
            zero = jnp.zeros_like(x16)
            xd = jnp.concatenate([jnp.where(low, x16, zero), jnp.where(low, zero, x16)], axis=0)
            od = jnp.concatenate([jnp.where(low, o16, zero), jnp.where(low, zero, o16)], axis=0)
            yy = mm(m, xd)
            pp = mm(o16, xd, NT)
            dx = mm(mt, od)
            dgs[b] = dgs[b] + w0 * pp[:, 0:128] + w1 * pp[:, 128:256]
            dxin[rows, cj] = dx
            q1s[rows, cj] = o16.astype(F32) * yy - x16.astype(F32) * dx

        blocks(inside)

    i320 = lax.broadcasted_iota(jnp.int32, (320, 320), 0)
    k320 = lax.broadcasted_iota(jnp.int32, (320, 320), 1)
    tens = lax.shift_right_logical(i320 * 6554, 16)
    source = ((tens & 3) * 8 + lax.shift_right_logical(tens, 2)) * 10 + i320 - tens * 10
    perm = jnp.where(k320 == source, 1.0, 0.0).astype(F32).astype(BF16)
    for q in range(4):
        hidt[320 * q : 320 * q + 320, :] = mm(perm, hidf[:, 320 * q : 320 * q + 320], NT).astype(BF16)
    got(27, cot.at[0:384, :])
    w_done(2)
    pair_forward(2)
    pair_inside(2)
    pair_forward(3)
    pair_inside(3)
    w_done(3)
    pair_forward(4)
    pair_inside(4)
    for p in range(4):
        for q in range(4):
            hidx[320 * p + 80 * q : 320 * p + 80 * q + 80, :] = hidt[320 * q + 80 * p : 320 * q + 80 * p + 80, :]
    w_done(1)
    pair_forward(0)
    pair_inside(0)
    pair_forward(1)
    pair_inside(1)

    def turn(b, rows):
        dcf[rows, :] = mm(dgs[b], bmf[rows, :], NN, highest)
        dbf[rows, :] = mm(dgs[b], cmf[rows, :], TN, highest)

    blocks(turn)
    got(29, ttr)

    lanes = lax.broadcasted_iota(jnp.int32, (256, 128), 0)
    outl = lax.broadcasted_iota(jnp.int32, (256, 128), 1)

    def sums(z, j):
        hi = z.astype(BF16)
        lo = (z - hi.astype(F32)).astype(BF16)
        choose = (outl == 2 * j + lax.rem(lax.div(lanes, 64), 2)).astype(F32).astype(BF16)
        return mm(jnp.concatenate([hi, lo], axis=1), choose)

    yes = [jnp.where(y >= k, 1.0, 0.0).astype(F32) for k in (1, 2, 3)]
    no = [jnp.where(y + k <= 3, 1.0, 0.0).astype(F32) for k in (1, 2, 3)]
    inner = [jnp.zeros((8, 128), F32) for _ in range(4)]
    gain = [jnp.zeros((8, 128), F32)]

    def pair_outside(j):
        cj = slice(128 * j, 128 * j + 128)
        got(30 + j, str_.at[:, :, cj])
        t = [ttr[k, 0:1, cj] for k in range(3)]
        came = [str_[k, :, cj].astype(F32) for k in range(3)]
        s = yes[0] * came[0] + (yes[1] * jnp.exp(t[0])) * came[1] + (yes[2] * jnp.exp(t[0] + t[1])) * came[2]
        d = no[0] * came[2] + (no[1] * jnp.exp(t[2])) * came[1] + (no[2] * jnp.exp(t[2] + t[1])) * came[0]
        for b in (3, 2, 1, 0):
            db[b, :, cj] = d.astype(BF16)
            dd[b] = d
            d = jnp.exp(total(b, cj)) * d + dl[b, :, cj]
        for b in range(4):
            sb[b, :, cj] = s.astype(BF16)
            grown = jnp.exp(total(b, cj)) * s
            inner[b] = inner[b] + sums((grown * dd[b]).reshape(16, 8, 128).sum(axis=0), j)
            s = grown + sl[b, :, cj]

        def outside(b, rows):
            o = cot[rows, cj].astype(F32)
            yst = mm(cmf[rows, :].astype(BF16), sb[b, :, cj]) * ecs[rows, cj]
            dxst = mm(bmf[rows, :].astype(BF16), db[b, :, cj]) * tls[rows, cj]
            val = vv[rows, cj]
            dxs = dxin[rows, cj] + dxst
            z = jnp.concatenate([q1s[rows, cj] + o * yst, xb[rows, cj].astype(F32) * dxst, dxs * val], axis=0)
            red[b] = red[b] + sums(z, j)
            dval = dxs * sexp[rows, cj] + pair(skip, j) * o
            rr[rows, cj] = (dval * silu_grad(projv[rows, cj])).astype(BF16)
            gain[0] = gain[0] + sums((o * val).reshape(16, 8, 128).sum(axis=0), j)

        blocks(outside)

    class Stream:
        def __init__(self, base, group, lo, hi, kind, bufs):
            self.base, self.group, self.lo, self.hi, self.left = base, group, lo, hi, hidx if kind else hidt
            self.dw, self.s1, self.r1, self.s2, self.r2, self.s3, self.r3, self.s4, self.r4, self.sd, self.rd = bufs
            self.index, self.dev, self.index2, self.dev2 = (y, ydev, x, xdev) if kind == 0 else (x, xdev, y, ydev)

        def send(self, i, src, dst, dev):
            return send(self.base + i, src, dst, dev, self.group)

        def first(self):
            for i in (2, 1, 3, 0):
                rows = ds(lax.rem(self.index + i, 4) * 320, 320)
                self.dw[rows, :] = mm(self.left[rows, :], rr[:, self.lo : self.hi])
                if i == 2:
                    self.s1[...] = self.dw[rows, :].astype(BF16)
                    self.one = (
                        self.send(0, self.s1.at[0:160, :], self.r1.at[0], self.dev(1)),
                        self.send(1, self.s1.at[160:320, :], self.r1.at[1], self.dev(-1)),
                    )

        def second(self):
            nxt = lax.rem(self.index + 1, 4) * 320
            prv = lax.rem(self.index + 3, 4) * 320
            self.one[0].wait_recv()
            self.s2[0, 0:160, :] = (self.dw[ds(nxt, 160), :] + self.r1[0].astype(F32)).astype(BF16)
            self.s2[0, 160:320, :] = self.dw[ds(nxt + 160, 160), :].astype(BF16)
            self.send(2, self.s2.at[0], self.r2.at[0], self.dev(1))
            self.one[1].wait_recv()
            self.s2[1, 0:160, :] = self.dw[ds(prv, 160), :].astype(BF16)
            self.s2[1, 160:320, :] = (self.dw[ds(prv + 160, 160), :] + self.r1[1].astype(F32)).astype(BF16)
            self.send(2, self.s2.at[1], self.r2.at[1], self.dev(-1))

        def third(self):
            got(self.base + 2, self.r2)
            here = ds(self.index * 320, 320)
            summed = self.dw[here, :] + self.r2[0].astype(F32) + self.r2[1].astype(F32)
            self.dw[here, :] = summed
            self.s3[...] = summed.astype(BF16)
            for k in (2, 1, 3):
                piece = self.s3.at[ds(lax.rem(self.index2 + k, 4) * 80, 80), :]
                self.send(3, piece, self.r3.at[k - 1], self.dev2(k))

        def fourth(self):
            got(self.base + 3, self.r3)
            rows = ds(self.index * 320 + self.index2 * 80, 80)
            self.s4[...] = self.dw[rows, :] + self.r3[0].astype(F32) + self.r3[1].astype(F32) + self.r3[2].astype(F32)
            self.four = self.send(4, self.s4.at[ds((1 - zh) * 40, 40), :], self.r4, zpair)

        def owners(self):
            self.four.wait_recv()
            chunk = self.s4[ds(zh * 40, 40), :] + self.r4[...]
            for i in range(4):
                self.sd[i, 0:10, :] = chunk[10 * i : 10 * i + 10, :]
            self.rd[g] = self.sd[r]
            for k in (2, 3, 1):
                zlk, ck, dev = rank(k)
                self.send(5, self.sd.at[zlk * 2 + ck], self.rd.at[g], dev)

        def finish(self):
            got(self.base + 5, self.rd.at[0:3])

        def close(self):
            sent(self.group, self.dw.at[0:688, :])

    alpha = Stream(46, 13, 256, 640, 0, (dwa, sa1, ra1, sa2, ra2, sa3, ra3, sa4, ra4, sda, rda))
    beta = Stream(52, 14, 0, 256, 1, (dwb, sb1, rb1, sb2, rb2, sb3, rb3, sb4, rb4, sdb, rdb))
    gamma = Stream(58, 15, 640, 896, 1, (dwc, sc1, rc1, sc2, rc2, sc3, rc3, sc4, rc4, sdc, rdc))

    pair_outside(2)
    pair_outside(3)
    pair_outside(4)
    alpha.first()
    pair_outside(0)
    pair_outside(1)

    ownl = coli < 10
    bias_sum = decay_sum = jnp.zeros((8, 128), F32)
    for b in range(4):
        rows = slice(128 * b, 128 * b + 128)
        dcf[rows, :] = dcf[rows, :] + mm(oe[rows, :], sb[b], NT)
        dbf[rows, :] = dbf[rows, :] + mm(xt[rows, :], db[b], NT)
        dlog = mm(upper, red[b, 0:128], NN, highest) + mm(strict, red[b, 128:256], NN, highest)
        dlog = jnp.where(ownl, dlog + inner[b].sum(axis=0, keepdims=True), 0.0)
        ddt = (red[b, 256:384] + neg * dlog) * jax.nn.sigmoid(projs[rows, 128:256] + bias)
        ddt = jnp.where(ownl, ddt, 0.0)
        rr[rows, 768:896] = ddt.astype(BF16)
        bias_sum = bias_sum + ddt.reshape(16, 8, 128).sum(axis=0)
        decay_sum = decay_sum + (dlog * lgd[rows, :]).reshape(16, 8, 128).sum(axis=0)
    first = c == 0
    place = jnp.where(jnp.logical_and(rowi < 10, coli == rowi + 10 * g), 1.0, 0.0).astype(F32)
    t1s[...] = jnp.where(first, dcf[...], dbf[...])
    t1 = send(35, t1s, t1r, core, 9)
    beta.first()
    row8 = lax.broadcasted_iota(jnp.int32, (8, 128), 0)
    packed = jnp.where(
        row8 == 0, bias_sum.sum(axis=0, keepdims=True),
        jnp.where(row8 == 1, decay_sum.sum(axis=0, keepdims=True),
                  jnp.where(row8 == 2, gain[0].sum(axis=0, keepdims=True), 0.0)),
    )
    heads_y[y] = mm(packed, place, NN, highest)
    for k in (1, 2, 3):
        send(38, heads_y.at[y], heads_y.at[y], ydev(k), 10)
    alpha.second()
    t1.wait_recv()
    mixed = jnp.where(first, dbf[...], dcf[...]) + t1r[...]
    rr[:, 640:768] = (mixed * silu_grad(projs[:, ds(256 * c, 128, 128)])).astype(BF16)
    gamma.first()
    for n in range(5):
        part = slice(256 * n, 256 * n + 256)
        hgp[:, part] = (
            mm(rr[:, 0:640], wf[part, 0:640], NT)
            + mm(rr[:, 640:768], wf[part, ds(lane0, 128)], NT)
            + mm(rr[:, 768:896], wf[part, 768:896], NT)
        )
    mate_row = ds((zl * 2 + 1 - c) * 128, 128)
    far_mate = ds(((1 - zl) * 2 + 1 - c) * 128, 128)
    far_row = ds(((1 - zl) * 2 + c) * 128, 128)
    hgs[1] = hgp[far_mate, :].astype(BF16)
    hg_far = send(43, hgs.at[1], hgr.at[1], core, 11)
    hgs[0] = hgp[mate_row, :].astype(BF16)
    hg_near = send(42, hgs.at[0], hgr.at[0], core, 11)
    beta.second()
    hg_far.wait_recv()
    hgs[2] = (hgp[far_row, :] + hgr[1].astype(F32)).astype(BF16)
    hg_z = send(44, hgs.at[2], hgr.at[2], rank(2)[2], 11)
    alpha.third()
    gamma.second()
    beta.third()
    got(38, heads_y.at[0:3])
    heads_x[x] = (heads_y[0] + heads_y[1]) + (heads_y[2] + heads_y[3])
    for k in (1, 2, 3):
        send(39, heads_x.at[x], heads_x.at[x], xdev(k), 10)
    alpha.fourth()
    gamma.third()
    beta.fourth()
    got(39, heads_x.at[0:3])
    heads_z[zh] = (heads_x[0] + heads_x[1]) + (heads_x[2] + heads_x[3])
    head_z = send(40, heads_z.at[zh], heads_z.at[zh], zpair, 10)
    alpha.owners()
    gamma.fourth()
    beta.owners()
    hg_near.wait_recv()
    hg_z.wait_recv()
    hgo[...] = (hgp[here_id, :] + hgr[0].astype(F32) + hgr[2].astype(F32)).astype(BF16)
    hg_out = pltpu.make_async_copy(hgo, hg_ref, ls.at[5])
    hg_out.start()
    head_z.wait_recv()
    heads_g[r] = heads_z[0] + heads_z[1]
    for k in (1, 2, 3):
        send(41, heads_g.at[r], heads_g.at[r], rank(k)[2], 10)
    gamma.owners()
    alpha.finish()
    for k in range(4):
        wgo[:, 640 * k + 256 : 640 * k + 640] = rda[k, 0:10, :]
    beta.finish()
    for k in range(4):
        wgo[:, 640 * k : 640 * k + 256] = rdb[k, 0:10, :]
    got(41, heads_g.at[0:3])
    hdo[...] = (heads_g[0] + heads_g[1]) + (heads_g[2] + heads_g[3])
    hd_out = pltpu.make_async_copy(hdo, hd_ref, ls.at[6])
    hd_out.start()
    gamma.finish()
    wgo[:, 2560:2688] = rdc[0, 0:10, 0:128] + rdc[2, 0:10, 0:128]
    wgo[:, 2688:2816] = rdc[1, 0:10, 0:128] + rdc[3, 0:10, 0:128]
    for k in range(4):
        wgo[:, 2816 + 10 * k : 2826 + 10 * k] = rdc[k, 0:10, 128:138]
    wg_out = pltpu.make_async_copy(wgo, wg_ref, ls.at[7])
    wg_out.start()
    for m in range(4):
        sent(m, wf.at[0:1120, cols(m)])
    sent(4, hidf.at[0:384, :])
    sent(5, cot.at[0:384, :])
    sent(6, wf.at[:, ds(lane0, 128)])
    sent(7, ttr)
    sent(8, str_)
    sent(9, t1r)
    sent(10, bmf.at[0:80, :])
    sent(11, hgs)
    for stream in (alpha, beta, gamma):
        stream.close()
    hg_out.wait()
    hd_out.wait()
    wg_out.wait()


def scratch():
    def v(shape, dtype=F32):
        return pltpu.VMEM(shape, dtype)

    def stream(n):
        return [
            v((D, n)), v((320, n), BF16), v((2, 160, n), BF16), v((2, 320, n), BF16), v((2, 320, n), BF16),
            v((320, n), BF16), v((3, 80, n), BF16), v((80, n)), v((40, n)), v((4, 16, n)), v((4, 16, n)),
        ]

    wide, wide16 = v((512, COLS)), v((512, COLS), BF16)
    thin = v((512, 128))
    return [
        v((512, D), BF16), v((D, 512), BF16), v((D, 512), BF16), wide16, v((160, 2856), BF16), v((D, 1024), BF16),
        v((512, 384)), wide, thin, thin, thin, thin, v((4, 16, 128)), thin,
        v((4, 128, 128)), v((4, 128, 128)), v((4, 128, 128)),
        wide, wide, wide, wide, wide16, wide16, wide16, v((32, COLS)),
        v((4, 128, COLS)), v((4, 128, COLS)), v((2, 128, COLS), BF16), v((8, COLS)),
        v((3, 128, COLS), BF16), v((3, 8, COLS)), wide, wide, thin, thin,
        v((4, 128, COLS), BF16), v((4, 128, COLS), BF16), v((4, 128, 128)), v((4, 384, 128)),
        v((512, 896), BF16), thin, thin,
        v((512, D)), v((3, 128, D), BF16), v((3, 128, D), BF16),
        *stream(384), *stream(256), *stream(256),
        v((4, 8, 128)), v((4, 8, 128)), v((2, 8, 128)), v((4, 8, 128)),
        v((128, D), BF16), v((10, 2856)), v((8, 128)),
        pltpu.SemaphoreType.DMA((16,)), pltpu.SemaphoreType.DMA((64,)), pltpu.SemaphoreType.DMA((8,)),
    ]


def emit(hg_ref, wg_ref, hd_ref, hg_out, wg_out, hd_out):
    hg_out[...] = hg_ref[...]
    wg_out[...] = wg_ref[...]
    hd_out[...] = hd_ref[0:3, 0:HEADS]


def body(hidden, output_grad, input_weight, step_bias, decay_log, skip_gain):
    anyspace = pl.BlockSpec(memory_space=pl.ANY)
    vmem = pl.BlockSpec(memory_space=pltpu.VMEM)
    hg, wg, hd = pl.pallas_call(
        kernel,
        out_shape=(
            jax.ShapeDtypeStruct((128, D), BF16),
            jax.ShapeDtypeStruct((10, 2856), F32),
            jax.ShapeDtypeStruct((8, 128), F32),
        ),
        in_specs=[anyspace, anyspace, anyspace, vmem, vmem, vmem],
        out_specs=(anyspace, anyspace, anyspace),
        scratch_shapes=scratch(),
        compiler_params=pltpu.CompilerParams(has_side_effects=True, collective_id=0, vmem_limit_bytes=64000000),
    )(hidden[0], output_grad[0], input_weight, step_bias[None], decay_log[None], skip_gain[None])
    hg, wg, hd = pl.pallas_call(
        emit,
        out_shape=(
            jax.ShapeDtypeStruct((128, D), BF16),
            jax.ShapeDtypeStruct((10, 2856), F32),
            jax.ShapeDtypeStruct((3, HEADS), F32),
        ),
        in_specs=[vmem, vmem, vmem],
        out_specs=(vmem, vmem, vmem),
    )(hg, wg, hd)
    return (hg[None], wg, hd)


def solution(mesh):
    torus = Mesh(
        mesh.devices.reshape(4, 2, 2, 4, 2), ("seq_0", "seq_1", "seq_2", "zero_0", "zero_1")
    )
    in_specs = (P(ZERO, SEQ, None), P(ZERO, SEQ, None), P(ZERO, None), P(), P(), P())
    out_specs = (P(ZERO, SEQ, None), P(SEQ_ZERO, None), P())
    return jax.shard_map(body, mesh=torus, in_specs=in_specs, out_specs=out_specs, check_vma=False)
```

```python
import functools

import jax
import jax.numpy as jnp
from jax import lax
from jax.experimental import pallas as pl
from jax.experimental.pallas import tpu as pltpu
from jax.sharding import Mesh
from jax.sharding import PartitionSpec as P

HEADS = 40
STATE = 128
INNER = 2560
D = 1280
COLS = 640
ZERO = ("zero_0", "zero_1")
SEQ = ("seq_0", "seq_1", "seq_2")
SEQ_ZERO = ("seq_0", "seq_1", "seq_2", "zero_0", "zero_1")
MESH = pl.DeviceIdType.MESH
F32 = jnp.float32
BF16 = jnp.bfloat16
highest = lax.Precision.HIGHEST
NN = (((1,), (0,)), ((), ()))
NT = (((1,), (1,)), ((), ()))
TN = (((0,), (0,)), ((), ()))


def mm(a, b, dims=NN, precision=None):
    return lax.dot_general(a, b, dims, preferred_element_type=F32, precision=precision)


def ds(start, size, align=None):
    return pl.ds(pl.multiple_of(start, align or size), size)


def silu_grad(v):
    sig = jax.nn.sigmoid(v)
    return sig * (1.0 + v * (1.0 - sig))


def kernel(
    hid_ref, cot_ref, w_ref, bias_ref, decay_ref, skip_ref,
    hg_ref, wg_ref, hd_ref,
    hidf, hidt, hidx, cot, wraw, wf, projs, projv, bmf, cmf, lgd, cums, cumt, stp, gs, gts, dgs,
    sexp, ecs, tls, vv, xb, xt, oe, tot,
    sl, dl, stt, tts, str_, ttr, q1s, dxin, dbf, dcf, sb, db, dd, red,
    rr, t1s, t1r, hgp, hgs, hgr,
    dwa, sa1, ra1, sa2, ra2, sa3, ra3, sa4, ra4, sda, rda,
    dwb, sb1, rb1, sb2, rb2, sb3, rb3, sb4, rb4, sdb, rdb,
    dwc, sc1, rc1, sc2, rc2, sc3, rc3, sc4, rc4, sdc, rdc,
    heads_y, heads_x, heads_z, heads_g, hgo, wgo, hdo,
    ss, rs, ls,
):
    y, zl, c = (lax.axis_index(n) for n in SEQ)
    x, zh = (lax.axis_index(n) for n in ZERO)
    r = zl * 2 + c
    a = lax.rem(zl + zh, 2)
    g = a * 2 + c

    def send(i, src, dst, where, group):
        copy = pltpu.make_async_remote_copy(
            src_ref=src, dst_ref=dst, send_sem=ss.at[group], recv_sem=rs.at[i],
            device_id=where, device_id_type=MESH,
        )
        copy.start()
        return copy

    def bytes_of(ref, i=0, group=0):
        return pltpu.make_async_remote_copy(
            src_ref=ref, dst_ref=ref, send_sem=ss.at[group], recv_sem=rs.at[i],
            device_id={"seq_2": 1 - c}, device_id_type=MESH,
        )

    def got(i, ref):
        bytes_of(ref, i=i).wait_recv()

    def sent(group, ref):
        bytes_of(ref, group=group).wait_send()

    def rank(k):
        zlk = lax.rem(zl + k // 2, 2)
        ck = lax.rem(c + k % 2, 2)
        return zlk, ck, {"seq_1": zlk, "seq_2": ck}

    def xdev(k):
        return {"zero_0": lax.rem(x + k + 4, 4)}

    def ydev(k):
        return {"seq_0": lax.rem(y + k + 4, 4)}

    zpair = {"seq_1": 1 - zl, "zero_1": 1 - zh}
    core = {"seq_2": 1 - c}
    here_id = ds(r * 128, 128)

    def shard(xk, zk, lo=0, size=160):
        return ds((lax.rem(xk + 4, 4) * 2 + zk) * 160 + lo, size, 16)

    own = shard(x, zh)
    lane0 = 640 + 256 * c
    local = [
        pltpu.make_async_copy(w_ref, wraw, ls.at[0]),
        pltpu.make_async_copy(w_ref.at[:, ds(g * COLS, COLS, 128)], wf.at[own, 0:640], ls.at[1]),
        pltpu.make_async_copy(w_ref.at[:, ds(2560 + 128 * c, 128)], wf.at[own, ds(lane0, 128)], ls.at[2]),
        pltpu.make_async_copy(hid_ref, hidf.at[here_id, :], ls.at[3]),
        pltpu.make_async_copy(cot_ref.at[:, ds(g * COLS, COLS, 128)], cot.at[here_id, :], ls.at[4]),
    ]
    for copy in local:
        copy.start()

    barrier = pltpu.get_barrier_semaphore()

    def greet(dev):
        pl.semaphore_signal(barrier, inc=1, device_id=dev, device_id_type=MESH)

    greet(zpair)
    for k in (1, 2, 3):
        greet(xdev(k))
        greet(ydev(k))
        greet(rank(k)[2])
    coli = lax.broadcasted_iota(jnp.int32, (128, 128), 1)
    rowi = lax.broadcasted_iota(jnp.int32, (128, 128), 0)
    local[0].wait()
    tail = jnp.concatenate([wraw[:, 2816:2856].astype(F32), jnp.zeros((160, 88), F32)], axis=1)
    tail = pltpu.roll(tail, lax.rem(128 - 10 * g, 128), 1)
    keep10 = lax.broadcasted_iota(jnp.int32, (160, 128), 1) < 10
    wf[own, 768:896] = jnp.where(keep10, tail, 0.0).astype(BF16)

    def lanes10(ref):
        full = jnp.concatenate([ref[...], jnp.zeros((1, 88), F32)], axis=1)
        return pltpu.roll(jnp.broadcast_to(full, (8, 128)), lax.rem(128 - 10 * g, 128), 1)[0:1, :]

    bias = lanes10(bias_ref)
    neg = -jnp.exp(lanes10(decay_ref))
    skip = lanes10(skip_ref)
    for copy in local[1:]:
        copy.wait()
    pl.semaphore_wait(barrier, 10)

    def cols(m):
        return (ds(640 + 128 * c, 256, 128), slice(0, 256), slice(256, 512), slice(512, 640))[m]

    w = {}

    def wsend(m, i, rows, dev):
        ref = wf.at[rows, cols(m)]
        slot = min(i, 5) if m < 2 else {1: 1, 2: 2, 5: 3, 6: 4}.get(i, 5)
        w[m, i] = send(6 * m + slot, ref, ref, dev, m)

    def w_own_x(m):
        wsend(m, 1, own, xdev(1))
        wsend(m, 2, own, xdev(-1))

    def w_own_z(m):
        wsend(m, 0, own, zpair)

    def w_other(m):
        w[m, 0].wait_recv()
        wsend(m, 3, shard(x, 1 - zh), xdev(1))
        wsend(m, 4, shard(x, 1 - zh), xdev(-1))

    def w_forward(m):
        w[m, 1].wait_recv()
        wsend(m, 5, shard(x - 1, zh, 0, 80), xdev(1))
        w[m, 2].wait_recv()
        wsend(m, 6, shard(x + 1, zh, 80, 80), xdev(-1))

    def w_forward_other(m):
        w[m, 3].wait_recv()
        wsend(m, 7, shard(x - 1, 1 - zh, 0, 80), xdev(1))
        w[m, 4].wait_recv()
        wsend(m, 8, shard(x + 1, 1 - zh, 80, 80), xdev(-1))

    def w_across(m):
        wsend(m, 3, shard(x - 1, zh), zpair)
        wsend(m, 4, shard(x + 1, zh), zpair)

    def w_across_far(m):
        w[m, 5].wait_recv()
        wsend(m, 7, shard(x + 2, zh, 0, 80), zpair)
        w[m, 6].wait_recv()
        wsend(m, 8, shard(x + 2, zh, 80, 80), zpair)

    def w_done(m):
        got(6 * m + 5, wf.at[0 : 320 if m < 2 else 640, cols(m)])

    def hand(k):
        ref = wf.at[ds(lax.rem(x + k + 4, 4) * 320, 320), ds(lane0, 128)]
        send(28, ref, ref, core, 6)

    w_own_z(0)
    w_own_x(0)
    h_z = send(24, hid_ref, hidf.at[here_id, :], rank(2)[2], 4)
    w_own_x(2)
    w_own_z(1)
    h_c = send(25, hid_ref, hidf.at[here_id, :], core, 4)
    for k in (2, 3, 1):
        zlk, ck, dev = rank(k)
        gk = lax.rem(zlk + zh, 2) * 2 + ck
        send(27, cot_ref.at[:, ds(gk * COLS, COLS, 128)], cot.at[here_id, :], dev, 5)
    w_own_z(2)
    w_own_z(3)
    w_other(0)
    w_forward(0)
    w_forward(2)
    w_across(2)
    w_own_x(3)
    w_forward_other(0)
    w_own_x(1)
    for k in (-1, 0, 1):
        hand(k)
    h_z.wait_recv()
    zrows = ds((rank(2)[0] * 2 + c) * 128, 128)
    h_f = send(26, hidf.at[zrows, :], hidf.at[zrows, :], core, 4)
    w_across_far(2)
    w_forward(3)
    w_across(3)
    w_other(1)
    w_done(0)
    hand(2)
    h_c.wait_recv()
    h_f.wait_recv()

    low = coli < 64
    causal = rowi >= coli
    anti = rowi <= coli
    tri = causal.astype(F32)
    upper = anti.astype(F32)
    strict = (rowi > coli).astype(F32)

    def pair(v, j):
        return jnp.where(low[0 : v.shape[0]], v[:, 2 * j : 2 * j + 1], v[:, 2 * j + 1 : 2 * j + 2])

    def blocks(f, unroll=True):
        if unroll:
            for b in range(4):
                f(b, pl.ds(b * 128, 128))
        else:
            def step(b, carry):
                f(b, ds(b * 128, 128))
                return carry

            lax.fori_loop(0, 4, step, 0)

    def steps(b, rows):
        projs[rows, ds(128 * c, 256, 128)] = mm(hidf[rows, :], wf[:, ds(640 + 128 * c, 256, 128)])
        pre = projs[rows, 128:256] + bias
        step = jnp.maximum(pre, 0.0) + jnp.log1p(jnp.exp(-jnp.abs(pre)))
        lg = neg * step
        cum = mm(tri, lg, NN, highest)
        stp[rows, :] = step
        lgd[rows, :] = lg
        cums[rows, :] = cum
        cumt[b] = cum.T[0:16, :]
        dgs[b] = jnp.zeros((128, 128), F32)
        red[b] = jnp.zeros((384, 128), F32)

    def maps(b, rows):
        projs[rows, ds(256 - 256 * c, 128)] = mm(hidf[rows, :], wf[:, ds(896 - 256 * c, 128)])
        bm = jax.nn.silu(projs[rows, 0:128])
        cm = jax.nn.silu(projs[rows, 256:384])
        bmf[rows, :] = bm
        cmf[rows, :] = cm
        scores = mm(cm, bm, NT, highest)
        gs[b] = scores
        gts[b] = scores.T

    blocks(steps)
    for j in range(5):
        cj = slice(128 * j, 128 * j + 128)
        for b in range(4):
            last_row = cums[128 * b + 127 : 128 * b + 128, :]
            tot[8 * b : 8 * b + 8, cj] = pair(jnp.broadcast_to(last_row, (8, 128)), j)
    tts[...] = tot[0:8, :] + tot[8:16, :] + tot[16:24, :] + tot[24:32, :]
    for k in (1, 2, 3):
        send(29, tts, ttr.at[k - 1], ydev(k), 7)

    i320 = lax.broadcasted_iota(jnp.int32, (320, 320), 0)
    k320 = lax.broadcasted_iota(jnp.int32, (320, 320), 1)
    tens = lax.shift_right_logical(i320 * 6554, 16)
    source = ((tens & 3) * 8 + lax.shift_right_logical(tens, 2)) * 10 + i320 - tens * 10
    perm = jnp.where(k320 == source, 1.0, 0.0).astype(F32).astype(BF16)
    for q in range(4):
        hidt[320 * q : 320 * q + 320, :] = mm(perm, hidf[:, 320 * q : 320 * q + 320], NT).astype(BF16)
    w_forward(1)
    got(28, wf.at[:, ds(896 - 256 * c, 128)])
    maps(0, pl.ds(0, 128))
    w_across_far(3)
    maps(1, pl.ds(128, 128))
    maps(2, pl.ds(256, 128))
    w_forward_other(1)
    maps(3, pl.ds(384, 128))

    def total(b, cj):
        return tot[8 * b : 8 * b + 1, cj]

    def pair_forward(j):
        cj = slice(128 * j, 128 * j + 128)

        wide = slice(128 * j, min(128 * j + 256, 640))

        def project(b, rows):
            projv[rows, wide] = mm(hidf[rows, :], wf[:, wide])

        def local_part(b, rows):
            ce = pair(cums[rows, :], j)
            se = pair(stp[rows, :], j)
            ec = jnp.exp(ce)
            tl = jnp.exp(ce[127:128, :] - ce)
            val = jax.nn.silu(projv[rows, cj])
            xs = val * se
            sexp[rows, cj] = se
            ecs[rows, cj] = ec
            tls[rows, cj] = tl
            vv[rows, cj] = val
            xb[rows, cj] = xs.astype(BF16)
            x16 = (xs * tl).astype(BF16)
            o16 = (cot[rows, cj].astype(F32) * ec).astype(BF16)
            xt[rows, cj] = x16
            oe[rows, cj] = o16
            sl[b, :, cj] = mm(bmf[rows, :].astype(BF16), x16, TN)
            dl[b, :, cj] = mm(cmf[rows, :].astype(BF16), o16, TN)

        if j % 2 == 0:
            blocks(project)
        blocks(local_part)
        s = sl[0, :, cj]
        d = dl[3, :, cj]
        for b in range(1, 4):
            s = jnp.exp(total(b, cj)) * s + sl[b, :, cj]
            d = jnp.exp(total(3 - b, cj)) * d + dl[3 - b, :, cj]
        stt[0, :, cj] = s.astype(BF16)
        stt[1, :, cj] = d.astype(BF16)
        for k in (1, 2, 3):
            wraps = lax.div(y + k, 4)
            send(30 + j, stt.at[wraps, :, cj], str_.at[k - 1, :, cj], ydev(k), 8)

    def pair_inside(j):
        cj = slice(128 * j, 128 * j + 128)

        def inside(b, rows):
            cum = cums[rows, :]
            c0, c1 = cum[:, 2 * j : 2 * j + 1], cum[:, 2 * j + 1 : 2 * j + 2]
            r0, r1 = cumt[b, 2 * j : 2 * j + 1, :], cumt[b, 2 * j + 1 : 2 * j + 2, :]
            w0 = jnp.where(causal, jnp.exp(jnp.where(causal, c0 - r0, 0.0)), 0.0)
            w1 = jnp.where(causal, jnp.exp(jnp.where(causal, c1 - r1, 0.0)), 0.0)
            u0 = jnp.where(anti, jnp.exp(jnp.where(anti, r0 - c0, 0.0)), 0.0)
            u1 = jnp.where(anti, jnp.exp(jnp.where(anti, r1 - c1, 0.0)), 0.0)
            scores, scores_t = gs[b], gts[b]
            m = jnp.concatenate([scores * w0, scores * w1], axis=1).astype(BF16)
            mt = jnp.concatenate([scores_t * u0, scores_t * u1], axis=1).astype(BF16)
            x16 = xb[rows, cj]
            o16 = cot[rows, cj]
            zero = jnp.zeros_like(x16)
            xd = jnp.concatenate([jnp.where(low, x16, zero), jnp.where(low, zero, x16)], axis=0)
            od = jnp.concatenate([jnp.where(low, o16, zero), jnp.where(low, zero, o16)], axis=0)
            yy = mm(m, xd)
            pp = mm(o16, xd, NT)
            dx = mm(mt, od)
            dgs[b] = dgs[b] + w0 * pp[:, 0:128] + w1 * pp[:, 128:256]
            dxin[rows, cj] = dx
            q1s[rows, cj] = o16.astype(F32) * yy - x16.astype(F32) * dx

        blocks(inside)

    got(27, cot.at[0:384, :])
    w_done(2)
    pair_forward(2)
    pair_inside(2)
    pair_forward(3)
    pair_inside(3)
    w_done(3)
    pair_forward(4)
    pair_inside(4)
    for p in range(4):
        for q in range(4):
            hidx[320 * p + 80 * q : 320 * p + 80 * q + 80, :] = hidt[320 * q + 80 * p : 320 * q + 80 * p + 80, :]
    w_done(1)
    pair_forward(0)
    pair_inside(0)
    pair_forward(1)
    pair_inside(1)

    def turn(b, rows):
        dcf[rows, :] = mm(dgs[b], bmf[rows, :], NN, highest)
        dbf[rows, :] = mm(dgs[b], cmf[rows, :], TN, highest)

    blocks(turn)
    got(29, ttr)

    lanes = lax.broadcasted_iota(jnp.int32, (256, 128), 0)
    outl = lax.broadcasted_iota(jnp.int32, (256, 128), 1)

    def sums(z, j):
        hi = z.astype(BF16)
        lo = (z - hi.astype(F32)).astype(BF16)
        choose = (outl == 2 * j + lax.rem(lax.div(lanes, 64), 2)).astype(F32).astype(BF16)
        return mm(jnp.concatenate([hi, lo], axis=1), choose)

    yes = [jnp.where(y >= k, 1.0, 0.0).astype(F32) for k in (1, 2, 3)]
    no = [jnp.where(y + k <= 3, 1.0, 0.0).astype(F32) for k in (1, 2, 3)]
    inner = [jnp.zeros((8, 128), F32) for _ in range(4)]
    gain = [jnp.zeros((8, 128), F32)]

    def pair_outside(j):
        cj = slice(128 * j, 128 * j + 128)
        got(30 + j, str_.at[:, :, cj])
        t = [ttr[k, 0:1, cj] for k in range(3)]
        came = [str_[k, :, cj].astype(F32) for k in range(3)]
        s = yes[0] * came[0] + (yes[1] * jnp.exp(t[0])) * came[1] + (yes[2] * jnp.exp(t[0] + t[1])) * came[2]
        d = no[0] * came[2] + (no[1] * jnp.exp(t[2])) * came[1] + (no[2] * jnp.exp(t[2] + t[1])) * came[0]
        for b in (3, 2, 1, 0):
            db[b, :, cj] = d.astype(BF16)
            dd[b] = d
            d = jnp.exp(total(b, cj)) * d + dl[b, :, cj]
        for b in range(4):
            sb[b, :, cj] = s.astype(BF16)
            grown = jnp.exp(total(b, cj)) * s
            inner[b] = inner[b] + sums((grown * dd[b]).reshape(16, 8, 128).sum(axis=0), j)
            s = grown + sl[b, :, cj]

        def outside(b, rows):
            o = cot[rows, cj].astype(F32)
            yst = mm(cmf[rows, :].astype(BF16), sb[b, :, cj]) * ecs[rows, cj]
            dxst = mm(bmf[rows, :].astype(BF16), db[b, :, cj]) * tls[rows, cj]
            val = vv[rows, cj]
            dxs = dxin[rows, cj] + dxst
            z = jnp.concatenate([q1s[rows, cj] + o * yst, xb[rows, cj].astype(F32) * dxst, dxs * val], axis=0)
            red[b] = red[b] + sums(z, j)
            dval = dxs * sexp[rows, cj] + pair(skip, j) * o
            rr[rows, cj] = (dval * silu_grad(projv[rows, cj])).astype(BF16)
            gain[0] = gain[0] + sums((o * val).reshape(16, 8, 128).sum(axis=0), j)

        blocks(outside)

    class Stream:
        def __init__(self, base, group, lo, hi, kind, bufs):
            self.base, self.group, self.lo, self.hi, self.left = base, group, lo, hi, hidx if kind else hidt
            self.dw, self.s1, self.r1, self.s2, self.r2, self.s3, self.r3, self.s4, self.r4, self.sd, self.rd = bufs
            self.index, self.dev, self.index2, self.dev2 = (y, ydev, x, xdev) if kind == 0 else (x, xdev, y, ydev)

        def send(self, i, src, dst, dev):
            return send(self.base + i, src, dst, dev, self.group)

        def first(self):
            for i in (2, 1, 3, 0):
                rows = ds(lax.rem(self.index + i, 4) * 320, 320)
                cols = slice(self.lo, self.hi) if self.hi else ds(640 + 128 * c, 256, 128)
                self.dw[rows, :] = mm(self.left[rows, :], rr[:, cols])
                if i == 2:
                    self.s1[...] = self.dw[rows, :].astype(BF16)
                    self.one = (
                        self.send(0, self.s1.at[0:160, :], self.r1.at[0], self.dev(1)),
                        self.send(1, self.s1.at[160:320, :], self.r1.at[1], self.dev(-1)),
                    )

        def second(self):
            nxt = lax.rem(self.index + 1, 4) * 320
            prv = lax.rem(self.index + 3, 4) * 320
            self.one[0].wait_recv()
            self.s2[0, 0:160, :] = (self.dw[ds(nxt, 160), :] + self.r1[0].astype(F32)).astype(BF16)
            self.s2[0, 160:320, :] = self.dw[ds(nxt + 160, 160), :].astype(BF16)
            self.send(2, self.s2.at[0], self.r2.at[0], self.dev(1))
            self.one[1].wait_recv()
            self.s2[1, 0:160, :] = self.dw[ds(prv, 160), :].astype(BF16)
            self.s2[1, 160:320, :] = (self.dw[ds(prv + 160, 160), :] + self.r1[1].astype(F32)).astype(BF16)
            self.send(2, self.s2.at[1], self.r2.at[1], self.dev(-1))

        def third(self):
            got(self.base + 2, self.r2)
            here = ds(self.index * 320, 320)
            summed = self.dw[here, :] + self.r2[0].astype(F32) + self.r2[1].astype(F32)
            self.dw[here, :] = summed
            self.s3[...] = summed.astype(BF16)
            for k in (2, 1, 3):
                piece = self.s3.at[ds(lax.rem(self.index2 + k, 4) * 80, 80), :]
                self.send(3, piece, self.r3.at[k - 1], self.dev2(k))

        def fourth(self):
            got(self.base + 3, self.r3)
            rows = ds(self.index * 320 + self.index2 * 80, 80)
            self.s4[...] = self.dw[rows, :] + self.r3[0].astype(F32) + self.r3[1].astype(F32) + self.r3[2].astype(F32)
            self.four = self.send(4, self.s4.at[ds((1 - zh) * 40, 40), :], self.r4, zpair)

        def owners(self):
            self.four.wait_recv()
            chunk = self.s4[ds(zh * 40, 40), :] + self.r4[...]
            for i in range(4):
                self.sd[i, 0:10, :] = chunk[10 * i : 10 * i + 10, :]
            self.rd[g] = self.sd[r]
            for k in (2, 3, 1):
                zlk, ck, dev = rank(k)
                self.send(5, self.sd.at[zlk * 2 + ck], self.rd.at[g], dev)

        def finish(self):
            got(self.base + 5, self.rd.at[0:3])

        def close(self):
            sent(self.group, self.dw.at[0:688, :])

    alpha = Stream(46, 13, 256, 640, 0, (dwa, sa1, ra1, sa2, ra2, sa3, ra3, sa4, ra4, sda, rda))
    beta = Stream(52, 14, 0, 256, 1, (dwb, sb1, rb1, sb2, rb2, sb3, rb3, sb4, rb4, sdb, rdb))
    gamma = Stream(58, 15, 640, None, 1, (dwc, sc1, rc1, sc2, rc2, sc3, rc3, sc4, rc4, sdc, rdc))

    pair_outside(2)
    pair_outside(3)
    pair_outside(4)
    alpha.first()
    pair_outside(0)
    pair_outside(1)

    ownl = coli < 10
    bias_sum = decay_sum = jnp.zeros((8, 128), F32)
    for b in range(4):
        rows = slice(128 * b, 128 * b + 128)
        dcf[rows, :] = dcf[rows, :] + mm(oe[rows, :], sb[b], NT)
        dbf[rows, :] = dbf[rows, :] + mm(xt[rows, :], db[b], NT)
        dlog = mm(upper, red[b, 0:128], NN, highest) + mm(strict, red[b, 128:256], NN, highest)
        dlog = jnp.where(ownl, dlog + inner[b].sum(axis=0, keepdims=True), 0.0)
        ddt = (red[b, 256:384] + neg * dlog) * jax.nn.sigmoid(projs[rows, 128:256] + bias)
        ddt = jnp.where(ownl, ddt, 0.0)
        rr[rows, 768:896] = ddt.astype(BF16)
        bias_sum = bias_sum + ddt.reshape(16, 8, 128).sum(axis=0)
        decay_sum = decay_sum + (dlog * lgd[rows, :]).reshape(16, 8, 128).sum(axis=0)
    first = c == 0
    place = jnp.where(jnp.logical_and(rowi < 10, coli == rowi + 10 * g), 1.0, 0.0).astype(F32)
    t1s[...] = jnp.where(first, dcf[...], dbf[...])
    t1 = send(35, t1s, t1r, core, 9)
    beta.first()
    row8 = lax.broadcasted_iota(jnp.int32, (8, 128), 0)
    packed = jnp.where(
        row8 == 0, bias_sum.sum(axis=0, keepdims=True),
        jnp.where(row8 == 1, decay_sum.sum(axis=0, keepdims=True),
                  jnp.where(row8 == 2, gain[0].sum(axis=0, keepdims=True), 0.0)),
    )
    heads_y[y] = mm(packed, place, NN, highest)
    for k in (1, 2, 3):
        send(38, heads_y.at[y], heads_y.at[y], ydev(k), 10)
    alpha.second()
    t1.wait_recv()
    mixed = jnp.where(first, dbf[...], dcf[...]) + t1r[...]
    rr[:, ds(lane0, 128)] = (mixed * silu_grad(projs[:, ds(256 * c, 128, 128)])).astype(BF16)
    rr[:, ds(896 - 256 * c, 128)] = jnp.zeros((512, 128), BF16)
    gamma.first()
    for n in range(5):
        part = slice(256 * n, 256 * n + 256)
        hgp[:, part] = mm(rr[...], wf[part, :], NT)
    mate_row = ds((zl * 2 + 1 - c) * 128, 128)
    far_mate = ds(((1 - zl) * 2 + 1 - c) * 128, 128)
    far_row = ds(((1 - zl) * 2 + c) * 128, 128)
    hgs[1] = hgp[far_mate, :].astype(BF16)
    hg_far = send(43, hgs.at[1], hgr.at[1], core, 11)
    hgs[0] = hgp[mate_row, :].astype(BF16)
    hg_near = send(42, hgs.at[0], hgr.at[0], core, 11)
    beta.second()
    hg_far.wait_recv()
    hgs[2] = (hgp[far_row, :] + hgr[1].astype(F32)).astype(BF16)
    hg_z = send(44, hgs.at[2], hgr.at[2], rank(2)[2], 11)
    gamma.second()
    alpha.third()
    beta.third()
    got(38, heads_y.at[0:3])
    heads_x[x] = (heads_y[0] + heads_y[1]) + (heads_y[2] + heads_y[3])
    for k in (1, 2, 3):
        send(39, heads_x.at[x], heads_x.at[x], xdev(k), 10)
    gamma.third()
    beta.fourth()
    got(39, heads_x.at[0:3])
    heads_z[zh] = (heads_x[0] + heads_x[1]) + (heads_x[2] + heads_x[3])
    head_z = send(40, heads_z.at[zh], heads_z.at[zh], zpair, 10)
    alpha.fourth()
    gamma.fourth()
    beta.owners()
    alpha.owners()
    hg_near.wait_recv()
    hg_z.wait_recv()
    hgo[...] = (hgp[here_id, :] + hgr[0].astype(F32) + hgr[2].astype(F32)).astype(BF16)
    hg_out = pltpu.make_async_copy(hgo, hg_ref, ls.at[5])
    hg_out.start()
    head_z.wait_recv()
    heads_g[r] = heads_z[0] + heads_z[1]
    for k in (1, 2, 3):
        send(41, heads_g.at[r], heads_g.at[r], rank(k)[2], 10)
    gamma.owners()
    beta.finish()
    for k in range(4):
        wgo[:, 640 * k : 640 * k + 256] = rdb[k, 0:10, :]
    alpha.finish()
    for k in range(4):
        wgo[:, 640 * k + 256 : 640 * k + 640] = rda[k, 0:10, :]
    got(41, heads_g.at[0:3])
    hdo[...] = (heads_g[0] + heads_g[1]) + (heads_g[2] + heads_g[3])
    hd_out = pltpu.make_async_copy(hdo, hd_ref, ls.at[6])
    hd_out.start()
    gamma.finish()
    wgo[:, 2560:2688] = rdc[0, 0:10, 0:128] + rdc[2, 0:10, 0:128]
    wgo[:, 2688:2816] = rdc[1, 0:10, 128:256] + rdc[3, 0:10, 128:256]
    for k in range(4):
        lane = 128 - 128 * (k % 2)
        wgo[:, 2816 + 10 * k : 2826 + 10 * k] = rdc[k, 0:10, lane : lane + 10]
    wg_out = pltpu.make_async_copy(wgo, wg_ref, ls.at[7])
    wg_out.start()
    for m in range(4):
        sent(m, wf.at[0:1120, cols(m)])
    sent(4, hidf.at[0:384, :])
    sent(5, cot.at[0:384, :])
    sent(6, wf.at[:, ds(lane0, 128)])
    sent(7, ttr)
    sent(8, str_)
    sent(9, t1r)
    sent(10, bmf.at[0:80, :])
    sent(11, hgs)
    for stream in (alpha, beta, gamma):
        stream.close()
    hg_out.wait()
    hd_out.wait()
    wg_out.wait()


def scratch():
    def v(shape, dtype=F32):
        return pltpu.VMEM(shape, dtype)

    def stream(n):
        return [
            v((D, n)), v((320, n), BF16), v((2, 160, n), BF16), v((2, 320, n), BF16), v((2, 320, n), BF16),
            v((320, n), BF16), v((3, 80, n), BF16), v((80, n)), v((40, n)), v((4, 16, n)), v((4, 16, n)),
        ]

    wide, wide16 = v((512, COLS)), v((512, COLS), BF16)
    thin = v((512, 128))
    return [
        v((512, D), BF16), v((D, 512), BF16), v((D, 512), BF16), wide16, v((160, 2856), BF16), v((D, 1024), BF16),
        v((512, 384)), wide, thin, thin, thin, thin, v((4, 16, 128)), thin,
        v((4, 128, 128)), v((4, 128, 128)), v((4, 128, 128)),
        wide, wide, wide, wide, wide16, wide16, wide16, v((32, COLS)),
        v((4, 128, COLS)), v((4, 128, COLS)), v((2, 128, COLS), BF16), v((8, COLS)),
        v((3, 128, COLS), BF16), v((3, 8, COLS)), wide, wide, thin, thin,
        v((4, 128, COLS), BF16), v((4, 128, COLS), BF16), v((4, 128, 128)), v((4, 384, 128)),
        v((512, 1024), BF16), thin, thin,
        v((512, D)), v((3, 128, D), BF16), v((3, 128, D), BF16),
        *stream(384), *stream(256), *stream(256),
        v((4, 8, 128)), v((4, 8, 128)), v((2, 8, 128)), v((4, 8, 128)),
        v((128, D), BF16), v((10, 2856)), v((8, 128)),
        pltpu.SemaphoreType.DMA((16,)), pltpu.SemaphoreType.DMA((64,)), pltpu.SemaphoreType.DMA((8,)),
    ]


def emit(hg_ref, wg_ref, hd_ref, hg_out, wg_out, hd_out):
    hg_out[...] = hg_ref[...]
    wg_out[...] = wg_ref[...]
    hd_out[...] = hd_ref[0:3, 0:HEADS]


def body(hidden, output_grad, input_weight, step_bias, decay_log, skip_gain):
    anyspace = pl.BlockSpec(memory_space=pl.ANY)
    vmem = pl.BlockSpec(memory_space=pltpu.VMEM)
    hg, wg, hd = pl.pallas_call(
        kernel,
        out_shape=(
            jax.ShapeDtypeStruct((128, D), BF16),
            jax.ShapeDtypeStruct((10, 2856), F32),
            jax.ShapeDtypeStruct((8, 128), F32),
        ),
        in_specs=[anyspace, anyspace, anyspace, vmem, vmem, vmem],
        out_specs=(anyspace, anyspace, anyspace),
        scratch_shapes=scratch(),
        compiler_params=pltpu.CompilerParams(has_side_effects=True, collective_id=0, vmem_limit_bytes=64000000),
    )(hidden[0], output_grad[0], input_weight, step_bias[None], decay_log[None], skip_gain[None])
    hg, wg, hd = pl.pallas_call(
        emit,
        out_shape=(
            jax.ShapeDtypeStruct((128, D), BF16),
            jax.ShapeDtypeStruct((10, 2856), F32),
            jax.ShapeDtypeStruct((3, HEADS), F32),
        ),
        in_specs=[vmem, vmem, vmem],
        out_specs=(vmem, vmem, vmem),
    )(hg, wg, hd)
    return (hg[None], wg, hd)


def solution(mesh):
    torus = Mesh(
        mesh.devices.reshape(4, 2, 2, 4, 2), ("seq_0", "seq_1", "seq_2", "zero_0", "zero_1")
    )
    in_specs = (P(ZERO, SEQ, None), P(ZERO, SEQ, None), P(ZERO, None), P(), P(), P())
    out_specs = (P(ZERO, SEQ, None), P(SEQ_ZERO, None), P())
    return jax.shard_map(body, mesh=torus, in_specs=in_specs, out_specs=out_specs, check_vma=False)
```

```python
import functools

import jax
import jax.numpy as jnp
from jax import lax
from jax.experimental import pallas as pl
from jax.experimental.pallas import tpu as pltpu
from jax.sharding import Mesh
from jax.sharding import PartitionSpec as P

HEADS = 40
STATE = 128
INNER = 2560
D = 1280
COLS = 640
ZERO = ("zero_0", "zero_1")
SEQ = ("seq_0", "seq_1", "seq_2")
SEQ_ZERO = ("seq_0", "seq_1", "seq_2", "zero_0", "zero_1")
MESH = pl.DeviceIdType.MESH
F32 = jnp.float32
BF16 = jnp.bfloat16
highest = lax.Precision.HIGHEST
NN = (((1,), (0,)), ((), ()))
NT = (((1,), (1,)), ((), ()))
TN = (((0,), (0,)), ((), ()))


def mm(a, b, dims=NN, precision=None):
    return lax.dot_general(a, b, dims, preferred_element_type=F32, precision=precision)


def ds(start, size, align=None):
    return pl.ds(pl.multiple_of(start, align or size), size)


def silu_grad(v):
    sig = jax.nn.sigmoid(v)
    return sig * (1.0 + v * (1.0 - sig))


def kernel(
    hid_ref, cot_ref, w_ref, bias_ref, decay_ref, skip_ref,
    hg_ref, wg_ref, hd_ref,
    hidf, hidt, hidx, cot, wraw, wf, projs, projv, bmf, cmf, lgd, cums, cumt, stp, gs, gts, dgs,
    sexp, ecs, tls, vv, xb, xt, oe, tot,
    sl, dl, stt, tts, str_, ttr, q1s, dxin, dbf, dcf, sb, db, dd, red,
    rr, t1s, t1r, hgp, hgs, hgr,
    dwa, sa1, ra1, sa2, ra2, sa3, ra3, sa4, ra4, sda, rda,
    dwb, sb1, rb1, sb2, rb2, sb3, rb3, sb4, rb4, sdb, rdb,
    dwc, sc1, rc1, sc2, rc2, sc3, rc3, sc4, rc4, sdc, rdc,
    heads_y, heads_x, heads_z, heads_g, hgo, wgo, hdo,
    ss, rs, ls,
):
    y, zl, c = (lax.axis_index(n) for n in SEQ)
    x, zh = (lax.axis_index(n) for n in ZERO)
    r = zl * 2 + c
    a = lax.rem(zl + zh, 2)
    g = a * 2 + c

    def send(i, src, dst, where, group):
        copy = pltpu.make_async_remote_copy(
            src_ref=src, dst_ref=dst, send_sem=ss.at[group], recv_sem=rs.at[i],
            device_id=where, device_id_type=MESH,
        )
        copy.start()
        return copy

    def bytes_of(ref, i=0, group=0):
        return pltpu.make_async_remote_copy(
            src_ref=ref, dst_ref=ref, send_sem=ss.at[group], recv_sem=rs.at[i],
            device_id={"seq_2": 1 - c}, device_id_type=MESH,
        )

    def got(i, ref):
        bytes_of(ref, i=i).wait_recv()

    def sent(group, ref):
        bytes_of(ref, group=group).wait_send()

    def rank(k):
        zlk = lax.rem(zl + k // 2, 2)
        ck = lax.rem(c + k % 2, 2)
        return zlk, ck, {"seq_1": zlk, "seq_2": ck}

    def xdev(k):
        return {"zero_0": lax.rem(x + k + 4, 4)}

    def ydev(k):
        return {"seq_0": lax.rem(y + k + 4, 4)}

    zpair = {"seq_1": 1 - zl, "zero_1": 1 - zh}
    core = {"seq_2": 1 - c}
    here_id = ds(r * 128, 128)

    def shard(xk, zk, lo=0, size=160):
        return ds((lax.rem(xk + 4, 4) * 2 + zk) * 160 + lo, size, 16)

    own = shard(x, zh)
    lane0 = 640 + 256 * c
    local = [
        pltpu.make_async_copy(w_ref, wraw, ls.at[0]),
        pltpu.make_async_copy(w_ref.at[:, ds(g * COLS, COLS, 128)], wf.at[own, 0:640], ls.at[1]),
        pltpu.make_async_copy(w_ref.at[:, ds(2560 + 128 * c, 128)], wf.at[own, ds(lane0, 128)], ls.at[2]),
        pltpu.make_async_copy(hid_ref, hidf.at[here_id, :], ls.at[3]),
        pltpu.make_async_copy(cot_ref.at[:, ds(g * COLS, COLS, 128)], cot.at[here_id, :], ls.at[4]),
    ]
    for copy in local:
        copy.start()

    barrier = pltpu.get_barrier_semaphore()

    def greet(dev):
        pl.semaphore_signal(barrier, inc=1, device_id=dev, device_id_type=MESH)

    greet(zpair)
    for k in (1, 2, 3):
        greet(xdev(k))
        greet(ydev(k))
        greet(rank(k)[2])
    coli = lax.broadcasted_iota(jnp.int32, (128, 128), 1)
    rowi = lax.broadcasted_iota(jnp.int32, (128, 128), 0)
    local[0].wait()
    tail = jnp.concatenate([wraw[:, 2816:2856].astype(F32), jnp.zeros((160, 88), F32)], axis=1)
    tail = pltpu.roll(tail, lax.rem(128 - 10 * g, 128), 1)
    keep10 = lax.broadcasted_iota(jnp.int32, (160, 128), 1) < 10
    wf[own, 768:896] = jnp.where(keep10, tail, 0.0).astype(BF16)

    def lanes10(ref):
        full = jnp.concatenate([ref[...], jnp.zeros((1, 88), F32)], axis=1)
        return pltpu.roll(jnp.broadcast_to(full, (8, 128)), lax.rem(128 - 10 * g, 128), 1)[0:1, :]

    bias = lanes10(bias_ref)
    neg = -jnp.exp(lanes10(decay_ref))
    skip = lanes10(skip_ref)
    for copy in local[1:]:
        copy.wait()
    pl.semaphore_wait(barrier, 10)

    def cols(m):
        return (ds(640 + 128 * c, 256, 128), slice(0, 256), slice(256, 512), slice(512, 640))[m]

    w = {}

    def wsend(m, i, rows, dev):
        ref = wf.at[rows, cols(m)]
        slot = min(i, 5) if m < 2 else {1: 1, 2: 2, 5: 3, 6: 4}.get(i, 5)
        w[m, i] = send(6 * m + slot, ref, ref, dev, m)

    def w_own_x(m):
        wsend(m, 1, own, xdev(1))
        wsend(m, 2, own, xdev(-1))

    def w_own_z(m):
        wsend(m, 0, own, zpair)

    def w_other(m):
        w[m, 0].wait_recv()
        wsend(m, 3, shard(x, 1 - zh), xdev(1))
        wsend(m, 4, shard(x, 1 - zh), xdev(-1))

    def w_forward(m):
        w[m, 1].wait_recv()
        wsend(m, 5, shard(x - 1, zh, 0, 80), xdev(1))
        w[m, 2].wait_recv()
        wsend(m, 6, shard(x + 1, zh, 80, 80), xdev(-1))

    def w_forward_other(m):
        w[m, 3].wait_recv()
        wsend(m, 7, shard(x - 1, 1 - zh, 0, 80), xdev(1))
        w[m, 4].wait_recv()
        wsend(m, 8, shard(x + 1, 1 - zh, 80, 80), xdev(-1))

    def w_across(m):
        wsend(m, 3, shard(x - 1, zh), zpair)
        wsend(m, 4, shard(x + 1, zh), zpair)

    def w_across_far(m):
        w[m, 5].wait_recv()
        wsend(m, 7, shard(x + 2, zh, 0, 80), zpair)
        w[m, 6].wait_recv()
        wsend(m, 8, shard(x + 2, zh, 80, 80), zpair)

    def w_done(m):
        got(6 * m + 5, wf.at[0 : 320 if m < 2 else 640, cols(m)])

    def hand(k):
        ref = wf.at[ds(lax.rem(x + k + 4, 4) * 320, 320), ds(lane0, 128)]
        send(28, ref, ref, core, 6)

    w_own_z(0)
    w_own_x(0)
    h_z = send(24, hid_ref, hidf.at[here_id, :], rank(2)[2], 4)
    w_own_x(2)
    w_own_z(1)
    h_c = send(25, hid_ref, hidf.at[here_id, :], core, 4)
    for k in (2, 3, 1):
        zlk, ck, dev = rank(k)
        gk = lax.rem(zlk + zh, 2) * 2 + ck
        send(27, cot_ref.at[:, ds(gk * COLS, COLS, 128)], cot.at[here_id, :], dev, 5)
    w_own_z(2)
    w_own_z(3)
    w_other(0)
    w_forward(0)
    w_forward(2)
    w_across(2)
    w_own_x(3)
    w_forward_other(0)
    w_own_x(1)
    for k in (-1, 0, 1):
        hand(k)
    h_z.wait_recv()
    zrows = ds((rank(2)[0] * 2 + c) * 128, 128)
    h_f = send(26, hidf.at[zrows, :], hidf.at[zrows, :], core, 4)
    w_across_far(2)
    w_forward(3)
    w_across(3)
    w_other(1)
    w_done(0)
    hand(2)
    h_c.wait_recv()
    h_f.wait_recv()

    low = coli < 64
    causal = rowi >= coli
    anti = rowi <= coli
    tri = causal.astype(F32)
    upper = anti.astype(F32)
    strict = (rowi > coli).astype(F32)

    def pair(v, j):
        return jnp.where(low[0 : v.shape[0]], v[:, 2 * j : 2 * j + 1], v[:, 2 * j + 1 : 2 * j + 2])

    def blocks(f, unroll=True):
        if unroll:
            for b in range(4):
                f(b, pl.ds(b * 128, 128))
        else:
            def step(b, carry):
                f(b, ds(b * 128, 128))
                return carry

            lax.fori_loop(0, 4, step, 0)

    def steps(b, rows):
        projs[rows, ds(128 * c, 256, 128)] = mm(hidf[rows, :], wf[:, ds(640 + 128 * c, 256, 128)])
        pre = projs[rows, 128:256] + bias
        step = jnp.maximum(pre, 0.0) + jnp.log1p(jnp.exp(-jnp.abs(pre)))
        lg = neg * step
        cum = mm(tri, lg, NN, highest)
        stp[rows, :] = step
        lgd[rows, :] = lg
        cums[rows, :] = cum
        cumt[b] = cum.T[0:16, :]
        dgs[b] = jnp.zeros((128, 128), F32)
        red[b] = jnp.zeros((384, 128), F32)

    def maps(b, rows):
        projs[rows, ds(256 - 256 * c, 128)] = mm(hidf[rows, :], wf[:, ds(896 - 256 * c, 128)])
        bm = jax.nn.silu(projs[rows, 0:128])
        cm = jax.nn.silu(projs[rows, 256:384])
        bmf[rows, :] = bm
        cmf[rows, :] = cm
        scores = mm(cm, bm, NT, highest)
        gs[b] = scores
        gts[b] = scores.T

    blocks(steps)
    for j in range(5):
        cj = slice(128 * j, 128 * j + 128)
        for b in range(4):
            last_row = cums[128 * b + 127 : 128 * b + 128, :]
            tot[8 * b : 8 * b + 8, cj] = pair(jnp.broadcast_to(last_row, (8, 128)), j)
    tts[...] = tot[0:8, :] + tot[8:16, :] + tot[16:24, :] + tot[24:32, :]
    for k in (1, 2, 3):
        send(29, tts, ttr.at[k - 1], ydev(k), 7)

    i320 = lax.broadcasted_iota(jnp.int32, (320, 320), 0)
    k320 = lax.broadcasted_iota(jnp.int32, (320, 320), 1)
    tens = lax.shift_right_logical(i320 * 6554, 16)
    source = ((tens & 3) * 8 + lax.shift_right_logical(tens, 2)) * 10 + i320 - tens * 10
    perm = jnp.where(k320 == source, 1.0, 0.0).astype(F32).astype(BF16)
    for q in range(4):
        hidt[320 * q : 320 * q + 320, :] = mm(perm, hidf[:, 320 * q : 320 * q + 320], NT).astype(BF16)
    w_forward(1)
    got(28, wf.at[:, ds(896 - 256 * c, 128)])
    maps(0, pl.ds(0, 128))
    w_across_far(3)
    maps(1, pl.ds(128, 128))
    maps(2, pl.ds(256, 128))
    w_forward_other(1)
    maps(3, pl.ds(384, 128))

    def total(b, cj):
        return tot[8 * b : 8 * b + 1, cj]

    def pair_forward(j):
        cj = slice(128 * j, 128 * j + 128)

        wide = slice(128 * j, min(128 * j + 256, 640))

        def project(b, rows):
            projv[rows, wide] = mm(hidf[rows, :], wf[:, wide])

        def local_part(b, rows):
            ce = pair(cums[rows, :], j)
            se = pair(stp[rows, :], j)
            ec = jnp.exp(ce)
            tl = jnp.exp(ce[127:128, :] - ce)
            val = jax.nn.silu(projv[rows, cj])
            xs = val * se
            sexp[rows, cj] = se
            ecs[rows, cj] = ec
            tls[rows, cj] = tl
            vv[rows, cj] = val
            xb[rows, cj] = xs.astype(BF16)
            x16 = (xs * tl).astype(BF16)
            o16 = (cot[rows, cj].astype(F32) * ec).astype(BF16)
            xt[rows, cj] = x16
            oe[rows, cj] = o16
            sl[b, :, cj] = mm(bmf[rows, :].astype(BF16), x16, TN)
            dl[b, :, cj] = mm(cmf[rows, :].astype(BF16), o16, TN)

        if j % 2 == 0:
            blocks(project)
        blocks(local_part)
        s = sl[0, :, cj]
        d = dl[3, :, cj]
        for b in range(1, 4):
            s = jnp.exp(total(b, cj)) * s + sl[b, :, cj]
            d = jnp.exp(total(3 - b, cj)) * d + dl[3 - b, :, cj]
        stt[0, :, cj] = s.astype(BF16)
        stt[1, :, cj] = d.astype(BF16)
        for k in (1, 2, 3):
            wraps = lax.div(y + k, 4)
            send(30 + j, stt.at[wraps, :, cj], str_.at[k - 1, :, cj], ydev(k), 8)

    def pair_inside(j):
        cj = slice(128 * j, 128 * j + 128)

        def inside(b, rows):
            cum = cums[rows, :]
            c0, c1 = cum[:, 2 * j : 2 * j + 1], cum[:, 2 * j + 1 : 2 * j + 2]
            r0, r1 = cumt[b, 2 * j : 2 * j + 1, :], cumt[b, 2 * j + 1 : 2 * j + 2, :]
            w0 = jnp.where(causal, jnp.exp(jnp.where(causal, c0 - r0, 0.0)), 0.0)
            w1 = jnp.where(causal, jnp.exp(jnp.where(causal, c1 - r1, 0.0)), 0.0)
            u0 = jnp.where(anti, jnp.exp(jnp.where(anti, r0 - c0, 0.0)), 0.0)
            u1 = jnp.where(anti, jnp.exp(jnp.where(anti, r1 - c1, 0.0)), 0.0)
            scores, scores_t = gs[b], gts[b]
            m = jnp.concatenate([scores * w0, scores * w1], axis=1).astype(BF16)
            mt = jnp.concatenate([scores_t * u0, scores_t * u1], axis=1).astype(BF16)
            x16 = xb[rows, cj]
            o16 = cot[rows, cj]
            zero = jnp.zeros_like(x16)
            xd = jnp.concatenate([jnp.where(low, x16, zero), jnp.where(low, zero, x16)], axis=0)
            od = jnp.concatenate([jnp.where(low, o16, zero), jnp.where(low, zero, o16)], axis=0)
            yy = mm(m, xd)
            pp = mm(o16, xd, NT)
            dx = mm(mt, od)
            dgs[b] = dgs[b] + w0 * pp[:, 0:128] + w1 * pp[:, 128:256]
            dxin[rows, cj] = dx
            q1s[rows, cj] = o16.astype(F32) * yy - x16.astype(F32) * dx

        blocks(inside)

    got(27, cot.at[0:384, :])
    w_done(2)
    pair_forward(2)
    pair_inside(2)
    pair_forward(3)
    pair_inside(3)
    w_done(3)
    pair_forward(4)
    pair_inside(4)
    for p in range(4):
        for q in range(4):
            hidx[320 * p + 80 * q : 320 * p + 80 * q + 80, :] = hidt[320 * q + 80 * p : 320 * q + 80 * p + 80, :]
    w_done(1)
    pair_forward(0)
    pair_inside(0)
    pair_forward(1)
    pair_inside(1)

    def turn(b, rows):
        dcf[rows, :] = mm(dgs[b], bmf[rows, :], NN, highest) + mm(oe[rows, :], sb[b], NT)
        dbf[rows, :] = mm(dgs[b], cmf[rows, :], TN, highest) + mm(xt[rows, :], db[b], NT)

    got(29, ttr)

    lanes = lax.broadcasted_iota(jnp.int32, (256, 128), 0)
    outl = lax.broadcasted_iota(jnp.int32, (256, 128), 1)

    def sums(z, j):
        hi = z.astype(BF16)
        lo = (z - hi.astype(F32)).astype(BF16)
        choose = (outl == 2 * j + lax.rem(lax.div(lanes, 64), 2)).astype(F32).astype(BF16)
        return mm(jnp.concatenate([hi, lo], axis=1), choose)

    yes = [jnp.where(y >= k, 1.0, 0.0).astype(F32) for k in (1, 2, 3)]
    no = [jnp.where(y + k <= 3, 1.0, 0.0).astype(F32) for k in (1, 2, 3)]
    inner = [jnp.zeros((8, 128), F32) for _ in range(4)]
    gain = [jnp.zeros((8, 128), F32)]

    def pair_outside(j):
        cj = slice(128 * j, 128 * j + 128)
        got(30 + j, str_.at[:, :, cj])
        t = [ttr[k, 0:1, cj] for k in range(3)]
        came = [str_[k, :, cj].astype(F32) for k in range(3)]
        s = yes[0] * came[0] + (yes[1] * jnp.exp(t[0])) * came[1] + (yes[2] * jnp.exp(t[0] + t[1])) * came[2]
        d = no[0] * came[2] + (no[1] * jnp.exp(t[2])) * came[1] + (no[2] * jnp.exp(t[2] + t[1])) * came[0]
        for b in (3, 2, 1, 0):
            db[b, :, cj] = d.astype(BF16)
            dd[b] = d
            d = jnp.exp(total(b, cj)) * d + dl[b, :, cj]
        for b in range(4):
            sb[b, :, cj] = s.astype(BF16)
            grown = jnp.exp(total(b, cj)) * s
            inner[b] = inner[b] + sums((grown * dd[b]).reshape(16, 8, 128).sum(axis=0), j)
            s = grown + sl[b, :, cj]

        def outside(b, rows):
            o = cot[rows, cj].astype(F32)
            yst = mm(cmf[rows, :].astype(BF16), sb[b, :, cj]) * ecs[rows, cj]
            dxst = mm(bmf[rows, :].astype(BF16), db[b, :, cj]) * tls[rows, cj]
            val = vv[rows, cj]
            dxs = dxin[rows, cj] + dxst
            z = jnp.concatenate([q1s[rows, cj] + o * yst, xb[rows, cj].astype(F32) * dxst, dxs * val], axis=0)
            red[b] = red[b] + sums(z, j)
            dval = dxs * sexp[rows, cj] + pair(skip, j) * o
            rr[rows, cj] = (dval * silu_grad(projv[rows, cj])).astype(BF16)
            gain[0] = gain[0] + sums((o * val).reshape(16, 8, 128).sum(axis=0), j)

        blocks(outside)

    class Stream:
        def __init__(self, base, group, parts, kind, bufs):
            self.base, self.group, self.parts, self.left = base, group, parts, hidx if kind else hidt
            self.dw, self.s1, self.r1, self.s2, self.r2, self.s3, self.r3, self.s4, self.r4, self.sd, self.rd = bufs
            self.index, self.dev, self.index2, self.dev2 = (y, ydev, x, xdev) if kind == 0 else (x, xdev, y, ydev)

        def send(self, i, src, dst, dev):
            return send(self.base + i, src, dst, dev, self.group)

        def first(self):
            for i in (2, 1, 3, 0):
                rows = ds(lax.rem(self.index + i, 4) * 320, 320)
                for cols, target in self.parts:
                    self.dw[rows, target] = mm(self.left[rows, :], rr[:, cols])
                if i == 2:
                    self.s1[...] = self.dw[rows, :].astype(BF16)
                    self.one = (
                        self.send(0, self.s1.at[0:160, :], self.r1.at[0], self.dev(1)),
                        self.send(1, self.s1.at[160:320, :], self.r1.at[1], self.dev(-1)),
                    )

        def second(self):
            nxt = lax.rem(self.index + 1, 4) * 320
            prv = lax.rem(self.index + 3, 4) * 320
            self.one[0].wait_recv()
            self.s2[0, 0:160, :] = (self.dw[ds(nxt, 160), :] + self.r1[0].astype(F32)).astype(BF16)
            self.s2[0, 160:320, :] = self.dw[ds(nxt + 160, 160), :].astype(BF16)
            self.send(2, self.s2.at[0], self.r2.at[0], self.dev(1))
            self.one[1].wait_recv()
            self.s2[1, 0:160, :] = self.dw[ds(prv, 160), :].astype(BF16)
            self.s2[1, 160:320, :] = (self.dw[ds(prv + 160, 160), :] + self.r1[1].astype(F32)).astype(BF16)
            self.send(2, self.s2.at[1], self.r2.at[1], self.dev(-1))

        def third(self):
            got(self.base + 2, self.r2)
            here = ds(self.index * 320, 320)
            summed = self.dw[here, :] + self.r2[0].astype(F32) + self.r2[1].astype(F32)
            self.dw[here, :] = summed
            self.s3[...] = summed.astype(BF16)
            for k in (2, 1, 3):
                piece = self.s3.at[ds(lax.rem(self.index2 + k, 4) * 80, 80), :]
                self.send(3, piece, self.r3.at[k - 1], self.dev2(k))

        def fourth(self):
            got(self.base + 3, self.r3)
            rows = ds(self.index * 320 + self.index2 * 80, 80)
            self.s4[...] = self.dw[rows, :] + self.r3[0].astype(F32) + self.r3[1].astype(F32) + self.r3[2].astype(F32)
            self.four = self.send(4, self.s4.at[ds((1 - zh) * 40, 40), :], self.r4, zpair)

        def owners(self):
            self.four.wait_recv()
            chunk = self.s4[ds(zh * 40, 40), :] + self.r4[...]
            for i in range(4):
                self.sd[i, 0:10, :] = chunk[10 * i : 10 * i + 10, :]
            self.rd[g] = self.sd[r]
            for k in (2, 3, 1):
                zlk, ck, dev = rank(k)
                self.send(5, self.sd.at[zlk * 2 + ck], self.rd.at[g], dev)

        def finish(self):
            got(self.base + 5, self.rd.at[0:3])

        def close(self):
            sent(self.group, self.dw.at[0:688, :])

    alpha = Stream(46, 13, [(slice(256, 640), slice(0, 384))], 0, (dwa, sa1, ra1, sa2, ra2, sa3, ra3, sa4, ra4, sda, rda))
    beta = Stream(52, 14, [(slice(0, 256), slice(0, 256)), (slice(768, 896), slice(256, 384))], 1, (dwb, sb1, rb1, sb2, rb2, sb3, rb3, sb4, rb4, sdb, rdb))
    gamma = Stream(58, 15, [(ds(lane0, 128), slice(0, 128))], 0, (dwc, sc1, rc1, sc2, rc2, sc3, rc3, sc4, rc4, sdc, rdc))

    pair_outside(2)
    pair_outside(3)
    pair_outside(4)
    alpha.first()
    pair_outside(0)
    pair_outside(1)

    blocks(turn)
    first = c == 0
    t1s[...] = jnp.where(first, dcf[...], dbf[...])
    t1 = send(35, t1s, t1r, core, 9)

    ownl = coli < 10
    bias_sum = decay_sum = jnp.zeros((8, 128), F32)
    for b in range(4):
        rows = slice(128 * b, 128 * b + 128)
        dlog = mm(upper, red[b, 0:128], NN, highest) + mm(strict, red[b, 128:256], NN, highest)
        dlog = jnp.where(ownl, dlog + inner[b].sum(axis=0, keepdims=True), 0.0)
        ddt = (red[b, 256:384] + neg * dlog) * jax.nn.sigmoid(projs[rows, 128:256] + bias)
        ddt = jnp.where(ownl, ddt, 0.0)
        rr[rows, 768:896] = ddt.astype(BF16)
        bias_sum = bias_sum + ddt.reshape(16, 8, 128).sum(axis=0)
        decay_sum = decay_sum + (dlog * lgd[rows, :]).reshape(16, 8, 128).sum(axis=0)
    place = jnp.where(jnp.logical_and(rowi < 10, coli == rowi + 10 * g), 1.0, 0.0).astype(F32)
    beta.first()
    row8 = lax.broadcasted_iota(jnp.int32, (8, 128), 0)
    packed = jnp.where(
        row8 == 0, bias_sum.sum(axis=0, keepdims=True),
        jnp.where(row8 == 1, decay_sum.sum(axis=0, keepdims=True),
                  jnp.where(row8 == 2, gain[0].sum(axis=0, keepdims=True), 0.0)),
    )
    heads_y[y] = mm(packed, place, NN, highest)
    for k in (1, 2, 3):
        send(38, heads_y.at[y], heads_y.at[y], ydev(k), 10)
    alpha.second()
    t1.wait_recv()
    mixed = jnp.where(first, dbf[...], dcf[...]) + t1r[...]
    rr[:, ds(lane0, 128)] = (mixed * silu_grad(projs[:, ds(256 * c, 128, 128)])).astype(BF16)
    rr[:, ds(896 - 256 * c, 128)] = jnp.zeros((512, 128), BF16)
    gamma.first()
    for n in range(5):
        part = slice(256 * n, 256 * n + 256)
        hgp[:, part] = mm(rr[...], wf[part, :], NT)
    mate_row = ds((zl * 2 + 1 - c) * 128, 128)
    far_mate = ds(((1 - zl) * 2 + 1 - c) * 128, 128)
    far_row = ds(((1 - zl) * 2 + c) * 128, 128)
    hgs[1] = hgp[far_mate, :].astype(BF16)
    hg_far = send(43, hgs.at[1], hgr.at[1], core, 11)
    hgs[0] = hgp[mate_row, :].astype(BF16)
    hg_near = send(42, hgs.at[0], hgr.at[0], core, 11)
    beta.second()
    hg_far.wait_recv()
    hgs[2] = (hgp[far_row, :] + hgr[1].astype(F32)).astype(BF16)
    hg_z = send(44, hgs.at[2], hgr.at[2], rank(2)[2], 11)
    alpha.third()
    gamma.second()
    beta.third()
    got(38, heads_y.at[0:3])
    heads_x[x] = (heads_y[0] + heads_y[1]) + (heads_y[2] + heads_y[3])
    for k in (1, 2, 3):
        send(39, heads_x.at[x], heads_x.at[x], xdev(k), 10)
    gamma.third()
    alpha.fourth()
    got(39, heads_x.at[0:3])
    heads_z[zh] = (heads_x[0] + heads_x[1]) + (heads_x[2] + heads_x[3])
    head_z = send(40, heads_z.at[zh], heads_z.at[zh], zpair, 10)
    gamma.fourth()
    beta.fourth()
    alpha.owners()
    gamma.owners()
    hg_near.wait_recv()
    hg_z.wait_recv()
    hgo[...] = (hgp[here_id, :] + hgr[0].astype(F32) + hgr[2].astype(F32)).astype(BF16)
    hg_out = pltpu.make_async_copy(hgo, hg_ref, ls.at[5])
    hg_out.start()
    head_z.wait_recv()
    heads_g[r] = heads_z[0] + heads_z[1]
    for k in (1, 2, 3):
        send(41, heads_g.at[r], heads_g.at[r], rank(k)[2], 10)
    beta.owners()
    alpha.finish()
    for k in range(4):
        wgo[:, 640 * k + 256 : 640 * k + 640] = rda[k, 0:10, :]
    got(41, heads_g.at[0:3])
    hdo[...] = (heads_g[0] + heads_g[1]) + (heads_g[2] + heads_g[3])
    hd_out = pltpu.make_async_copy(hdo, hd_ref, ls.at[6])
    hd_out.start()
    gamma.finish()
    wgo[:, 2560:2688] = rdc[0, 0:10, :] + rdc[2, 0:10, :]
    wgo[:, 2688:2816] = rdc[1, 0:10, :] + rdc[3, 0:10, :]
    beta.finish()
    for k in range(4):
        wgo[:, 640 * k : 640 * k + 256] = rdb[k, 0:10, 0:256]
        wgo[:, 2816 + 10 * k : 2826 + 10 * k] = rdb[k, 0:10, 256:266]
    wg_out = pltpu.make_async_copy(wgo, wg_ref, ls.at[7])
    wg_out.start()
    for m in range(4):
        sent(m, wf.at[0:1120, cols(m)])
    sent(4, hidf.at[0:384, :])
    sent(5, cot.at[0:384, :])
    sent(6, wf.at[:, ds(lane0, 128)])
    sent(7, ttr)
    sent(8, str_)
    sent(9, t1r)
    sent(10, bmf.at[0:80, :])
    sent(11, hgs)
    for stream in (alpha, beta, gamma):
        stream.close()
    hg_out.wait()
    hd_out.wait()
    wg_out.wait()


def scratch():
    def v(shape, dtype=F32):
        return pltpu.VMEM(shape, dtype)

    def stream(n):
        return [
            v((D, n)), v((320, n), BF16), v((2, 160, n), BF16), v((2, 320, n), BF16), v((2, 320, n), BF16),
            v((320, n), BF16), v((3, 80, n), BF16), v((80, n)), v((40, n)), v((4, 16, n)), v((4, 16, n)),
        ]

    wide, wide16 = v((512, COLS)), v((512, COLS), BF16)
    thin = v((512, 128))
    return [
        v((512, D), BF16), v((D, 512), BF16), v((D, 512), BF16), wide16, v((160, 2856), BF16), v((D, 1024), BF16),
        v((512, 384)), wide, thin, thin, thin, thin, v((4, 16, 128)), thin,
        v((4, 128, 128)), v((4, 128, 128)), v((4, 128, 128)),
        wide, wide, wide, wide, wide16, wide16, wide16, v((32, COLS)),
        v((4, 128, COLS)), v((4, 128, COLS)), v((2, 128, COLS), BF16), v((8, COLS)),
        v((3, 128, COLS), BF16), v((3, 8, COLS)), wide, wide, thin, thin,
        v((4, 128, COLS), BF16), v((4, 128, COLS), BF16), v((4, 128, 128)), v((4, 384, 128)),
        v((512, 1024), BF16), thin, thin,
        v((512, D)), v((3, 128, D), BF16), v((3, 128, D), BF16),
        *stream(384), *stream(384), *stream(128),
        v((4, 8, 128)), v((4, 8, 128)), v((2, 8, 128)), v((4, 8, 128)),
        v((128, D), BF16), v((10, 2856)), v((8, 128)),
        pltpu.SemaphoreType.DMA((16,)), pltpu.SemaphoreType.DMA((64,)), pltpu.SemaphoreType.DMA((8,)),
    ]


def emit(hg_ref, wg_ref, hd_ref, hg_out, wg_out, hd_out):
    hg_out[...] = hg_ref[...]
    wg_out[...] = wg_ref[...]
    hd_out[...] = hd_ref[0:3, 0:HEADS]


def body(hidden, output_grad, input_weight, step_bias, decay_log, skip_gain):
    anyspace = pl.BlockSpec(memory_space=pl.ANY)
    vmem = pl.BlockSpec(memory_space=pltpu.VMEM)
    hg, wg, hd = pl.pallas_call(
        kernel,
        out_shape=(
            jax.ShapeDtypeStruct((128, D), BF16),
            jax.ShapeDtypeStruct((10, 2856), F32),
            jax.ShapeDtypeStruct((8, 128), F32),
        ),
        in_specs=[anyspace, anyspace, anyspace, vmem, vmem, vmem],
        out_specs=(anyspace, anyspace, anyspace),
        scratch_shapes=scratch(),
        compiler_params=pltpu.CompilerParams(has_side_effects=True, collective_id=0, vmem_limit_bytes=64000000),
    )(hidden[0], output_grad[0], input_weight, step_bias[None], decay_log[None], skip_gain[None])
    hg, wg, hd = pl.pallas_call(
        emit,
        out_shape=(
            jax.ShapeDtypeStruct((128, D), BF16),
            jax.ShapeDtypeStruct((10, 2856), F32),
            jax.ShapeDtypeStruct((3, HEADS), F32),
        ),
        in_specs=[vmem, vmem, vmem],
        out_specs=(vmem, vmem, vmem),
    )(hg, wg, hd)
    return (hg[None], wg, hd)


def solution(mesh):
    torus = Mesh(
        mesh.devices.reshape(4, 2, 2, 4, 2), ("seq_0", "seq_1", "seq_2", "zero_0", "zero_1")
    )
    in_specs = (P(ZERO, SEQ, None), P(ZERO, SEQ, None), P(ZERO, None), P(), P(), P())
    out_specs = (P(ZERO, SEQ, None), P(SEQ_ZERO, None), P())
    return jax.shard_map(body, mesh=torus, in_specs=in_specs, out_specs=out_specs, check_vma=False)
```

```python
import functools

import jax
import jax.numpy as jnp
from jax import lax
from jax.experimental import pallas as pl
from jax.experimental.pallas import tpu as pltpu
from jax.sharding import Mesh
from jax.sharding import PartitionSpec as P

HEADS = 40
STATE = 128
INNER = 2560
D = 1280
COLS = 640
ZERO = ("zero_0", "zero_1")
SEQ = ("seq_0", "seq_1", "seq_2")
SEQ_ZERO = ("seq_0", "seq_1", "seq_2", "zero_0", "zero_1")
MESH = pl.DeviceIdType.MESH
F32 = jnp.float32
BF16 = jnp.bfloat16
highest = lax.Precision.HIGHEST
NN = (((1,), (0,)), ((), ()))
NT = (((1,), (1,)), ((), ()))
TN = (((0,), (0,)), ((), ()))


def mm(a, b, dims=NN, precision=None):
    return lax.dot_general(a, b, dims, preferred_element_type=F32, precision=precision)


def parts(v, count):
    out = []
    for _ in range(count):
        out.append(v.astype(BF16))
        v = v - out[-1].astype(F32)
    return out


def mm3(a, b, dims=NN):
    (ah, al), (bh, bl) = parts(a, 2), parts(b, 2)
    (ka,), (kb,) = dims[0]
    return mm(jnp.concatenate([ah, al, ah], axis=ka), jnp.concatenate([bh, bh, bl], axis=kb), dims)


def ds(start, size, align=None):
    return pl.ds(pl.multiple_of(start, align or size), size)


def silu_grad(v):
    sig = jax.nn.sigmoid(v)
    return sig * (1.0 + v * (1.0 - sig))


def kernel(
    hid_ref, cot_ref, w_ref, bias_ref, decay_ref, skip_ref,
    hg_ref, wg_ref, hd_ref,
    hidf, hidt, hidx, cot, wraw, wf, projs, projv, bmf, cmf, lgd, cums, cumt, stp, gs, gts, dgs,
    sexp, ecs, tls, vv, xb, xt, oe, tot,
    sl, dl, stt, tts, str_, ttr, q1s, dxin, dbf, dcf, sb, db, dd, red,
    rr, t1s, t1r, hgp, hgs, hgr,
    dwa, sa1, ra1, sa2, ra2, sa3, ra3, sa4, ra4, sda, rda,
    dwb, sb1, rb1, sb2, rb2, sb3, rb3, sb4, rb4, sdb, rdb,
    dwc, sc1, rc1, sc2, rc2, sc3, rc3, sc4, rc4, sdc, rdc,
    dwd, sd1, rd1, sd2, rd2, sd3, rd3, sd4, rd4, sdd, rdd,
    heads_y, heads_x, heads_z, heads_g, hgo, wgo, hdo,
    ss, rs, ls,
):
    y, zl, c = (lax.axis_index(n) for n in SEQ)
    x, zh = (lax.axis_index(n) for n in ZERO)
    r = zl * 2 + c
    a = lax.rem(zl + zh, 2)
    g = a * 2 + c

    def send(i, src, dst, where, group):
        copy = pltpu.make_async_remote_copy(
            src_ref=src, dst_ref=dst, send_sem=ss.at[group], recv_sem=rs.at[i],
            device_id=where, device_id_type=MESH,
        )
        copy.start()
        return copy

    def bytes_of(ref, i=0, group=0):
        return pltpu.make_async_remote_copy(
            src_ref=ref, dst_ref=ref, send_sem=ss.at[group], recv_sem=rs.at[i],
            device_id={"seq_2": 1 - c}, device_id_type=MESH,
        )

    def got(i, ref):
        bytes_of(ref, i=i).wait_recv()

    def sent(group, ref):
        bytes_of(ref, group=group).wait_send()

    def rank(k):
        zlk = lax.rem(zl + k // 2, 2)
        ck = lax.rem(c + k % 2, 2)
        return zlk, ck, {"seq_1": zlk, "seq_2": ck}

    def xdev(k):
        return {"zero_0": lax.rem(x + k + 4, 4)}

    def ydev(k):
        return {"seq_0": lax.rem(y + k + 4, 4)}

    zpair = {"seq_1": 1 - zl, "zero_1": 1 - zh}
    core = {"seq_2": 1 - c}
    here_id = ds(r * 128, 128)

    def shard(xk, zk, lo=0, size=160):
        return ds((lax.rem(xk + 4, 4) * 2 + zk) * 160 + lo, size, 16)

    own = shard(x, zh)
    lane0 = 640 + 256 * c
    local = [
        pltpu.make_async_copy(w_ref, wraw, ls.at[0]),
        pltpu.make_async_copy(w_ref.at[:, ds(g * COLS, COLS, 128)], wf.at[own, 0:640], ls.at[1]),
        pltpu.make_async_copy(w_ref.at[:, ds(2560 + 128 * c, 128)], wf.at[own, ds(lane0, 128)], ls.at[2]),
        pltpu.make_async_copy(hid_ref, hidf.at[here_id, :], ls.at[3]),
        pltpu.make_async_copy(cot_ref.at[:, ds(g * COLS, COLS, 128)], cot.at[here_id, :], ls.at[4]),
    ]
    for copy in local:
        copy.start()

    barrier = pltpu.get_barrier_semaphore()

    def greet(dev):
        pl.semaphore_signal(barrier, inc=1, device_id=dev, device_id_type=MESH)

    greet(zpair)
    for k in (1, 2, 3):
        greet(xdev(k))
        greet(ydev(k))
        greet(rank(k)[2])
    coli = lax.broadcasted_iota(jnp.int32, (128, 128), 1)
    rowi = lax.broadcasted_iota(jnp.int32, (128, 128), 0)
    local[0].wait()
    tail = jnp.concatenate([wraw[:, 2816:2856].astype(F32), jnp.zeros((160, 88), F32)], axis=1)
    tail = pltpu.roll(tail, lax.rem(128 - 10 * g, 128), 1)
    keep10 = lax.broadcasted_iota(jnp.int32, (160, 128), 1) < 10
    wf[own, 768:896] = jnp.where(keep10, tail, 0.0).astype(BF16)

    def lanes10(ref):
        full = jnp.concatenate([ref[...], jnp.zeros((1, 88), F32)], axis=1)
        return pltpu.roll(jnp.broadcast_to(full, (8, 128)), lax.rem(128 - 10 * g, 128), 1)[0:1, :]

    bias = lanes10(bias_ref)
    neg = -jnp.exp(lanes10(decay_ref))
    skip = lanes10(skip_ref)
    for copy in local[1:]:
        copy.wait()
    pl.semaphore_wait(barrier, 10)

    def cols(m):
        return (ds(640 + 128 * c, 256, 128), slice(0, 256), slice(256, 512), slice(512, 640))[m]

    w = {}

    def wsend(m, i, rows, dev):
        ref = wf.at[rows, cols(m)]
        slot = min(i, 5) if m < 2 else {1: 1, 2: 2, 5: 3, 6: 4}.get(i, 5)
        w[m, i] = send(6 * m + slot, ref, ref, dev, m)

    def w_own_x(m):
        wsend(m, 1, own, xdev(1))
        wsend(m, 2, own, xdev(-1))

    def w_own_z(m):
        wsend(m, 0, own, zpair)

    def w_other(m):
        w[m, 0].wait_recv()
        wsend(m, 3, shard(x, 1 - zh), xdev(1))
        wsend(m, 4, shard(x, 1 - zh), xdev(-1))

    def w_forward(m):
        w[m, 1].wait_recv()
        wsend(m, 5, shard(x - 1, zh, 0, 80), xdev(1))
        w[m, 2].wait_recv()
        wsend(m, 6, shard(x + 1, zh, 80, 80), xdev(-1))

    def w_forward_other(m):
        w[m, 3].wait_recv()
        wsend(m, 7, shard(x - 1, 1 - zh, 0, 80), xdev(1))
        w[m, 4].wait_recv()
        wsend(m, 8, shard(x + 1, 1 - zh, 80, 80), xdev(-1))

    def w_across(m):
        wsend(m, 3, shard(x - 1, zh), zpair)
        wsend(m, 4, shard(x + 1, zh), zpair)

    def w_across_far(m):
        w[m, 5].wait_recv()
        wsend(m, 7, shard(x + 2, zh, 0, 80), zpair)
        w[m, 6].wait_recv()
        wsend(m, 8, shard(x + 2, zh, 80, 80), zpair)

    def w_done(m):
        got(6 * m + 5, wf.at[0 : 320 if m < 2 else 640, cols(m)])

    def hand(k):
        ref = wf.at[ds(lax.rem(x + k + 4, 4) * 320, 320), ds(lane0, 128)]
        send(28, ref, ref, core, 6)

    w_own_z(0)
    w_own_x(0)
    h_z = send(24, hid_ref, hidf.at[here_id, :], rank(2)[2], 4)
    w_own_x(2)
    w_own_z(1)
    h_c = send(25, hid_ref, hidf.at[here_id, :], core, 4)
    for k in (2, 3, 1):
        zlk, ck, dev = rank(k)
        gk = lax.rem(zlk + zh, 2) * 2 + ck
        send(27, cot_ref.at[:, ds(gk * COLS, COLS, 128)], cot.at[here_id, :], dev, 5)
    w_own_z(2)
    w_own_z(3)
    w_other(0)
    w_forward(0)
    w_forward(2)
    w_across(2)
    w_own_x(3)
    w_forward_other(0)
    w_own_x(1)
    for k in (-1, 0, 1):
        hand(k)
    h_z.wait_recv()
    zrows = ds((rank(2)[0] * 2 + c) * 128, 128)
    h_f = send(26, hidf.at[zrows, :], hidf.at[zrows, :], core, 4)
    w_across_far(2)
    w_forward(3)
    w_across(3)
    w_other(1)
    w_done(0)
    hand(2)
    h_c.wait_recv()
    h_f.wait_recv()

    low = coli < 64
    causal = rowi >= coli
    anti = rowi <= coli
    tri = causal.astype(F32).astype(BF16)
    tri3 = jnp.concatenate([tri] * 3, axis=1)
    upper = anti.astype(F32).astype(BF16)
    strict = (rowi > coli).astype(F32).astype(BF16)
    sums4 = jnp.concatenate([upper] * 3 + [strict] * 3, axis=1)

    def pair(v, j):
        return jnp.where(low[0 : v.shape[0]], v[:, 2 * j : 2 * j + 1], v[:, 2 * j + 1 : 2 * j + 2])

    def blocks(f, unroll=True):
        if unroll:
            for b in range(4):
                f(b, pl.ds(b * 128, 128))
        else:
            def step(b, carry):
                f(b, ds(b * 128, 128))
                return carry

            lax.fori_loop(0, 4, step, 0)

    def steps(b, rows):
        projs[rows, ds(128 * c, 256, 128)] = mm(hidf[rows, :], wf[:, ds(640 + 128 * c, 256, 128)])
        pre = projs[rows, 128:256] + bias
        step = jnp.maximum(pre, 0.0) + jnp.log1p(jnp.exp(-jnp.abs(pre)))
        lg = neg * step
        cum = mm(tri3, jnp.concatenate(parts(lg, 3), axis=0))
        stp[rows, :] = step
        lgd[rows, :] = lg
        cums[rows, :] = cum
        cumt[b] = cum.T[0:16, :]
        dgs[b] = jnp.zeros((128, 128), F32)
        red[b] = jnp.zeros((384, 128), F32)

    def maps(b, rows):
        projs[rows, ds(256 - 256 * c, 128)] = mm(hidf[rows, :], wf[:, ds(896 - 256 * c, 128)])
        bm = jax.nn.silu(projs[rows, 0:128])
        cm = jax.nn.silu(projs[rows, 256:384])
        bmf[rows, :] = bm
        cmf[rows, :] = cm
        scores = mm3(cm, bm, NT)
        gs[b] = scores
        gts[b] = scores.T

    blocks(steps)
    for j in range(5):
        cj = slice(128 * j, 128 * j + 128)
        for b in range(4):
            last_row = cums[128 * b + 127 : 128 * b + 128, :]
            tot[8 * b : 8 * b + 8, cj] = pair(jnp.broadcast_to(last_row, (8, 128)), j)
    tts[...] = tot[0:8, :] + tot[8:16, :] + tot[16:24, :] + tot[24:32, :]
    for k in (1, 2, 3):
        send(29, tts, ttr.at[k - 1], ydev(k), 7)

    i320 = lax.broadcasted_iota(jnp.int32, (320, 320), 0)
    k320 = lax.broadcasted_iota(jnp.int32, (320, 320), 1)
    tens = lax.shift_right_logical(i320 * 6554, 16)
    source = ((tens & 3) * 8 + lax.shift_right_logical(tens, 2)) * 10 + i320 - tens * 10
    perm = jnp.where(k320 == source, 1.0, 0.0).astype(F32).astype(BF16)
    for q in range(4):
        hidt[320 * q : 320 * q + 320, :] = mm(perm, hidf[:, 320 * q : 320 * q + 320], NT).astype(BF16)
    w_forward(1)
    got(28, wf.at[:, ds(896 - 256 * c, 128)])
    maps(0, pl.ds(0, 128))
    w_across_far(3)
    maps(1, pl.ds(128, 128))
    maps(2, pl.ds(256, 128))
    w_forward_other(1)
    maps(3, pl.ds(384, 128))

    def total(b, cj):
        return tot[8 * b : 8 * b + 1, cj]

    def pair_forward(j):
        cj = slice(128 * j, 128 * j + 128)

        wide = slice(128 * j, min(128 * j + 256, 640))

        def project(b, rows):
            projv[rows, wide] = mm(hidf[rows, :], wf[:, wide])

        def local_part(b, rows):
            ce = pair(cums[rows, :], j)
            se = pair(stp[rows, :], j)
            ec = jnp.exp(ce)
            tl = jnp.exp(ce[127:128, :] - ce)
            val = jax.nn.silu(projv[rows, cj])
            xs = val * se
            sexp[rows, cj] = se
            ecs[rows, cj] = ec
            tls[rows, cj] = tl
            vv[rows, cj] = val
            xb[rows, cj] = xs.astype(BF16)
            x16 = (xs * tl).astype(BF16)
            o16 = (cot[rows, cj].astype(F32) * ec).astype(BF16)
            xt[rows, cj] = x16
            oe[rows, cj] = o16
            sl[b, :, cj] = mm(bmf[rows, :].astype(BF16), x16, TN)
            dl[b, :, cj] = mm(cmf[rows, :].astype(BF16), o16, TN)

        if j % 2 == 0:
            blocks(project)
        blocks(local_part)
        s = sl[0, :, cj]
        d = dl[3, :, cj]
        for b in range(1, 4):
            s = jnp.exp(total(b, cj)) * s + sl[b, :, cj]
            d = jnp.exp(total(3 - b, cj)) * d + dl[3 - b, :, cj]
        stt[0, :, cj] = s.astype(BF16)
        stt[1, :, cj] = d.astype(BF16)
        for k in (1, 2, 3):
            wraps = lax.div(y + k, 4)
            send(30 + j, stt.at[wraps, :, cj], str_.at[k - 1, :, cj], ydev(k), 8)

    def pair_inside(j):
        cj = slice(128 * j, 128 * j + 128)

        def inside(b, rows):
            cum = cums[rows, :]
            c0, c1 = cum[:, 2 * j : 2 * j + 1], cum[:, 2 * j + 1 : 2 * j + 2]
            r0, r1 = cumt[b, 2 * j : 2 * j + 1, :], cumt[b, 2 * j + 1 : 2 * j + 2, :]
            w0 = jnp.where(causal, jnp.exp(jnp.where(causal, c0 - r0, 0.0)), 0.0)
            w1 = jnp.where(causal, jnp.exp(jnp.where(causal, c1 - r1, 0.0)), 0.0)
            u0 = jnp.where(anti, jnp.exp(jnp.where(anti, r0 - c0, 0.0)), 0.0)
            u1 = jnp.where(anti, jnp.exp(jnp.where(anti, r1 - c1, 0.0)), 0.0)
            scores, scores_t = gs[b], gts[b]
            m = jnp.concatenate([scores * w0, scores * w1], axis=1).astype(BF16)
            mt = jnp.concatenate([scores_t * u0, scores_t * u1], axis=1).astype(BF16)
            x16 = xb[rows, cj]
            o16 = cot[rows, cj]
            zero = jnp.zeros_like(x16)
            xd = jnp.concatenate([jnp.where(low, x16, zero), jnp.where(low, zero, x16)], axis=0)
            od = jnp.concatenate([jnp.where(low, o16, zero), jnp.where(low, zero, o16)], axis=0)
            yy = mm(m, xd)
            pp = mm(o16, xd, NT)
            dx = mm(mt, od)
            dgs[b] = dgs[b] + w0 * pp[:, 0:128] + w1 * pp[:, 128:256]
            dxin[rows, cj] = dx
            q1s[rows, cj] = o16.astype(F32) * yy - x16.astype(F32) * dx

        blocks(inside)

    got(27, cot.at[0:384, :])
    w_done(2)
    pair_forward(2)
    pair_inside(2)
    pair_forward(3)
    pair_inside(3)
    w_done(3)
    pair_forward(4)
    pair_inside(4)
    for p in range(4):
        for q in range(4):
            hidx[320 * p + 80 * q : 320 * p + 80 * q + 80, :] = hidt[320 * q + 80 * p : 320 * q + 80 * p + 80, :]
    w_done(1)
    pair_forward(0)
    pair_inside(0)
    pair_forward(1)
    pair_inside(1)

    def turn(b, rows):
        dcf[rows, :] = mm3(dgs[b], bmf[rows, :], NN) + mm(oe[rows, :], sb[b], NT)
        dbf[rows, :] = mm3(dgs[b], cmf[rows, :], TN) + mm(xt[rows, :], db[b], NT)

    got(29, ttr)

    lanes = lax.broadcasted_iota(jnp.int32, (256, 128), 0)
    outl = lax.broadcasted_iota(jnp.int32, (256, 128), 1)

    def sums(z, j):
        hi = z.astype(BF16)
        lo = (z - hi.astype(F32)).astype(BF16)
        choose = (outl == 2 * j + lax.rem(lax.div(lanes, 64), 2)).astype(F32).astype(BF16)
        return mm(jnp.concatenate([hi, lo], axis=1), choose)

    yes = [jnp.where(y >= k, 1.0, 0.0).astype(F32) for k in (1, 2, 3)]
    no = [jnp.where(y + k <= 3, 1.0, 0.0).astype(F32) for k in (1, 2, 3)]
    inner = [jnp.zeros((8, 128), F32) for _ in range(4)]
    gain = [jnp.zeros((8, 128), F32)]

    def pair_outside(j):
        cj = slice(128 * j, 128 * j + 128)
        got(30 + j, str_.at[:, :, cj])
        t = [ttr[k, 0:1, cj] for k in range(3)]
        came = [str_[k, :, cj].astype(F32) for k in range(3)]
        s = yes[0] * came[0] + (yes[1] * jnp.exp(t[0])) * came[1] + (yes[2] * jnp.exp(t[0] + t[1])) * came[2]
        d = no[0] * came[2] + (no[1] * jnp.exp(t[2])) * came[1] + (no[2] * jnp.exp(t[2] + t[1])) * came[0]
        for b in (3, 2, 1, 0):
            db[b, :, cj] = d.astype(BF16)
            dd[b] = d
            d = jnp.exp(total(b, cj)) * d + dl[b, :, cj]
        for b in range(4):
            sb[b, :, cj] = s.astype(BF16)
            grown = jnp.exp(total(b, cj)) * s
            inner[b] = inner[b] + sums((grown * dd[b]).reshape(16, 8, 128).sum(axis=0), j)
            s = grown + sl[b, :, cj]

        def outside(b, rows):
            o = cot[rows, cj].astype(F32)
            yst = mm(cmf[rows, :].astype(BF16), sb[b, :, cj]) * ecs[rows, cj]
            dxst = mm(bmf[rows, :].astype(BF16), db[b, :, cj]) * tls[rows, cj]
            val = vv[rows, cj]
            dxs = dxin[rows, cj] + dxst
            z = jnp.concatenate([q1s[rows, cj] + o * yst, xb[rows, cj].astype(F32) * dxst, dxs * val], axis=0)
            red[b] = red[b] + sums(z, j)
            dval = dxs * sexp[rows, cj] + pair(skip, j) * o
            rr[rows, cj] = (dval * silu_grad(projv[rows, cj])).astype(BF16)
            gain[0] = gain[0] + sums((o * val).reshape(16, 8, 128).sum(axis=0), j)

        blocks(outside)

    class Stream:
        def __init__(self, base, group, parts, kind, bufs):
            self.base, self.group, self.parts, self.left = base, group, parts, hidx if kind else hidt
            self.dw, self.s1, self.r1, self.s2, self.r2, self.s3, self.r3, self.s4, self.r4, self.sd, self.rd = bufs
            self.index, self.dev, self.index2, self.dev2 = (y, ydev, x, xdev) if kind == 0 else (x, xdev, y, ydev)

        def send(self, i, src, dst, dev):
            return send(self.base + i, src, dst, dev, self.group)

        def block(self, i):
            rows = ds(lax.rem(self.index + i, 4) * 320, 320)
            for cols, target in self.parts:
                self.dw[rows, target] = mm(self.left[rows, :], rr[:, cols])
            return rows

        def first(self):
            rows = self.block(2)
            self.s1[...] = self.dw[rows, :].astype(BF16)
            self.one = (
                self.send(0, self.s1.at[0:160, :], self.r1.at[0], self.dev(1)),
                self.send(1, self.s1.at[160:320, :], self.r1.at[1], self.dev(-1)),
            )

        def rest(self):
            for i in (1, 3, 0):
                self.block(i)

        def second(self):
            nxt = lax.rem(self.index + 1, 4) * 320
            prv = lax.rem(self.index + 3, 4) * 320
            self.one[0].wait_recv()
            self.s2[0, 0:160, :] = (self.dw[ds(nxt, 160), :] + self.r1[0].astype(F32)).astype(BF16)
            self.s2[0, 160:320, :] = self.dw[ds(nxt + 160, 160), :].astype(BF16)
            self.send(2, self.s2.at[0], self.r2.at[0], self.dev(1))
            self.one[1].wait_recv()
            self.s2[1, 0:160, :] = self.dw[ds(prv, 160), :].astype(BF16)
            self.s2[1, 160:320, :] = (self.dw[ds(prv + 160, 160), :] + self.r1[1].astype(F32)).astype(BF16)
            self.send(2, self.s2.at[1], self.r2.at[1], self.dev(-1))

        def third(self):
            got(self.base + 2, self.r2)
            here = ds(self.index * 320, 320)
            summed = self.dw[here, :] + self.r2[0].astype(F32) + self.r2[1].astype(F32)
            self.dw[here, :] = summed
            self.s3[...] = summed.astype(BF16)
            for k in (2, 1, 3):
                piece = self.s3.at[ds(lax.rem(self.index2 + k, 4) * 80, 80), :]
                self.send(3, piece, self.r3.at[k - 1], self.dev2(k))

        def fourth(self):
            got(self.base + 3, self.r3)
            rows = ds(self.index * 320 + self.index2 * 80, 80)
            self.s4[...] = self.dw[rows, :] + self.r3[0].astype(F32) + self.r3[1].astype(F32) + self.r3[2].astype(F32)
            self.four = self.send(4, self.s4.at[ds((1 - zh) * 40, 40), :], self.r4, zpair)

        def owners(self):
            self.four.wait_recv()
            chunk = self.s4[ds(zh * 40, 40), :] + self.r4[...]
            for i in range(4):
                self.sd[i, 0:10, :] = chunk[10 * i : 10 * i + 10, :]
            self.rd[g] = self.sd[r]
            for k in (2, 3, 1):
                zlk, ck, dev = rank(k)
                self.send(5, self.sd.at[zlk * 2 + ck], self.rd.at[g], dev)

        def finish(self):
            got(self.base + 5, self.rd.at[0:3])

        def close(self):
            sent(self.group, self.dw.at[0:688, :])

    alpha = Stream(46, 13, [(slice(256, 640), slice(0, 384))], 0, (dwa, sa1, ra1, sa2, ra2, sa3, ra3, sa4, ra4, sda, rda))
    beta = Stream(52, 14, [(slice(0, 256), slice(0, 256))], 1, (dwb, sb1, rb1, sb2, rb2, sb3, rb3, sb4, rb4, sdb, rdb))
    gamma = Stream(58, 15, [(ds(lane0, 128), slice(0, 128))], 0, (dwc, sc1, rc1, sc2, rc2, sc3, rc3, sc4, rc4, sdc, rdc))
    delta = Stream(64, 16, [(slice(768, 896), slice(0, 128))], 1, (dwd, sd1, rd1, sd2, rd2, sd3, rd3, sd4, rd4, sdd, rdd))

    pair_outside(2)
    pair_outside(3)
    pair_outside(4)
    alpha.first()
    pair_outside(0)
    pair_outside(1)
    beta.first()

    blocks(turn)
    first = c == 0
    t1s[...] = jnp.where(first, dcf[...], dbf[...])
    t1 = send(35, t1s, t1r, core, 9)
    alpha.rest()
    alpha.second()

    ownl = coli < 10
    bias_sum = decay_sum = jnp.zeros((8, 128), F32)
    for b in range(4):
        rows = slice(128 * b, 128 * b + 128)
        dlog = mm(sums4, jnp.concatenate(parts(red[b, 0:128], 3) + parts(red[b, 128:256], 3), axis=0))
        dlog = jnp.where(ownl, dlog + inner[b].sum(axis=0, keepdims=True), 0.0)
        ddt = (red[b, 256:384] + neg * dlog) * jax.nn.sigmoid(projs[rows, 128:256] + bias)
        ddt = jnp.where(ownl, ddt, 0.0)
        rr[rows, 768:896] = ddt.astype(BF16)
        bias_sum = bias_sum + ddt.reshape(16, 8, 128).sum(axis=0)
        decay_sum = decay_sum + (dlog * lgd[rows, :]).reshape(16, 8, 128).sum(axis=0)
    place = jnp.where(jnp.logical_and(rowi < 10, coli == rowi + 10 * g), 1.0, 0.0).astype(F32)
    delta.first()
    row8 = lax.broadcasted_iota(jnp.int32, (8, 128), 0)
    packed = jnp.where(
        row8 == 0, bias_sum.sum(axis=0, keepdims=True),
        jnp.where(row8 == 1, decay_sum.sum(axis=0, keepdims=True),
                  jnp.where(row8 == 2, gain[0].sum(axis=0, keepdims=True), 0.0)),
    )
    heads_y[y] = mm(packed, place, NN, highest)
    for k in (1, 2, 3):
        send(38, heads_y.at[y], heads_y.at[y], ydev(k), 10)
    t1.wait_recv()
    mixed = jnp.where(first, dbf[...], dcf[...]) + t1r[...]
    rr[:, ds(lane0, 128)] = (mixed * silu_grad(projs[:, ds(256 * c, 128, 128)])).astype(BF16)
    rr[:, ds(896 - 256 * c, 128)] = jnp.zeros((512, 128), BF16)
    gamma.first()
    beta.rest()
    beta.second()
    delta.rest()
    gamma.rest()
    for n in range(5):
        part = slice(256 * n, 256 * n + 256)
        hgp[:, part] = mm(rr[...], wf[part, :], NT)
    mate_row = ds((zl * 2 + 1 - c) * 128, 128)
    far_mate = ds(((1 - zl) * 2 + 1 - c) * 128, 128)
    far_row = ds(((1 - zl) * 2 + c) * 128, 128)
    hgs[1] = hgp[far_mate, :].astype(BF16)
    hg_far = send(43, hgs.at[1], hgr.at[1], core, 11)
    hgs[0] = hgp[mate_row, :].astype(BF16)
    hg_near = send(42, hgs.at[0], hgr.at[0], core, 11)
    delta.second()
    hg_far.wait_recv()
    hgs[2] = (hgp[far_row, :] + hgr[1].astype(F32)).astype(BF16)
    hg_z = send(44, hgs.at[2], hgr.at[2], rank(2)[2], 11)
    alpha.third()
    beta.third()
    gamma.second()
    delta.third()
    got(38, heads_y.at[0:3])
    heads_x[x] = (heads_y[0] + heads_y[1]) + (heads_y[2] + heads_y[3])
    for k in (1, 2, 3):
        send(39, heads_x.at[x], heads_x.at[x], xdev(k), 10)
    beta.fourth()
    alpha.fourth()
    gamma.third()
    got(39, heads_x.at[0:3])
    heads_z[zh] = (heads_x[0] + heads_x[1]) + (heads_x[2] + heads_x[3])
    head_z = send(40, heads_z.at[zh], heads_z.at[zh], zpair, 10)
    delta.fourth()
    beta.owners()
    alpha.owners()
    gamma.fourth()
    delta.owners()
    hg_near.wait_recv()
    hg_z.wait_recv()
    hgo[...] = (hgp[here_id, :] + hgr[0].astype(F32) + hgr[2].astype(F32)).astype(BF16)
    hg_out = pltpu.make_async_copy(hgo, hg_ref, ls.at[5])
    hg_out.start()
    head_z.wait_recv()
    heads_g[r] = heads_z[0] + heads_z[1]
    for k in (1, 2, 3):
        send(41, heads_g.at[r], heads_g.at[r], rank(k)[2], 10)
    beta.finish()
    for k in range(4):
        wgo[:, 640 * k : 640 * k + 256] = rdb[k, 0:10, :]
    gamma.owners()
    alpha.finish()
    for k in range(4):
        wgo[:, 640 * k + 256 : 640 * k + 640] = rda[k, 0:10, :]
    got(41, heads_g.at[0:3])
    hdo[...] = (heads_g[0] + heads_g[1]) + (heads_g[2] + heads_g[3])
    hd_out = pltpu.make_async_copy(hdo, hd_ref, ls.at[6])
    hd_out.start()
    delta.finish()
    for k in range(4):
        wgo[:, 2816 + 10 * k : 2826 + 10 * k] = rdd[k, 0:10, 0:10]
    gamma.finish()
    wgo[:, 2560:2688] = rdc[0, 0:10, :] + rdc[2, 0:10, :]
    wgo[:, 2688:2816] = rdc[1, 0:10, :] + rdc[3, 0:10, :]
    wg_out = pltpu.make_async_copy(wgo, wg_ref, ls.at[7])
    wg_out.start()
    for m in range(4):
        sent(m, wf.at[0:1120, cols(m)])
    sent(4, hidf.at[0:384, :])
    sent(5, cot.at[0:384, :])
    sent(6, wf.at[:, ds(lane0, 128)])
    sent(7, ttr)
    sent(8, str_)
    sent(9, t1r)
    sent(10, bmf.at[0:80, :])
    sent(11, hgs)
    for stream in (alpha, beta, gamma, delta):
        stream.close()
    hg_out.wait()
    hd_out.wait()
    wg_out.wait()


def scratch():
    def v(shape, dtype=F32):
        return pltpu.VMEM(shape, dtype)

    def stream(n):
        return [
            v((D, n)), v((320, n), BF16), v((2, 160, n), BF16), v((2, 320, n), BF16), v((2, 320, n), BF16),
            v((320, n), BF16), v((3, 80, n), BF16), v((80, n)), v((40, n)), v((4, 16, n)), v((4, 16, n)),
        ]

    wide, wide16 = v((512, COLS)), v((512, COLS), BF16)
    thin = v((512, 128))
    return [
        v((512, D), BF16), v((D, 512), BF16), v((D, 512), BF16), wide16, v((160, 2856), BF16), v((D, 1024), BF16),
        v((512, 384)), wide, thin, thin, thin, thin, v((4, 16, 128)), thin,
        v((4, 128, 128)), v((4, 128, 128)), v((4, 128, 128)),
        wide, wide, wide, wide, wide16, wide16, wide16, v((32, COLS)),
        v((4, 128, COLS)), v((4, 128, COLS)), v((2, 128, COLS), BF16), v((8, COLS)),
        v((3, 128, COLS), BF16), v((3, 8, COLS)), wide, wide, thin, thin,
        v((4, 128, COLS), BF16), v((4, 128, COLS), BF16), v((4, 128, 128)), v((4, 384, 128)),
        v((512, 1024), BF16), thin, thin,
        v((512, D)), v((3, 128, D), BF16), v((3, 128, D), BF16),
        *stream(384), *stream(256), *stream(128), *stream(128),
        v((4, 8, 128)), v((4, 8, 128)), v((2, 8, 128)), v((4, 8, 128)),
        v((128, D), BF16), v((10, 2856)), v((8, 128)),
        pltpu.SemaphoreType.DMA((17,)), pltpu.SemaphoreType.DMA((70,)), pltpu.SemaphoreType.DMA((8,)),
    ]


def emit(hg_ref, wg_ref, hd_ref, hg_out, wg_out, hd_out):
    hg_out[...] = hg_ref[...]
    wg_out[...] = wg_ref[...]
    hd_out[...] = hd_ref[0:3, 0:HEADS]


def body(hidden, output_grad, input_weight, step_bias, decay_log, skip_gain):
    anyspace = pl.BlockSpec(memory_space=pl.ANY)
    vmem = pl.BlockSpec(memory_space=pltpu.VMEM)
    hg, wg, hd = pl.pallas_call(
        kernel,
        out_shape=(
            jax.ShapeDtypeStruct((128, D), BF16),
            jax.ShapeDtypeStruct((10, 2856), F32),
            jax.ShapeDtypeStruct((8, 128), F32),
        ),
        in_specs=[anyspace, anyspace, anyspace, vmem, vmem, vmem],
        out_specs=(anyspace, anyspace, anyspace),
        scratch_shapes=scratch(),
        compiler_params=pltpu.CompilerParams(has_side_effects=True, collective_id=0, vmem_limit_bytes=64000000),
    )(hidden[0], output_grad[0], input_weight, step_bias[None], decay_log[None], skip_gain[None])
    hg, wg, hd = pl.pallas_call(
        emit,
        out_shape=(
            jax.ShapeDtypeStruct((128, D), BF16),
            jax.ShapeDtypeStruct((10, 2856), F32),
            jax.ShapeDtypeStruct((3, HEADS), F32),
        ),
        in_specs=[vmem, vmem, vmem],
        out_specs=(vmem, vmem, vmem),
    )(hg, wg, hd)
    return (hg[None], wg, hd)


def solution(mesh):
    torus = Mesh(
        mesh.devices.reshape(4, 2, 2, 4, 2), ("seq_0", "seq_1", "seq_2", "zero_0", "zero_1")
    )
    in_specs = (P(ZERO, SEQ, None), P(ZERO, SEQ, None), P(ZERO, None), P(), P(), P())
    out_specs = (P(ZERO, SEQ, None), P(SEQ_ZERO, None), P())
    return jax.shard_map(body, mesh=torus, in_specs=in_specs, out_specs=out_specs, check_vma=False)
```

```python
import functools

import jax
import jax.numpy as jnp
from jax import lax
from jax.experimental import pallas as pl
from jax.experimental.pallas import tpu as pltpu
from jax.sharding import Mesh
from jax.sharding import PartitionSpec as P

HEADS = 40
STATE = 128
INNER = 2560
D = 1280
COLS = 640
ZERO = ("zero_0", "zero_1")
SEQ = ("seq_0", "seq_1", "seq_2")
SEQ_ZERO = ("seq_0", "seq_1", "seq_2", "zero_0", "zero_1")
MESH = pl.DeviceIdType.MESH
F32 = jnp.float32
BF16 = jnp.bfloat16
highest = lax.Precision.HIGHEST
NN = (((1,), (0,)), ((), ()))
NT = (((1,), (1,)), ((), ()))
TN = (((0,), (0,)), ((), ()))


def mm(a, b, dims=NN, precision=None):
    return lax.dot_general(a, b, dims, preferred_element_type=F32, precision=precision)


def parts(v, count):
    out = []
    for _ in range(count):
        out.append(v.astype(BF16))
        v = v - out[-1].astype(F32)
    return out


def mm3(a, b, dims=NN):
    (ah, al), (bh, bl) = parts(a, 2), parts(b, 2)
    (ka,), (kb,) = dims[0]
    return mm(jnp.concatenate([ah, al, ah], axis=ka), jnp.concatenate([bh, bh, bl], axis=kb), dims)


def ds(start, size, align=None):
    return pl.ds(pl.multiple_of(start, align or size), size)


def silu_grad(v):
    sig = jax.nn.sigmoid(v)
    return sig * (1.0 + v * (1.0 - sig))


def kernel(
    hid_ref, cot_ref, w_ref, bias_ref, decay_ref, skip_ref,
    hg_ref, wg_ref, hd_ref,
    stepw, stepa, hidf, hidt, hidx, cot, wraw, wf, projs, projv, bmf, cmf, lgd, cums, cumt, stp, gs, gts, dgs,
    sexp, ecs, tls, vv, xb, xt, oe, tot,
    sl, dl, stt, tts, str_, ttr, q1s, dxin, dbf, dcf, sb, db, dd, red,
    rr, t1s, t1r, hgp, hgs, hgr,
    dwa, sa1, ra1, sa2, ra2, sa3, ra3, sa4, ra4, sda, rda,
    dwb, sb1, rb1, sb2, rb2, sb3, rb3, sb4, rb4, sdb, rdb,
    dwc, sc1, rc1, sc2, rc2, sc3, rc3, sc4, rc4, sdc, rdc,
    dwd, sd1, rd1, sd2, rd2, sd3, rd3, sd4, rd4, sdd, rdd,
    heads_y, heads_x, heads_z, heads_g, hgo, wgo, hdo,
    ss, rs, ls,
):
    y, zl, c = (lax.axis_index(n) for n in SEQ)
    x, zh = (lax.axis_index(n) for n in ZERO)
    r = zl * 2 + c
    a = lax.rem(zl + zh, 2)
    g = a * 2 + c

    def send(i, src, dst, where, group):
        copy = pltpu.make_async_remote_copy(
            src_ref=src, dst_ref=dst, send_sem=ss.at[group], recv_sem=rs.at[i],
            device_id=where, device_id_type=MESH,
        )
        copy.start()
        return copy

    def bytes_of(ref, i=0, group=0):
        return pltpu.make_async_remote_copy(
            src_ref=ref, dst_ref=ref, send_sem=ss.at[group], recv_sem=rs.at[i],
            device_id={"seq_2": 1 - c}, device_id_type=MESH,
        )

    def got(i, ref):
        bytes_of(ref, i=i).wait_recv()

    def sent(group, ref):
        bytes_of(ref, group=group).wait_send()

    def rank(k):
        zlk = lax.rem(zl + k // 2, 2)
        ck = lax.rem(c + k % 2, 2)
        return zlk, ck, {"seq_1": zlk, "seq_2": ck}

    def xdev(k):
        return {"zero_0": lax.rem(x + k + 4, 4)}

    def ydev(k):
        return {"seq_0": lax.rem(y + k + 4, 4)}

    zpair = {"seq_1": 1 - zl, "zero_1": 1 - zh}
    core = {"seq_2": 1 - c}
    here_id = ds(r * 128, 128)

    def shard(xk, zk, lo=0, size=160):
        return ds((lax.rem(xk + 4, 4) * 2 + zk) * 160 + lo, size, 16)

    own = shard(x, zh)
    lane0 = 640 + 256 * c
    local = [
        pltpu.make_async_copy(w_ref, wraw, ls.at[0]),
        pltpu.make_async_copy(w_ref.at[:, ds(g * COLS, COLS, 128)], wf.at[own, 0:640], ls.at[1]),
        pltpu.make_async_copy(w_ref.at[:, ds(2560 + 128 * c, 128)], wf.at[own, ds(lane0, 128)], ls.at[2]),
        pltpu.make_async_copy(hid_ref, hidf.at[here_id, :], ls.at[3]),
        pltpu.make_async_copy(cot_ref.at[:, ds(g * COLS, COLS, 128)], cot.at[here_id, :], ls.at[4]),
    ]
    for copy in local:
        copy.start()

    barrier = pltpu.get_barrier_semaphore()

    def greet(dev):
        pl.semaphore_signal(barrier, inc=1, device_id=dev, device_id_type=MESH)

    greet(zpair)
    for k in (1, 2, 3):
        greet(xdev(k))
        greet(ydev(k))
        greet(rank(k)[2])
    coli = lax.broadcasted_iota(jnp.int32, (128, 128), 1)
    rowi = lax.broadcasted_iota(jnp.int32, (128, 128), 0)
    local[0].wait()
    stepa[...] = jnp.zeros_like(stepa)
    tail = jnp.concatenate([wraw[:, 2816:2856].astype(F32), jnp.zeros((160, 88), F32)], axis=1)
    tail = pltpu.roll(tail, lax.rem(128 - 10 * g, 128), 1)
    keep10 = lax.broadcasted_iota(jnp.int32, (160, 128), 1) < 10
    tail = jnp.concatenate([jnp.where(keep10, tail, 0.0), jnp.zeros((96, 128), F32)], axis=0)
    stepw[x * 2 + zh] = tail.T[0:16, :].astype(BF16)

    def lanes10(ref):
        full = jnp.concatenate([ref[...], jnp.zeros((1, 88), F32)], axis=1)
        return pltpu.roll(jnp.broadcast_to(full, (8, 128)), lax.rem(128 - 10 * g, 128), 1)[0:1, :]

    bias = lanes10(bias_ref)
    neg = -jnp.exp(lanes10(decay_ref))
    skip = lanes10(skip_ref)
    for copy in local[1:]:
        copy.wait()
    pl.semaphore_wait(barrier, 10)

    def cols(m):
        return (ds(lane0, 128), slice(0, 256), slice(256, 512), slice(512, 640))[m]

    w = {}

    def wsend(m, i, rows, dev):
        ref = wf.at[rows, cols(m)]
        slot = min(i, 5) if m < 2 else {1: 1, 2: 2, 5: 3, 6: 4}.get(i, 5)
        w[m, i] = send(6 * m + slot, ref, ref, dev, m)

    def w_own_x(m):
        wsend(m, 1, own, xdev(1))
        wsend(m, 2, own, xdev(-1))

    def w_own_z(m):
        wsend(m, 0, own, zpair)

    def w_other(m):
        w[m, 0].wait_recv()
        wsend(m, 3, shard(x, 1 - zh), xdev(1))
        wsend(m, 4, shard(x, 1 - zh), xdev(-1))

    def w_forward(m):
        w[m, 1].wait_recv()
        wsend(m, 5, shard(x - 1, zh, 0, 80), xdev(1))
        w[m, 2].wait_recv()
        wsend(m, 6, shard(x + 1, zh, 80, 80), xdev(-1))

    def w_forward_other(m):
        w[m, 3].wait_recv()
        wsend(m, 7, shard(x - 1, 1 - zh, 0, 80), xdev(1))
        w[m, 4].wait_recv()
        wsend(m, 8, shard(x + 1, 1 - zh, 80, 80), xdev(-1))

    def w_across(m):
        wsend(m, 3, shard(x - 1, zh), zpair)
        wsend(m, 4, shard(x + 1, zh), zpair)

    def w_across_far(m):
        w[m, 5].wait_recv()
        wsend(m, 7, shard(x + 2, zh, 0, 80), zpair)
        w[m, 6].wait_recv()
        wsend(m, 8, shard(x + 2, zh, 80, 80), zpair)

    def w_done(m):
        got(6 * m + 5, wf.at[0 : 320 if m < 2 else 640, cols(m)])

    def step_send(i, xk, zk, dev):
        ref = stepw.at[lax.rem(x + xk + 4, 4) * 2 + zk]
        return send(i, ref, ref, dev, 17)

    def hand(k):
        ref = wf.at[ds(lax.rem(x + k + 4, 4) * 320, 320), ds(lane0, 128)]
        send(28, ref, ref, core, 6)

    step_z = step_send(70, 0, zh, zpair)
    step_x = [step_send(71, 0, zh, xdev(1)), step_send(72, 0, zh, xdev(-1))]
    w_own_z(0)
    w_own_x(0)
    h_z = send(24, hid_ref, hidf.at[here_id, :], rank(2)[2], 4)
    w_own_x(2)
    w_own_z(1)
    h_c = send(25, hid_ref, hidf.at[here_id, :], core, 4)
    for k in (2, 3, 1):
        zlk, ck, dev = rank(k)
        gk = lax.rem(zlk + zh, 2) * 2 + ck
        send(27, cot_ref.at[:, ds(gk * COLS, COLS, 128)], cot.at[here_id, :], dev, 5)
    w_own_z(2)
    w_own_z(3)
    step_z.wait_recv()
    step_o = [step_send(73, 0, 1 - zh, xdev(1)), step_send(74, 0, 1 - zh, xdev(-1))]
    w_other(0)
    for copy in step_x:
        copy.wait_recv()
    step_send(75, -1, zh, xdev(1))
    w_forward(0)
    w_forward(2)
    w_across(2)
    w_own_x(3)
    for copy in step_o:
        copy.wait_recv()
    step_send(75, -1, 1 - zh, xdev(1))
    w_forward_other(0)
    w_own_x(1)
    for k in (-1, 0, 1):
        hand(k)
    h_z.wait_recv()
    zrows = ds((rank(2)[0] * 2 + c) * 128, 128)
    h_f = send(26, hidf.at[zrows, :], hidf.at[zrows, :], core, 4)
    w_across_far(2)
    w_forward(3)
    w_across(3)
    w_other(1)
    w_done(0)
    hand(2)
    got(75, stepw.at[0:2])
    for k in range(8):
        stepa[0:16, 160 * k : 160 * k + 160] = stepw[k][:, 0:160].astype(F32)
    wf[:, 768:896] = stepa[...].T.astype(BF16)
    h_c.wait_recv()
    h_f.wait_recv()

    low = coli < 64
    causal = rowi >= coli
    anti = rowi <= coli
    tri = causal.astype(F32).astype(BF16)
    tri3 = jnp.concatenate([tri] * 3, axis=1)
    upper = anti.astype(F32).astype(BF16)
    strict = (rowi > coli).astype(F32).astype(BF16)
    sums4 = jnp.concatenate([upper] * 3 + [strict] * 3, axis=1)

    def pair(v, j):
        return jnp.where(low[0 : v.shape[0]], v[:, 2 * j : 2 * j + 1], v[:, 2 * j + 1 : 2 * j + 2])

    def blocks(f, unroll=True):
        if unroll:
            for b in range(4):
                f(b, pl.ds(b * 128, 128))
        else:
            def step(b, carry):
                f(b, ds(b * 128, 128))
                return carry

            lax.fori_loop(0, 4, step, 0)

    def steps(b, rows):
        projs[rows, ds(128 * c, 256, 128)] = mm(hidf[rows, :], wf[:, ds(640 + 128 * c, 256, 128)])
        pre = projs[rows, 128:256] + bias
        step = jnp.maximum(pre, 0.0) + jnp.log1p(jnp.exp(-jnp.abs(pre)))
        lg = neg * step
        cum = mm(tri3, jnp.concatenate(parts(lg, 3), axis=0))
        stp[rows, :] = step
        lgd[rows, :] = lg
        cums[rows, :] = cum
        cumt[b] = cum.T[0:16, :]
        dgs[b] = jnp.zeros((128, 128), F32)
        red[b] = jnp.zeros((384, 128), F32)

    def maps(b, rows):
        projs[rows, ds(256 - 256 * c, 128)] = mm(hidf[rows, :], wf[:, ds(896 - 256 * c, 128)])
        bm = jax.nn.silu(projs[rows, 0:128])
        cm = jax.nn.silu(projs[rows, 256:384])
        bmf[rows, :] = bm
        cmf[rows, :] = cm
        scores = mm3(cm, bm, NT)
        gs[b] = scores
        gts[b] = scores.T

    blocks(steps)
    for j in range(5):
        cj = slice(128 * j, 128 * j + 128)
        for b in range(4):
            last_row = cums[128 * b + 127 : 128 * b + 128, :]
            tot[8 * b : 8 * b + 8, cj] = pair(jnp.broadcast_to(last_row, (8, 128)), j)
    tts[...] = tot[0:8, :] + tot[8:16, :] + tot[16:24, :] + tot[24:32, :]
    for k in (1, 2, 3):
        send(29, tts, ttr.at[k - 1], ydev(k), 7)

    i320 = lax.broadcasted_iota(jnp.int32, (320, 320), 0)
    k320 = lax.broadcasted_iota(jnp.int32, (320, 320), 1)
    tens = lax.shift_right_logical(i320 * 6554, 16)
    source = ((tens & 3) * 8 + lax.shift_right_logical(tens, 2)) * 10 + i320 - tens * 10
    perm = jnp.where(k320 == source, 1.0, 0.0).astype(F32).astype(BF16)
    for q in range(4):
        hidt[320 * q : 320 * q + 320, :] = mm(perm, hidf[:, 320 * q : 320 * q + 320], NT).astype(BF16)
    w_forward(1)
    got(28, wf.at[:, ds(896 - 256 * c, 128)])
    maps(0, pl.ds(0, 128))
    w_across_far(3)
    maps(1, pl.ds(128, 128))
    maps(2, pl.ds(256, 128))
    w_forward_other(1)
    maps(3, pl.ds(384, 128))

    def total(b, cj):
        return tot[8 * b : 8 * b + 1, cj]

    def pair_forward(j):
        cj = slice(128 * j, 128 * j + 128)

        wide = slice(128 * j, min(128 * j + 256, 640))

        def project(b, rows):
            projv[rows, wide] = mm(hidf[rows, :], wf[:, wide])

        def local_part(b, rows):
            ce = pair(cums[rows, :], j)
            se = pair(stp[rows, :], j)
            ec = jnp.exp(ce)
            tl = jnp.exp(ce[127:128, :] - ce)
            val = jax.nn.silu(projv[rows, cj])
            xs = val * se
            sexp[rows, cj] = se
            ecs[rows, cj] = ec
            tls[rows, cj] = tl
            vv[rows, cj] = val
            xb[rows, cj] = xs.astype(BF16)
            x16 = (xs * tl).astype(BF16)
            o16 = (cot[rows, cj].astype(F32) * ec).astype(BF16)
            xt[rows, cj] = x16
            oe[rows, cj] = o16
            sl[b, :, cj] = mm(bmf[rows, :].astype(BF16), x16, TN)
            dl[b, :, cj] = mm(cmf[rows, :].astype(BF16), o16, TN)

        if j % 2 == 0:
            blocks(project)
        blocks(local_part)
        s = sl[0, :, cj]
        d = dl[3, :, cj]
        for b in range(1, 4):
            s = jnp.exp(total(b, cj)) * s + sl[b, :, cj]
            d = jnp.exp(total(3 - b, cj)) * d + dl[3 - b, :, cj]
        stt[0, :, cj] = s.astype(BF16)
        stt[1, :, cj] = d.astype(BF16)
        for k in (1, 2, 3):
            wraps = lax.div(y + k, 4)
            send(30 + j, stt.at[wraps, :, cj], str_.at[k - 1, :, cj], ydev(k), 8)

    def pair_inside(j):
        cj = slice(128 * j, 128 * j + 128)

        def inside(b, rows):
            cum = cums[rows, :]
            c0, c1 = cum[:, 2 * j : 2 * j + 1], cum[:, 2 * j + 1 : 2 * j + 2]
            r0, r1 = cumt[b, 2 * j : 2 * j + 1, :], cumt[b, 2 * j + 1 : 2 * j + 2, :]
            w0 = jnp.where(causal, jnp.exp(jnp.where(causal, c0 - r0, 0.0)), 0.0)
            w1 = jnp.where(causal, jnp.exp(jnp.where(causal, c1 - r1, 0.0)), 0.0)
            u0 = jnp.where(anti, jnp.exp(jnp.where(anti, r0 - c0, 0.0)), 0.0)
            u1 = jnp.where(anti, jnp.exp(jnp.where(anti, r1 - c1, 0.0)), 0.0)
            scores, scores_t = gs[b], gts[b]
            m = jnp.concatenate([scores * w0, scores * w1], axis=1).astype(BF16)
            mt = jnp.concatenate([scores_t * u0, scores_t * u1], axis=1).astype(BF16)
            x16 = xb[rows, cj]
            o16 = cot[rows, cj]
            zero = jnp.zeros_like(x16)
            xd = jnp.concatenate([jnp.where(low, x16, zero), jnp.where(low, zero, x16)], axis=0)
            od = jnp.concatenate([jnp.where(low, o16, zero), jnp.where(low, zero, o16)], axis=0)
            yy = mm(m, xd)
            pp = mm(o16, xd, NT)
            dx = mm(mt, od)
            dgs[b] = dgs[b] + w0 * pp[:, 0:128] + w1 * pp[:, 128:256]
            dxin[rows, cj] = dx
            q1s[rows, cj] = o16.astype(F32) * yy - x16.astype(F32) * dx

        blocks(inside)

    got(27, cot.at[0:384, :])
    w_done(2)
    pair_forward(2)
    pair_inside(2)
    pair_forward(3)
    pair_inside(3)
    w_done(3)
    pair_forward(4)
    pair_inside(4)
    for p in range(4):
        for q in range(4):
            hidx[320 * p + 80 * q : 320 * p + 80 * q + 80, :] = hidt[320 * q + 80 * p : 320 * q + 80 * p + 80, :]
    w_done(1)
    pair_forward(0)
    pair_inside(0)
    pair_forward(1)
    pair_inside(1)

    def turn(b, rows):
        dcf[rows, :] = mm3(dgs[b], bmf[rows, :], NN) + mm(oe[rows, :], sb[b], NT)
        dbf[rows, :] = mm3(dgs[b], cmf[rows, :], TN) + mm(xt[rows, :], db[b], NT)

    got(29, ttr)

    lanes = lax.broadcasted_iota(jnp.int32, (256, 128), 0)
    outl = lax.broadcasted_iota(jnp.int32, (256, 128), 1)

    def sums(z, j):
        hi = z.astype(BF16)
        lo = (z - hi.astype(F32)).astype(BF16)
        choose = (outl == 2 * j + lax.rem(lax.div(lanes, 64), 2)).astype(F32).astype(BF16)
        return mm(jnp.concatenate([hi, lo], axis=1), choose)

    yes = [jnp.where(y >= k, 1.0, 0.0).astype(F32) for k in (1, 2, 3)]
    no = [jnp.where(y + k <= 3, 1.0, 0.0).astype(F32) for k in (1, 2, 3)]
    inner = [jnp.zeros((8, 128), F32) for _ in range(4)]
    gain = [jnp.zeros((8, 128), F32)]

    def pair_outside(j):
        cj = slice(128 * j, 128 * j + 128)
        got(30 + j, str_.at[:, :, cj])
        t = [ttr[k, 0:1, cj] for k in range(3)]
        came = [str_[k, :, cj].astype(F32) for k in range(3)]
        s = yes[0] * came[0] + (yes[1] * jnp.exp(t[0])) * came[1] + (yes[2] * jnp.exp(t[0] + t[1])) * came[2]
        d = no[0] * came[2] + (no[1] * jnp.exp(t[2])) * came[1] + (no[2] * jnp.exp(t[2] + t[1])) * came[0]
        for b in (3, 2, 1, 0):
            db[b, :, cj] = d.astype(BF16)
            dd[b] = d
            d = jnp.exp(total(b, cj)) * d + dl[b, :, cj]
        for b in range(4):
            sb[b, :, cj] = s.astype(BF16)
            grown = jnp.exp(total(b, cj)) * s
            inner[b] = inner[b] + sums((grown * dd[b]).reshape(16, 8, 128).sum(axis=0), j)
            s = grown + sl[b, :, cj]

        def outside(b, rows):
            o = cot[rows, cj].astype(F32)
            yst = mm(cmf[rows, :].astype(BF16), sb[b, :, cj]) * ecs[rows, cj]
            dxst = mm(bmf[rows, :].astype(BF16), db[b, :, cj]) * tls[rows, cj]
            val = vv[rows, cj]
            dxs = dxin[rows, cj] + dxst
            z = jnp.concatenate([q1s[rows, cj] + o * yst, xb[rows, cj].astype(F32) * dxst, dxs * val], axis=0)
            red[b] = red[b] + sums(z, j)
            dval = dxs * sexp[rows, cj] + pair(skip, j) * o
            rr[rows, cj] = (dval * silu_grad(projv[rows, cj])).astype(BF16)
            gain[0] = gain[0] + sums((o * val).reshape(16, 8, 128).sum(axis=0), j)

        blocks(outside)

    class Stream:
        def __init__(self, base, group, parts, kind, bufs):
            self.base, self.group, self.parts, self.left = base, group, parts, hidx if kind else hidt
            self.dw, self.s1, self.r1, self.s2, self.r2, self.s3, self.r3, self.s4, self.r4, self.sd, self.rd = bufs
            self.index, self.dev, self.index2, self.dev2 = (y, ydev, x, xdev) if kind == 0 else (x, xdev, y, ydev)

        def send(self, i, src, dst, dev):
            return send(self.base + i, src, dst, dev, self.group)

        def block(self, i):
            rows = ds(lax.rem(self.index + i, 4) * 320, 320)
            for cols, target in self.parts:
                self.dw[rows, target] = mm(self.left[rows, :], rr[:, cols])
            return rows

        def first(self):
            rows = self.block(2)
            self.s1[...] = self.dw[rows, :].astype(BF16)
            self.one = (
                self.send(0, self.s1.at[0:160, :], self.r1.at[0], self.dev(1)),
                self.send(1, self.s1.at[160:320, :], self.r1.at[1], self.dev(-1)),
            )

        def rest(self):
            for i in (1, 3, 0):
                self.block(i)

        def second(self):
            nxt = lax.rem(self.index + 1, 4) * 320
            prv = lax.rem(self.index + 3, 4) * 320
            self.one[0].wait_recv()
            self.s2[0, 0:160, :] = (self.dw[ds(nxt, 160), :] + self.r1[0].astype(F32)).astype(BF16)
            self.s2[0, 160:320, :] = self.dw[ds(nxt + 160, 160), :].astype(BF16)
            self.send(2, self.s2.at[0], self.r2.at[0], self.dev(1))
            self.one[1].wait_recv()
            self.s2[1, 0:160, :] = self.dw[ds(prv, 160), :].astype(BF16)
            self.s2[1, 160:320, :] = (self.dw[ds(prv + 160, 160), :] + self.r1[1].astype(F32)).astype(BF16)
            self.send(2, self.s2.at[1], self.r2.at[1], self.dev(-1))

        def third(self):
            got(self.base + 2, self.r2)
            here = ds(self.index * 320, 320)
            summed = self.dw[here, :] + self.r2[0].astype(F32) + self.r2[1].astype(F32)
            self.dw[here, :] = summed
            self.s3[...] = summed.astype(BF16)
            for k in (2, 1, 3):
                piece = self.s3.at[ds(lax.rem(self.index2 + k, 4) * 80, 80), :]
                self.send(3, piece, self.r3.at[k - 1], self.dev2(k))

        def fourth(self):
            got(self.base + 3, self.r3)
            rows = ds(self.index * 320 + self.index2 * 80, 80)
            self.s4[...] = self.dw[rows, :] + self.r3[0].astype(F32) + self.r3[1].astype(F32) + self.r3[2].astype(F32)
            self.four = self.send(4, self.s4.at[ds((1 - zh) * 40, 40), :], self.r4, zpair)

        def owners(self):
            self.four.wait_recv()
            chunk = self.s4[ds(zh * 40, 40), :] + self.r4[...]
            for i in range(4):
                self.sd[i, 0:10, :] = chunk[10 * i : 10 * i + 10, :]
            self.rd[g] = self.sd[r]
            for k in (2, 3, 1):
                zlk, ck, dev = rank(k)
                self.send(5, self.sd.at[zlk * 2 + ck], self.rd.at[g], dev)

        def finish(self):
            got(self.base + 5, self.rd.at[0:3])

        def close(self):
            sent(self.group, self.dw.at[0:688, :])

    alpha = Stream(46, 13, [(slice(256, 640), slice(0, 384))], 0, (dwa, sa1, ra1, sa2, ra2, sa3, ra3, sa4, ra4, sda, rda))
    beta = Stream(52, 14, [(slice(0, 256), slice(0, 256))], 1, (dwb, sb1, rb1, sb2, rb2, sb3, rb3, sb4, rb4, sdb, rdb))
    gamma = Stream(58, 15, [(ds(lane0, 128), slice(0, 128))], 0, (dwc, sc1, rc1, sc2, rc2, sc3, rc3, sc4, rc4, sdc, rdc))
    delta = Stream(64, 16, [(slice(768, 896), slice(0, 128))], 1, (dwd, sd1, rd1, sd2, rd2, sd3, rd3, sd4, rd4, sdd, rdd))

    pair_outside(2)
    pair_outside(3)
    pair_outside(4)
    alpha.first()
    pair_outside(0)
    pair_outside(1)
    beta.first()

    blocks(turn)
    first = c == 0
    t1s[...] = jnp.where(first, dcf[...], dbf[...])
    t1 = send(35, t1s, t1r, core, 9)
    alpha.rest()
    alpha.second()

    ownl = coli < 10
    bias_sum = decay_sum = jnp.zeros((8, 128), F32)
    for b in range(4):
        rows = slice(128 * b, 128 * b + 128)
        dlog = mm(sums4, jnp.concatenate(parts(red[b, 0:128], 3) + parts(red[b, 128:256], 3), axis=0))
        dlog = jnp.where(ownl, dlog + inner[b].sum(axis=0, keepdims=True), 0.0)
        ddt = (red[b, 256:384] + neg * dlog) * jax.nn.sigmoid(projs[rows, 128:256] + bias)
        ddt = jnp.where(ownl, ddt, 0.0)
        rr[rows, 768:896] = ddt.astype(BF16)
        bias_sum = bias_sum + ddt.reshape(16, 8, 128).sum(axis=0)
        decay_sum = decay_sum + (dlog * lgd[rows, :]).reshape(16, 8, 128).sum(axis=0)
    place = jnp.where(jnp.logical_and(rowi < 10, coli == rowi + 10 * g), 1.0, 0.0).astype(F32)
    delta.first()
    row8 = lax.broadcasted_iota(jnp.int32, (8, 128), 0)
    packed = jnp.where(
        row8 == 0, bias_sum.sum(axis=0, keepdims=True),
        jnp.where(row8 == 1, decay_sum.sum(axis=0, keepdims=True),
                  jnp.where(row8 == 2, gain[0].sum(axis=0, keepdims=True), 0.0)),
    )
    heads_y[y] = mm(packed, place, NN, highest)
    for k in (1, 2, 3):
        send(38, heads_y.at[y], heads_y.at[y], ydev(k), 10)
    t1.wait_recv()
    mixed = jnp.where(first, dbf[...], dcf[...]) + t1r[...]
    rr[:, ds(lane0, 128)] = (mixed * silu_grad(projs[:, ds(256 * c, 128, 128)])).astype(BF16)
    rr[:, ds(896 - 256 * c, 128)] = jnp.zeros((512, 128), BF16)
    gamma.first()
    beta.rest()
    beta.second()
    delta.rest()
    gamma.rest()
    for n in range(5):
        part = slice(256 * n, 256 * n + 256)
        hgp[:, part] = mm(rr[...], wf[part, :], NT)
    mate_row = ds((zl * 2 + 1 - c) * 128, 128)
    far_mate = ds(((1 - zl) * 2 + 1 - c) * 128, 128)
    far_row = ds(((1 - zl) * 2 + c) * 128, 128)
    hgs[1] = hgp[far_mate, :].astype(BF16)
    hg_far = send(43, hgs.at[1], hgr.at[1], core, 11)
    hgs[0] = hgp[mate_row, :].astype(BF16)
    hg_near = send(42, hgs.at[0], hgr.at[0], core, 11)
    delta.second()
    hg_far.wait_recv()
    hgs[2] = (hgp[far_row, :] + hgr[1].astype(F32)).astype(BF16)
    hg_z = send(44, hgs.at[2], hgr.at[2], rank(2)[2], 11)
    alpha.third()
    gamma.second()
    beta.third()
    delta.third()
    got(38, heads_y.at[0:3])
    heads_x[x] = (heads_y[0] + heads_y[1]) + (heads_y[2] + heads_y[3])
    for k in (1, 2, 3):
        send(39, heads_x.at[x], heads_x.at[x], xdev(k), 10)
    gamma.third()
    alpha.fourth()
    beta.fourth()
    got(39, heads_x.at[0:3])
    heads_z[zh] = (heads_x[0] + heads_x[1]) + (heads_x[2] + heads_x[3])
    head_z = send(40, heads_z.at[zh], heads_z.at[zh], zpair, 10)
    gamma.fourth()
    delta.fourth()
    alpha.owners()
    beta.owners()
    gamma.owners()
    delta.owners()
    hg_near.wait_recv()
    hg_z.wait_recv()
    hgo[...] = (hgp[here_id, :] + hgr[0].astype(F32) + hgr[2].astype(F32)).astype(BF16)
    hg_out = pltpu.make_async_copy(hgo, hg_ref, ls.at[5])
    hg_out.start()
    head_z.wait_recv()
    heads_g[r] = heads_z[0] + heads_z[1]
    for k in (1, 2, 3):
        send(41, heads_g.at[r], heads_g.at[r], rank(k)[2], 10)
    beta.finish()
    for k in range(4):
        wgo[:, 640 * k : 640 * k + 256] = rdb[k, 0:10, :]
    alpha.finish()
    for k in range(4):
        wgo[:, 640 * k + 256 : 640 * k + 640] = rda[k, 0:10, :]
    got(41, heads_g.at[0:3])
    hdo[...] = (heads_g[0] + heads_g[1]) + (heads_g[2] + heads_g[3])
    hd_out = pltpu.make_async_copy(hdo, hd_ref, ls.at[6])
    hd_out.start()
    delta.finish()
    for k in range(4):
        wgo[:, 2816 + 10 * k : 2826 + 10 * k] = rdd[k, 0:10, 0:10]
    gamma.finish()
    wgo[:, 2560:2688] = rdc[0, 0:10, :] + rdc[2, 0:10, :]
    wgo[:, 2688:2816] = rdc[1, 0:10, :] + rdc[3, 0:10, :]
    wg_out = pltpu.make_async_copy(wgo, wg_ref, ls.at[7])
    wg_out.start()
    for m in range(4):
        sent(m, wf.at[0:1120, cols(m)])
    sent(4, hidf.at[0:384, :])
    sent(17, stepw.at[0:7])
    sent(5, cot.at[0:384, :])
    sent(6, wf.at[:, ds(lane0, 128)])
    sent(7, ttr)
    sent(8, str_)
    sent(9, t1r)
    sent(10, bmf.at[0:80, :])
    sent(11, hgs)
    for stream in (alpha, beta, gamma, delta):
        stream.close()
    hg_out.wait()
    hd_out.wait()
    wg_out.wait()


def scratch():
    def v(shape, dtype=F32):
        return pltpu.VMEM(shape, dtype)

    def stream(n):
        return [
            v((D, n)), v((320, n), BF16), v((2, 160, n), BF16), v((2, 320, n), BF16), v((2, 320, n), BF16),
            v((320, n), BF16), v((3, 80, n), BF16), v((80, n)), v((40, n)), v((4, 16, n)), v((4, 16, n)),
        ]

    wide, wide16 = v((512, COLS)), v((512, COLS), BF16)
    thin = v((512, 128))
    return [
        v((8, 16, 256), BF16), v((128, D)),
        v((512, D), BF16), v((D, 512), BF16), v((D, 512), BF16), wide16, v((160, 2856), BF16), v((D, 1024), BF16),
        v((512, 384)), wide, thin, thin, thin, thin, v((4, 16, 128)), thin,
        v((4, 128, 128)), v((4, 128, 128)), v((4, 128, 128)),
        wide, wide, wide, wide, wide16, wide16, wide16, v((32, COLS)),
        v((4, 128, COLS)), v((4, 128, COLS)), v((2, 128, COLS), BF16), v((8, COLS)),
        v((3, 128, COLS), BF16), v((3, 8, COLS)), wide, wide, thin, thin,
        v((4, 128, COLS), BF16), v((4, 128, COLS), BF16), v((4, 128, 128)), v((4, 384, 128)),
        v((512, 1024), BF16), thin, thin,
        v((512, D)), v((3, 128, D), BF16), v((3, 128, D), BF16),
        *stream(384), *stream(256), *stream(128), *stream(128),
        v((4, 8, 128)), v((4, 8, 128)), v((2, 8, 128)), v((4, 8, 128)),
        v((128, D), BF16), v((10, 2856)), v((8, 128)),
        pltpu.SemaphoreType.DMA((18,)), pltpu.SemaphoreType.DMA((76,)), pltpu.SemaphoreType.DMA((8,)),
    ]


def emit(hg_ref, wg_ref, hd_ref, hg_out, wg_out, hd_out):
    hg_out[...] = hg_ref[...]
    wg_out[...] = wg_ref[...]
    hd_out[...] = hd_ref[0:3, 0:HEADS]


def body(hidden, output_grad, input_weight, step_bias, decay_log, skip_gain):
    anyspace = pl.BlockSpec(memory_space=pl.ANY)
    vmem = pl.BlockSpec(memory_space=pltpu.VMEM)
    hg, wg, hd = pl.pallas_call(
        kernel,
        out_shape=(
            jax.ShapeDtypeStruct((128, D), BF16),
            jax.ShapeDtypeStruct((10, 2856), F32),
            jax.ShapeDtypeStruct((8, 128), F32),
        ),
        in_specs=[anyspace, anyspace, anyspace, vmem, vmem, vmem],
        out_specs=(anyspace, anyspace, anyspace),
        scratch_shapes=scratch(),
        compiler_params=pltpu.CompilerParams(has_side_effects=True, collective_id=0, vmem_limit_bytes=64000000),
    )(hidden[0], output_grad[0], input_weight, step_bias[None], decay_log[None], skip_gain[None])
    hg, wg, hd = pl.pallas_call(
        emit,
        out_shape=(
            jax.ShapeDtypeStruct((128, D), BF16),
            jax.ShapeDtypeStruct((10, 2856), F32),
            jax.ShapeDtypeStruct((3, HEADS), F32),
        ),
        in_specs=[vmem, vmem, vmem],
        out_specs=(vmem, vmem, vmem),
    )(hg, wg, hd)
    return (hg[None], wg, hd)


def solution(mesh):
    torus = Mesh(
        mesh.devices.reshape(4, 2, 2, 4, 2), ("seq_0", "seq_1", "seq_2", "zero_0", "zero_1")
    )
    in_specs = (P(ZERO, SEQ, None), P(ZERO, SEQ, None), P(ZERO, None), P(), P(), P())
    out_specs = (P(ZERO, SEQ, None), P(SEQ_ZERO, None), P())
    return jax.shard_map(body, mesh=torus, in_specs=in_specs, out_specs=out_specs, check_vma=False)
```

```python
import functools

import jax
import jax.numpy as jnp
from jax import lax
from jax.experimental import pallas as pl
from jax.experimental.pallas import tpu as pltpu
from jax.sharding import Mesh
from jax.sharding import PartitionSpec as P

HEADS = 40
STATE = 128
INNER = 2560
D = 1280
COLS = 640
ZERO = ("zero_0", "zero_1")
SEQ = ("seq_0", "seq_1", "seq_2")
SEQ_ZERO = ("seq_0", "seq_1", "seq_2", "zero_0", "zero_1")
MESH = pl.DeviceIdType.MESH
F32 = jnp.float32
BF16 = jnp.bfloat16
highest = lax.Precision.HIGHEST
NN = (((1,), (0,)), ((), ()))
NT = (((1,), (1,)), ((), ()))
TN = (((0,), (0,)), ((), ()))


def mm(a, b, dims=NN, precision=None):
    return lax.dot_general(a, b, dims, preferred_element_type=F32, precision=precision)


def parts(v, count):
    out = []
    for _ in range(count):
        out.append(v.astype(BF16))
        v = v - out[-1].astype(F32)
    return out


def mm3(a, b, dims=NN):
    (ah, al), (bh, bl) = parts(a, 2), parts(b, 2)
    (ka,), (kb,) = dims[0]
    return mm(jnp.concatenate([ah, al, ah], axis=ka), jnp.concatenate([bh, bh, bl], axis=kb), dims)


def ds(start, size, align=None):
    return pl.ds(pl.multiple_of(start, align or size), size)


def silu_grad(v):
    sig = jax.nn.sigmoid(v)
    return sig * (1.0 + v * (1.0 - sig))


def kernel(
    hid_ref, cot_ref, w_ref, bias_ref, decay_ref, skip_ref,
    hg_ref, wg_ref, hd_ref,
    stepw, stepa, hidf, hidt, hidx, cot, wraw, wf, projs, projv, bmf, cmf, lgd, cums, cumt, stp, gs, gts, dgs,
    sexp, ecs, tls, vv, xb, xt, oe, tot,
    sl, dl, stt, tts, str_, ttr, q1s, dxin, dbf, dcf, sb, db, dd, red,
    rr, t1s, t1r, hgp, hgs, hgr,
    heads_y, heads_x, heads_z, heads_g, hgo, wgo, hdo,
    ss, rs, ls, *bufs,
):
    y, zl, c = (lax.axis_index(n) for n in SEQ)
    x, zh = (lax.axis_index(n) for n in ZERO)
    r = zl * 2 + c
    a = lax.rem(zl + zh, 2)
    g = a * 2 + c

    def send(i, src, dst, where, group):
        copy = pltpu.make_async_remote_copy(
            src_ref=src, dst_ref=dst, send_sem=ss.at[group], recv_sem=rs.at[i],
            device_id=where, device_id_type=MESH,
        )
        copy.start()
        return copy

    def bytes_of(ref, i=0, group=0):
        return pltpu.make_async_remote_copy(
            src_ref=ref, dst_ref=ref, send_sem=ss.at[group], recv_sem=rs.at[i],
            device_id={"seq_2": 1 - c}, device_id_type=MESH,
        )

    def got(i, ref):
        bytes_of(ref, i=i).wait_recv()

    def sent(group, ref):
        bytes_of(ref, group=group).wait_send()

    def rank(k):
        zlk = lax.rem(zl + k // 2, 2)
        ck = lax.rem(c + k % 2, 2)
        return zlk, ck, {"seq_1": zlk, "seq_2": ck}

    def xdev(k):
        return {"zero_0": lax.rem(x + k + 4, 4)}

    def ydev(k):
        return {"seq_0": lax.rem(y + k + 4, 4)}

    zpair = {"seq_1": 1 - zl, "zero_1": 1 - zh}
    core = {"seq_2": 1 - c}
    here_id = ds(r * 128, 128)

    def shard(xk, zk, lo=0, size=160):
        return ds((lax.rem(xk + 4, 4) * 2 + zk) * 160 + lo, size, 16)

    own = shard(x, zh)
    lane0 = 640 + 256 * c
    local = [
        pltpu.make_async_copy(w_ref, wraw, ls.at[0]),
        pltpu.make_async_copy(w_ref.at[:, ds(g * COLS, COLS, 128)], wf.at[own, 0:640], ls.at[1]),
        pltpu.make_async_copy(w_ref.at[:, ds(2560 + 128 * c, 128)], wf.at[own, ds(lane0, 128)], ls.at[2]),
        pltpu.make_async_copy(hid_ref, hidf.at[here_id, :], ls.at[3]),
        pltpu.make_async_copy(cot_ref.at[:, ds(g * COLS, COLS, 128)], cot.at[here_id, :], ls.at[4]),
    ]
    for copy in local:
        copy.start()

    barrier = pltpu.get_barrier_semaphore()

    def greet(dev):
        pl.semaphore_signal(barrier, inc=1, device_id=dev, device_id_type=MESH)

    greet(zpair)
    for k in (1, 2, 3):
        greet(xdev(k))
        greet(ydev(k))
        greet(rank(k)[2])
    coli = lax.broadcasted_iota(jnp.int32, (128, 128), 1)
    rowi = lax.broadcasted_iota(jnp.int32, (128, 128), 0)
    local[0].wait()
    stepa[...] = jnp.zeros_like(stepa)
    tail = jnp.concatenate([wraw[:, 2816:2856].astype(F32), jnp.zeros((160, 88), F32)], axis=1)
    tail = pltpu.roll(tail, lax.rem(128 - 10 * g, 128), 1)
    keep10 = lax.broadcasted_iota(jnp.int32, (160, 128), 1) < 10
    tail = jnp.concatenate([jnp.where(keep10, tail, 0.0), jnp.zeros((96, 128), F32)], axis=0)
    stepw[x * 2 + zh] = tail.T[0:16, :].astype(BF16)

    def lanes10(ref):
        full = jnp.concatenate([ref[...], jnp.zeros((1, 88), F32)], axis=1)
        return pltpu.roll(jnp.broadcast_to(full, (8, 128)), lax.rem(128 - 10 * g, 128), 1)[0:1, :]

    bias = lanes10(bias_ref)
    neg = -jnp.exp(lanes10(decay_ref))
    skip = lanes10(skip_ref)
    for copy in local[1:]:
        copy.wait()
    pl.semaphore_wait(barrier, 10)

    def cols(m):
        return (ds(lane0, 128), slice(0, 256), slice(256, 512), slice(512, 640))[m]

    w = {}

    def wsend(m, i, rows, dev):
        ref = wf.at[rows, cols(m)]
        slot = min(i, 5) if m < 2 else {1: 1, 2: 2, 5: 3, 6: 4}.get(i, 5)
        w[m, i] = send(6 * m + slot, ref, ref, dev, m)

    def w_own_x(m):
        wsend(m, 1, own, xdev(1))
        wsend(m, 2, own, xdev(-1))

    def w_own_z(m):
        wsend(m, 0, own, zpair)

    def w_other(m):
        w[m, 0].wait_recv()
        wsend(m, 3, shard(x, 1 - zh), xdev(1))
        wsend(m, 4, shard(x, 1 - zh), xdev(-1))

    def w_forward(m):
        w[m, 1].wait_recv()
        wsend(m, 5, shard(x - 1, zh, 0, 80), xdev(1))
        w[m, 2].wait_recv()
        wsend(m, 6, shard(x + 1, zh, 80, 80), xdev(-1))

    def w_forward_other(m):
        w[m, 3].wait_recv()
        wsend(m, 7, shard(x - 1, 1 - zh, 0, 80), xdev(1))
        w[m, 4].wait_recv()
        wsend(m, 8, shard(x + 1, 1 - zh, 80, 80), xdev(-1))

    def w_across(m):
        wsend(m, 3, shard(x - 1, zh), zpair)
        wsend(m, 4, shard(x + 1, zh), zpair)

    def w_across_far(m):
        w[m, 5].wait_recv()
        wsend(m, 7, shard(x + 2, zh, 0, 80), zpair)
        w[m, 6].wait_recv()
        wsend(m, 8, shard(x + 2, zh, 80, 80), zpair)

    def w_done(m):
        got(6 * m + 5, wf.at[0 : 320 if m < 2 else 640, cols(m)])

    def step_send(i, xk, zk, dev):
        ref = stepw.at[lax.rem(x + xk + 4, 4) * 2 + zk]
        return send(i, ref, ref, dev, 20)

    def hand(k):
        ref = wf.at[ds(lax.rem(x + k + 4, 4) * 320, 320), ds(lane0, 128)]
        send(28, ref, ref, core, 6)

    step_z = step_send(88, 0, zh, zpair)
    step_x = [step_send(89, 0, zh, xdev(1)), step_send(90, 0, zh, xdev(-1))]
    w_own_z(0)
    w_own_x(0)
    h_z = send(24, hid_ref, hidf.at[here_id, :], rank(2)[2], 4)
    w_own_x(2)
    w_own_z(1)
    h_c = send(25, hid_ref, hidf.at[here_id, :], core, 4)
    for k in (2, 3, 1):
        zlk, ck, dev = rank(k)
        gk = lax.rem(zlk + zh, 2) * 2 + ck
        send(27, cot_ref.at[:, ds(gk * COLS, COLS, 128)], cot.at[here_id, :], dev, 5)
    w_own_z(2)
    w_own_z(3)
    step_z.wait_recv()
    step_o = [step_send(91, 0, 1 - zh, xdev(1)), step_send(92, 0, 1 - zh, xdev(-1))]
    w_other(0)
    for copy in step_x:
        copy.wait_recv()
    step_send(93, -1, zh, xdev(1))
    w_forward(0)
    w_forward(2)
    w_across(2)
    w_own_x(3)
    for copy in step_o:
        copy.wait_recv()
    step_send(93, -1, 1 - zh, xdev(1))
    w_forward_other(0)
    w_own_x(1)
    for k in (-1, 0, 1):
        hand(k)
    h_z.wait_recv()
    zrows = ds((rank(2)[0] * 2 + c) * 128, 128)
    h_f = send(26, hidf.at[zrows, :], hidf.at[zrows, :], core, 4)
    w_across_far(2)
    w_forward(3)
    w_across(3)
    w_other(1)
    w_done(0)
    hand(2)
    got(93, stepw.at[0:2])
    for k in range(8):
        stepa[0:16, 160 * k : 160 * k + 160] = stepw[k][:, 0:160].astype(F32)
    wf[:, 768:896] = stepa[...].T.astype(BF16)

    low = coli < 64
    causal = rowi >= coli
    anti = rowi <= coli
    tri = causal.astype(F32).astype(BF16)
    tri3 = jnp.concatenate([tri] * 3, axis=1)
    upper = anti.astype(F32).astype(BF16)
    strict = (rowi > coli).astype(F32).astype(BF16)
    sums4 = jnp.concatenate([upper] * 3 + [strict] * 3, axis=1)

    def pair(v, j):
        return jnp.where(low[0 : v.shape[0]], v[:, 2 * j : 2 * j + 1], v[:, 2 * j + 1 : 2 * j + 2])

    def blocks(f, unroll=True):
        if unroll:
            for b in range(4):
                f(b, pl.ds(b * 128, 128))
        else:
            def step(b, carry):
                f(b, ds(b * 128, 128))
                return carry

            lax.fori_loop(0, 4, step, 0)

    def steps(b, rows):
        projs[rows, ds(128 * c, 256, 128)] = mm(hidf[rows, :], wf[:, ds(640 + 128 * c, 256, 128)])
        pre = projs[rows, 128:256] + bias
        step = jnp.maximum(pre, 0.0) + jnp.log1p(jnp.exp(-jnp.abs(pre)))
        lg = neg * step
        cum = mm(tri3, jnp.concatenate(parts(lg, 3), axis=0))
        stp[rows, :] = step
        lgd[rows, :] = lg
        cums[rows, :] = cum
        cumt[b] = cum.T[0:16, :]
        dgs[b] = jnp.zeros((128, 128), F32)
        red[b] = jnp.zeros((384, 128), F32)

    def maps(b, rows):
        projs[rows, ds(256 - 256 * c, 128)] = mm(hidf[rows, :], wf[:, ds(896 - 256 * c, 128)])
        bm = jax.nn.silu(projs[rows, 0:128])
        cm = jax.nn.silu(projs[rows, 256:384])
        bmf[rows, :] = bm
        cmf[rows, :] = cm
        scores = mm3(cm, bm, NT)
        gs[b] = scores
        gts[b] = scores.T

    h_c.wait_recv()
    for k in range(4):
        if k == 3:
            h_f.wait_recv()
        b = rank(k)[0] * 2 + rank(k)[1]
        steps(b, ds(b * 128, 128))
    for j in range(5):
        cj = slice(128 * j, 128 * j + 128)
        for b in range(4):
            last_row = cums[128 * b + 127 : 128 * b + 128, :]
            tot[8 * b : 8 * b + 8, cj] = pair(jnp.broadcast_to(last_row, (8, 128)), j)
    tts[...] = tot[0:8, :] + tot[8:16, :] + tot[16:24, :] + tot[24:32, :]
    for k in (1, 2, 3):
        send(29, tts, ttr.at[k - 1], ydev(k), 7)

    i320 = lax.broadcasted_iota(jnp.int32, (320, 320), 0)
    k320 = lax.broadcasted_iota(jnp.int32, (320, 320), 1)
    tens = lax.shift_right_logical(i320 * 6554, 16)
    source = ((tens & 3) * 8 + lax.shift_right_logical(tens, 2)) * 10 + i320 - tens * 10
    perm = jnp.where(k320 == source, 1.0, 0.0).astype(F32).astype(BF16)
    for q in range(4):
        hidt[320 * q : 320 * q + 320, :] = mm(perm, hidf[:, 320 * q : 320 * q + 320], NT).astype(BF16)
    w_forward(1)
    got(28, wf.at[:, ds(896 - 256 * c, 128)])
    maps(0, pl.ds(0, 128))
    w_across_far(3)
    maps(1, pl.ds(128, 128))
    maps(2, pl.ds(256, 128))
    w_forward_other(1)
    maps(3, pl.ds(384, 128))

    def total(b, cj):
        return tot[8 * b : 8 * b + 1, cj]

    def pair_forward(j):
        cj = slice(128 * j, 128 * j + 128)

        wide = slice(128 * j, min(128 * j + 256, 640))

        def project(b, rows):
            projv[rows, wide] = mm(hidf[rows, :], wf[:, wide])

        def local_part(b, rows):
            ce = pair(cums[rows, :], j)
            se = pair(stp[rows, :], j)
            ec = jnp.exp(ce)
            tl = jnp.exp(ce[127:128, :] - ce)
            val = jax.nn.silu(projv[rows, cj])
            xs = val * se
            sexp[rows, cj] = se
            ecs[rows, cj] = ec
            tls[rows, cj] = tl
            vv[rows, cj] = val
            xb[rows, cj] = xs.astype(BF16)
            x16 = (xs * tl).astype(BF16)
            o16 = (cot[rows, cj].astype(F32) * ec).astype(BF16)
            xt[rows, cj] = x16
            oe[rows, cj] = o16
            sl[b, :, cj] = mm(bmf[rows, :].astype(BF16), x16, TN)
            dl[b, :, cj] = mm(cmf[rows, :].astype(BF16), o16, TN)

        if j % 2 == 0:
            blocks(project)
        blocks(local_part)
        s = sl[0, :, cj]
        d = dl[3, :, cj]
        for b in range(1, 4):
            s = jnp.exp(total(b, cj)) * s + sl[b, :, cj]
            d = jnp.exp(total(3 - b, cj)) * d + dl[3 - b, :, cj]
        stt[0, :, cj] = s.astype(BF16)
        stt[1, :, cj] = d.astype(BF16)
        for k in (1, 2, 3):
            wraps = lax.div(y + k, 4)
            send(30 + j, stt.at[wraps, :, cj], str_.at[k - 1, :, cj], ydev(k), 8)

    def pair_inside(j):
        cj = slice(128 * j, 128 * j + 128)

        def inside(b, rows):
            cum = cums[rows, :]
            c0, c1 = cum[:, 2 * j : 2 * j + 1], cum[:, 2 * j + 1 : 2 * j + 2]
            r0, r1 = cumt[b, 2 * j : 2 * j + 1, :], cumt[b, 2 * j + 1 : 2 * j + 2, :]
            w0 = jnp.where(causal, jnp.exp(jnp.where(causal, c0 - r0, 0.0)), 0.0)
            w1 = jnp.where(causal, jnp.exp(jnp.where(causal, c1 - r1, 0.0)), 0.0)
            u0 = jnp.where(anti, jnp.exp(jnp.where(anti, r0 - c0, 0.0)), 0.0)
            u1 = jnp.where(anti, jnp.exp(jnp.where(anti, r1 - c1, 0.0)), 0.0)
            scores, scores_t = gs[b], gts[b]
            m = jnp.concatenate([scores * w0, scores * w1], axis=1).astype(BF16)
            mt = jnp.concatenate([scores_t * u0, scores_t * u1], axis=1).astype(BF16)
            x16 = xb[rows, cj]
            o16 = cot[rows, cj]
            zero = jnp.zeros_like(x16)
            xd = jnp.concatenate([jnp.where(low, x16, zero), jnp.where(low, zero, x16)], axis=0)
            od = jnp.concatenate([jnp.where(low, o16, zero), jnp.where(low, zero, o16)], axis=0)
            yy = mm(m, xd)
            pp = mm(o16, xd, NT)
            dx = mm(mt, od)
            dgs[b] = dgs[b] + w0 * pp[:, 0:128] + w1 * pp[:, 128:256]
            dxin[rows, cj] = dx
            q1s[rows, cj] = o16.astype(F32) * yy - x16.astype(F32) * dx

        blocks(inside)

    got(27, cot.at[0:384, :])
    w_done(2)
    pair_forward(2)
    pair_inside(2)
    pair_forward(3)
    pair_inside(3)
    w_done(3)
    pair_forward(4)
    pair_inside(4)
    for p in range(4):
        for q in range(4):
            hidx[320 * p + 80 * q : 320 * p + 80 * q + 80, :] = hidt[320 * q + 80 * p : 320 * q + 80 * p + 80, :]
    w_done(1)
    pair_forward(0)
    pair_inside(0)
    pair_forward(1)
    pair_inside(1)

    def turn(b, rows):
        dcf[rows, :] = mm3(dgs[b], bmf[rows, :], NN) + mm(oe[rows, :], sb[b], NT)
        dbf[rows, :] = mm3(dgs[b], cmf[rows, :], TN) + mm(xt[rows, :], db[b], NT)

    got(29, ttr)

    lanes = lax.broadcasted_iota(jnp.int32, (256, 128), 0)
    outl = lax.broadcasted_iota(jnp.int32, (256, 128), 1)

    def sums(z, j):
        hi = z.astype(BF16)
        lo = (z - hi.astype(F32)).astype(BF16)
        choose = (outl == 2 * j + lax.rem(lax.div(lanes, 64), 2)).astype(F32).astype(BF16)
        return mm(jnp.concatenate([hi, lo], axis=1), choose)

    yes = [jnp.where(y >= k, 1.0, 0.0).astype(F32) for k in (1, 2, 3)]
    no = [jnp.where(y + k <= 3, 1.0, 0.0).astype(F32) for k in (1, 2, 3)]
    inner = [jnp.zeros((8, 128), F32) for _ in range(4)]
    gain = [jnp.zeros((8, 128), F32)]

    def pair_outside(j):
        cj = slice(128 * j, 128 * j + 128)
        got(30 + j, str_.at[:, :, cj])
        t = [ttr[k, 0:1, cj] for k in range(3)]
        came = [str_[k, :, cj].astype(F32) for k in range(3)]
        s = yes[0] * came[0] + (yes[1] * jnp.exp(t[0])) * came[1] + (yes[2] * jnp.exp(t[0] + t[1])) * came[2]
        d = no[0] * came[2] + (no[1] * jnp.exp(t[2])) * came[1] + (no[2] * jnp.exp(t[2] + t[1])) * came[0]
        for b in (3, 2, 1, 0):
            db[b, :, cj] = d.astype(BF16)
            dd[b] = d
            d = jnp.exp(total(b, cj)) * d + dl[b, :, cj]
        for b in range(4):
            sb[b, :, cj] = s.astype(BF16)
            grown = jnp.exp(total(b, cj)) * s
            inner[b] = inner[b] + sums((grown * dd[b]).reshape(16, 8, 128).sum(axis=0), j)
            s = grown + sl[b, :, cj]

        def outside(b, rows):
            o = cot[rows, cj].astype(F32)
            yst = mm(cmf[rows, :].astype(BF16), sb[b, :, cj]) * ecs[rows, cj]
            dxst = mm(bmf[rows, :].astype(BF16), db[b, :, cj]) * tls[rows, cj]
            val = vv[rows, cj]
            dxs = dxin[rows, cj] + dxst
            z = jnp.concatenate([q1s[rows, cj] + o * yst, xb[rows, cj].astype(F32) * dxst, dxs * val], axis=0)
            red[b] = red[b] + sums(z, j)
            dval = dxs * sexp[rows, cj] + pair(skip, j) * o
            rr[rows, cj] = (dval * silu_grad(projv[rows, cj])).astype(BF16)
            gain[0] = gain[0] + sums((o * val).reshape(16, 8, 128).sum(axis=0), j)

        blocks(outside)

    class Stream:
        def __init__(self, base, group, parts, kind, bufs):
            self.base, self.group, self.parts, self.left = base, group, parts, hidx if kind else hidt
            self.dw, self.s1, self.r1, self.s2, self.r2, self.s3, self.r3, self.s4, self.r4, self.sd, self.rd = bufs
            self.index, self.dev, self.index2, self.dev2 = (y, ydev, x, xdev) if kind == 0 else (x, xdev, y, ydev)

        def send(self, i, src, dst, dev):
            return send(self.base + i, src, dst, dev, self.group)

        def block(self, i):
            rows = ds(lax.rem(self.index + i, 4) * 320, 320)
            for cols, target in self.parts:
                self.dw[rows, target] = mm(self.left[rows, :], rr[:, cols])
            return rows

        def first(self):
            rows = self.block(2)
            self.s1[...] = self.dw[rows, :].astype(BF16)
            self.one = (
                self.send(0, self.s1.at[0:160, :], self.r1.at[0], self.dev(1)),
                self.send(1, self.s1.at[160:320, :], self.r1.at[1], self.dev(-1)),
            )

        def rest(self):
            for i in (1, 3, 0):
                self.block(i)

        def second(self):
            nxt = lax.rem(self.index + 1, 4) * 320
            prv = lax.rem(self.index + 3, 4) * 320
            self.one[0].wait_recv()
            self.s2[0, 0:160, :] = (self.dw[ds(nxt, 160), :] + self.r1[0].astype(F32)).astype(BF16)
            self.s2[0, 160:320, :] = self.dw[ds(nxt + 160, 160), :].astype(BF16)
            self.send(2, self.s2.at[0], self.r2.at[0], self.dev(1))
            self.one[1].wait_recv()
            self.s2[1, 0:160, :] = self.dw[ds(prv, 160), :].astype(BF16)
            self.s2[1, 160:320, :] = (self.dw[ds(prv + 160, 160), :] + self.r1[1].astype(F32)).astype(BF16)
            self.send(2, self.s2.at[1], self.r2.at[1], self.dev(-1))

        def third(self):
            got(self.base + 2, self.r2)
            here = ds(self.index * 320, 320)
            summed = self.dw[here, :] + self.r2[0].astype(F32) + self.r2[1].astype(F32)
            self.dw[here, :] = summed
            self.s3[...] = summed.astype(BF16)
            for k in (2, 1, 3):
                piece = self.s3.at[ds(lax.rem(self.index2 + k, 4) * 80, 80), :]
                self.send(3, piece, self.r3.at[k - 1], self.dev2(k))

        def fourth(self):
            got(self.base + 3, self.r3)
            rows = ds(self.index * 320 + self.index2 * 80, 80)
            self.s4[...] = self.dw[rows, :] + self.r3[0].astype(F32) + self.r3[1].astype(F32) + self.r3[2].astype(F32)
            self.four = self.send(4, self.s4.at[ds((1 - zh) * 40, 40), :], self.r4, zpair)

        def owners(self):
            self.four.wait_recv()
            chunk = self.s4[ds(zh * 40, 40), :] + self.r4[...]
            for i in range(4):
                self.sd[i, 0:10, :] = chunk[10 * i : 10 * i + 10, :]
            self.rd[g] = self.sd[r]
            for k in (2, 3, 1):
                zlk, ck, dev = rank(k)
                self.send(5, self.sd.at[zlk * 2 + ck], self.rd.at[g], dev)

        def finish(self):
            got(self.base + 5, self.rd.at[0:3])

        def close(self):
            sent(self.group, self.dw.at[0:688, :])

    tiles = [slice(128 * t, 128 * t + 128) for t in range(5)] + [slice(768, 896), ds(lane0, 128)]
    kinds = (0, 1, 0, 1, 0, 1, 0)
    p0, p1, p2, p3, p4, st, mp = streams = [
        Stream(46 + 6 * t, 13 + t, [(tiles[t], slice(0, 128))], kinds[t], bufs[11 * t : 11 * t + 11]) for t in range(7)
    ]

    pair_outside(2)
    p2.first()
    pair_outside(3)
    p3.first()
    p2.rest()
    pair_outside(4)
    p4.first()
    p3.rest()
    pair_outside(0)
    p0.first()
    p2.second()
    pair_outside(1)
    p1.first()
    p3.second()

    blocks(turn)
    first = c == 0
    t1s[...] = jnp.where(first, dcf[...], dbf[...])
    t1 = send(35, t1s, t1r, core, 9)
    p4.rest()
    p4.second()

    ownl = coli < 10
    bias_sum = decay_sum = jnp.zeros((8, 128), F32)
    for b in range(4):
        rows = slice(128 * b, 128 * b + 128)
        dlog = mm(sums4, jnp.concatenate(parts(red[b, 0:128], 3) + parts(red[b, 128:256], 3), axis=0))
        dlog = jnp.where(ownl, dlog + inner[b].sum(axis=0, keepdims=True), 0.0)
        ddt = (red[b, 256:384] + neg * dlog) * jax.nn.sigmoid(projs[rows, 128:256] + bias)
        ddt = jnp.where(ownl, ddt, 0.0)
        rr[rows, 768:896] = ddt.astype(BF16)
        bias_sum = bias_sum + ddt.reshape(16, 8, 128).sum(axis=0)
        decay_sum = decay_sum + (dlog * lgd[rows, :]).reshape(16, 8, 128).sum(axis=0)
    place = jnp.where(jnp.logical_and(rowi < 10, coli == rowi + 10 * g), 1.0, 0.0).astype(F32)
    st.first()
    row8 = lax.broadcasted_iota(jnp.int32, (8, 128), 0)
    packed = jnp.where(
        row8 == 0, bias_sum.sum(axis=0, keepdims=True),
        jnp.where(row8 == 1, decay_sum.sum(axis=0, keepdims=True),
                  jnp.where(row8 == 2, gain[0].sum(axis=0, keepdims=True), 0.0)),
    )
    heads_y[y] = mm(packed, place, NN, highest)
    for k in (1, 2, 3):
        send(38, heads_y.at[y], heads_y.at[y], ydev(k), 10)
    t1.wait_recv()
    mixed = jnp.where(first, dbf[...], dcf[...]) + t1r[...]
    rr[:, ds(lane0, 128)] = (mixed * silu_grad(projs[:, ds(256 * c, 128, 128)])).astype(BF16)
    rr[:, ds(896 - 256 * c, 128)] = jnp.zeros((512, 128), BF16)
    mp.first()
    p0.rest()
    p0.second()
    p1.rest()
    p1.second()
    p2.third()

    def token(lo, hi):
        for n in range(lo, hi):
            part = slice(256 * n, 256 * n + 256)
            hgp[:, part] = mm(rr[...], wf[part, :], NT)

    st.rest()
    token(0, 2)
    p3.third()
    mp.rest()
    st.second()
    token(2, 4)
    mp.second()
    p4.third()
    token(4, 5)
    mate_row = ds((zl * 2 + 1 - c) * 128, 128)
    far_mate = ds(((1 - zl) * 2 + 1 - c) * 128, 128)
    far_row = ds(((1 - zl) * 2 + c) * 128, 128)
    hgs[1] = hgp[far_mate, :].astype(BF16)
    hg_far = send(43, hgs.at[1], hgr.at[1], core, 11)
    hgs[0] = hgp[mate_row, :].astype(BF16)
    hg_near = send(42, hgs.at[0], hgr.at[0], core, 11)
    p2.fourth()
    p0.third()
    hg_far.wait_recv()
    hgs[2] = (hgp[far_row, :] + hgr[1].astype(F32)).astype(BF16)
    hg_z = send(44, hgs.at[2], hgr.at[2], rank(2)[2], 11)
    p1.third()
    p3.fourth()
    got(38, heads_y.at[0:3])
    heads_x[x] = (heads_y[0] + heads_y[1]) + (heads_y[2] + heads_y[3])
    for k in (1, 2, 3):
        send(39, heads_x.at[x], heads_x.at[x], xdev(k), 10)
    st.third()
    mp.third()
    p4.fourth()
    p2.owners()
    p0.fourth()
    got(39, heads_x.at[0:3])
    heads_z[zh] = (heads_x[0] + heads_x[1]) + (heads_x[2] + heads_x[3])
    head_z = send(40, heads_z.at[zh], heads_z.at[zh], zpair, 10)
    p3.owners()
    p1.fourth()
    p4.owners()
    st.fourth()
    mp.fourth()
    p0.owners()
    p1.owners()
    st.owners()
    mp.owners()
    hg_near.wait_recv()
    hg_z.wait_recv()
    hgo[...] = (hgp[here_id, :] + hgr[0].astype(F32) + hgr[2].astype(F32)).astype(BF16)
    hg_out = pltpu.make_async_copy(hgo, hg_ref, ls.at[5])
    hg_out.start()
    head_z.wait_recv()
    heads_g[r] = heads_z[0] + heads_z[1]
    for k in (1, 2, 3):
        send(41, heads_g.at[r], heads_g.at[r], rank(k)[2], 10)
    got(41, heads_g.at[0:3])
    hdo[...] = (heads_g[0] + heads_g[1]) + (heads_g[2] + heads_g[3])
    hd_out = pltpu.make_async_copy(hdo, hd_ref, ls.at[6])
    hd_out.start()
    for t, stream in ((2, p2), (3, p3), (4, p4), (0, p0), (1, p1)):
        stream.finish()
        for k in range(4):
            wgo[:, 640 * k + 128 * t : 640 * k + 128 * t + 128] = stream.rd[k, 0:10, :]
    st.finish()
    for k in range(4):
        wgo[:, 2816 + 10 * k : 2826 + 10 * k] = st.rd[k, 0:10, 0:10]
    mp.finish()
    wgo[:, 2560:2688] = mp.rd[0, 0:10, :] + mp.rd[2, 0:10, :]
    wgo[:, 2688:2816] = mp.rd[1, 0:10, :] + mp.rd[3, 0:10, :]
    wg_out = pltpu.make_async_copy(wgo, wg_ref, ls.at[7])
    wg_out.start()
    for m in range(4):
        sent(m, wf.at[0:1120, cols(m)])
    sent(4, hidf.at[0:384, :])
    sent(20, stepw.at[0:7])
    sent(5, cot.at[0:384, :])
    sent(6, wf.at[:, ds(lane0, 128)])
    sent(7, ttr)
    sent(8, str_)
    sent(9, t1r)
    sent(10, bmf.at[0:80, :])
    sent(11, hgs)
    for stream in streams:
        stream.close()
    hg_out.wait()
    hd_out.wait()
    wg_out.wait()


def scratch():
    def v(shape, dtype=F32):
        return pltpu.VMEM(shape, dtype)

    def stream(n):
        return [
            v((D, n)), v((320, n), BF16), v((2, 160, n), BF16), v((2, 320, n), BF16), v((2, 320, n), BF16),
            v((320, n), BF16), v((3, 80, n), BF16), v((80, n)), v((40, n)), v((4, 16, n)), v((4, 16, n)),
        ]

    wide, wide16 = v((512, COLS)), v((512, COLS), BF16)
    thin = v((512, 128))
    return [
        v((8, 16, 256), BF16), v((128, D)),
        v((512, D), BF16), v((D, 512), BF16), v((D, 512), BF16), wide16, v((160, 2856), BF16), v((D, 1024), BF16),
        v((512, 384)), wide, thin, thin, thin, thin, v((4, 16, 128)), thin,
        v((4, 128, 128)), v((4, 128, 128)), v((4, 128, 128)),
        wide, wide, wide, wide, wide16, wide16, wide16, v((32, COLS)),
        v((4, 128, COLS)), v((4, 128, COLS)), v((2, 128, COLS), BF16), v((8, COLS)),
        v((3, 128, COLS), BF16), v((3, 8, COLS)), wide, wide, thin, thin,
        v((4, 128, COLS), BF16), v((4, 128, COLS), BF16), v((4, 128, 128)), v((4, 384, 128)),
        v((512, 1024), BF16), thin, thin,
        v((512, D)), v((3, 128, D), BF16), v((3, 128, D), BF16),
        v((4, 8, 128)), v((4, 8, 128)), v((2, 8, 128)), v((4, 8, 128)),
        v((128, D), BF16), v((10, 2856)), v((8, 128)),
        pltpu.SemaphoreType.DMA((21,)), pltpu.SemaphoreType.DMA((94,)), pltpu.SemaphoreType.DMA((8,)),
        *(buf for _ in range(7) for buf in stream(128)),
    ]


def emit(hg_ref, wg_ref, hd_ref, hg_out, wg_out, hd_out):
    hg_out[...] = hg_ref[...]
    wg_out[...] = wg_ref[...]
    hd_out[...] = hd_ref[0:3, 0:HEADS]


def body(hidden, output_grad, input_weight, step_bias, decay_log, skip_gain):
    anyspace = pl.BlockSpec(memory_space=pl.ANY)
    vmem = pl.BlockSpec(memory_space=pltpu.VMEM)
    hg, wg, hd = pl.pallas_call(
        kernel,
        out_shape=(
            jax.ShapeDtypeStruct((128, D), BF16),
            jax.ShapeDtypeStruct((10, 2856), F32),
            jax.ShapeDtypeStruct((8, 128), F32),
        ),
        in_specs=[anyspace, anyspace, anyspace, vmem, vmem, vmem],
        out_specs=(anyspace, anyspace, anyspace),
        scratch_shapes=scratch(),
        compiler_params=pltpu.CompilerParams(has_side_effects=True, collective_id=0, vmem_limit_bytes=64000000),
    )(hidden[0], output_grad[0], input_weight, step_bias[None], decay_log[None], skip_gain[None])
    hg, wg, hd = pl.pallas_call(
        emit,
        out_shape=(
            jax.ShapeDtypeStruct((128, D), BF16),
            jax.ShapeDtypeStruct((10, 2856), F32),
            jax.ShapeDtypeStruct((3, HEADS), F32),
        ),
        in_specs=[vmem, vmem, vmem],
        out_specs=(vmem, vmem, vmem),
    )(hg, wg, hd)
    return (hg[None], wg, hd)


def solution(mesh):
    torus = Mesh(
        mesh.devices.reshape(4, 2, 2, 4, 2), ("seq_0", "seq_1", "seq_2", "zero_0", "zero_1")
    )
    in_specs = (P(ZERO, SEQ, None), P(ZERO, SEQ, None), P(ZERO, None), P(), P(), P())
    out_specs = (P(ZERO, SEQ, None), P(SEQ_ZERO, None), P())
    return jax.shard_map(body, mesh=torus, in_specs=in_specs, out_specs=out_specs, check_vma=False)
```

```python
import functools

import jax
import jax.numpy as jnp
from jax import lax
from jax.experimental import pallas as pl
from jax.experimental.pallas import tpu as pltpu
from jax.sharding import Mesh
from jax.sharding import PartitionSpec as P

HEADS = 40
STATE = 128
INNER = 2560
D = 1280
COLS = 640
ZERO = ("zero_0", "zero_1")
SEQ = ("seq_0", "seq_1", "seq_2")
SEQ_ZERO = ("seq_0", "seq_1", "seq_2", "zero_0", "zero_1")
MESH = pl.DeviceIdType.MESH
F32 = jnp.float32
BF16 = jnp.bfloat16
highest = lax.Precision.HIGHEST
NN = (((1,), (0,)), ((), ()))
NT = (((1,), (1,)), ((), ()))
TN = (((0,), (0,)), ((), ()))


def mm(a, b, dims=NN, precision=None):
    return lax.dot_general(a, b, dims, preferred_element_type=F32, precision=precision)


def parts(v, count):
    out = []
    for _ in range(count):
        out.append(v.astype(BF16))
        v = v - out[-1].astype(F32)
    return out


def mm3(a, b, dims=NN):
    (ah, al), (bh, bl) = parts(a, 2), parts(b, 2)
    (ka,), (kb,) = dims[0]
    return mm(jnp.concatenate([ah, al, ah], axis=ka), jnp.concatenate([bh, bh, bl], axis=kb), dims)


def ds(start, size, align=None):
    return pl.ds(pl.multiple_of(start, align or size), size)


def silu_grad(v):
    sig = jax.nn.sigmoid(v)
    return sig * (1.0 + v * (1.0 - sig))


def kernel(
    hid_ref, cot_ref, w_ref, bias_ref, decay_ref, skip_ref,
    hg_ref, wg_ref, hd_ref,
    stepw, stepa, hidf, hidt, hidx, cot, wraw, wf, projs, projv, bmf, cmf, lgd, cums, cumt, stp, gs, gts, dgs,
    sexp, ecs, tls, vv, xb, xt, oe, tot,
    sl, dl, stt, tts, str_, ttr, q1s, dxin, dbf, dcf, sb, db, dd, red,
    rr, t1s, t1r, hgp, hgs, hgr,
    heads_y, heads_x, heads_z, heads_g, hgo, wgo, hdo,
    ss, rs, ls, *bufs,
):
    y, zl, c = (lax.axis_index(n) for n in SEQ)
    x, zh = (lax.axis_index(n) for n in ZERO)
    r = zl * 2 + c
    a = lax.rem(zl + zh, 2)
    g = a * 2 + c

    def send(i, src, dst, where, group):
        copy = pltpu.make_async_remote_copy(
            src_ref=src, dst_ref=dst, send_sem=ss.at[group], recv_sem=rs.at[i],
            device_id=where, device_id_type=MESH,
        )
        copy.start()
        return copy

    def bytes_of(ref, i=0, group=0):
        return pltpu.make_async_remote_copy(
            src_ref=ref, dst_ref=ref, send_sem=ss.at[group], recv_sem=rs.at[i],
            device_id={"seq_2": 1 - c}, device_id_type=MESH,
        )

    def got(i, ref):
        bytes_of(ref, i=i).wait_recv()

    def sent(group, ref):
        bytes_of(ref, group=group).wait_send()

    def rank(k):
        zlk = lax.rem(zl + k // 2, 2)
        ck = lax.rem(c + k % 2, 2)
        return zlk, ck, {"seq_1": zlk, "seq_2": ck}

    def xdev(k):
        return {"zero_0": lax.rem(x + k + 4, 4)}

    def ydev(k):
        return {"seq_0": lax.rem(y + k + 4, 4)}

    zpair = {"seq_1": 1 - zl, "zero_1": 1 - zh}
    core = {"seq_2": 1 - c}
    here_id = ds(r * 128, 128)

    def shard(xk, zk, lo=0, size=160):
        return ds((lax.rem(xk + 4, 4) * 2 + zk) * 160 + lo, size, 16)

    own = shard(x, zh)
    lane0 = 640 + 256 * c
    local = [
        pltpu.make_async_copy(w_ref, wraw, ls.at[0]),
        pltpu.make_async_copy(w_ref.at[:, ds(g * COLS, COLS, 128)], wf.at[own, 0:640], ls.at[1]),
        pltpu.make_async_copy(w_ref.at[:, ds(2560 + 128 * c, 128)], wf.at[own, ds(lane0, 128)], ls.at[2]),
        pltpu.make_async_copy(hid_ref, hidf.at[here_id, :], ls.at[3]),
        pltpu.make_async_copy(cot_ref.at[:, ds(g * COLS, COLS, 128)], cot.at[here_id, :], ls.at[4]),
    ]
    for copy in local:
        copy.start()

    barrier = pltpu.get_barrier_semaphore()

    def greet(dev):
        pl.semaphore_signal(barrier, inc=1, device_id=dev, device_id_type=MESH)

    greet(zpair)
    for k in (1, 2, 3):
        greet(xdev(k))
        greet(ydev(k))
        greet(rank(k)[2])
    coli = lax.broadcasted_iota(jnp.int32, (128, 128), 1)
    rowi = lax.broadcasted_iota(jnp.int32, (128, 128), 0)
    local[0].wait()
    stepa[...] = jnp.zeros_like(stepa)
    tail = jnp.concatenate([wraw[:, 2816:2856].astype(F32), jnp.zeros((160, 88), F32)], axis=1)
    tail = pltpu.roll(tail, lax.rem(128 - 10 * g, 128), 1)
    keep10 = lax.broadcasted_iota(jnp.int32, (160, 128), 1) < 10
    tail = jnp.concatenate([jnp.where(keep10, tail, 0.0), jnp.zeros((96, 128), F32)], axis=0)
    stepw[x * 2 + zh] = tail.T[0:16, :].astype(BF16)

    def lanes10(ref):
        full = jnp.concatenate([ref[...], jnp.zeros((1, 88), F32)], axis=1)
        return pltpu.roll(jnp.broadcast_to(full, (8, 128)), lax.rem(128 - 10 * g, 128), 1)[0:1, :]

    bias = lanes10(bias_ref)
    neg = -jnp.exp(lanes10(decay_ref))
    skip = lanes10(skip_ref)
    for copy in local[1:]:
        copy.wait()
    pl.semaphore_wait(barrier, 10)

    def cols(m):
        return (ds(lane0, 128), slice(0, 256), slice(256, 512), slice(512, 640))[m]

    w = {}

    def wsend(m, i, rows, dev):
        ref = wf.at[rows, cols(m)]
        slot = min(i, 5) if m < 2 else {1: 1, 2: 2, 5: 3, 6: 4}.get(i, 5)
        w[m, i] = send(6 * m + slot, ref, ref, dev, m)

    def w_own_x(m):
        wsend(m, 1, own, xdev(1))
        wsend(m, 2, own, xdev(-1))

    def w_own_z(m):
        wsend(m, 0, own, zpair)

    def w_other(m):
        w[m, 0].wait_recv()
        wsend(m, 3, shard(x, 1 - zh), xdev(1))
        wsend(m, 4, shard(x, 1 - zh), xdev(-1))

    def w_forward(m):
        w[m, 1].wait_recv()
        wsend(m, 5, shard(x - 1, zh, 0, 80), xdev(1))
        w[m, 2].wait_recv()
        wsend(m, 6, shard(x + 1, zh, 80, 80), xdev(-1))

    def w_forward_other(m):
        w[m, 3].wait_recv()
        wsend(m, 7, shard(x - 1, 1 - zh, 0, 80), xdev(1))
        w[m, 4].wait_recv()
        wsend(m, 8, shard(x + 1, 1 - zh, 80, 80), xdev(-1))

    def w_across(m):
        wsend(m, 3, shard(x - 1, zh), zpair)
        wsend(m, 4, shard(x + 1, zh), zpair)

    def w_across_far(m):
        w[m, 5].wait_recv()
        wsend(m, 7, shard(x + 2, zh, 0, 80), zpair)
        w[m, 6].wait_recv()
        wsend(m, 8, shard(x + 2, zh, 80, 80), zpair)

    def w_done(m):
        got(6 * m + 5, wf.at[0 : 320 if m < 2 else 640, cols(m)])

    def step_send(i, xk, zk, dev):
        ref = stepw.at[lax.rem(x + xk + 4, 4) * 2 + zk]
        return send(i, ref, ref, dev, 20)

    def hand(k):
        ref = wf.at[ds(lax.rem(x + k + 4, 4) * 320, 320), ds(lane0, 128)]
        send(28, ref, ref, core, 6)

    step_z = step_send(88, 0, zh, zpair)
    step_x = [step_send(89, 0, zh, xdev(1)), step_send(90, 0, zh, xdev(-1))]
    w_own_z(0)
    w_own_x(0)
    h_z = send(24, hid_ref, hidf.at[here_id, :], rank(2)[2], 4)
    w_own_x(2)
    w_own_z(1)
    h_c = send(25, hid_ref, hidf.at[here_id, :], core, 4)
    for k in (2, 3, 1):
        zlk, ck, dev = rank(k)
        gk = lax.rem(zlk + zh, 2) * 2 + ck
        send(27, cot_ref.at[:, ds(gk * COLS, COLS, 128)], cot.at[here_id, :], dev, 5)
    w_own_z(2)
    w_own_z(3)
    step_z.wait_recv()
    step_o = [step_send(91, 0, 1 - zh, xdev(1)), step_send(92, 0, 1 - zh, xdev(-1))]
    w_other(0)
    for copy in step_x:
        copy.wait_recv()
    step_send(93, -1, zh, xdev(1))
    w_forward(0)
    w_forward(2)
    w_across(2)
    w_own_x(3)
    for copy in step_o:
        copy.wait_recv()
    step_send(93, -1, 1 - zh, xdev(1))
    w_forward_other(0)
    w_own_x(1)
    for k in (-1, 0, 1):
        hand(k)
    i320 = lax.broadcasted_iota(jnp.int32, (320, 320), 0)
    k320 = lax.broadcasted_iota(jnp.int32, (320, 320), 1)
    tens = lax.shift_right_logical(i320 * 6554, 16)
    source = ((tens & 3) * 8 + lax.shift_right_logical(tens, 2)) * 10 + i320 - tens * 10
    perm = jnp.where(k320 == source, 1.0, 0.0).astype(F32).astype(BF16)

    def transpose(k):
        rows = ds((rank(k)[0] * 2 + rank(k)[1]) * 128, 128)
        for q in range(4):
            part = slice(320 * q, 320 * q + 320)
            hidt[part, rows] = mm(perm, hidf[rows, part], NT).astype(BF16)

    transpose(0)
    h_c.wait_recv()
    transpose(1)
    h_z.wait_recv()
    zrows = ds((rank(2)[0] * 2 + c) * 128, 128)
    h_f = send(26, hidf.at[zrows, :], hidf.at[zrows, :], core, 4)
    w_across_far(2)
    w_forward(3)
    w_across(3)
    w_other(1)
    w_done(0)
    hand(2)
    got(93, stepw.at[0:2])
    for k in range(8):
        stepa[0:16, 160 * k : 160 * k + 160] = stepw[k][:, 0:160].astype(F32)
    wf[:, 768:896] = stepa[...].T.astype(BF16)

    low = coli < 64
    causal = rowi >= coli
    anti = rowi <= coli
    tri = causal.astype(F32).astype(BF16)
    tri3 = jnp.concatenate([tri] * 3, axis=1)
    upper = anti.astype(F32).astype(BF16)
    strict = (rowi > coli).astype(F32).astype(BF16)
    sums4 = jnp.concatenate([upper] * 3 + [strict] * 3, axis=1)

    def pair(v, j):
        return jnp.where(low[0 : v.shape[0]], v[:, 2 * j : 2 * j + 1], v[:, 2 * j + 1 : 2 * j + 2])

    def blocks(f, unroll=True):
        if unroll:
            for b in range(4):
                f(b, pl.ds(b * 128, 128))
        else:
            def step(b, carry):
                f(b, ds(b * 128, 128))
                return carry

            lax.fori_loop(0, 4, step, 0)

    def steps(b, rows):
        projs[rows, ds(128 * c, 256, 128)] = mm(hidf[rows, :], wf[:, ds(640 + 128 * c, 256, 128)])
        pre = projs[rows, 128:256] + bias
        step = jnp.maximum(pre, 0.0) + jnp.log1p(jnp.exp(-jnp.abs(pre)))
        lg = neg * step
        cum = mm(tri3, jnp.concatenate(parts(lg, 3), axis=0))
        stp[rows, :] = step
        lgd[rows, :] = lg
        cums[rows, :] = cum
        cumt[b] = cum.T[0:16, :]
        dgs[b] = jnp.zeros((128, 128), F32)
        red[b] = jnp.zeros((384, 128), F32)

    def maps(b, rows):
        projs[rows, ds(256 - 256 * c, 128)] = mm(hidf[rows, :], wf[:, ds(896 - 256 * c, 128)])
        bm = jax.nn.silu(projs[rows, 0:128])
        cm = jax.nn.silu(projs[rows, 256:384])
        bmf[rows, :] = bm
        cmf[rows, :] = cm
        scores = mm3(cm, bm, NT)
        gs[b] = scores
        gts[b] = scores.T

    for k in range(4):
        if k == 3:
            h_f.wait_recv()
        b = rank(k)[0] * 2 + rank(k)[1]
        steps(b, ds(b * 128, 128))
    for j in range(5):
        cj = slice(128 * j, 128 * j + 128)
        for b in range(4):
            last_row = cums[128 * b + 127 : 128 * b + 128, :]
            tot[8 * b : 8 * b + 8, cj] = pair(jnp.broadcast_to(last_row, (8, 128)), j)
    tts[...] = tot[0:8, :] + tot[8:16, :] + tot[16:24, :] + tot[24:32, :]
    for k in (1, 2, 3):
        send(29, tts, ttr.at[k - 1], ydev(k), 7)

    transpose(2)
    transpose(3)
    w_forward(1)
    got(28, wf.at[:, ds(896 - 256 * c, 128)])
    maps(0, pl.ds(0, 128))
    w_across_far(3)
    maps(1, pl.ds(128, 128))
    maps(2, pl.ds(256, 128))
    w_forward_other(1)
    maps(3, pl.ds(384, 128))

    def total(b, cj):
        return tot[8 * b : 8 * b + 1, cj]

    def pair_forward(j):
        cj = slice(128 * j, 128 * j + 128)

        wide = slice(128 * j, min(128 * j + 256, 640))

        def project(b, rows):
            projv[rows, wide] = mm(hidf[rows, :], wf[:, wide])

        def local_part(b, rows):
            ce = pair(cums[rows, :], j)
            se = pair(stp[rows, :], j)
            ec = jnp.exp(ce)
            tl = jnp.exp(ce[127:128, :] - ce)
            val = jax.nn.silu(projv[rows, cj])
            xs = val * se
            sexp[rows, cj] = se
            ecs[rows, cj] = ec
            tls[rows, cj] = tl
            vv[rows, cj] = val
            xb[rows, cj] = xs.astype(BF16)
            x16 = (xs * tl).astype(BF16)
            o16 = (cot[rows, cj].astype(F32) * ec).astype(BF16)
            xt[rows, cj] = x16
            oe[rows, cj] = o16
            sl[b, :, cj] = mm(bmf[rows, :].astype(BF16), x16, TN)
            dl[b, :, cj] = mm(cmf[rows, :].astype(BF16), o16, TN)

        if j % 2 == 0:
            blocks(project)
        blocks(local_part)
        s = sl[0, :, cj]
        d = dl[3, :, cj]
        for b in range(1, 4):
            s = jnp.exp(total(b, cj)) * s + sl[b, :, cj]
            d = jnp.exp(total(3 - b, cj)) * d + dl[3 - b, :, cj]
        stt[0, :, cj] = s.astype(BF16)
        stt[1, :, cj] = d.astype(BF16)
        for k in (1, 2, 3):
            wraps = lax.div(y + k, 4)
            send(30 + j, stt.at[wraps, :, cj], str_.at[k - 1, :, cj], ydev(k), 8)

    def pair_inside(j):
        cj = slice(128 * j, 128 * j + 128)

        def inside(b, rows):
            cum = cums[rows, :]
            c0, c1 = cum[:, 2 * j : 2 * j + 1], cum[:, 2 * j + 1 : 2 * j + 2]
            r0, r1 = cumt[b, 2 * j : 2 * j + 1, :], cumt[b, 2 * j + 1 : 2 * j + 2, :]
            w0 = jnp.where(causal, jnp.exp(jnp.where(causal, c0 - r0, 0.0)), 0.0)
            w1 = jnp.where(causal, jnp.exp(jnp.where(causal, c1 - r1, 0.0)), 0.0)
            u0 = jnp.where(anti, jnp.exp(jnp.where(anti, r0 - c0, 0.0)), 0.0)
            u1 = jnp.where(anti, jnp.exp(jnp.where(anti, r1 - c1, 0.0)), 0.0)
            scores, scores_t = gs[b], gts[b]
            m = jnp.concatenate([scores * w0, scores * w1], axis=1).astype(BF16)
            mt = jnp.concatenate([scores_t * u0, scores_t * u1], axis=1).astype(BF16)
            x16 = xb[rows, cj]
            o16 = cot[rows, cj]
            zero = jnp.zeros_like(x16)
            xd = jnp.concatenate([jnp.where(low, x16, zero), jnp.where(low, zero, x16)], axis=0)
            od = jnp.concatenate([jnp.where(low, o16, zero), jnp.where(low, zero, o16)], axis=0)
            yy = mm(m, xd)
            pp = mm(o16, xd, NT)
            dx = mm(mt, od)
            dgs[b] = dgs[b] + w0 * pp[:, 0:128] + w1 * pp[:, 128:256]
            dxin[rows, cj] = dx
            q1s[rows, cj] = o16.astype(F32) * yy - x16.astype(F32) * dx

        blocks(inside)

    got(27, cot.at[0:384, :])
    w_done(2)
    pair_forward(2)
    pair_inside(2)
    pair_forward(3)
    pair_inside(3)
    w_done(3)
    pair_forward(4)
    pair_inside(4)
    for p in range(4):
        for q in range(4):
            hidx[320 * p + 80 * q : 320 * p + 80 * q + 80, :] = hidt[320 * q + 80 * p : 320 * q + 80 * p + 80, :]
    w_done(1)
    pair_forward(0)
    pair_inside(0)
    pair_forward(1)
    pair_inside(1)

    def turn(b, rows):
        dcf[rows, :] = mm3(dgs[b], bmf[rows, :], NN) + mm(oe[rows, :], sb[b], NT)
        dbf[rows, :] = mm3(dgs[b], cmf[rows, :], TN) + mm(xt[rows, :], db[b], NT)

    got(29, ttr)

    lanes = lax.broadcasted_iota(jnp.int32, (256, 128), 0)
    outl = lax.broadcasted_iota(jnp.int32, (256, 128), 1)

    def sums(z, j):
        hi = z.astype(BF16)
        lo = (z - hi.astype(F32)).astype(BF16)
        choose = (outl == 2 * j + lax.rem(lax.div(lanes, 64), 2)).astype(F32).astype(BF16)
        return mm(jnp.concatenate([hi, lo], axis=1), choose)

    yes = [jnp.where(y >= k, 1.0, 0.0).astype(F32) for k in (1, 2, 3)]
    no = [jnp.where(y + k <= 3, 1.0, 0.0).astype(F32) for k in (1, 2, 3)]
    inner = [jnp.zeros((8, 128), F32) for _ in range(4)]
    gain = [jnp.zeros((8, 128), F32)]

    def pair_outside(j):
        cj = slice(128 * j, 128 * j + 128)
        got(30 + j, str_.at[:, :, cj])
        t = [ttr[k, 0:1, cj] for k in range(3)]
        came = [str_[k, :, cj].astype(F32) for k in range(3)]
        s = yes[0] * came[0] + (yes[1] * jnp.exp(t[0])) * came[1] + (yes[2] * jnp.exp(t[0] + t[1])) * came[2]
        d = no[0] * came[2] + (no[1] * jnp.exp(t[2])) * came[1] + (no[2] * jnp.exp(t[2] + t[1])) * came[0]
        for b in (3, 2, 1, 0):
            db[b, :, cj] = d.astype(BF16)
            dd[b] = d
            d = jnp.exp(total(b, cj)) * d + dl[b, :, cj]
        for b in range(4):
            sb[b, :, cj] = s.astype(BF16)
            grown = jnp.exp(total(b, cj)) * s
            inner[b] = inner[b] + sums((grown * dd[b]).reshape(16, 8, 128).sum(axis=0), j)
            s = grown + sl[b, :, cj]

        def outside(b, rows):
            o = cot[rows, cj].astype(F32)
            yst = mm(cmf[rows, :].astype(BF16), sb[b, :, cj]) * ecs[rows, cj]
            dxst = mm(bmf[rows, :].astype(BF16), db[b, :, cj]) * tls[rows, cj]
            val = vv[rows, cj]
            dxs = dxin[rows, cj] + dxst
            z = jnp.concatenate([q1s[rows, cj] + o * yst, xb[rows, cj].astype(F32) * dxst, dxs * val], axis=0)
            red[b] = red[b] + sums(z, j)
            dval = dxs * sexp[rows, cj] + pair(skip, j) * o
            rr[rows, cj] = (dval * silu_grad(projv[rows, cj])).astype(BF16)
            gain[0] = gain[0] + sums((o * val).reshape(16, 8, 128).sum(axis=0), j)

        blocks(outside)

    class Stream:
        def __init__(self, base, group, parts, kind, bufs):
            self.base, self.group, self.parts, self.left = base, group, parts, hidx if kind else hidt
            self.dw, self.s1, self.r1, self.s2, self.r2, self.s3, self.r3, self.s4, self.r4, self.sd, self.rd = bufs
            self.index, self.dev, self.index2, self.dev2 = (y, ydev, x, xdev) if kind == 0 else (x, xdev, y, ydev)

        def send(self, i, src, dst, dev):
            return send(self.base + i, src, dst, dev, self.group)

        def block(self, i):
            rows = ds(lax.rem(self.index + i, 4) * 320, 320)
            for cols, target in self.parts:
                self.dw[rows, target] = mm(self.left[rows, :], rr[:, cols])
            return rows

        def first(self):
            rows = self.block(2)
            self.s1[...] = self.dw[rows, :].astype(BF16)
            self.one = (
                self.send(0, self.s1.at[0:160, :], self.r1.at[0], self.dev(1)),
                self.send(1, self.s1.at[160:320, :], self.r1.at[1], self.dev(-1)),
            )

        def rest(self):
            for i in (1, 3, 0):
                self.block(i)

        def second(self):
            nxt = lax.rem(self.index + 1, 4) * 320
            prv = lax.rem(self.index + 3, 4) * 320
            self.one[0].wait_recv()
            self.s2[0, 0:160, :] = (self.dw[ds(nxt, 160), :] + self.r1[0].astype(F32)).astype(BF16)
            self.s2[0, 160:320, :] = self.dw[ds(nxt + 160, 160), :].astype(BF16)
            self.send(2, self.s2.at[0], self.r2.at[0], self.dev(1))
            self.one[1].wait_recv()
            self.s2[1, 0:160, :] = self.dw[ds(prv, 160), :].astype(BF16)
            self.s2[1, 160:320, :] = (self.dw[ds(prv + 160, 160), :] + self.r1[1].astype(F32)).astype(BF16)
            self.send(2, self.s2.at[1], self.r2.at[1], self.dev(-1))

        def third(self):
            got(self.base + 2, self.r2)
            here = ds(self.index * 320, 320)
            summed = self.dw[here, :] + self.r2[0].astype(F32) + self.r2[1].astype(F32)
            self.dw[here, :] = summed
            self.s3[...] = summed.astype(BF16)
            for k in (2, 1, 3):
                piece = self.s3.at[ds(lax.rem(self.index2 + k, 4) * 80, 80), :]
                self.send(3, piece, self.r3.at[k - 1], self.dev2(k))

        def fourth(self):
            got(self.base + 3, self.r3)
            rows = ds(self.index * 320 + self.index2 * 80, 80)
            self.s4[...] = self.dw[rows, :] + self.r3[0].astype(F32) + self.r3[1].astype(F32) + self.r3[2].astype(F32)
            self.four = self.send(4, self.s4.at[ds((1 - zh) * 40, 40), :], self.r4, zpair)

        def owners(self):
            self.four.wait_recv()
            chunk = self.s4[ds(zh * 40, 40), :] + self.r4[...]
            for i in range(4):
                self.sd[i, 0:10, :] = chunk[10 * i : 10 * i + 10, :]
            self.rd[g] = self.sd[r]
            for k in (2, 3, 1):
                zlk, ck, dev = rank(k)
                self.send(5, self.sd.at[zlk * 2 + ck], self.rd.at[g], dev)

        def finish(self):
            got(self.base + 5, self.rd.at[0:3])

        def close(self):
            sent(self.group, self.dw.at[0:688, :])

    tiles = [slice(128 * t, 128 * t + 128) for t in range(5)] + [slice(768, 896), ds(lane0, 128)]
    kinds = (0, 1, 0, 1, 0, 1, 0)
    p0, p1, p2, p3, p4, st, mp = streams = [
        Stream(46 + 6 * t, 13 + t, [(tiles[t], slice(0, 128))], kinds[t], bufs[11 * t : 11 * t + 11]) for t in range(7)
    ]

    pair_outside(2)
    p2.first()
    pair_outside(3)
    p3.first()
    p2.rest()
    pair_outside(4)
    p4.first()
    p3.rest()
    pair_outside(0)
    p0.first()
    p2.second()
    pair_outside(1)
    p1.first()
    p3.second()

    blocks(turn)
    first = c == 0
    t1s[...] = jnp.where(first, dcf[...], dbf[...])
    t1 = send(35, t1s, t1r, core, 9)
    p4.rest()
    p4.second()

    ownl = coli < 10
    bias_sum = decay_sum = jnp.zeros((8, 128), F32)
    for b in range(4):
        rows = slice(128 * b, 128 * b + 128)
        dlog = mm(sums4, jnp.concatenate(parts(red[b, 0:128], 3) + parts(red[b, 128:256], 3), axis=0))
        dlog = jnp.where(ownl, dlog + inner[b].sum(axis=0, keepdims=True), 0.0)
        ddt = (red[b, 256:384] + neg * dlog) * jax.nn.sigmoid(projs[rows, 128:256] + bias)
        ddt = jnp.where(ownl, ddt, 0.0)
        rr[rows, 768:896] = ddt.astype(BF16)
        bias_sum = bias_sum + ddt.reshape(16, 8, 128).sum(axis=0)
        decay_sum = decay_sum + (dlog * lgd[rows, :]).reshape(16, 8, 128).sum(axis=0)
    place = jnp.where(jnp.logical_and(rowi < 10, coli == rowi + 10 * g), 1.0, 0.0).astype(F32)
    st.first()
    row8 = lax.broadcasted_iota(jnp.int32, (8, 128), 0)
    packed = jnp.where(
        row8 == 0, bias_sum.sum(axis=0, keepdims=True),
        jnp.where(row8 == 1, decay_sum.sum(axis=0, keepdims=True),
                  jnp.where(row8 == 2, gain[0].sum(axis=0, keepdims=True), 0.0)),
    )
    heads_y[y] = mm(packed, place, NN, highest)
    for k in (1, 2, 3):
        send(38, heads_y.at[y], heads_y.at[y], ydev(k), 10)
    t1.wait_recv()
    mixed = jnp.where(first, dbf[...], dcf[...]) + t1r[...]
    rr[:, ds(lane0, 128)] = (mixed * silu_grad(projs[:, ds(256 * c, 128, 128)])).astype(BF16)
    rr[:, ds(896 - 256 * c, 128)] = jnp.zeros((512, 128), BF16)
    mp.first()

    def token(half):
        rows = ds(half * 256, 256)
        for n in range(5):
            part = slice(256 * n, 256 * n + 256)
            hgp[rows, part] = mm(rr[rows, :], wf[part, :], NT)

    mate_row = ds((zl * 2 + 1 - c) * 128, 128)
    far_mate = ds(((1 - zl) * 2 + 1 - c) * 128, 128)
    far_row = ds(((1 - zl) * 2 + c) * 128, 128)
    token(1 - zl)
    hgs[1] = hgp[far_mate, :].astype(BF16)
    hg_far = send(43, hgs.at[1], hgr.at[1], core, 11)
    p0.rest()
    p0.second()
    p1.rest()
    p1.second()
    p2.third()
    hg_far.wait_recv()
    hgs[2] = (hgp[far_row, :] + hgr[1].astype(F32)).astype(BF16)
    hg_z = send(44, hgs.at[2], hgr.at[2], rank(2)[2], 11)
    st.rest()
    st.second()
    p3.third()
    mp.rest()
    mp.second()
    p4.third()
    token(zl)
    hgs[0] = hgp[mate_row, :].astype(BF16)
    hg_near = send(42, hgs.at[0], hgr.at[0], core, 11)
    p2.fourth()
    p0.third()
    p1.third()
    p3.fourth()
    got(38, heads_y.at[0:3])
    heads_x[x] = (heads_y[0] + heads_y[1]) + (heads_y[2] + heads_y[3])
    for k in (1, 2, 3):
        send(39, heads_x.at[x], heads_x.at[x], xdev(k), 10)
    st.third()
    mp.third()
    p4.fourth()
    p2.owners()
    p0.fourth()
    got(39, heads_x.at[0:3])
    heads_z[zh] = (heads_x[0] + heads_x[1]) + (heads_x[2] + heads_x[3])
    head_z = send(40, heads_z.at[zh], heads_z.at[zh], zpair, 10)
    p3.owners()
    p1.fourth()
    p4.owners()
    st.fourth()
    mp.fourth()
    hg_near.wait_recv()
    hg_z.wait_recv()
    hgo[...] = (hgp[here_id, :] + hgr[0].astype(F32) + hgr[2].astype(F32)).astype(BF16)
    hg_out = pltpu.make_async_copy(hgo, hg_ref, ls.at[5])
    hg_out.start()
    p0.owners()
    p1.owners()
    st.owners()
    mp.owners()
    head_z.wait_recv()
    heads_g[r] = heads_z[0] + heads_z[1]
    for k in (1, 2, 3):
        send(41, heads_g.at[r], heads_g.at[r], rank(k)[2], 10)
    got(41, heads_g.at[0:3])
    hdo[...] = (heads_g[0] + heads_g[1]) + (heads_g[2] + heads_g[3])
    hd_out = pltpu.make_async_copy(hdo, hd_ref, ls.at[6])
    hd_out.start()
    for t, stream in ((2, p2), (3, p3), (4, p4), (0, p0), (1, p1)):
        stream.finish()
        for k in range(4):
            wgo[:, 640 * k + 128 * t : 640 * k + 128 * t + 128] = stream.rd[k, 0:10, :]
    st.finish()
    for k in range(4):
        wgo[:, 2816 + 10 * k : 2826 + 10 * k] = st.rd[k, 0:10, 0:10]
    mp.finish()
    wgo[:, 2560:2688] = mp.rd[0, 0:10, :] + mp.rd[2, 0:10, :]
    wgo[:, 2688:2816] = mp.rd[1, 0:10, :] + mp.rd[3, 0:10, :]
    wg_out = pltpu.make_async_copy(wgo, wg_ref, ls.at[7])
    wg_out.start()
    for m in range(4):
        sent(m, wf.at[0:1120, cols(m)])
    sent(4, hidf.at[0:384, :])
    sent(20, stepw.at[0:7])
    sent(5, cot.at[0:384, :])
    sent(6, wf.at[:, ds(lane0, 128)])
    sent(7, ttr)
    sent(8, str_)
    sent(9, t1r)
    sent(10, bmf.at[0:80, :])
    sent(11, hgs)
    for stream in streams:
        stream.close()
    hg_out.wait()
    hd_out.wait()
    wg_out.wait()


def scratch():
    def v(shape, dtype=F32):
        return pltpu.VMEM(shape, dtype)

    def stream(n):
        return [
            v((D, n)), v((320, n), BF16), v((2, 160, n), BF16), v((2, 320, n), BF16), v((2, 320, n), BF16),
            v((320, n), BF16), v((3, 80, n), BF16), v((80, n)), v((40, n)), v((4, 16, n)), v((4, 16, n)),
        ]

    wide, wide16 = v((512, COLS)), v((512, COLS), BF16)
    thin = v((512, 128))
    return [
        v((8, 16, 256), BF16), v((128, D)),
        v((512, D), BF16), v((D, 512), BF16), v((D, 512), BF16), wide16, v((160, 2856), BF16), v((D, 1024), BF16),
        v((512, 384)), wide, thin, thin, thin, thin, v((4, 16, 128)), thin,
        v((4, 128, 128)), v((4, 128, 128)), v((4, 128, 128)),
        wide, wide, wide, wide, wide16, wide16, wide16, v((32, COLS)),
        v((4, 128, COLS)), v((4, 128, COLS)), v((2, 128, COLS), BF16), v((8, COLS)),
        v((3, 128, COLS), BF16), v((3, 8, COLS)), wide, wide, thin, thin,
        v((4, 128, COLS), BF16), v((4, 128, COLS), BF16), v((4, 128, 128)), v((4, 384, 128)),
        v((512, 1024), BF16), thin, thin,
        v((512, D)), v((3, 128, D), BF16), v((3, 128, D), BF16),
        v((4, 8, 128)), v((4, 8, 128)), v((2, 8, 128)), v((4, 8, 128)),
        v((128, D), BF16), v((10, 2856)), v((8, 128)),
        pltpu.SemaphoreType.DMA((21,)), pltpu.SemaphoreType.DMA((94,)), pltpu.SemaphoreType.DMA((8,)),
        *(buf for _ in range(7) for buf in stream(128)),
    ]


def emit(hg_ref, wg_ref, hd_ref, hg_out, wg_out, hd_out):
    hg_out[...] = hg_ref[...]
    wg_out[...] = wg_ref[...]
    hd_out[...] = hd_ref[0:3, 0:HEADS]


def body(hidden, output_grad, input_weight, step_bias, decay_log, skip_gain):
    anyspace = pl.BlockSpec(memory_space=pl.ANY)
    vmem = pl.BlockSpec(memory_space=pltpu.VMEM)
    hg, wg, hd = pl.pallas_call(
        kernel,
        out_shape=(
            jax.ShapeDtypeStruct((128, D), BF16),
            jax.ShapeDtypeStruct((10, 2856), F32),
            jax.ShapeDtypeStruct((8, 128), F32),
        ),
        in_specs=[anyspace, anyspace, anyspace, vmem, vmem, vmem],
        out_specs=(anyspace, anyspace, anyspace),
        scratch_shapes=scratch(),
        compiler_params=pltpu.CompilerParams(has_side_effects=True, collective_id=0, vmem_limit_bytes=64000000),
    )(hidden[0], output_grad[0], input_weight, step_bias[None], decay_log[None], skip_gain[None])
    hg, wg, hd = pl.pallas_call(
        emit,
        out_shape=(
            jax.ShapeDtypeStruct((128, D), BF16),
            jax.ShapeDtypeStruct((10, 2856), F32),
            jax.ShapeDtypeStruct((3, HEADS), F32),
        ),
        in_specs=[vmem, vmem, vmem],
        out_specs=(vmem, vmem, vmem),
    )(hg, wg, hd)
    return (hg[None], wg, hd)


def solution(mesh):
    torus = Mesh(
        mesh.devices.reshape(4, 2, 2, 4, 2), ("seq_0", "seq_1", "seq_2", "zero_0", "zero_1")
    )
    in_specs = (P(ZERO, SEQ, None), P(ZERO, SEQ, None), P(ZERO, None), P(), P(), P())
    out_specs = (P(ZERO, SEQ, None), P(SEQ_ZERO, None), P())
    return jax.shard_map(body, mesh=torus, in_specs=in_specs, out_specs=out_specs, check_vma=False)
```

```python
import functools

import jax
import jax.numpy as jnp
from jax import lax
from jax.experimental import pallas as pl
from jax.experimental.pallas import tpu as pltpu
from jax.sharding import Mesh
from jax.sharding import PartitionSpec as P

HEADS = 40
STATE = 128
INNER = 2560
D = 1280
COLS = 640
ZERO = ("zero_0", "zero_1")
SEQ = ("seq_0", "seq_1", "seq_2")
SEQ_ZERO = ("seq_0", "seq_1", "seq_2", "zero_0", "zero_1")
MESH = pl.DeviceIdType.MESH
F32 = jnp.float32
BF16 = jnp.bfloat16
highest = lax.Precision.HIGHEST
NN = (((1,), (0,)), ((), ()))
NT = (((1,), (1,)), ((), ()))
TN = (((0,), (0,)), ((), ()))


def mm(a, b, dims=NN, precision=None):
    return lax.dot_general(a, b, dims, preferred_element_type=F32, precision=precision)


def parts(v, count):
    out = []
    for _ in range(count):
        out.append(v.astype(BF16))
        v = v - out[-1].astype(F32)
    return out


def mm3(a, b, dims=NN):
    (ah, al), (bh, bl) = parts(a, 2), parts(b, 2)
    (ka,), (kb,) = dims[0]
    return mm(jnp.concatenate([ah, al, ah], axis=ka), jnp.concatenate([bh, bh, bl], axis=kb), dims)


def ds(start, size, align=None):
    return pl.ds(pl.multiple_of(start, align or size), size)


def silu_grad(v):
    sig = jax.nn.sigmoid(v)
    return sig * (1.0 + v * (1.0 - sig))


def kernel(
    hid_ref, cot_ref, w_ref, bias_ref, decay_ref, skip_ref,
    hg_ref, wg_ref, hd_ref,
    stepw, stepa, hidf, hidt, hidx, cot, wraw, wf, projs, projv, bmf, cmf, lgd, cums, cumt, stp, gs, gts, dgs,
    sexp, ecs, tls, vv, xb, xt, oe, tot,
    sl, dl, stt, tts, str_, ttr, q1s, dxin, dbf, dcf, sb, db, dd, red,
    rr, t1s, t1r, hgp, hgs, hgr,
    heads_y, heads_x, heads_z, heads_g, hgo, wgo, hdo,
    ss, rs, ls, *bufs,
):
    y, zl, c = (lax.axis_index(n) for n in SEQ)
    x, zh = (lax.axis_index(n) for n in ZERO)
    r = zl * 2 + c
    a = lax.rem(zl + zh, 2)
    g = a * 2 + c

    def send(i, src, dst, where, group):
        copy = pltpu.make_async_remote_copy(
            src_ref=src, dst_ref=dst, send_sem=ss.at[group], recv_sem=rs.at[i],
            device_id=where, device_id_type=MESH,
        )
        copy.start()
        return copy

    def bytes_of(ref, i=0, group=0):
        return pltpu.make_async_remote_copy(
            src_ref=ref, dst_ref=ref, send_sem=ss.at[group], recv_sem=rs.at[i],
            device_id={"seq_2": 1 - c}, device_id_type=MESH,
        )

    def got(i, ref):
        bytes_of(ref, i=i).wait_recv()

    def sent(group, ref):
        bytes_of(ref, group=group).wait_send()

    def rank(k):
        zlk = lax.rem(zl + k // 2, 2)
        ck = lax.rem(c + k % 2, 2)
        return zlk, ck, {"seq_1": zlk, "seq_2": ck}

    def xdev(k):
        return {"zero_0": lax.rem(x + k + 4, 4)}

    def ydev(k):
        return {"seq_0": lax.rem(y + k + 4, 4)}

    zpair = {"seq_1": 1 - zl, "zero_1": 1 - zh}
    core = {"seq_2": 1 - c}
    here_id = ds(r * 128, 128)

    def shard(xk, zk, lo=0, size=160):
        return ds((lax.rem(xk + 4, 4) * 2 + zk) * 160 + lo, size, 16)

    own = shard(x, zh)
    lane0 = 640 + 256 * c
    local = [
        pltpu.make_async_copy(w_ref, wraw, ls.at[0]),
        pltpu.make_async_copy(w_ref.at[:, ds(g * COLS, COLS, 128)], wf.at[own, 0:640], ls.at[1]),
        pltpu.make_async_copy(w_ref.at[:, ds(2560 + 128 * c, 128)], wf.at[own, ds(lane0, 128)], ls.at[2]),
        pltpu.make_async_copy(hid_ref, hidf.at[here_id, :], ls.at[3]),
        pltpu.make_async_copy(cot_ref.at[:, ds(g * COLS, COLS, 128)], cot.at[here_id, :], ls.at[4]),
    ]
    for copy in local:
        copy.start()

    barrier = pltpu.get_barrier_semaphore()

    def greet(dev):
        pl.semaphore_signal(barrier, inc=1, device_id=dev, device_id_type=MESH)

    greet(zpair)
    for k in (1, 2, 3):
        greet(xdev(k))
        greet(ydev(k))
        greet(rank(k)[2])
    coli = lax.broadcasted_iota(jnp.int32, (128, 128), 1)
    rowi = lax.broadcasted_iota(jnp.int32, (128, 128), 0)
    local[0].wait()
    stepa[...] = jnp.zeros_like(stepa)
    tail = jnp.concatenate([wraw[:, 2816:2856].astype(F32), jnp.zeros((160, 88), F32)], axis=1)
    tail = pltpu.roll(tail, lax.rem(128 - 10 * g, 128), 1)
    keep10 = lax.broadcasted_iota(jnp.int32, (160, 128), 1) < 10
    tail = jnp.concatenate([jnp.where(keep10, tail, 0.0), jnp.zeros((96, 128), F32)], axis=0)
    stepw[x * 2 + zh] = tail.T[0:16, :].astype(BF16)

    def lanes10(ref):
        full = jnp.concatenate([ref[...], jnp.zeros((1, 88), F32)], axis=1)
        return pltpu.roll(jnp.broadcast_to(full, (8, 128)), lax.rem(128 - 10 * g, 128), 1)[0:1, :]

    bias = lanes10(bias_ref)
    neg = -jnp.exp(lanes10(decay_ref))
    skip = lanes10(skip_ref)
    for copy in local[1:]:
        copy.wait()
    pl.semaphore_wait(barrier, 10)

    def cols(m):
        return (ds(lane0, 128), slice(0, 256), slice(256, 512), slice(512, 640))[m]

    w = {}

    def wsend(m, i, rows, dev):
        ref = wf.at[rows, cols(m)]
        slot = min(i, 5) if m < 2 else {1: 1, 2: 2, 5: 3, 6: 4}.get(i, 5)
        w[m, i] = send(6 * m + slot, ref, ref, dev, m)

    def w_own_x(m):
        wsend(m, 1, own, xdev(1))
        wsend(m, 2, own, xdev(-1))

    def w_own_z(m):
        wsend(m, 0, own, zpair)

    def w_other(m):
        w[m, 0].wait_recv()
        wsend(m, 3, shard(x, 1 - zh), xdev(1))
        wsend(m, 4, shard(x, 1 - zh), xdev(-1))

    def w_forward(m):
        w[m, 1].wait_recv()
        wsend(m, 5, shard(x - 1, zh, 0, 80), xdev(1))
        w[m, 2].wait_recv()
        wsend(m, 6, shard(x + 1, zh, 80, 80), xdev(-1))

    def w_forward_other(m):
        w[m, 3].wait_recv()
        wsend(m, 7, shard(x - 1, 1 - zh, 0, 80), xdev(1))
        w[m, 4].wait_recv()
        wsend(m, 8, shard(x + 1, 1 - zh, 80, 80), xdev(-1))

    def w_across(m):
        wsend(m, 3, shard(x - 1, zh), zpair)
        wsend(m, 4, shard(x + 1, zh), zpair)

    def w_across_far(m):
        w[m, 5].wait_recv()
        wsend(m, 7, shard(x + 2, zh, 0, 80), zpair)
        w[m, 6].wait_recv()
        wsend(m, 8, shard(x + 2, zh, 80, 80), zpair)

    def w_done(m):
        got(6 * m + 5, wf.at[0 : 320 if m < 2 else 640, cols(m)])

    def step_send(i, xk, zk, dev):
        ref = stepw.at[lax.rem(x + xk + 4, 4) * 2 + zk]
        return send(i, ref, ref, dev, 20)

    def hand(k):
        ref = wf.at[ds(lax.rem(x + k + 4, 4) * 320, 320), ds(lane0, 128)]
        send(28, ref, ref, core, 6)

    step_z = step_send(88, 0, zh, zpair)
    step_x = [step_send(89, 0, zh, xdev(1)), step_send(90, 0, zh, xdev(-1))]
    w_own_z(0)
    w_own_x(0)
    h_z = send(24, hid_ref, hidf.at[here_id, :], rank(2)[2], 4)
    w_own_x(2)
    w_own_z(1)
    h_c = send(25, hid_ref, hidf.at[here_id, :], core, 4)
    for k in (2, 3, 1):
        zlk, ck, dev = rank(k)
        gk = lax.rem(zlk + zh, 2) * 2 + ck
        send(27, cot_ref.at[:, ds(gk * COLS, COLS, 128)], cot.at[here_id, :], dev, 5)
    w_own_z(2)
    w_own_z(3)
    step_z.wait_recv()
    step_o = [step_send(91, 0, 1 - zh, xdev(1)), step_send(92, 0, 1 - zh, xdev(-1))]
    w_other(0)
    for copy in step_x:
        copy.wait_recv()
    step_send(93, -1, zh, xdev(1))
    w_forward(0)
    w_forward(2)
    w_across(2)
    w_own_x(3)
    for copy in step_o:
        copy.wait_recv()
    step_send(93, -1, 1 - zh, xdev(1))
    w_forward_other(0)
    w_own_x(1)
    for k in (-1, 0, 1):
        hand(k)
    i320 = lax.broadcasted_iota(jnp.int32, (320, 320), 0)
    k320 = lax.broadcasted_iota(jnp.int32, (320, 320), 1)
    tens = lax.shift_right_logical(i320 * 6554, 16)
    source = ((tens & 3) * 8 + lax.shift_right_logical(tens, 2)) * 10 + i320 - tens * 10
    perm = jnp.where(k320 == source, 1.0, 0.0).astype(F32).astype(BF16)

    def transpose(k):
        rows = ds((rank(k)[0] * 2 + rank(k)[1]) * 128, 128)
        for q in range(4):
            part = slice(320 * q, 320 * q + 320)
            hidt[part, rows] = mm(perm, hidf[rows, part], NT).astype(BF16)

    transpose(0)
    h_c.wait_recv()
    transpose(1)
    h_z.wait_recv()
    zrows = ds((rank(2)[0] * 2 + c) * 128, 128)
    h_f = send(26, hidf.at[zrows, :], hidf.at[zrows, :], core, 4)
    w_across_far(2)
    w_forward(3)
    w_across(3)
    w_other(1)
    w_done(0)
    hand(2)
    got(93, stepw.at[0:2])
    for k in range(8):
        stepa[0:16, 160 * k : 160 * k + 160] = stepw[k][:, 0:160].astype(F32)
    wf[:, 768:896] = stepa[...].T.astype(BF16)

    low = coli < 64
    causal = rowi >= coli
    anti = rowi <= coli
    tri = causal.astype(F32).astype(BF16)
    tri3 = jnp.concatenate([tri] * 3, axis=1)
    upper = anti.astype(F32).astype(BF16)
    strict = (rowi > coli).astype(F32).astype(BF16)
    sums4 = jnp.concatenate([upper] * 3 + [strict] * 3, axis=1)

    def pair(v, j):
        return jnp.where(low[0 : v.shape[0]], v[:, 2 * j : 2 * j + 1], v[:, 2 * j + 1 : 2 * j + 2])

    def blocks(f, unroll=True):
        if unroll:
            for b in range(4):
                f(b, pl.ds(b * 128, 128))
        else:
            def step(b, carry):
                f(b, ds(b * 128, 128))
                return carry

            lax.fori_loop(0, 4, step, 0)

    def steps(b, rows):
        projs[rows, ds(128 * c, 256, 128)] = mm(hidf[rows, :], wf[:, ds(640 + 128 * c, 256, 128)])
        pre = projs[rows, 128:256] + bias
        step = jnp.maximum(pre, 0.0) + jnp.log1p(jnp.exp(-jnp.abs(pre)))
        lg = neg * step
        cum = mm(tri3, jnp.concatenate(parts(lg, 3), axis=0))
        stp[rows, :] = step
        lgd[rows, :] = lg
        cums[rows, :] = cum
        cumt[b] = cum.T[0:16, :]
        dgs[b] = jnp.zeros((128, 128), F32)
        red[b] = jnp.zeros((384, 128), F32)

    def maps(b, rows):
        projs[rows, ds(256 - 256 * c, 128)] = mm(hidf[rows, :], wf[:, ds(896 - 256 * c, 128)])
        bm = jax.nn.silu(projs[rows, 0:128])
        cm = jax.nn.silu(projs[rows, 256:384])
        bmf[rows, :] = bm
        cmf[rows, :] = cm
        scores = mm3(cm, bm, NT)
        gs[b] = scores
        gts[b] = scores.T

    for k in range(4):
        if k == 3:
            h_f.wait_recv()
        b = rank(k)[0] * 2 + rank(k)[1]
        steps(b, ds(b * 128, 128))
    for j in range(5):
        cj = slice(128 * j, 128 * j + 128)
        for b in range(4):
            last_row = cums[128 * b + 127 : 128 * b + 128, :]
            tot[8 * b : 8 * b + 8, cj] = pair(jnp.broadcast_to(last_row, (8, 128)), j)
    tts[...] = tot[0:8, :] + tot[8:16, :] + tot[16:24, :] + tot[24:32, :]
    for k in (1, 2, 3):
        send(29, tts, ttr.at[k - 1], ydev(k), 7)

    transpose(2)
    transpose(3)
    w_forward(1)
    got(28, wf.at[:, ds(896 - 256 * c, 128)])
    maps(0, pl.ds(0, 128))
    w_across_far(3)
    maps(1, pl.ds(128, 128))
    maps(2, pl.ds(256, 128))
    w_forward_other(1)
    maps(3, pl.ds(384, 128))

    def total(b, cj):
        return tot[8 * b : 8 * b + 1, cj]

    def pair_forward(j):
        cj = slice(128 * j, 128 * j + 128)

        wide = slice(128 * j, min(128 * j + 256, 640))

        def project(b, rows):
            projv[rows, wide] = mm(hidf[rows, :], wf[:, wide])

        def local_part(b, rows):
            ce = pair(cums[rows, :], j)
            se = pair(stp[rows, :], j)
            ec = jnp.exp(ce)
            tl = jnp.exp(ce[127:128, :] - ce)
            val = jax.nn.silu(projv[rows, cj])
            xs = val * se
            sexp[rows, cj] = se
            ecs[rows, cj] = ec
            tls[rows, cj] = tl
            vv[rows, cj] = val
            xb[rows, cj] = xs.astype(BF16)
            x16 = (xs * tl).astype(BF16)
            o16 = (cot[rows, cj].astype(F32) * ec).astype(BF16)
            xt[rows, cj] = x16
            oe[rows, cj] = o16
            sl[b, :, cj] = mm(bmf[rows, :].astype(BF16), x16, TN)
            dl[b, :, cj] = mm(cmf[rows, :].astype(BF16), o16, TN)

        if j % 2 == 0:
            blocks(project)
        blocks(local_part)
        s = sl[0, :, cj]
        d = dl[3, :, cj]
        for b in range(1, 4):
            s = jnp.exp(total(b, cj)) * s + sl[b, :, cj]
            d = jnp.exp(total(3 - b, cj)) * d + dl[3 - b, :, cj]
        stt[0, :, cj] = s.astype(BF16)
        stt[1, :, cj] = d.astype(BF16)
        for k in (1, 2, 3):
            wraps = lax.div(y + k, 4)
            send(30 + j, stt.at[wraps, :, cj], str_.at[k - 1, :, cj], ydev(k), 8)

    def pair_inside(j):
        cj = slice(128 * j, 128 * j + 128)

        def inside(b, rows):
            cum = cums[rows, :]
            c0, c1 = cum[:, 2 * j : 2 * j + 1], cum[:, 2 * j + 1 : 2 * j + 2]
            r0, r1 = cumt[b, 2 * j : 2 * j + 1, :], cumt[b, 2 * j + 1 : 2 * j + 2, :]
            w0 = jnp.where(causal, jnp.exp(jnp.where(causal, c0 - r0, 0.0)), 0.0)
            w1 = jnp.where(causal, jnp.exp(jnp.where(causal, c1 - r1, 0.0)), 0.0)
            u0 = jnp.where(anti, jnp.exp(jnp.where(anti, r0 - c0, 0.0)), 0.0)
            u1 = jnp.where(anti, jnp.exp(jnp.where(anti, r1 - c1, 0.0)), 0.0)
            scores, scores_t = gs[b], gts[b]
            m = jnp.concatenate([scores * w0, scores * w1], axis=1).astype(BF16)
            mt = jnp.concatenate([scores_t * u0, scores_t * u1], axis=1).astype(BF16)
            x16 = xb[rows, cj]
            o16 = cot[rows, cj]
            zero = jnp.zeros_like(x16)
            xd = jnp.concatenate([jnp.where(low, x16, zero), jnp.where(low, zero, x16)], axis=0)
            od = jnp.concatenate([jnp.where(low, o16, zero), jnp.where(low, zero, o16)], axis=0)
            yy = mm(m, xd)
            pp = mm(o16, xd, NT)
            dx = mm(mt, od)
            dgs[b] = dgs[b] + w0 * pp[:, 0:128] + w1 * pp[:, 128:256]
            dxin[rows, cj] = dx
            q1s[rows, cj] = o16.astype(F32) * yy - x16.astype(F32) * dx

        blocks(inside)

    got(27, cot.at[0:384, :])
    w_done(2)
    pair_forward(2)
    pair_inside(2)
    pair_forward(3)
    pair_inside(3)
    w_done(3)
    pair_forward(4)
    pair_inside(4)
    for p in range(4):
        for q in range(4):
            hidx[320 * p + 80 * q : 320 * p + 80 * q + 80, :] = hidt[320 * q + 80 * p : 320 * q + 80 * p + 80, :]
    w_done(1)
    pair_forward(0)
    pair_inside(0)
    pair_forward(1)
    pair_inside(1)

    def turn(b, rows):
        dcf[rows, :] = mm3(dgs[b], bmf[rows, :], NN) + mm(oe[rows, :], sb[b], NT)
        dbf[rows, :] = mm3(dgs[b], cmf[rows, :], TN) + mm(xt[rows, :], db[b], NT)

    got(29, ttr)

    lanes = lax.broadcasted_iota(jnp.int32, (256, 128), 0)
    outl = lax.broadcasted_iota(jnp.int32, (256, 128), 1)

    def sums(z, j):
        hi = z.astype(BF16)
        lo = (z - hi.astype(F32)).astype(BF16)
        choose = (outl == 2 * j + lax.rem(lax.div(lanes, 64), 2)).astype(F32).astype(BF16)
        return mm(jnp.concatenate([hi, lo], axis=1), choose)

    yes = [jnp.where(y >= k, 1.0, 0.0).astype(F32) for k in (1, 2, 3)]
    no = [jnp.where(y + k <= 3, 1.0, 0.0).astype(F32) for k in (1, 2, 3)]
    inner = [jnp.zeros((8, 128), F32) for _ in range(4)]
    gain = [jnp.zeros((8, 128), F32)]

    def pair_outside(j):
        cj = slice(128 * j, 128 * j + 128)
        got(30 + j, str_.at[:, :, cj])
        t = [ttr[k, 0:1, cj] for k in range(3)]
        came = [str_[k, :, cj].astype(F32) for k in range(3)]
        s = yes[0] * came[0] + (yes[1] * jnp.exp(t[0])) * came[1] + (yes[2] * jnp.exp(t[0] + t[1])) * came[2]
        d = no[0] * came[2] + (no[1] * jnp.exp(t[2])) * came[1] + (no[2] * jnp.exp(t[2] + t[1])) * came[0]
        for b in (3, 2, 1, 0):
            db[b, :, cj] = d.astype(BF16)
            dd[b] = d
            d = jnp.exp(total(b, cj)) * d + dl[b, :, cj]
        for b in range(4):
            sb[b, :, cj] = s.astype(BF16)
            grown = jnp.exp(total(b, cj)) * s
            inner[b] = inner[b] + sums((grown * dd[b]).reshape(16, 8, 128).sum(axis=0), j)
            s = grown + sl[b, :, cj]

        def outside(b, rows):
            o = cot[rows, cj].astype(F32)
            yst = mm(cmf[rows, :].astype(BF16), sb[b, :, cj]) * ecs[rows, cj]
            dxst = mm(bmf[rows, :].astype(BF16), db[b, :, cj]) * tls[rows, cj]
            val = vv[rows, cj]
            dxs = dxin[rows, cj] + dxst
            z = jnp.concatenate([q1s[rows, cj] + o * yst, xb[rows, cj].astype(F32) * dxst, dxs * val], axis=0)
            red[b] = red[b] + sums(z, j)
            dval = dxs * sexp[rows, cj] + pair(skip, j) * o
            rr[rows, cj] = (dval * silu_grad(projv[rows, cj])).astype(BF16)
            gain[0] = gain[0] + sums((o * val).reshape(16, 8, 128).sum(axis=0), j)

        blocks(outside)

    class Stream:
        def __init__(self, base, group, parts, kind, bufs):
            self.base, self.group, self.parts, self.left = base, group, parts, hidx if kind else hidt
            self.dw, self.s1, self.r1, self.s2, self.r2, self.s3, self.r3, self.s4, self.r4, self.sd, self.rd = bufs
            self.index, self.dev, self.index2, self.dev2 = (y, ydev, x, xdev) if kind == 0 else (x, xdev, y, ydev)

        def send(self, i, src, dst, dev):
            return send(self.base + i, src, dst, dev, self.group)

        def block(self, i):
            rows = ds(lax.rem(self.index + i, 4) * 320, 320)
            for cols, target in self.parts:
                self.dw[rows, target] = mm(self.left[rows, :], rr[:, cols])
            return rows

        def first(self):
            rows = self.block(2)
            self.s1[...] = self.dw[rows, :].astype(BF16)
            self.one = (
                self.send(0, self.s1.at[0:160, :], self.r1.at[0], self.dev(1)),
                self.send(1, self.s1.at[160:320, :], self.r1.at[1], self.dev(-1)),
            )

        def rest(self):
            for i in (1, 3, 0):
                self.block(i)

        def second(self):
            nxt = lax.rem(self.index + 1, 4) * 320
            prv = lax.rem(self.index + 3, 4) * 320
            self.one[0].wait_recv()
            self.s2[0, 0:160, :] = (self.dw[ds(nxt, 160), :] + self.r1[0].astype(F32)).astype(BF16)
            self.s2[0, 160:320, :] = self.dw[ds(nxt + 160, 160), :].astype(BF16)
            self.send(2, self.s2.at[0], self.r2.at[0], self.dev(1))
            self.one[1].wait_recv()
            self.s2[1, 0:160, :] = self.dw[ds(prv, 160), :].astype(BF16)
            self.s2[1, 160:320, :] = (self.dw[ds(prv + 160, 160), :] + self.r1[1].astype(F32)).astype(BF16)
            self.send(2, self.s2.at[1], self.r2.at[1], self.dev(-1))

        def third(self):
            got(self.base + 2, self.r2)
            here = ds(self.index * 320, 320)
            summed = self.dw[here, :] + self.r2[0].astype(F32) + self.r2[1].astype(F32)
            self.dw[here, :] = summed
            self.s3[...] = summed.astype(BF16)
            for k in (2, 1, 3):
                piece = self.s3.at[ds(lax.rem(self.index2 + k, 4) * 80, 80), :]
                self.send(3, piece, self.r3.at[k - 1], self.dev2(k))

        def fourth(self):
            got(self.base + 3, self.r3)
            rows = ds(self.index * 320 + self.index2 * 80, 80)
            self.s4[...] = self.dw[rows, :] + self.r3[0].astype(F32) + self.r3[1].astype(F32) + self.r3[2].astype(F32)
            self.four = self.send(4, self.s4.at[ds((1 - zh) * 40, 40), :], self.r4, zpair)

        def owners(self):
            self.four.wait_recv()
            chunk = self.s4[ds(zh * 40, 40), :] + self.r4[...]
            for i in range(4):
                self.sd[i, 0:10, :] = chunk[10 * i : 10 * i + 10, :]
            self.rd[g] = self.sd[r]
            for k in (2, 3, 1):
                zlk, ck, dev = rank(k)
                self.send(5, self.sd.at[zlk * 2 + ck], self.rd.at[g], dev)

        def finish(self):
            got(self.base + 5, self.rd.at[0:3])

        def close(self):
            sent(self.group, self.dw.at[0:688, :])

    tiles = [slice(128 * t, 128 * t + 128) for t in range(5)] + [slice(768, 896), ds(lane0, 128)]
    kinds = (0, 1, 0, 1, 0, 1, 0)
    p0, p1, p2, p3, p4, st, mp = streams = [
        Stream(46 + 6 * t, 13 + t, [(tiles[t], slice(0, 128))], kinds[t], bufs[11 * t : 11 * t + 11]) for t in range(7)
    ]

    pair_outside(2)
    p2.first()
    pair_outside(3)
    p3.first()
    p2.rest()
    pair_outside(4)
    p4.first()
    p3.rest()
    pair_outside(0)
    p0.first()
    p2.second()
    pair_outside(1)
    p1.first()
    p3.second()

    blocks(turn)
    first = c == 0
    t1s[...] = jnp.where(first, dcf[...], dbf[...])
    t1 = send(35, t1s, t1r, core, 9)
    p4.rest()
    p4.second()

    ownl = coli < 10
    bias_sum = decay_sum = jnp.zeros((8, 128), F32)
    for b in range(4):
        rows = slice(128 * b, 128 * b + 128)
        dlog = mm(sums4, jnp.concatenate(parts(red[b, 0:128], 3) + parts(red[b, 128:256], 3), axis=0))
        dlog = jnp.where(ownl, dlog + inner[b].sum(axis=0, keepdims=True), 0.0)
        ddt = (red[b, 256:384] + neg * dlog) * jax.nn.sigmoid(projs[rows, 128:256] + bias)
        ddt = jnp.where(ownl, ddt, 0.0)
        rr[rows, 768:896] = ddt.astype(BF16)
        bias_sum = bias_sum + ddt.reshape(16, 8, 128).sum(axis=0)
        decay_sum = decay_sum + (dlog * lgd[rows, :]).reshape(16, 8, 128).sum(axis=0)
    place = jnp.where(jnp.logical_and(rowi < 10, coli == rowi + 10 * g), 1.0, 0.0).astype(F32)
    st.first()
    row8 = lax.broadcasted_iota(jnp.int32, (8, 128), 0)
    packed = jnp.where(
        row8 == 0, bias_sum.sum(axis=0, keepdims=True),
        jnp.where(row8 == 1, decay_sum.sum(axis=0, keepdims=True),
                  jnp.where(row8 == 2, gain[0].sum(axis=0, keepdims=True), 0.0)),
    )
    heads_y[y] = mm(packed, place, NN, highest)
    for k in (1, 2, 3):
        send(38, heads_y.at[y], heads_y.at[y], ydev(k), 10)
    p0.rest()
    p0.second()
    t1.wait_recv()
    mixed = jnp.where(first, dbf[...], dcf[...]) + t1r[...]
    rr[:, ds(lane0, 128)] = (mixed * silu_grad(projs[:, ds(256 * c, 128, 128)])).astype(BF16)
    rr[:, ds(896 - 256 * c, 128)] = jnp.zeros((512, 128), BF16)
    mp.first()

    def token(half):
        rows = ds(half * 256, 256)
        for n in range(5):
            part = slice(256 * n, 256 * n + 256)
            hgp[rows, part] = mm(rr[rows, :], wf[part, :], NT)

    mate_row = ds((zl * 2 + 1 - c) * 128, 128)
    far_mate = ds(((1 - zl) * 2 + 1 - c) * 128, 128)
    far_row = ds(((1 - zl) * 2 + c) * 128, 128)
    p1.rest()
    p1.second()
    p2.third()
    st.rest()
    st.second()
    p3.third()
    token(1 - zl)
    hgs[1] = hgp[far_mate, :].astype(BF16)
    hg_far = send(43, hgs.at[1], hgr.at[1], core, 11)
    mp.rest()
    mp.second()
    p4.third()
    hg_far.wait_recv()
    hgs[2] = (hgp[far_row, :] + hgr[1].astype(F32)).astype(BF16)
    hg_z = send(44, hgs.at[2], hgr.at[2], rank(2)[2], 11)
    p0.third()
    token(zl)
    hgs[0] = hgp[mate_row, :].astype(BF16)
    hg_near = send(42, hgs.at[0], hgr.at[0], core, 11)
    p1.third()
    p2.fourth()
    p3.fourth()
    st.third()
    mp.third()
    got(38, heads_y.at[0:3])
    heads_x[x] = (heads_y[0] + heads_y[1]) + (heads_y[2] + heads_y[3])
    for k in (1, 2, 3):
        send(39, heads_x.at[x], heads_x.at[x], xdev(k), 10)
    p4.fourth()
    p0.fourth()
    p2.owners()
    p3.owners()
    p1.fourth()
    st.fourth()
    got(39, heads_x.at[0:3])
    heads_z[zh] = (heads_x[0] + heads_x[1]) + (heads_x[2] + heads_x[3])
    head_z = send(40, heads_z.at[zh], heads_z.at[zh], zpair, 10)
    mp.fourth()
    p4.owners()
    p0.owners()
    hg_near.wait_recv()
    hg_z.wait_recv()
    hgo[...] = (hgp[here_id, :] + hgr[0].astype(F32) + hgr[2].astype(F32)).astype(BF16)
    hg_out = pltpu.make_async_copy(hgo, hg_ref, ls.at[5])
    hg_out.start()
    p1.owners()
    st.owners()
    mp.owners()
    head_z.wait_recv()
    heads_g[r] = heads_z[0] + heads_z[1]
    for k in (1, 2, 3):
        send(41, heads_g.at[r], heads_g.at[r], rank(k)[2], 10)
    for t, stream in ((2, p2), (3, p3), (4, p4), (0, p0), (1, p1)):
        stream.finish()
        for k in range(4):
            wgo[:, 640 * k + 128 * t : 640 * k + 128 * t + 128] = stream.rd[k, 0:10, :]
    got(41, heads_g.at[0:3])
    hdo[...] = (heads_g[0] + heads_g[1]) + (heads_g[2] + heads_g[3])
    hd_out = pltpu.make_async_copy(hdo, hd_ref, ls.at[6])
    hd_out.start()
    st.finish()
    for k in range(4):
        wgo[:, 2816 + 10 * k : 2826 + 10 * k] = st.rd[k, 0:10, 0:10]
    mp.finish()
    wgo[:, 2560:2688] = mp.rd[0, 0:10, :] + mp.rd[2, 0:10, :]
    wgo[:, 2688:2816] = mp.rd[1, 0:10, :] + mp.rd[3, 0:10, :]
    wg_out = pltpu.make_async_copy(wgo, wg_ref, ls.at[7])
    wg_out.start()
    for m in range(4):
        sent(m, wf.at[0:1120, cols(m)])
    sent(4, hidf.at[0:384, :])
    sent(20, stepw.at[0:7])
    sent(5, cot.at[0:384, :])
    sent(6, wf.at[:, ds(lane0, 128)])
    sent(7, ttr)
    sent(8, str_)
    sent(9, t1r)
    sent(10, bmf.at[0:80, :])
    sent(11, hgs)
    for stream in streams:
        stream.close()
    hg_out.wait()
    hd_out.wait()
    wg_out.wait()


def scratch():
    def v(shape, dtype=F32):
        return pltpu.VMEM(shape, dtype)

    def stream(n):
        return [
            v((D, n)), v((320, n), BF16), v((2, 160, n), BF16), v((2, 320, n), BF16), v((2, 320, n), BF16),
            v((320, n), BF16), v((3, 80, n), BF16), v((80, n)), v((40, n)), v((4, 16, n)), v((4, 16, n)),
        ]

    wide, wide16 = v((512, COLS)), v((512, COLS), BF16)
    thin = v((512, 128))
    return [
        v((8, 16, 256), BF16), v((128, D)),
        v((512, D), BF16), v((D, 512), BF16), v((D, 512), BF16), wide16, v((160, 2856), BF16), v((D, 1024), BF16),
        v((512, 384)), wide, thin, thin, thin, thin, v((4, 16, 128)), thin,
        v((4, 128, 128)), v((4, 128, 128)), v((4, 128, 128)),
        wide, wide, wide, wide, wide16, wide16, wide16, v((32, COLS)),
        v((4, 128, COLS)), v((4, 128, COLS)), v((2, 128, COLS), BF16), v((8, COLS)),
        v((3, 128, COLS), BF16), v((3, 8, COLS)), wide, wide, thin, thin,
        v((4, 128, COLS), BF16), v((4, 128, COLS), BF16), v((4, 128, 128)), v((4, 384, 128)),
        v((512, 1024), BF16), thin, thin,
        v((512, D)), v((3, 128, D), BF16), v((3, 128, D), BF16),
        v((4, 8, 128)), v((4, 8, 128)), v((2, 8, 128)), v((4, 8, 128)),
        v((128, D), BF16), v((10, 2856)), v((8, 128)),
        pltpu.SemaphoreType.DMA((21,)), pltpu.SemaphoreType.DMA((94,)), pltpu.SemaphoreType.DMA((8,)),
        *(buf for _ in range(7) for buf in stream(128)),
    ]


def emit(hg_ref, wg_ref, hd_ref, hg_out, wg_out, hd_out):
    hg_out[...] = hg_ref[...]
    wg_out[...] = wg_ref[...]
    hd_out[...] = hd_ref[0:3, 0:HEADS]


def body(hidden, output_grad, input_weight, step_bias, decay_log, skip_gain):
    anyspace = pl.BlockSpec(memory_space=pl.ANY)
    vmem = pl.BlockSpec(memory_space=pltpu.VMEM)
    hg, wg, hd = pl.pallas_call(
        kernel,
        out_shape=(
            jax.ShapeDtypeStruct((128, D), BF16),
            jax.ShapeDtypeStruct((10, 2856), F32),
            jax.ShapeDtypeStruct((8, 128), F32),
        ),
        in_specs=[anyspace, anyspace, anyspace, vmem, vmem, vmem],
        out_specs=(anyspace, anyspace, anyspace),
        scratch_shapes=scratch(),
        compiler_params=pltpu.CompilerParams(has_side_effects=True, collective_id=0, vmem_limit_bytes=64000000),
    )(hidden[0], output_grad[0], input_weight, step_bias[None], decay_log[None], skip_gain[None])
    hg, wg, hd = pl.pallas_call(
        emit,
        out_shape=(
            jax.ShapeDtypeStruct((128, D), BF16),
            jax.ShapeDtypeStruct((10, 2856), F32),
            jax.ShapeDtypeStruct((3, HEADS), F32),
        ),
        in_specs=[vmem, vmem, vmem],
        out_specs=(vmem, vmem, vmem),
    )(hg, wg, hd)
    return (hg[None], wg, hd)


def solution(mesh):
    torus = Mesh(
        mesh.devices.reshape(4, 2, 2, 4, 2), ("seq_0", "seq_1", "seq_2", "zero_0", "zero_1")
    )
    in_specs = (P(ZERO, SEQ, None), P(ZERO, SEQ, None), P(ZERO, None), P(), P(), P())
    out_specs = (P(ZERO, SEQ, None), P(SEQ_ZERO, None), P())
    return jax.shard_map(body, mesh=torus, in_specs=in_specs, out_specs=out_specs, check_vma=False)
```

```python
import functools

import jax
import jax.numpy as jnp
from jax import lax
from jax.experimental import pallas as pl
from jax.experimental.pallas import tpu as pltpu
from jax.sharding import Mesh
from jax.sharding import PartitionSpec as P

HEADS = 40
STATE = 128
INNER = 2560
D = 1280
COLS = 640
ZERO = ("zero_0", "zero_1")
SEQ = ("seq_0", "seq_1", "seq_2")
SEQ_ZERO = ("seq_0", "seq_1", "seq_2", "zero_0", "zero_1")
MESH = pl.DeviceIdType.MESH
F32 = jnp.float32
BF16 = jnp.bfloat16
highest = lax.Precision.HIGHEST
NN = (((1,), (0,)), ((), ()))
NT = (((1,), (1,)), ((), ()))
TN = (((0,), (0,)), ((), ()))


def mm(a, b, dims=NN, precision=None):
    return lax.dot_general(a, b, dims, preferred_element_type=F32, precision=precision)


def parts(v, count):
    out = []
    for _ in range(count):
        out.append(v.astype(BF16))
        v = v - out[-1].astype(F32)
    return out


def mm3(a, b, dims=NN):
    (ah, al), (bh, bl) = parts(a, 2), parts(b, 2)
    (ka,), (kb,) = dims[0]
    return mm(jnp.concatenate([ah, al, ah], axis=ka), jnp.concatenate([bh, bh, bl], axis=kb), dims)


def ds(start, size, align=None):
    return pl.ds(pl.multiple_of(start, align or size), size)


def silu_grad(v):
    sig = jax.nn.sigmoid(v)
    return sig * (1.0 + v * (1.0 - sig))


def kernel(
    hid_ref, cot_ref, w_ref, bias_ref, decay_ref, skip_ref,
    hg_ref, wg_ref, hd_ref,
    stepw, stepa, hidf, hidt, hidx, cot, wraw, wf, projs, projv, bmf, cmf, lgd, cums, cumt, stp, gs, gts, dgs,
    sexp, ecs, tls, vv, xb, xt, oe, tot,
    sl, dl, stt, tts, str_, ttr, q1s, dxin, dbf, dcf, sb, db, dd, red,
    rr, t1s, t1r, hgp, hgs, hgr,
    heads_y, heads_x, heads_z, heads_g, hgo, wgo, hdo,
    ss, rs, ls, *bufs,
):
    y, zl, c = (lax.axis_index(n) for n in SEQ)
    x, zh = (lax.axis_index(n) for n in ZERO)
    r = zl * 2 + c
    a = lax.rem(zl + zh, 2)
    g = a * 2 + c

    def send(i, src, dst, where, group):
        copy = pltpu.make_async_remote_copy(
            src_ref=src, dst_ref=dst, send_sem=ss.at[group], recv_sem=rs.at[i],
            device_id=where, device_id_type=MESH,
        )
        copy.start()
        return copy

    def bytes_of(ref, i=0, group=0):
        return pltpu.make_async_remote_copy(
            src_ref=ref, dst_ref=ref, send_sem=ss.at[group], recv_sem=rs.at[i],
            device_id={"seq_2": 1 - c}, device_id_type=MESH,
        )

    def got(i, ref):
        bytes_of(ref, i=i).wait_recv()

    def sent(group, ref):
        bytes_of(ref, group=group).wait_send()

    def rank(k):
        zlk = lax.rem(zl + k // 2, 2)
        ck = lax.rem(c + k % 2, 2)
        return zlk, ck, {"seq_1": zlk, "seq_2": ck}

    def xdev(k):
        return {"zero_0": lax.rem(x + k + 4, 4)}

    def ydev(k):
        return {"seq_0": lax.rem(y + k + 4, 4)}

    zpair = {"seq_1": 1 - zl, "zero_1": 1 - zh}
    core = {"seq_2": 1 - c}
    here_id = ds(r * 128, 128)

    def shard(xk, zk, lo=0, size=160):
        return ds((lax.rem(xk + 4, 4) * 2 + zk) * 160 + lo, size, 16)

    own = shard(x, zh)
    lane0 = 640 + 256 * c
    local = [
        pltpu.make_async_copy(w_ref, wraw, ls.at[0]),
        pltpu.make_async_copy(w_ref.at[:, ds(g * COLS, COLS, 128)], wf.at[own, 0:640], ls.at[1]),
        pltpu.make_async_copy(w_ref.at[:, ds(2560 + 128 * c, 128)], wf.at[own, ds(lane0, 128)], ls.at[2]),
        pltpu.make_async_copy(hid_ref, hidf.at[here_id, :], ls.at[3]),
        pltpu.make_async_copy(cot_ref.at[:, ds(g * COLS, COLS, 128)], cot.at[here_id, :], ls.at[4]),
    ]
    for copy in local:
        copy.start()

    barrier = pltpu.get_barrier_semaphore()

    def greet(dev):
        pl.semaphore_signal(barrier, inc=1, device_id=dev, device_id_type=MESH)

    greet(zpair)
    for k in (1, 2, 3):
        greet(xdev(k))
        greet(ydev(k))
        greet(rank(k)[2])
    coli = lax.broadcasted_iota(jnp.int32, (128, 128), 1)
    rowi = lax.broadcasted_iota(jnp.int32, (128, 128), 0)
    local[0].wait()
    stepa[...] = jnp.zeros_like(stepa)
    tail = jnp.concatenate([wraw[:, 2816:2856].astype(F32), jnp.zeros((160, 88), F32)], axis=1)
    tail = pltpu.roll(tail, lax.rem(128 - 10 * g, 128), 1)
    keep10 = lax.broadcasted_iota(jnp.int32, (160, 128), 1) < 10
    tail = jnp.concatenate([jnp.where(keep10, tail, 0.0), jnp.zeros((96, 128), F32)], axis=0)
    stepw[x * 2 + zh] = tail.T[0:16, :].astype(BF16)

    def lanes10(ref):
        full = jnp.concatenate([ref[...], jnp.zeros((1, 88), F32)], axis=1)
        return pltpu.roll(jnp.broadcast_to(full, (8, 128)), lax.rem(128 - 10 * g, 128), 1)[0:1, :]

    bias = lanes10(bias_ref)
    neg = -jnp.exp(lanes10(decay_ref))
    skip = lanes10(skip_ref)
    for copy in local[1:]:
        copy.wait()
    pl.semaphore_wait(barrier, 10)

    def cols(m):
        return (ds(lane0, 128), slice(0, 256), slice(256, 512), slice(512, 640))[m]

    w = {}

    def wsend(m, i, rows, dev):
        ref = wf.at[rows, cols(m)]
        slot = min(i, 5) if m < 2 else {1: 1, 2: 2, 5: 3, 6: 4}.get(i, 5)
        w[m, i] = send(6 * m + slot, ref, ref, dev, m)

    def w_own_x(m):
        wsend(m, 1, own, xdev(1))
        wsend(m, 2, own, xdev(-1))

    def w_own_z(m):
        wsend(m, 0, own, zpair)

    def w_other(m):
        w[m, 0].wait_recv()
        wsend(m, 3, shard(x, 1 - zh), xdev(1))
        wsend(m, 4, shard(x, 1 - zh), xdev(-1))

    def w_forward(m):
        w[m, 1].wait_recv()
        wsend(m, 5, shard(x - 1, zh, 0, 80), xdev(1))
        w[m, 2].wait_recv()
        wsend(m, 6, shard(x + 1, zh, 80, 80), xdev(-1))

    def w_forward_other(m):
        w[m, 3].wait_recv()
        wsend(m, 7, shard(x - 1, 1 - zh, 0, 80), xdev(1))
        w[m, 4].wait_recv()
        wsend(m, 8, shard(x + 1, 1 - zh, 80, 80), xdev(-1))

    def w_across(m):
        wsend(m, 3, shard(x - 1, zh), zpair)
        wsend(m, 4, shard(x + 1, zh), zpair)

    def w_across_far(m):
        w[m, 5].wait_recv()
        wsend(m, 7, shard(x + 2, zh, 0, 80), zpair)
        w[m, 6].wait_recv()
        wsend(m, 8, shard(x + 2, zh, 80, 80), zpair)

    def w_done(m):
        got(6 * m + 5, wf.at[0 : 320 if m < 2 else 640, cols(m)])

    def step_send(i, xk, zk, dev):
        ref = stepw.at[lax.rem(x + xk + 4, 4) * 2 + zk]
        return send(i, ref, ref, dev, 20)

    def hand(k):
        ref = wf.at[ds(lax.rem(x + k + 4, 4) * 320, 320), ds(lane0, 128)]
        send(28, ref, ref, core, 6)

    step_z = step_send(88, 0, zh, zpair)
    step_x = [step_send(89, 0, zh, xdev(1)), step_send(90, 0, zh, xdev(-1))]
    w_own_z(0)
    w_own_x(0)
    h_z = send(24, hid_ref, hidf.at[here_id, :], rank(2)[2], 4)
    w_own_x(2)
    w_own_z(1)
    h_c = send(25, hid_ref, hidf.at[here_id, :], core, 4)
    for k in (2, 3, 1):
        zlk, ck, dev = rank(k)
        gk = lax.rem(zlk + zh, 2) * 2 + ck
        send(27, cot_ref.at[:, ds(gk * COLS, COLS, 128)], cot.at[here_id, :], dev, 5)
    w_own_z(2)
    w_own_z(3)
    step_z.wait_recv()
    step_o = [step_send(91, 0, 1 - zh, xdev(1)), step_send(92, 0, 1 - zh, xdev(-1))]
    w_other(0)
    for copy in step_x:
        copy.wait_recv()
    step_send(93, -1, zh, xdev(1))
    w_forward(0)
    w_forward(2)
    w_across(2)
    w_own_x(3)
    for copy in step_o:
        copy.wait_recv()
    step_send(93, -1, 1 - zh, xdev(1))
    w_forward_other(0)
    w_own_x(1)
    for k in (-1, 0, 1):
        hand(k)
    i320 = lax.broadcasted_iota(jnp.int32, (320, 320), 0)
    k320 = lax.broadcasted_iota(jnp.int32, (320, 320), 1)
    tens = lax.shift_right_logical(i320 * 6554, 16)
    source = ((tens & 3) * 8 + lax.shift_right_logical(tens, 2)) * 10 + i320 - tens * 10
    perm = jnp.where(k320 == source, 1.0, 0.0).astype(F32).astype(BF16)

    def transpose(k):
        rows = ds((rank(k)[0] * 2 + rank(k)[1]) * 128, 128)
        for q in range(4):
            part = slice(320 * q, 320 * q + 320)
            hidt[part, rows] = mm(perm, hidf[rows, part], NT).astype(BF16)

    transpose(0)
    h_c.wait_recv()
    transpose(1)
    h_z.wait_recv()
    zrows = ds((rank(2)[0] * 2 + c) * 128, 128)
    h_f = send(26, hidf.at[zrows, :], hidf.at[zrows, :], core, 4)
    w_across_far(2)
    w_forward(3)
    w_across(3)
    w_other(1)
    w_done(0)
    hand(2)
    got(93, stepw.at[0:2])
    for k in range(8):
        stepa[0:16, 160 * k : 160 * k + 160] = stepw[k][:, 0:160].astype(F32)
    wf[:, 768:896] = stepa[...].T.astype(BF16)

    low = coli < 64
    causal = rowi >= coli
    anti = rowi <= coli
    tri = causal.astype(F32).astype(BF16)
    tri3 = jnp.concatenate([tri] * 3, axis=1)
    upper = anti.astype(F32).astype(BF16)
    strict = (rowi > coli).astype(F32).astype(BF16)
    sums4 = jnp.concatenate([upper] * 3 + [strict] * 3, axis=1)

    def pair(v, j):
        return jnp.where(low[0 : v.shape[0]], v[:, 2 * j : 2 * j + 1], v[:, 2 * j + 1 : 2 * j + 2])

    def blocks(f, unroll=True):
        if unroll:
            for b in range(4):
                f(b, pl.ds(b * 128, 128))
        else:
            def step(b, carry):
                f(b, ds(b * 128, 128))
                return carry

            lax.fori_loop(0, 4, step, 0)

    def steps(b, rows):
        projs[rows, ds(128 * c, 256, 128)] = mm(hidf[rows, :], wf[:, ds(640 + 128 * c, 256, 128)])
        pre = projs[rows, 128:256] + bias
        step = jnp.maximum(pre, 0.0) + jnp.log1p(jnp.exp(-jnp.abs(pre)))
        lg = neg * step
        cum = mm(tri3, jnp.concatenate(parts(lg, 3), axis=0))
        stp[rows, :] = step
        lgd[rows, :] = lg
        cums[rows, :] = cum
        cumt[b] = cum.T[0:16, :]
        dgs[b] = jnp.zeros((128, 128), F32)
        red[b] = jnp.zeros((384, 128), F32)

    def maps(b, rows):
        projs[rows, ds(256 - 256 * c, 128)] = mm(hidf[rows, :], wf[:, ds(896 - 256 * c, 128)])
        bm = jax.nn.silu(projs[rows, 0:128])
        cm = jax.nn.silu(projs[rows, 256:384])
        bmf[rows, :] = bm
        cmf[rows, :] = cm
        scores = mm3(cm, bm, NT)
        gs[b] = scores
        gts[b] = scores.T

    for k in range(4):
        if k == 3:
            h_f.wait_recv()
        b = rank(k)[0] * 2 + rank(k)[1]
        steps(b, ds(b * 128, 128))
    for j in range(5):
        cj = slice(128 * j, 128 * j + 128)
        for b in range(4):
            last_row = cums[128 * b + 127 : 128 * b + 128, :]
            tot[8 * b : 8 * b + 8, cj] = pair(jnp.broadcast_to(last_row, (8, 128)), j)
    tts[...] = tot[0:8, :] + tot[8:16, :] + tot[16:24, :] + tot[24:32, :]
    for k in (1, 2, 3):
        send(29, tts, ttr.at[k - 1], ydev(k), 7)

    transpose(2)
    transpose(3)
    w_forward(1)
    got(28, wf.at[:, ds(896 - 256 * c, 128)])
    maps(0, pl.ds(0, 128))
    w_across_far(3)
    maps(1, pl.ds(128, 128))
    maps(2, pl.ds(256, 128))
    w_forward_other(1)
    maps(3, pl.ds(384, 128))

    def total(b, cj):
        return tot[8 * b : 8 * b + 1, cj]

    def pair_forward(j):
        cj = slice(128 * j, 128 * j + 128)

        wide = slice(128 * j, min(128 * j + 256, 640))

        def project(b, rows):
            projv[rows, wide] = mm(hidf[rows, :], wf[:, wide])

        def local_part(b, rows):
            ce = pair(cums[rows, :], j)
            se = pair(stp[rows, :], j)
            ec = jnp.exp(ce)
            tl = jnp.exp(ce[127:128, :] - ce)
            val = jax.nn.silu(projv[rows, cj])
            xs = val * se
            sexp[rows, cj] = se
            ecs[rows, cj] = ec
            tls[rows, cj] = tl
            vv[rows, cj] = val
            xb[rows, cj] = xs.astype(BF16)
            x16 = (xs * tl).astype(BF16)
            o16 = (cot[rows, cj].astype(F32) * ec).astype(BF16)
            xt[rows, cj] = x16
            oe[rows, cj] = o16
            sl[b, :, cj] = mm(bmf[rows, :].astype(BF16), x16, TN)
            dl[b, :, cj] = mm(cmf[rows, :].astype(BF16), o16, TN)

        if j % 2 == 0:
            blocks(project)
        blocks(local_part)
        s = sl[0, :, cj]
        d = dl[3, :, cj]
        for b in range(1, 4):
            s = jnp.exp(total(b, cj)) * s + sl[b, :, cj]
            d = jnp.exp(total(3 - b, cj)) * d + dl[3 - b, :, cj]
        stt[0, :, cj] = s.astype(BF16)
        stt[1, :, cj] = d.astype(BF16)
        for k in (1, 2, 3):
            wraps = lax.div(y + k, 4)
            send(30 + j, stt.at[wraps, :, cj], str_.at[k - 1, :, cj], ydev(k), 8)

    def pair_inside(j):
        cj = slice(128 * j, 128 * j + 128)

        def inside(b, rows):
            cum = cums[rows, :]
            c0, c1 = cum[:, 2 * j : 2 * j + 1], cum[:, 2 * j + 1 : 2 * j + 2]
            r0, r1 = cumt[b, 2 * j : 2 * j + 1, :], cumt[b, 2 * j + 1 : 2 * j + 2, :]
            w0 = jnp.where(causal, jnp.exp(jnp.where(causal, c0 - r0, 0.0)), 0.0)
            w1 = jnp.where(causal, jnp.exp(jnp.where(causal, c1 - r1, 0.0)), 0.0)
            u0 = jnp.where(anti, jnp.exp(jnp.where(anti, r0 - c0, 0.0)), 0.0)
            u1 = jnp.where(anti, jnp.exp(jnp.where(anti, r1 - c1, 0.0)), 0.0)
            scores, scores_t = gs[b], gts[b]
            m = jnp.concatenate([scores * w0, scores * w1], axis=1).astype(BF16)
            mt = jnp.concatenate([scores_t * u0, scores_t * u1], axis=1).astype(BF16)
            x16 = xb[rows, cj]
            o16 = cot[rows, cj]
            zero = jnp.zeros_like(x16)
            xd = jnp.concatenate([jnp.where(low, x16, zero), jnp.where(low, zero, x16)], axis=0)
            od = jnp.concatenate([jnp.where(low, o16, zero), jnp.where(low, zero, o16)], axis=0)
            yy = mm(m, xd)
            pp = mm(o16, xd, NT)
            dx = mm(mt, od)
            dgs[b] = dgs[b] + w0 * pp[:, 0:128] + w1 * pp[:, 128:256]
            dxin[rows, cj] = dx
            q1s[rows, cj] = o16.astype(F32) * yy - x16.astype(F32) * dx

        blocks(inside)

    got(27, cot.at[0:384, :])
    w_done(2)
    pair_forward(2)
    pair_inside(2)
    pair_forward(3)
    pair_inside(3)
    w_done(3)
    pair_forward(4)
    pair_inside(4)
    for p in range(4):
        for q in range(4):
            hidx[320 * p + 80 * q : 320 * p + 80 * q + 80, :] = hidt[320 * q + 80 * p : 320 * q + 80 * p + 80, :]
    w_done(1)
    pair_forward(0)
    pair_inside(0)
    pair_forward(1)
    pair_inside(1)

    def turn(b, rows):
        dcf[rows, :] = mm3(dgs[b], bmf[rows, :], NN) + mm(oe[rows, :], sb[b], NT)
        dbf[rows, :] = mm3(dgs[b], cmf[rows, :], TN) + mm(xt[rows, :], db[b], NT)

    got(29, ttr)

    lanes = lax.broadcasted_iota(jnp.int32, (256, 128), 0)
    outl = lax.broadcasted_iota(jnp.int32, (256, 128), 1)

    def sums(z, j):
        hi = z.astype(BF16)
        lo = (z - hi.astype(F32)).astype(BF16)
        choose = (outl == 2 * j + lax.rem(lax.div(lanes, 64), 2)).astype(F32).astype(BF16)
        return mm(jnp.concatenate([hi, lo], axis=1), choose)

    yes = [jnp.where(y >= k, 1.0, 0.0).astype(F32) for k in (1, 2, 3)]
    no = [jnp.where(y + k <= 3, 1.0, 0.0).astype(F32) for k in (1, 2, 3)]
    inner = [jnp.zeros((8, 128), F32) for _ in range(4)]
    gain = [jnp.zeros((8, 128), F32)]

    def pair_outside(j):
        cj = slice(128 * j, 128 * j + 128)
        got(30 + j, str_.at[:, :, cj])
        t = [ttr[k, 0:1, cj] for k in range(3)]
        came = [str_[k, :, cj].astype(F32) for k in range(3)]
        s = yes[0] * came[0] + (yes[1] * jnp.exp(t[0])) * came[1] + (yes[2] * jnp.exp(t[0] + t[1])) * came[2]
        d = no[0] * came[2] + (no[1] * jnp.exp(t[2])) * came[1] + (no[2] * jnp.exp(t[2] + t[1])) * came[0]
        for b in (3, 2, 1, 0):
            db[b, :, cj] = d.astype(BF16)
            dd[b] = d
            d = jnp.exp(total(b, cj)) * d + dl[b, :, cj]
        for b in range(4):
            sb[b, :, cj] = s.astype(BF16)
            grown = jnp.exp(total(b, cj)) * s
            inner[b] = inner[b] + sums((grown * dd[b]).reshape(16, 8, 128).sum(axis=0), j)
            s = grown + sl[b, :, cj]

        def outside(b, rows):
            o = cot[rows, cj].astype(F32)
            yst = mm(cmf[rows, :].astype(BF16), sb[b, :, cj]) * ecs[rows, cj]
            dxst = mm(bmf[rows, :].astype(BF16), db[b, :, cj]) * tls[rows, cj]
            val = vv[rows, cj]
            dxs = dxin[rows, cj] + dxst
            z = jnp.concatenate([q1s[rows, cj] + o * yst, xb[rows, cj].astype(F32) * dxst, dxs * val], axis=0)
            red[b] = red[b] + sums(z, j)
            dval = dxs * sexp[rows, cj] + pair(skip, j) * o
            rr[rows, cj] = (dval * silu_grad(projv[rows, cj])).astype(BF16)
            gain[0] = gain[0] + sums((o * val).reshape(16, 8, 128).sum(axis=0), j)

        blocks(outside)

    class Stream:
        def __init__(self, base, group, parts, kind, bufs):
            self.base, self.group, self.parts, self.left = base, group, parts, hidx if kind else hidt
            self.dw, self.s1, self.r1, self.s2, self.r2, self.s3, self.r3, self.s4, self.r4, self.sd, self.rd = bufs
            self.index, self.dev, self.index2, self.dev2 = (y, ydev, x, xdev) if kind == 0 else (x, xdev, y, ydev)

        def send(self, i, src, dst, dev):
            return send(self.base + i, src, dst, dev, self.group)

        def block(self, i):
            rows = ds(lax.rem(self.index + i, 4) * 320, 320)
            for cols, target in self.parts:
                self.dw[rows, target] = mm(self.left[rows, :], rr[:, cols])
            return rows

        def first(self):
            rows = self.block(2)
            self.s1[...] = self.dw[rows, :].astype(BF16)
            self.one = (
                self.send(0, self.s1.at[0:160, :], self.r1.at[0], self.dev(1)),
                self.send(1, self.s1.at[160:320, :], self.r1.at[1], self.dev(-1)),
            )

        def rest(self):
            for i in (1, 3, 0):
                self.block(i)

        def second(self):
            nxt = lax.rem(self.index + 1, 4) * 320
            prv = lax.rem(self.index + 3, 4) * 320
            self.one[0].wait_recv()
            self.s2[0, 0:160, :] = (self.dw[ds(nxt, 160), :] + self.r1[0].astype(F32)).astype(BF16)
            self.s2[0, 160:320, :] = self.dw[ds(nxt + 160, 160), :].astype(BF16)
            self.send(2, self.s2.at[0], self.r2.at[0], self.dev(1))
            self.one[1].wait_recv()
            self.s2[1, 0:160, :] = self.dw[ds(prv, 160), :].astype(BF16)
            self.s2[1, 160:320, :] = (self.dw[ds(prv + 160, 160), :] + self.r1[1].astype(F32)).astype(BF16)
            self.send(2, self.s2.at[1], self.r2.at[1], self.dev(-1))

        def third(self):
            got(self.base + 2, self.r2)
            here = ds(self.index * 320, 320)
            summed = self.dw[here, :] + self.r2[0].astype(F32) + self.r2[1].astype(F32)
            self.dw[here, :] = summed
            self.s3[...] = summed.astype(BF16)
            for k in (2, 1, 3):
                piece = self.s3.at[ds(lax.rem(self.index2 + k, 4) * 80, 80), :]
                self.send(3, piece, self.r3.at[k - 1], self.dev2(k))

        def fourth(self):
            got(self.base + 3, self.r3)
            rows = ds(self.index * 320 + self.index2 * 80, 80)
            self.s4[...] = self.dw[rows, :] + self.r3[0].astype(F32) + self.r3[1].astype(F32) + self.r3[2].astype(F32)
            self.four = self.send(4, self.s4.at[ds((1 - zh) * 40, 40), :], self.r4, zpair)

        def owners(self):
            self.four.wait_recv()
            chunk = self.s4[ds(zh * 40, 40), :] + self.r4[...]
            for i in range(4):
                self.sd[i, 0:10, :] = chunk[10 * i : 10 * i + 10, :]
            self.rd[g] = self.sd[r]
            for k in (2, 3, 1):
                zlk, ck, dev = rank(k)
                self.send(5, self.sd.at[zlk * 2 + ck], self.rd.at[g], dev)

        def finish(self):
            got(self.base + 5, self.rd.at[0:3])

        def close(self):
            sent(self.group, self.dw.at[0:688, :])

    tiles = [slice(128 * t, 128 * t + 128) for t in range(5)] + [slice(768, 896), ds(lane0, 128)]
    kinds = (0, 1, 0, 1, 0, 1, 0)
    p0, p1, p2, p3, p4, st, mp = streams = [
        Stream(46 + 6 * t, 13 + t, [(tiles[t], slice(0, 128))], kinds[t], bufs[11 * t : 11 * t + 11]) for t in range(7)
    ]

    pair_outside(2)
    p2.first()
    pair_outside(3)
    p3.first()
    p2.rest()
    pair_outside(4)
    p4.first()
    p3.rest()
    pair_outside(0)
    p0.first()
    p2.second()
    pair_outside(1)
    p1.first()
    p3.second()

    blocks(turn)
    first = c == 0
    t1s[...] = jnp.where(first, dcf[...], dbf[...])
    t1 = send(35, t1s, t1r, core, 9)
    p4.rest()
    p4.second()

    ownl = coli < 10
    bias_sum = decay_sum = jnp.zeros((8, 128), F32)
    for b in range(4):
        rows = slice(128 * b, 128 * b + 128)
        dlog = mm(sums4, jnp.concatenate(parts(red[b, 0:128], 3) + parts(red[b, 128:256], 3), axis=0))
        dlog = jnp.where(ownl, dlog + inner[b].sum(axis=0, keepdims=True), 0.0)
        ddt = (red[b, 256:384] + neg * dlog) * jax.nn.sigmoid(projs[rows, 128:256] + bias)
        ddt = jnp.where(ownl, ddt, 0.0)
        rr[rows, 768:896] = ddt.astype(BF16)
        bias_sum = bias_sum + ddt.reshape(16, 8, 128).sum(axis=0)
        decay_sum = decay_sum + (dlog * lgd[rows, :]).reshape(16, 8, 128).sum(axis=0)
    place = jnp.where(jnp.logical_and(rowi < 10, coli == rowi + 10 * g), 1.0, 0.0).astype(F32)
    st.first()
    row8 = lax.broadcasted_iota(jnp.int32, (8, 128), 0)
    packed = jnp.where(
        row8 == 0, bias_sum.sum(axis=0, keepdims=True),
        jnp.where(row8 == 1, decay_sum.sum(axis=0, keepdims=True),
                  jnp.where(row8 == 2, gain[0].sum(axis=0, keepdims=True), 0.0)),
    )
    heads_y[y] = mm(packed, place, NN, highest)
    for k in (1, 2, 3):
        send(38, heads_y.at[y], heads_y.at[y], ydev(k), 10)
    p0.rest()
    p0.second()
    t1.wait_recv()
    mixed = jnp.where(first, dbf[...], dcf[...]) + t1r[...]
    rr[:, ds(lane0, 128)] = (mixed * silu_grad(projs[:, ds(256 * c, 128, 128)])).astype(BF16)
    rr[:, ds(896 - 256 * c, 128)] = jnp.zeros((512, 128), BF16)
    mp.first()

    def token(half):
        rows = ds(half * 256, 256)
        for n in range(5):
            part = slice(256 * n, 256 * n + 256)
            hgp[rows, part] = mm(rr[rows, :], wf[part, :], NT)

    mate_row = ds((zl * 2 + 1 - c) * 128, 128)
    far_mate = ds(((1 - zl) * 2 + 1 - c) * 128, 128)
    far_row = ds(((1 - zl) * 2 + c) * 128, 128)
    p1.rest()
    p1.second()
    p2.third()
    st.rest()
    st.second()
    p3.third()
    token(1 - zl)
    hgs[1] = hgp[far_mate, :].astype(BF16)
    hg_far = send(43, hgs.at[1], hgr.at[1], core, 11)
    mp.rest()
    mp.second()
    p4.third()
    hg_far.wait_recv()
    hgs[2] = (hgp[far_row, :] + hgr[1].astype(F32)).astype(BF16)
    hg_z = send(44, hgs.at[2], hgr.at[2], rank(2)[2], 11)
    p0.third()
    token(zl)
    hgs[0] = hgp[mate_row, :].astype(BF16)
    hg_near = send(42, hgs.at[0], hgr.at[0], core, 11)
    p1.third()
    p2.fourth()
    p3.fourth()
    st.third()
    mp.third()
    got(38, heads_y.at[0:3])
    heads_x[x] = (heads_y[0] + heads_y[1]) + (heads_y[2] + heads_y[3])
    for k in (1, 2, 3):
        send(39, heads_x.at[x], heads_x.at[x], xdev(k), 10)
    p4.fourth()
    p0.fourth()
    p2.owners()
    p3.owners()
    p1.fourth()
    st.fourth()
    got(39, heads_x.at[0:3])
    heads_z[zh] = (heads_x[0] + heads_x[1]) + (heads_x[2] + heads_x[3])
    head_z = send(40, heads_z.at[zh], heads_z.at[zh], zpair, 10)
    mp.fourth()
    p4.owners()
    p0.owners()
    p1.owners()
    st.owners()
    mp.owners()
    head_z.wait_recv()
    heads_g[r] = heads_z[0] + heads_z[1]
    for k in (1, 2, 3):
        send(41, heads_g.at[r], heads_g.at[r], rank(k)[2], 10)
    hg_near.wait_recv()
    hg_z.wait_recv()
    hgo[...] = (hgp[here_id, :] + hgr[0].astype(F32) + hgr[2].astype(F32)).astype(BF16)
    hg_out = pltpu.make_async_copy(hgo, hg_ref, ls.at[5])
    hg_out.start()
    for t, stream in ((2, p2), (3, p3), (4, p4), (0, p0), (1, p1)):
        stream.finish()
        for k in range(4):
            wgo[:, 640 * k + 128 * t : 640 * k + 128 * t + 128] = stream.rd[k, 0:10, :]
    got(41, heads_g.at[0:3])
    hdo[...] = (heads_g[0] + heads_g[1]) + (heads_g[2] + heads_g[3])
    hd_out = pltpu.make_async_copy(hdo, hd_ref, ls.at[6])
    hd_out.start()
    st.finish()
    for k in range(4):
        wgo[:, 2816 + 10 * k : 2826 + 10 * k] = st.rd[k, 0:10, 0:10]
    mp.finish()
    wgo[:, 2560:2688] = mp.rd[0, 0:10, :] + mp.rd[2, 0:10, :]
    wgo[:, 2688:2816] = mp.rd[1, 0:10, :] + mp.rd[3, 0:10, :]
    wg_out = pltpu.make_async_copy(wgo, wg_ref, ls.at[7])
    wg_out.start()
    for m in range(4):
        sent(m, wf.at[0:1120, cols(m)])
    sent(4, hidf.at[0:384, :])
    sent(20, stepw.at[0:7])
    sent(5, cot.at[0:384, :])
    sent(6, wf.at[:, ds(lane0, 128)])
    sent(7, ttr)
    sent(8, str_)
    sent(9, t1r)
    sent(10, bmf.at[0:80, :])
    sent(11, hgs)
    for stream in streams:
        stream.close()
    hg_out.wait()
    hd_out.wait()
    wg_out.wait()


def scratch():
    def v(shape, dtype=F32):
        return pltpu.VMEM(shape, dtype)

    def stream(n):
        return [
            v((D, n)), v((320, n), BF16), v((2, 160, n), BF16), v((2, 320, n), BF16), v((2, 320, n), BF16),
            v((320, n), BF16), v((3, 80, n), BF16), v((80, n)), v((40, n)), v((4, 16, n)), v((4, 16, n)),
        ]

    wide, wide16 = v((512, COLS)), v((512, COLS), BF16)
    thin = v((512, 128))
    return [
        v((8, 16, 256), BF16), v((128, D)),
        v((512, D), BF16), v((D, 512), BF16), v((D, 512), BF16), wide16, v((160, 2856), BF16), v((D, 1024), BF16),
        v((512, 384)), wide, thin, thin, thin, thin, v((4, 16, 128)), thin,
        v((4, 128, 128)), v((4, 128, 128)), v((4, 128, 128)),
        wide, wide, wide, wide, wide16, wide16, wide16, v((32, COLS)),
        v((4, 128, COLS)), v((4, 128, COLS)), v((2, 128, COLS), BF16), v((8, COLS)),
        v((3, 128, COLS), BF16), v((3, 8, COLS)), wide, wide, thin, thin,
        v((4, 128, COLS), BF16), v((4, 128, COLS), BF16), v((4, 128, 128)), v((4, 384, 128)),
        v((512, 1024), BF16), thin, thin,
        v((512, D)), v((3, 128, D), BF16), v((3, 128, D), BF16),
        v((4, 8, 128)), v((4, 8, 128)), v((2, 8, 128)), v((4, 8, 128)),
        v((128, D), BF16), v((10, 2856)), v((8, 128)),
        pltpu.SemaphoreType.DMA((21,)), pltpu.SemaphoreType.DMA((94,)), pltpu.SemaphoreType.DMA((8,)),
        *(buf for _ in range(7) for buf in stream(128)),
    ]


def emit(hg_ref, wg_ref, hd_ref, hg_out, wg_out, hd_out):
    hg_out[...] = hg_ref[...]
    wg_out[...] = wg_ref[...]
    hd_out[...] = hd_ref[0:3, 0:HEADS]


def body(hidden, output_grad, input_weight, step_bias, decay_log, skip_gain):
    anyspace = pl.BlockSpec(memory_space=pl.ANY)
    vmem = pl.BlockSpec(memory_space=pltpu.VMEM)
    hg, wg, hd = pl.pallas_call(
        kernel,
        out_shape=(
            jax.ShapeDtypeStruct((128, D), BF16),
            jax.ShapeDtypeStruct((10, 2856), F32),
            jax.ShapeDtypeStruct((8, 128), F32),
        ),
        in_specs=[anyspace, anyspace, anyspace, vmem, vmem, vmem],
        out_specs=(anyspace, anyspace, anyspace),
        scratch_shapes=scratch(),
        compiler_params=pltpu.CompilerParams(has_side_effects=True, collective_id=0, vmem_limit_bytes=64000000),
    )(hidden[0], output_grad[0], input_weight, step_bias[None], decay_log[None], skip_gain[None])
    hg, wg, hd = pl.pallas_call(
        emit,
        out_shape=(
            jax.ShapeDtypeStruct((128, D), BF16),
            jax.ShapeDtypeStruct((10, 2856), F32),
            jax.ShapeDtypeStruct((3, HEADS), F32),
        ),
        in_specs=[vmem, vmem, vmem],
        out_specs=(vmem, vmem, vmem),
    )(hg, wg, hd)
    return (hg[None], wg, hd)


def solution(mesh):
    torus = Mesh(
        mesh.devices.reshape(4, 2, 2, 4, 2), ("seq_0", "seq_1", "seq_2", "zero_0", "zero_1")
    )
    in_specs = (P(ZERO, SEQ, None), P(ZERO, SEQ, None), P(ZERO, None), P(), P(), P())
    out_specs = (P(ZERO, SEQ, None), P(SEQ_ZERO, None), P())
    return jax.shard_map(body, mesh=torus, in_specs=in_specs, out_specs=out_specs, check_vma=False)
```

```python
import functools

import jax
import jax.numpy as jnp
from jax import lax
from jax.experimental import pallas as pl
from jax.experimental.pallas import tpu as pltpu
from jax.sharding import Mesh
from jax.sharding import PartitionSpec as P

HEADS = 40
STATE = 128
INNER = 2560
D = 1280
COLS = 640
ZERO = ("zero_0", "zero_1")
SEQ = ("seq_0", "seq_1", "seq_2")
SEQ_ZERO = ("seq_0", "seq_1", "seq_2", "zero_0", "zero_1")
MESH = pl.DeviceIdType.MESH
F32 = jnp.float32
BF16 = jnp.bfloat16
highest = lax.Precision.HIGHEST
NN = (((1,), (0,)), ((), ()))
NT = (((1,), (1,)), ((), ()))
TN = (((0,), (0,)), ((), ()))


def mm(a, b, dims=NN, precision=None):
    return lax.dot_general(a, b, dims, preferred_element_type=F32, precision=precision)


def parts(v, count):
    out = []
    for _ in range(count):
        out.append(v.astype(BF16))
        v = v - out[-1].astype(F32)
    return out


def mm3(a, b, dims=NN):
    (ah, al), (bh, bl) = parts(a, 2), parts(b, 2)
    (ka,), (kb,) = dims[0]
    return mm(jnp.concatenate([ah, al, ah], axis=ka), jnp.concatenate([bh, bh, bl], axis=kb), dims)


def ds(start, size, align=None):
    return pl.ds(pl.multiple_of(start, align or size), size)


def silu_grad(v):
    sig = jax.nn.sigmoid(v)
    return sig * (1.0 + v * (1.0 - sig))


def kernel(
    hid_ref, cot_ref, w_ref, bias_ref, decay_ref, skip_ref,
    hg_ref, wg_ref, hd_ref,
    stepw, stepa, hidf, hidt, hidx, cot, wraw, wf, projs, projv, bmf, cmf, lgd, cums, cumt, stp, gs, gts, dgs,
    sexp, ecs, tls, vv, xb, xt, oe, tot,
    sl, dl, stt, tts, str_, ttr, q1s, dxin, dbf, dcf, sb, db, dd, red,
    rr, t1s, t1r, hgp, hgs, hgr,
    heads_y, heads_x, heads_z, heads_g, hgo, wgo, hdo,
    ss, rs, ls, *bufs,
):
    y, zl, c = (lax.axis_index(n) for n in SEQ)
    x, zh = (lax.axis_index(n) for n in ZERO)
    r = zl * 2 + c
    a = lax.rem(zl + zh, 2)
    g = a * 2 + c

    def send(i, src, dst, where, group):
        copy = pltpu.make_async_remote_copy(
            src_ref=src, dst_ref=dst, send_sem=ss.at[group], recv_sem=rs.at[i],
            device_id=where, device_id_type=MESH,
        )
        copy.start()
        return copy

    def bytes_of(ref, i=0, group=0):
        return pltpu.make_async_remote_copy(
            src_ref=ref, dst_ref=ref, send_sem=ss.at[group], recv_sem=rs.at[i],
            device_id={"seq_2": 1 - c}, device_id_type=MESH,
        )

    def got(i, ref):
        bytes_of(ref, i=i).wait_recv()

    def sent(group, ref):
        bytes_of(ref, group=group).wait_send()

    def rank(k):
        zlk = lax.rem(zl + k // 2, 2)
        ck = lax.rem(c + k % 2, 2)
        return zlk, ck, {"seq_1": zlk, "seq_2": ck}

    def xdev(k):
        return {"zero_0": lax.rem(x + k + 4, 4)}

    def ydev(k):
        return {"seq_0": lax.rem(y + k + 4, 4)}

    zpair = {"seq_1": 1 - zl, "zero_1": 1 - zh}
    core = {"seq_2": 1 - c}
    here_id = ds(r * 128, 128)

    def shard(xk, zk, lo=0, size=160):
        return ds((lax.rem(xk + 4, 4) * 2 + zk) * 160 + lo, size, 16)

    own = shard(x, zh)
    lane0 = 640 + 256 * c
    local = [
        pltpu.make_async_copy(w_ref, wraw, ls.at[0]),
        pltpu.make_async_copy(w_ref.at[:, ds(g * COLS, COLS, 128)], wf.at[own, 0:640], ls.at[1]),
        pltpu.make_async_copy(w_ref.at[:, ds(2560 + 128 * c, 128)], wf.at[own, ds(lane0, 128)], ls.at[2]),
        pltpu.make_async_copy(hid_ref, hidf.at[here_id, :], ls.at[3]),
        pltpu.make_async_copy(cot_ref.at[:, ds(g * COLS, COLS, 128)], cot.at[here_id, :], ls.at[4]),
    ]
    for copy in local:
        copy.start()

    barrier = pltpu.get_barrier_semaphore()

    def greet(dev):
        pl.semaphore_signal(barrier, inc=1, device_id=dev, device_id_type=MESH)

    greet(zpair)
    for k in (1, 2, 3):
        greet(xdev(k))
        greet(ydev(k))
        greet(rank(k)[2])
    coli = lax.broadcasted_iota(jnp.int32, (128, 128), 1)
    rowi = lax.broadcasted_iota(jnp.int32, (128, 128), 0)
    local[0].wait()
    stepa[...] = jnp.zeros_like(stepa)
    tail = jnp.concatenate([wraw[:, 2816:2856].astype(F32), jnp.zeros((160, 88), F32)], axis=1)
    tail = pltpu.roll(tail, lax.rem(128 - 10 * g, 128), 1)
    keep10 = lax.broadcasted_iota(jnp.int32, (160, 128), 1) < 10
    tail = jnp.concatenate([jnp.where(keep10, tail, 0.0), jnp.zeros((96, 128), F32)], axis=0)
    stepw[x * 2 + zh] = tail.T[0:16, :].astype(BF16)

    def lanes10(ref):
        full = jnp.concatenate([ref[...], jnp.zeros((1, 88), F32)], axis=1)
        return pltpu.roll(jnp.broadcast_to(full, (8, 128)), lax.rem(128 - 10 * g, 128), 1)[0:1, :]

    bias = lanes10(bias_ref)
    neg = -jnp.exp(lanes10(decay_ref))
    skip = lanes10(skip_ref)
    for copy in local[1:]:
        copy.wait()
    pl.semaphore_wait(barrier, 10)

    def cols(m):
        return (ds(lane0, 128), slice(0, 256), slice(256, 512), slice(512, 640))[m]

    w = {}

    def wsend(m, i, rows, dev):
        ref = wf.at[rows, cols(m)]
        slot = min(i, 5) if m < 2 else {1: 1, 2: 2, 5: 3, 6: 4}.get(i, 5)
        w[m, i] = send(6 * m + slot, ref, ref, dev, m)

    def w_own_x(m):
        wsend(m, 1, own, xdev(1))
        wsend(m, 2, own, xdev(-1))

    def w_own_z(m):
        wsend(m, 0, own, zpair)

    def w_other(m):
        w[m, 0].wait_recv()
        wsend(m, 3, shard(x, 1 - zh), xdev(1))
        wsend(m, 4, shard(x, 1 - zh), xdev(-1))

    def w_forward(m):
        w[m, 1].wait_recv()
        wsend(m, 5, shard(x - 1, zh, 0, 80), xdev(1))
        w[m, 2].wait_recv()
        wsend(m, 6, shard(x + 1, zh, 80, 80), xdev(-1))

    def w_forward_other(m):
        w[m, 3].wait_recv()
        wsend(m, 7, shard(x - 1, 1 - zh, 0, 80), xdev(1))
        w[m, 4].wait_recv()
        wsend(m, 8, shard(x + 1, 1 - zh, 80, 80), xdev(-1))

    def w_across(m):
        wsend(m, 3, shard(x - 1, zh), zpair)
        wsend(m, 4, shard(x + 1, zh), zpair)

    def w_across_far(m):
        w[m, 5].wait_recv()
        wsend(m, 7, shard(x + 2, zh, 0, 80), zpair)
        w[m, 6].wait_recv()
        wsend(m, 8, shard(x + 2, zh, 80, 80), zpair)

    def w_done(m):
        got(6 * m + 5, wf.at[0 : 320 if m < 2 else 640, cols(m)])

    def step_send(i, xk, zk, dev):
        ref = stepw.at[lax.rem(x + xk + 4, 4) * 2 + zk]
        return send(i, ref, ref, dev, 20)

    def hand(k):
        ref = wf.at[ds(lax.rem(x + k + 4, 4) * 320, 320), ds(lane0, 128)]
        send(28, ref, ref, core, 6)

    step_z = step_send(88, 0, zh, zpair)
    step_x = [step_send(89, 0, zh, xdev(1)), step_send(90, 0, zh, xdev(-1))]
    w_own_z(0)
    w_own_x(0)
    h_z = send(24, hid_ref, hidf.at[here_id, :], rank(2)[2], 4)
    w_own_x(2)
    w_own_z(1)
    h_c = send(25, hid_ref, hidf.at[here_id, :], core, 4)
    for k in (2, 3, 1):
        zlk, ck, dev = rank(k)
        gk = lax.rem(zlk + zh, 2) * 2 + ck
        send(27, cot_ref.at[:, ds(gk * COLS, COLS, 128)], cot.at[here_id, :], dev, 5)
    w_own_z(2)
    w_own_z(3)
    step_z.wait_recv()
    step_o = [step_send(91, 0, 1 - zh, xdev(1)), step_send(92, 0, 1 - zh, xdev(-1))]
    w_other(0)
    for copy in step_x:
        copy.wait_recv()
    step_send(93, -1, zh, xdev(1))
    w_forward(0)
    w_forward(2)
    w_across(2)
    w_own_x(3)
    for copy in step_o:
        copy.wait_recv()
    step_send(93, -1, 1 - zh, xdev(1))
    w_forward_other(0)
    w_own_x(1)
    for k in (-1, 0, 1):
        hand(k)
    i320 = lax.broadcasted_iota(jnp.int32, (320, 320), 0)
    k320 = lax.broadcasted_iota(jnp.int32, (320, 320), 1)
    tens = lax.shift_right_logical(i320 * 6554, 16)
    source = ((tens & 3) * 8 + lax.shift_right_logical(tens, 2)) * 10 + i320 - tens * 10
    perm = jnp.where(k320 == source, 1.0, 0.0).astype(F32).astype(BF16)

    def transpose(k):
        rows = ds((rank(k)[0] * 2 + rank(k)[1]) * 128, 128)
        for q in range(4):
            part = slice(320 * q, 320 * q + 320)
            hidt[part, rows] = mm(perm, hidf[rows, part], NT).astype(BF16)

    transpose(0)
    h_c.wait_recv()
    transpose(1)
    h_z.wait_recv()
    zrows = ds((rank(2)[0] * 2 + c) * 128, 128)
    h_f = send(26, hidf.at[zrows, :], hidf.at[zrows, :], core, 4)
    w_across_far(2)
    w_forward(3)
    w_across(3)
    w_other(1)
    w_done(0)
    hand(2)
    got(93, stepw.at[0:2])
    for k in range(8):
        stepa[0:16, 160 * k : 160 * k + 160] = stepw[k][:, 0:160].astype(F32)
    wf[:, 768:896] = stepa[...].T.astype(BF16)

    low = coli < 64
    causal = rowi >= coli
    anti = rowi <= coli
    tri = causal.astype(F32).astype(BF16)
    tri3 = jnp.concatenate([tri] * 3, axis=1)
    upper = anti.astype(F32).astype(BF16)
    strict = (rowi > coli).astype(F32).astype(BF16)
    sums4 = jnp.concatenate([upper] * 3 + [strict] * 3, axis=1)

    def pair(v, j):
        return jnp.where(low[0 : v.shape[0]], v[:, 2 * j : 2 * j + 1], v[:, 2 * j + 1 : 2 * j + 2])

    def blocks(f, unroll=True):
        if unroll:
            for b in range(4):
                f(b, pl.ds(b * 128, 128))
        else:
            def step(b, carry):
                f(b, ds(b * 128, 128))
                return carry

            lax.fori_loop(0, 4, step, 0)

    def steps(b, rows):
        projs[rows, ds(128 * c, 256, 128)] = mm(hidf[rows, :], wf[:, ds(640 + 128 * c, 256, 128)])
        pre = projs[rows, 128:256] + bias
        step = jnp.maximum(pre, 0.0) + jnp.log1p(jnp.exp(-jnp.abs(pre)))
        lg = neg * step
        cum = mm(tri3, jnp.concatenate(parts(lg, 3), axis=0))
        stp[rows, :] = step
        lgd[rows, :] = lg
        cums[rows, :] = cum
        cumt[b] = cum.T[0:16, :]
        dgs[b] = jnp.zeros((128, 128), F32)
        red[b] = jnp.zeros((384, 128), F32)

    def maps(b, rows):
        projs[rows, ds(256 - 256 * c, 128)] = mm(hidf[rows, :], wf[:, ds(896 - 256 * c, 128)])
        bm = jax.nn.silu(projs[rows, 0:128])
        cm = jax.nn.silu(projs[rows, 256:384])
        bmf[rows, :] = bm
        cmf[rows, :] = cm
        scores = mm3(cm, bm, NT)
        gs[b] = scores
        gts[b] = scores.T

    for k in range(4):
        if k == 3:
            h_f.wait_recv()
        b = rank(k)[0] * 2 + rank(k)[1]
        steps(b, ds(b * 128, 128))
    for j in range(5):
        cj = slice(128 * j, 128 * j + 128)
        for b in range(4):
            last_row = cums[128 * b + 127 : 128 * b + 128, :]
            tot[8 * b : 8 * b + 8, cj] = pair(jnp.broadcast_to(last_row, (8, 128)), j)
    tts[...] = tot[0:8, :] + tot[8:16, :] + tot[16:24, :] + tot[24:32, :]
    for k in (1, 2, 3):
        send(29, tts, ttr.at[k - 1], ydev(k), 7)

    transpose(2)
    transpose(3)
    w_forward(1)
    got(28, wf.at[:, ds(896 - 256 * c, 128)])
    maps(0, pl.ds(0, 128))
    w_across_far(3)
    maps(1, pl.ds(128, 128))
    maps(2, pl.ds(256, 128))
    w_forward_other(1)
    maps(3, pl.ds(384, 128))

    def total(b, cj):
        return tot[8 * b : 8 * b + 1, cj]

    def pair_forward(j):
        cj = slice(128 * j, 128 * j + 128)

        wide = slice(128 * j, min(128 * j + 256, 640))

        def project(b, rows):
            projv[rows, wide] = mm(hidf[rows, :], wf[:, wide])

        def local_part(b, rows):
            ce = pair(cums[rows, :], j)
            se = pair(stp[rows, :], j)
            ec = jnp.exp(ce)
            tl = jnp.exp(ce[127:128, :] - ce)
            val = jax.nn.silu(projv[rows, cj])
            xs = val * se
            sexp[rows, cj] = se
            ecs[rows, cj] = ec
            tls[rows, cj] = tl
            vv[rows, cj] = val
            xb[rows, cj] = xs.astype(BF16)
            x16 = (xs * tl).astype(BF16)
            o16 = (cot[rows, cj].astype(F32) * ec).astype(BF16)
            xt[rows, cj] = x16
            oe[rows, cj] = o16
            sl[b, :, cj] = mm(bmf[rows, :].astype(BF16), x16, TN)
            dl[b, :, cj] = mm(cmf[rows, :].astype(BF16), o16, TN)

        if j % 2 == 0:
            blocks(project)
        blocks(local_part)
        s = sl[0, :, cj]
        d = dl[3, :, cj]
        for b in range(1, 4):
            s = jnp.exp(total(b, cj)) * s + sl[b, :, cj]
            d = jnp.exp(total(3 - b, cj)) * d + dl[3 - b, :, cj]
        stt[0, :, cj] = s.astype(BF16)
        stt[1, :, cj] = d.astype(BF16)
        for k in (1, 2, 3):
            wraps = lax.div(y + k, 4)
            send(30 + j, stt.at[wraps, :, cj], str_.at[k - 1, :, cj], ydev(k), 8)

    def pair_inside(j):
        cj = slice(128 * j, 128 * j + 128)

        def inside(b, rows):
            cum = cums[rows, :]
            c0, c1 = cum[:, 2 * j : 2 * j + 1], cum[:, 2 * j + 1 : 2 * j + 2]
            r0, r1 = cumt[b, 2 * j : 2 * j + 1, :], cumt[b, 2 * j + 1 : 2 * j + 2, :]
            w0 = jnp.where(causal, jnp.exp(jnp.where(causal, c0 - r0, 0.0)), 0.0)
            w1 = jnp.where(causal, jnp.exp(jnp.where(causal, c1 - r1, 0.0)), 0.0)
            u0 = jnp.where(anti, jnp.exp(jnp.where(anti, r0 - c0, 0.0)), 0.0)
            u1 = jnp.where(anti, jnp.exp(jnp.where(anti, r1 - c1, 0.0)), 0.0)
            scores, scores_t = gs[b], gts[b]
            m = jnp.concatenate([scores * w0, scores * w1], axis=1).astype(BF16)
            mt = jnp.concatenate([scores_t * u0, scores_t * u1], axis=1).astype(BF16)
            x16 = xb[rows, cj]
            o16 = cot[rows, cj]
            zero = jnp.zeros_like(x16)
            xd = jnp.concatenate([jnp.where(low, x16, zero), jnp.where(low, zero, x16)], axis=0)
            od = jnp.concatenate([jnp.where(low, o16, zero), jnp.where(low, zero, o16)], axis=0)
            yy = mm(m, xd)
            pp = mm(o16, xd, NT)
            dx = mm(mt, od)
            dgs[b] = dgs[b] + w0 * pp[:, 0:128] + w1 * pp[:, 128:256]
            dxin[rows, cj] = dx
            q1s[rows, cj] = o16.astype(F32) * yy - x16.astype(F32) * dx

        blocks(inside)

    got(27, cot.at[0:384, :])
    w_done(2)
    pair_forward(2)
    pair_inside(2)
    pair_forward(3)
    pair_inside(3)
    w_done(3)
    pair_forward(4)
    pair_inside(4)
    for p in range(4):
        for q in range(4):
            hidx[320 * p + 80 * q : 320 * p + 80 * q + 80, :] = hidt[320 * q + 80 * p : 320 * q + 80 * p + 80, :]
    w_done(1)
    pair_forward(0)
    pair_inside(0)
    pair_forward(1)
    pair_inside(1)

    def turn(b, rows):
        dcf[rows, :] = mm3(dgs[b], bmf[rows, :], NN) + mm(oe[rows, :], sb[b], NT)
        dbf[rows, :] = mm3(dgs[b], cmf[rows, :], TN) + mm(xt[rows, :], db[b], NT)

    got(29, ttr)

    lanes = lax.broadcasted_iota(jnp.int32, (256, 128), 0)
    outl = lax.broadcasted_iota(jnp.int32, (256, 128), 1)

    def sums(z, j):
        hi = z.astype(BF16)
        lo = (z - hi.astype(F32)).astype(BF16)
        choose = (outl == 2 * j + lax.rem(lax.div(lanes, 64), 2)).astype(F32).astype(BF16)
        return mm(jnp.concatenate([hi, lo], axis=1), choose)

    yes = [jnp.where(y >= k, 1.0, 0.0).astype(F32) for k in (1, 2, 3)]
    no = [jnp.where(y + k <= 3, 1.0, 0.0).astype(F32) for k in (1, 2, 3)]
    inner = [jnp.zeros((8, 128), F32) for _ in range(4)]
    gain = [jnp.zeros((8, 128), F32)]

    def pair_outside(j):
        cj = slice(128 * j, 128 * j + 128)
        got(30 + j, str_.at[:, :, cj])
        t = [ttr[k, 0:1, cj] for k in range(3)]
        came = [str_[k, :, cj].astype(F32) for k in range(3)]
        s = yes[0] * came[0] + (yes[1] * jnp.exp(t[0])) * came[1] + (yes[2] * jnp.exp(t[0] + t[1])) * came[2]
        d = no[0] * came[2] + (no[1] * jnp.exp(t[2])) * came[1] + (no[2] * jnp.exp(t[2] + t[1])) * came[0]
        for b in (3, 2, 1, 0):
            db[b, :, cj] = d.astype(BF16)
            dd[b] = d
            d = jnp.exp(total(b, cj)) * d + dl[b, :, cj]
        for b in range(4):
            sb[b, :, cj] = s.astype(BF16)
            grown = jnp.exp(total(b, cj)) * s
            inner[b] = inner[b] + sums((grown * dd[b]).reshape(16, 8, 128).sum(axis=0), j)
            s = grown + sl[b, :, cj]

        def outside(b, rows):
            o = cot[rows, cj].astype(F32)
            yst = mm(cmf[rows, :].astype(BF16), sb[b, :, cj]) * ecs[rows, cj]
            dxst = mm(bmf[rows, :].astype(BF16), db[b, :, cj]) * tls[rows, cj]
            val = vv[rows, cj]
            dxs = dxin[rows, cj] + dxst
            z = jnp.concatenate([q1s[rows, cj] + o * yst, xb[rows, cj].astype(F32) * dxst, dxs * val], axis=0)
            red[b] = red[b] + sums(z, j)
            dval = dxs * sexp[rows, cj] + pair(skip, j) * o
            rr[rows, cj] = (dval * silu_grad(projv[rows, cj])).astype(BF16)
            gain[0] = gain[0] + sums((o * val).reshape(16, 8, 128).sum(axis=0), j)

        blocks(outside)

    class Stream:
        def __init__(self, base, group, parts, kind, bufs):
            self.base, self.group, self.parts, self.left = base, group, parts, hidx if kind else hidt
            self.dw, self.s1, self.r1, self.s2, self.r2, self.s3, self.r3, self.s4, self.r4, self.sd, self.rd = bufs
            self.index, self.dev, self.index2, self.dev2 = (y, ydev, x, xdev) if kind == 0 else (x, xdev, y, ydev)

        def send(self, i, src, dst, dev):
            return send(self.base + i, src, dst, dev, self.group)

        def block(self, i):
            rows = ds(lax.rem(self.index + i, 4) * 320, 320)
            for cols, target in self.parts:
                self.dw[rows, target] = mm(self.left[rows, :], rr[:, cols])
            return rows

        def first(self):
            rows = self.block(2)
            self.s1[...] = self.dw[rows, :].astype(BF16)
            self.one = (
                self.send(0, self.s1.at[0:160, :], self.r1.at[0], self.dev(1)),
                self.send(1, self.s1.at[160:320, :], self.r1.at[1], self.dev(-1)),
            )

        def rest(self):
            for i in (1, 3, 0):
                self.block(i)

        def second(self):
            nxt = lax.rem(self.index + 1, 4) * 320
            prv = lax.rem(self.index + 3, 4) * 320
            self.one[0].wait_recv()
            self.s2[0, 0:160, :] = (self.dw[ds(nxt, 160), :] + self.r1[0].astype(F32)).astype(BF16)
            self.s2[0, 160:320, :] = self.dw[ds(nxt + 160, 160), :].astype(BF16)
            self.send(2, self.s2.at[0], self.r2.at[0], self.dev(1))
            self.one[1].wait_recv()
            self.s2[1, 0:160, :] = self.dw[ds(prv, 160), :].astype(BF16)
            self.s2[1, 160:320, :] = (self.dw[ds(prv + 160, 160), :] + self.r1[1].astype(F32)).astype(BF16)
            self.send(2, self.s2.at[1], self.r2.at[1], self.dev(-1))

        def third(self):
            got(self.base + 2, self.r2)
            here = ds(self.index * 320, 320)
            summed = self.dw[here, :] + self.r2[0].astype(F32) + self.r2[1].astype(F32)
            self.dw[here, :] = summed
            self.s3[...] = summed.astype(BF16)
            for k in (2, 1, 3):
                piece = self.s3.at[ds(lax.rem(self.index2 + k, 4) * 80, 80), :]
                self.send(3, piece, self.r3.at[k - 1], self.dev2(k))

        def fourth(self):
            got(self.base + 3, self.r3)
            rows = ds(self.index * 320 + self.index2 * 80, 80)
            self.s4[...] = self.dw[rows, :] + self.r3[0].astype(F32) + self.r3[1].astype(F32) + self.r3[2].astype(F32)
            self.four = self.send(4, self.s4.at[ds((1 - zh) * 40, 40), :], self.r4, zpair)

        def owners(self):
            self.four.wait_recv()
            chunk = self.s4[ds(zh * 40, 40), :] + self.r4[...]
            for i in range(4):
                self.sd[i, 0:10, :] = chunk[10 * i : 10 * i + 10, :]
            self.rd[g] = self.sd[r]
            for k in (2, 3, 1):
                zlk, ck, dev = rank(k)
                self.send(5, self.sd.at[zlk * 2 + ck], self.rd.at[g], dev)

        def finish(self):
            got(self.base + 5, self.rd.at[0:3])

        def close(self):
            sent(self.group, self.dw.at[0:688, :])

    tiles = [slice(128 * t, 128 * t + 128) for t in range(5)] + [slice(768, 896), ds(lane0, 128)]
    kinds = (0, 1, 0, 1, 0, 1, 0)
    p0, p1, p2, p3, p4, st, mp = streams = [
        Stream(46 + 6 * t, 13 + t, [(tiles[t], slice(0, 128))], kinds[t], bufs[11 * t : 11 * t + 11]) for t in range(7)
    ]

    pair_outside(2)
    p2.first()
    pair_outside(3)
    p3.first()
    p2.rest()
    pair_outside(4)
    p4.first()
    pair_outside(0)
    p0.first()
    p2.second()
    pair_outside(1)
    p1.first()

    blocks(turn)
    first = c == 0
    t1s[...] = jnp.where(first, dcf[...], dbf[...])
    t1 = send(35, t1s, t1r, core, 9)
    p4.rest()
    p4.second()
    p3.rest()
    p3.second()

    ownl = coli < 10
    bias_sum = decay_sum = jnp.zeros((8, 128), F32)
    for b in range(4):
        rows = slice(128 * b, 128 * b + 128)
        dlog = mm(sums4, jnp.concatenate(parts(red[b, 0:128], 3) + parts(red[b, 128:256], 3), axis=0))
        dlog = jnp.where(ownl, dlog + inner[b].sum(axis=0, keepdims=True), 0.0)
        ddt = (red[b, 256:384] + neg * dlog) * jax.nn.sigmoid(projs[rows, 128:256] + bias)
        ddt = jnp.where(ownl, ddt, 0.0)
        rr[rows, 768:896] = ddt.astype(BF16)
        bias_sum = bias_sum + ddt.reshape(16, 8, 128).sum(axis=0)
        decay_sum = decay_sum + (dlog * lgd[rows, :]).reshape(16, 8, 128).sum(axis=0)
    place = jnp.where(jnp.logical_and(rowi < 10, coli == rowi + 10 * g), 1.0, 0.0).astype(F32)
    st.first()
    row8 = lax.broadcasted_iota(jnp.int32, (8, 128), 0)
    packed = jnp.where(
        row8 == 0, bias_sum.sum(axis=0, keepdims=True),
        jnp.where(row8 == 1, decay_sum.sum(axis=0, keepdims=True),
                  jnp.where(row8 == 2, gain[0].sum(axis=0, keepdims=True), 0.0)),
    )
    heads_y[y] = mm(packed, place, NN, highest)
    for k in (1, 2, 3):
        send(38, heads_y.at[y], heads_y.at[y], ydev(k), 10)
    p0.rest()
    p0.second()
    t1.wait_recv()
    mixed = jnp.where(first, dbf[...], dcf[...]) + t1r[...]
    rr[:, ds(lane0, 128)] = (mixed * silu_grad(projs[:, ds(256 * c, 128, 128)])).astype(BF16)
    rr[:, ds(896 - 256 * c, 128)] = jnp.zeros((512, 128), BF16)
    mp.first()

    def token(half):
        rows = ds(half * 256, 256)
        for n in range(5):
            part = slice(256 * n, 256 * n + 256)
            hgp[rows, part] = mm(rr[rows, :], wf[part, :], NT)

    mate_row = ds((zl * 2 + 1 - c) * 128, 128)
    far_mate = ds(((1 - zl) * 2 + 1 - c) * 128, 128)
    far_row = ds(((1 - zl) * 2 + c) * 128, 128)
    p1.rest()
    p1.second()
    p2.third()
    st.rest()
    st.second()
    p3.third()
    token(1 - zl)
    hgs[1] = hgp[far_mate, :].astype(BF16)
    hg_far = send(43, hgs.at[1], hgr.at[1], core, 11)
    mp.rest()
    mp.second()
    p4.third()
    hg_far.wait_recv()
    hgs[2] = (hgp[far_row, :] + hgr[1].astype(F32)).astype(BF16)
    hg_z = send(44, hgs.at[2], hgr.at[2], rank(2)[2], 11)
    p0.third()
    token(zl)
    hgs[0] = hgp[mate_row, :].astype(BF16)
    hg_near = send(42, hgs.at[0], hgr.at[0], core, 11)
    p1.third()
    p2.fourth()
    p3.fourth()
    st.third()
    mp.third()
    got(38, heads_y.at[0:3])
    heads_x[x] = (heads_y[0] + heads_y[1]) + (heads_y[2] + heads_y[3])
    for k in (1, 2, 3):
        send(39, heads_x.at[x], heads_x.at[x], xdev(k), 10)
    p4.fourth()
    p0.fourth()
    p2.owners()
    p3.owners()
    p1.fourth()
    st.fourth()
    got(39, heads_x.at[0:3])
    heads_z[zh] = (heads_x[0] + heads_x[1]) + (heads_x[2] + heads_x[3])
    head_z = send(40, heads_z.at[zh], heads_z.at[zh], zpair, 10)
    mp.fourth()
    p4.owners()
    p0.owners()
    p1.owners()
    st.owners()
    mp.owners()
    head_z.wait_recv()
    heads_g[r] = heads_z[0] + heads_z[1]
    for k in (1, 2, 3):
        send(41, heads_g.at[r], heads_g.at[r], rank(k)[2], 10)
    hg_near.wait_recv()
    hg_z.wait_recv()
    hgo[...] = (hgp[here_id, :] + hgr[0].astype(F32) + hgr[2].astype(F32)).astype(BF16)
    hg_out = pltpu.make_async_copy(hgo, hg_ref, ls.at[5])
    hg_out.start()
    for t, stream in ((2, p2), (3, p3), (4, p4), (0, p0), (1, p1)):
        stream.finish()
        for k in range(4):
            wgo[:, 640 * k + 128 * t : 640 * k + 128 * t + 128] = stream.rd[k, 0:10, :]
    got(41, heads_g.at[0:3])
    hdo[...] = (heads_g[0] + heads_g[1]) + (heads_g[2] + heads_g[3])
    hd_out = pltpu.make_async_copy(hdo, hd_ref, ls.at[6])
    hd_out.start()
    st.finish()
    for k in range(4):
        wgo[:, 2816 + 10 * k : 2826 + 10 * k] = st.rd[k, 0:10, 0:10]
    mp.finish()
    wgo[:, 2560:2688] = mp.rd[0, 0:10, :] + mp.rd[2, 0:10, :]
    wgo[:, 2688:2816] = mp.rd[1, 0:10, :] + mp.rd[3, 0:10, :]
    wg_out = pltpu.make_async_copy(wgo, wg_ref, ls.at[7])
    wg_out.start()
    for m in range(4):
        sent(m, wf.at[0:1120, cols(m)])
    sent(4, hidf.at[0:384, :])
    sent(20, stepw.at[0:7])
    sent(5, cot.at[0:384, :])
    sent(6, wf.at[:, ds(lane0, 128)])
    sent(7, ttr)
    sent(8, str_)
    sent(9, t1r)
    sent(10, bmf.at[0:80, :])
    sent(11, hgs)
    for stream in streams:
        stream.close()
    hg_out.wait()
    hd_out.wait()
    wg_out.wait()


def scratch():
    def v(shape, dtype=F32):
        return pltpu.VMEM(shape, dtype)

    def stream(n):
        return [
            v((D, n)), v((320, n), BF16), v((2, 160, n), BF16), v((2, 320, n), BF16), v((2, 320, n), BF16),
            v((320, n), BF16), v((3, 80, n), BF16), v((80, n)), v((40, n)), v((4, 16, n)), v((4, 16, n)),
        ]

    wide, wide16 = v((512, COLS)), v((512, COLS), BF16)
    thin = v((512, 128))
    return [
        v((8, 16, 256), BF16), v((128, D)),
        v((512, D), BF16), v((D, 512), BF16), v((D, 512), BF16), wide16, v((160, 2856), BF16), v((D, 1024), BF16),
        v((512, 384)), wide, thin, thin, thin, thin, v((4, 16, 128)), thin,
        v((4, 128, 128)), v((4, 128, 128)), v((4, 128, 128)),
        wide, wide, wide, wide, wide16, wide16, wide16, v((32, COLS)),
        v((4, 128, COLS)), v((4, 128, COLS)), v((2, 128, COLS), BF16), v((8, COLS)),
        v((3, 128, COLS), BF16), v((3, 8, COLS)), wide, wide, thin, thin,
        v((4, 128, COLS), BF16), v((4, 128, COLS), BF16), v((4, 128, 128)), v((4, 384, 128)),
        v((512, 1024), BF16), thin, thin,
        v((512, D)), v((3, 128, D), BF16), v((3, 128, D), BF16),
        v((4, 8, 128)), v((4, 8, 128)), v((2, 8, 128)), v((4, 8, 128)),
        v((128, D), BF16), v((10, 2856)), v((8, 128)),
        pltpu.SemaphoreType.DMA((21,)), pltpu.SemaphoreType.DMA((94,)), pltpu.SemaphoreType.DMA((8,)),
        *(buf for _ in range(7) for buf in stream(128)),
    ]


def emit(hg_ref, wg_ref, hd_ref, hg_out, wg_out, hd_out):
    hg_out[...] = hg_ref[...]
    wg_out[...] = wg_ref[...]
    hd_out[...] = hd_ref[0:3, 0:HEADS]


def body(hidden, output_grad, input_weight, step_bias, decay_log, skip_gain):
    anyspace = pl.BlockSpec(memory_space=pl.ANY)
    vmem = pl.BlockSpec(memory_space=pltpu.VMEM)
    hg, wg, hd = pl.pallas_call(
        kernel,
        out_shape=(
            jax.ShapeDtypeStruct((128, D), BF16),
            jax.ShapeDtypeStruct((10, 2856), F32),
            jax.ShapeDtypeStruct((8, 128), F32),
        ),
        in_specs=[anyspace, anyspace, anyspace, vmem, vmem, vmem],
        out_specs=(anyspace, anyspace, anyspace),
        scratch_shapes=scratch(),
        compiler_params=pltpu.CompilerParams(has_side_effects=True, collective_id=0, vmem_limit_bytes=64000000),
    )(hidden[0], output_grad[0], input_weight, step_bias[None], decay_log[None], skip_gain[None])
    hg, wg, hd = pl.pallas_call(
        emit,
        out_shape=(
            jax.ShapeDtypeStruct((128, D), BF16),
            jax.ShapeDtypeStruct((10, 2856), F32),
            jax.ShapeDtypeStruct((3, HEADS), F32),
        ),
        in_specs=[vmem, vmem, vmem],
        out_specs=(vmem, vmem, vmem),
    )(hg, wg, hd)
    return (hg[None], wg, hd)


def solution(mesh):
    torus = Mesh(
        mesh.devices.reshape(4, 2, 2, 4, 2), ("seq_0", "seq_1", "seq_2", "zero_0", "zero_1")
    )
    in_specs = (P(ZERO, SEQ, None), P(ZERO, SEQ, None), P(ZERO, None), P(), P(), P())
    out_specs = (P(ZERO, SEQ, None), P(SEQ_ZERO, None), P())
    return jax.shard_map(body, mesh=torus, in_specs=in_specs, out_specs=out_specs, check_vma=False)
```
